32 devices in a mesh: section: 2 (over core), seq: 4 (over y, x), head: 4 (over z).
Axes of the slice: x: 2, y: 2, z: 4, core: 2. Of those that a mesh axis runs over, the one named last changes fastest.
Arguments:
- tokens: bfloat16 [2, 2048, 1792], P(None, 'seq'), may hold values from -6 to 6
- lengths: int32 [2, 4], replicated, may hold values from 1 to 1024, 2048 in all within a row
- gain_attn: bfloat16 [2, 1792], P('section'), may hold values from 0.5 to 1.5
- w_query: bfloat16 [2, 1792, 256], P('section', 'seq', 'head'), may hold values from -0.125 to 0.125
- w_key: bfloat16 [2, 1792, 256], P('section', 'seq', 'head'), may hold values from -0.125 to 0.125
- w_value: bfloat16 [2, 1792, 1792], P('section', 'seq', 'head'), may hold values from -0.125 to 0.125
- w_gate_conv: bfloat16 [2, 1792, 1792], P('section', 'seq', 'head'), may hold values from -0.125 to 0.125
- conv_taps: bfloat16 [2, 3, 1792], P('section'), may hold values from -3 to 3
- w_out: bfloat16 [2, 1792, 1792], P('section', 'head', 'seq'), may hold values from -1 to 1
- gain_ffn: bfloat16 [2, 1792], P('section'), may hold values from 0.5 to 1.5
- w_gate: bfloat16 [2, 1792, 4864], P('section', 'seq', 'head'), may hold values from -0.125 to 0.125
- w_up: bfloat16 [2, 1792, 4864], P('section', 'seq', 'head'), may hold values from -0.125 to 0.125
- w_down: bfloat16 [2, 4864, 1792], P('section', 'head', 'seq'), may hold values from -0.078125 to 0.078125
- cotangent: bfloat16 [2, 2048, 1792], P(None, 'seq'), may hold values from -6 to 6
Outputs:
- activations: bfloat16 [2, 2, 2048, 1792], P('section', None, 'seq')
- input_grads: bfloat16 [2, 2, 2048, 1792], P('section', None, 'seq')
- grad_gain_attn: float32 [2, 1792], P('section')
- grad_w_query: float32 [2, 1792, 256], P('section', 'seq', 'head')
- grad_w_key: float32 [2, 1792, 256], P('section', 'seq', 'head')
- grad_w_value: float32 [2, 1792, 1792], P('section', 'seq', 'head')
- grad_w_gate_conv: float32 [2, 1792, 1792], P('section', 'seq', 'head')
- grad_conv_taps: float32 [2, 3, 1792], P('section')
- grad_w_out: float32 [2, 1792, 1792], P('section', 'head', 'seq')
- grad_gain_ffn: float32 [2, 1792], P('section')
- grad_w_gate: float32 [2, 1792, 4864], P('section', 'seq', 'head')
- grad_w_up: float32 [2, 1792, 4864], P('section', 'seq', 'head')
- grad_w_down: float32 [2, 4864, 1792], P('section', 'head', 'seq')
The draws below stay inside these ranges and needn't reach their ends.
Inputs may be any that keep to these rules, and one draw needn't show every extreme that they name: Each row holds the lengths of 4 sequences that fill the 2048 tokens of one micro-batch; in every row the longest is exactly 1024.
All inputs are finite; a program needn't handle non-finite values.
Results may differ from the reference program's by a relative error of at most 0.035.
Values may be sent and summed in bfloat16 or wider, within the bound.
A program may use at most 256 MiB of HBM per device.

```python
import math
import jax
import jax.numpy as jnp
import numpy as np
from jax import lax

D = 1792
H = 16
FK = 16
HD = 112
PHI = 273
FF = 4864
KW = 3
TOK_DEV = 512
MICRO = 2
SEQS = 4
TOK_MB = 2048
LONGEST = 1024


def levels(key, dims, shards, smallest, top_value):
    def one(dim, parts):
        heights = jax.random.uniform(jax.random.fold_in(jax.random.fold_in(key, 6), dim), (parts,), jnp.float32, smallest / len(shards), top_value / len(shards))
        return jnp.repeat(jnp.exp(heights), dims[dim] // parts).reshape((-1,) + (1,) * (len(dims) - dim - 1))

    gain = one(*shards[0])
    for cut in shards[1:]:
        gain = gain * one(*cut)
    return gain


def length_profile(count, total, limit, skew):
    weights = [(1 << 20) // math.isqrt(standing ** skew) + 1 for standing in range(2, count + 1)]
    rest, counts = total - limit - (count - 1), [1] * (count - 1)
    while rest > 0:
        free = [i for i in range(count - 1) if counts[i] < limit]
        mass, left = sum([weights[i] for i in free]), rest
        for i in free:
            more = min(limit - counts[i], max(1, left * weights[i] // mass), rest)
            counts[i] = counts[i] + more
            rest = rest - more
    return np.array([limit] + counts)


def ragged_sizes(stream_key, amount, total, limit, lean):
    if amount == 2:
        one = jax.random.randint(stream_key, (), max(1, total - limit), min(limit, total - 1) + 1)
        return jnp.stack([one, total - one])
    tallies = jnp.asarray(length_profile(amount, total, limit, lean), jnp.int32)
    couples = (amount - 1) // 2
    source_of, taker = tallies[1:1 + 2 * couples:2], tallies[2:2 + 2 * couples:2]
    margin = jnp.minimum(source_of - 1, limit - taker)
    passed = jax.random.randint(jax.random.fold_in(stream_key, 1), (couples,), 0, 1 << 20) % (margin + 1)
    tallies = tallies.at[1:1 + 2 * couples:2].set(source_of - passed).at[2:2 + 2 * couples:2].set(taker + passed)
    return tallies[jax.random.permutation(jax.random.fold_in(stream_key, 2), amount)]


def scatter_about(rng, extent, width, limit, cuts=(), held_as=jnp.bfloat16):
    gain = levels(rng, extent, cuts, -0.22, 0.18) if cuts else 1.0
    entries = jax.random.normal(rng, extent, jnp.float32) * width * gain
    return jnp.minimum(jnp.maximum(entries, -limit), limit).astype(held_as)


def setup_inputs(seed: int = 0) -> dict:
    key_of = jax.random.split(jax.random.key(seed), 15)
    tokens = scatter_about(key_of[0], (MICRO, TOK_MB, D), 1.0, 6.0, ((1, 4),))
    lengths = jax.vmap(lambda own: ragged_sizes(own, SEQS, TOK_MB, LONGEST, 2))(jax.random.split(key_of[1], MICRO)).reshape((MICRO, SEQS)).astype(jnp.int32)
    gain_attn = jnp.clip(1.0 + 0.1 * jax.random.normal(key_of[2], (2, D), jnp.float32), 0.5, 1.5).astype(jnp.bfloat16)
    w_query = scatter_about(key_of[3], (2, D, H * FK), D ** -0.5, 0.125, ((0, 2), (1, 4), (2, 4)))
    w_key = scatter_about(key_of[4], (2, D, H * FK), D ** -0.5, 0.125, ((0, 2), (1, 4), (2, 4)))
    w_value = scatter_about(key_of[5], (2, D, D), D ** -0.5, 0.125, ((0, 2), (1, 4), (2, 4)))
    w_gate_conv = scatter_about(key_of[6], (2, D, D), D ** -0.5, 0.125, ((0, 2), (1, 4), (2, 4)))
    conv_taps = scatter_about(key_of[7], (2, KW, D), 0.6, 3.0, ((0, 2),))
    w_out = scatter_about(key_of[8], (2, D, D), (D // 64) ** -0.5, 1.0, ((0, 2), (1, 4), (2, 4)))
    gain_ffn = jnp.clip(1.0 + 0.1 * jax.random.normal(key_of[9], (2, D), jnp.float32), 0.5, 1.5).astype(jnp.bfloat16)
    w_gate = scatter_about(key_of[10], (2, D, FF), D ** -0.5, 0.125, ((0, 2), (1, 4), (2, 4)))
    w_up = scatter_about(key_of[11], (2, D, FF), D ** -0.5, 0.125, ((0, 2), (1, 4), (2, 4)))
    w_down = scatter_about(key_of[12], (2, FF, D), FF ** -0.5, 0.078125, ((0, 2), (1, 4), (2, 4)))
    cotangent = scatter_about(key_of[13], (MICRO, TOK_MB, D), 1.0, 6.0, ((1, 4),))
    return dict(tokens=tokens, lengths=lengths, gain_attn=gain_attn, w_query=w_query, w_key=w_key, w_value=w_value, w_gate_conv=w_gate_conv, conv_taps=conv_taps, w_out=w_out, gain_ffn=gain_ffn, w_gate=w_gate, w_up=w_up, w_down=w_down, cotangent=cotangent)


@jax.custom_vjp
def low(v):
    return lax.optimization_barrier(v.astype(jnp.bfloat16)).astype(jnp.float32)

@jax.custom_vjp
def low_back(v):
    return v

def low_keep(v):
    return (low(v), None)

def low_pass(kept, grad):
    return (grad,)

def back_keep(v):
    return (v, None)

def back_low(kept, grad):
    return (low(grad),)
low.defvjp(low_keep, low_pass)
low_back.defvjp(back_keep, back_low)
precise = lax.Precision.HIGHEST
epsilon = 1e-05

def rms_norm(vector, scale_gain):
    return vector * lax.rsqrt(lax.optimization_barrier(jnp.mean(vector * vector, axis=-1, keepdims=True)) + epsilon) * scale_gain

def features(vector):
    second = vector[..., :, None] * vector[..., None, :] / (4.0 * math.sqrt(2.0))
    constant = jnp.ones(vector.shape[:-1] + (1,), jnp.float32)
    squares = second.reshape(vector.shape[:-1] + (vector.shape[-1] * vector.shape[-1],))
    return jnp.concatenate([constant, vector * 0.5, squares], axis=-1)

def seq_begin(lengths_row, positions):
    seq_starts = (jnp.cumsum(lengths_row) - lengths_row).astype(jnp.int32)
    chosen = jnp.where(seq_starts[None, :] <= positions[:, None], seq_starts[None, :], 0)
    return lax.optimization_barrier(jnp.max(chosen, axis=1)).astype(jnp.int32)

def attend_block(carried, block_inputs):
    running, norm_sum = carried
    queries, keys, values, starts_at, block_start = block_inputs
    row_count = starts_at.shape[0]
    scores = low_back(jnp.einsum('thf,shf->hts', queries, keys, precision=precise) / 4.0)
    places = jnp.arange(row_count, dtype=jnp.int32)
    visible = (starts_at[:, None] == starts_at[None, :]) & (places[None, :] <= places[:, None])
    weights = low(jnp.where(visible[None], 1.0 + scores + 0.5 * scores * scores, 0.0))
    phi_query = features(queries)
    phi_key = features(keys)
    carried_in = (starts_at < block_start).astype(jnp.float32)
    numerator = low_back(jnp.einsum('hts,she->the', weights, values, precision=precise) + carried_in[:, None, None] * jnp.einsum('thp,hpe->the', phi_query, running, precision=precise))
    denominator = jnp.transpose(lax.optimization_barrier(jnp.sum(weights, axis=2))) + carried_in[:, None] * jnp.einsum('thp,hp->th', phi_query, norm_sum, precision=precise)
    attended = numerator / denominator[:, :, None]
    last_rows = (starts_at == starts_at[row_count - 1]).astype(jnp.float32)
    restart = (starts_at[row_count - 1] >= block_start).astype(jnp.float32)
    phi_last = phi_key * last_rows[:, None, None]
    new_running = (1.0 - restart) * running + jnp.einsum('shp,she->hpe', phi_last, values, precision=precise)
    new_norm = (1.0 - restart) * norm_sum + lax.optimization_barrier(jnp.sum(phi_last, axis=0))
    return ((new_running, new_norm), attended)

def layer(inputs, params, starts_at):
    gain_attn, w_query, w_key, w_value, w_gate_conv, conv_taps, w_out, gain_ffn, w_gate, w_up, w_down = params
    row_total = inputs.shape[0]
    blocks = row_total // TOK_DEV
    normed = low(rms_norm(inputs, gain_attn))
    queries = low(low_back(jnp.dot(normed, w_query, precision=precise)))
    keys = low(low_back(jnp.dot(normed, w_key, precision=precise)))
    values = low(low_back(jnp.dot(normed, w_value, precision=precise)))
    gate_conv = low_back(jnp.dot(normed, w_gate_conv, precision=precise))
    initial = (jnp.zeros((H, PHI, HD), jnp.float32), jnp.zeros((H, PHI), jnp.float32))
    block_inputs = (queries.reshape(blocks, TOK_DEV, H, FK), keys.reshape(blocks, TOK_DEV, H, FK), values.reshape(blocks, TOK_DEV, H, HD), starts_at.reshape(blocks, TOK_DEV), jnp.arange(blocks, dtype=jnp.int32) * TOK_DEV)
    final_carry, attended = lax.scan(jax.checkpoint(attend_block), initial, block_inputs)
    attended = attended.reshape(row_total, D)
    positions = jnp.arange(row_total, dtype=jnp.int32)
    conv_out = conv_taps[0] * attended
    for offset in range(1, KW):
        earlier_rows = jnp.concatenate([jnp.zeros((offset, D), jnp.float32), attended[:row_total - offset]], axis=0)
        allowed = (positions - offset >= starts_at).astype(jnp.float32)
        conv_out = conv_out + conv_taps[offset] * earlier_rows * allowed[:, None]
    gated_out = low(conv_out * gate_conv)
    middle = inputs + low_back(jnp.dot(gated_out, w_out, precision=precise))
    normed_two = low(rms_norm(middle, gain_ffn))
    gate_pre = low_back(jnp.dot(normed_two, w_gate, precision=precise))
    upward = low_back(jnp.dot(normed_two, w_up, precision=precise))
    hidden = low(jax.nn.silu(gate_pre) * upward)
    return middle + low_back(jnp.dot(hidden, w_down, precision=precise))

def section_pass(inputs, params, starts_list):
    return jnp.stack([layer(inputs[micro_index], params, starts_list[micro_index]) for micro_index in range(MICRO)])

def reference(tokens, lengths, gain_attn, w_query, w_key, w_value, w_gate_conv, conv_taps, w_out, gain_ffn, w_gate, w_up, w_down, cotangent):
    positions = jnp.arange(TOK_MB, dtype=jnp.int32)
    starts_list = [seq_begin(lengths[micro_index], positions) for micro_index in range(MICRO)]
    weights_all = (gain_attn, w_query, w_key, w_value, w_gate_conv, conv_taps, w_out, gain_ffn, w_gate, w_up, w_down)
    first_params = tuple((weight[0].astype(jnp.float32) for weight in weights_all))
    second_params = tuple((weight[1].astype(jnp.float32) for weight in weights_all))

    def run_section(inputs, params):
        return section_pass(inputs, params, starts_list)
    first_out, first_back = jax.vjp(run_section, tokens.astype(jnp.float32), first_params)
    first_low = first_out.astype(jnp.bfloat16)
    second_out, second_back = jax.vjp(run_section, first_low.astype(jnp.float32), second_params)
    middle_grad, second_grads = second_back(cotangent.astype(jnp.float32))
    middle_low = middle_grad.astype(jnp.bfloat16)
    input_grad, first_grads = first_back(middle_low.astype(jnp.float32))
    activations = jnp.stack([first_low, second_out.astype(jnp.bfloat16)])
    input_grads = jnp.stack([input_grad.astype(jnp.bfloat16), middle_low])
    stacked = [jnp.stack([first_grads[param_index], second_grads[param_index]]) for param_index in range(11)]
    return (activations, input_grads, stacked[0], stacked[1], stacked[2], stacked[3], stacked[4], stacked[5], stacked[6], stacked[7], stacked[8], stacked[9], stacked[10])
```

```python
import math

import jax
import jax.numpy as jnp
from jax import lax
from jax.sharding import PartitionSpec as P

FK = 16
KW = 3


epsilon = 1e-05


def carried_in_2(x, axis, join, neutral):
    place = lax.axis_index(axis)
    gathered = jax.tree.map(
        lambda a, kind: lax.all_gather(a.astype(kind), axis),
        x,
        (jnp.bfloat16, jnp.bfloat16, jnp.bfloat16),
    )
    state = jax.tree.map(lambda a, e: jnp.zeros_like(a) + jnp.asarray(e, a.dtype), x, neutral)

    def one(turn, state):
        return join(
            state,
            jax.tree.map(
                lambda a, own: lax.dynamic_index_in_dim(a, turn, 0, False).astype(own.dtype),
                gathered,
                x,
            ),
        )

    return lax.fori_loop(0, place, one, state)


def carried_in_3(x, axis, combine, identity):
    devices, mine = (lax.axis_size(axis), lax.axis_index(axis))
    everything = jax.tree.map(
        lambda part, kind: lax.all_gather(part.astype(kind), axis),
        x,
        jax.tree.map(lambda a: jnp.bfloat16 if a.dtype == jnp.float32 else a.dtype, x),
    )
    start = jax.tree.map(
        lambda part, zero: jnp.broadcast_to(jnp.asarray(zero, part.dtype), part.shape), x, identity
    )

    def turn(k, before):
        at = devices - 1 - k
        reached = at > mine
        new = combine(
            before, jax.tree.map(lambda part, own: part[at].astype(own.dtype), everything, x)
        )
        return jax.tree.map(lambda a, b: jnp.where(reached, a, b), new, before)

    return lax.fori_loop(0, devices, turn, start)


def from_behind(x, axis, by):
    devices = lax.axis_size(axis)
    pairs = [(i, i + by) for i in range(devices) if 0 <= i + by < devices]
    return lax.ppermute(x, axis, pairs)


def rms_norm(vector, scale_gain):
    return (
        vector * lax.rsqrt(jnp.mean(vector * vector, axis=-1, keepdims=True) + epsilon) * scale_gain
    )


def features(vector):
    second = vector[..., :, None] * vector[..., None, :] / (4.0 * math.sqrt(2.0))
    constant = jnp.ones(vector.shape[:-1] + (1,), jnp.float32)
    squares = second.reshape(vector.shape[:-1] + (vector.shape[-1] * vector.shape[-1],))
    return jnp.concatenate([constant, vector * 0.5, squares], axis=-1)


def seq_begin(lengths_row, positions):
    seq_starts = jnp.cumsum(lengths_row) - lengths_row
    chosen = jnp.where(seq_starts[None, :] <= positions[:, None], seq_starts[None, :], 0)
    return jnp.max(chosen, axis=1)


def chain_combine(earlier_part, later_part):
    carried = 1.0 - later_part[2][0]
    return (
        later_part[0] + carried * earlier_part[0],
        later_part[1] + carried * earlier_part[1],
        jnp.maximum(earlier_part[2], later_part[2]),
    )


def carry_forward(local_state, local_norm, restart):
    identity = (
        jnp.zeros_like(local_state),
        jnp.zeros_like(local_norm),
        jnp.zeros((1,), jnp.float32),
    )
    prefix = carried_in_2((local_state, local_norm, restart[None]), "seq", chain_combine, identity)
    state_in, norm_in = (prefix[0], prefix[1])
    return (state_in, norm_in)


def carry_backward(state_grad, norm_grad, restart):
    identity = (jnp.zeros_like(state_grad), jnp.zeros_like(norm_grad), jnp.zeros((1,), jnp.float32))
    suffix = carried_in_3((state_grad, norm_grad, restart[None]), "seq", chain_combine, identity)
    state_out, norm_out = (suffix[0], suffix[1])
    return (state_out, norm_out)


def head_total(part_sum):
    return lax.psum(part_sum.astype(jnp.bfloat16), "head").astype(jnp.float32)


def head_back(part_sum):
    return lax.psum(part_sum.astype(jnp.bfloat16), "head").astype(jnp.float32)


def own_scores(query_heads, key_heads, starts_at):
    row_count = starts_at.shape[0]
    scores = (
        jnp.einsum("thf,shf->hts", query_heads, key_heads, preferred_element_type=jnp.float32)
        * 0.25
    )
    places = jnp.arange(row_count, dtype=jnp.int32)
    visible = (starts_at[:, None] == starts_at[None, :]) & (places[None, :] <= places[:, None])
    return (scores, visible)


def forward_layer(inputs, begin_ext, setting):
    weights_all, gain_one, gain_two, taps_local, block_start = setting
    (
        query_weight,
        key_weight,
        value_weight,
        gconv_weight,
        out_weight,
        gate_weight,
        up_weight,
        down_weight,
    ) = weights_all
    row_count = inputs.shape[0]
    starts_at = begin_ext[:row_count]
    positions = block_start + jnp.arange(row_count, dtype=jnp.int32)
    normed = rms_norm(inputs, gain_one).astype(jnp.bfloat16)
    queries = jnp.dot(normed, query_weight, preferred_element_type=jnp.float32).astype(jnp.bfloat16)
    keys_low = jnp.dot(normed, key_weight, preferred_element_type=jnp.float32).astype(jnp.bfloat16)
    values_low = jnp.dot(normed, value_weight, preferred_element_type=jnp.float32).astype(
        jnp.bfloat16
    )
    gate_conv = jnp.dot(normed, gconv_weight, preferred_element_type=jnp.float32)
    local_heads = queries.shape[1] // FK
    query_heads = queries.reshape(row_count, local_heads, FK)
    key_heads = keys_low.reshape(row_count, local_heads, FK)
    value_heads = values_low.reshape(row_count, local_heads, -1)
    scores, visible = own_scores(query_heads, key_heads, starts_at)
    attn_weights = jnp.where(visible[None], 1.0 + scores + 0.5 * scores * scores, 0.0).astype(
        jnp.bfloat16
    )
    phi_query = features(query_heads.astype(jnp.float32))
    phi_key = features(key_heads.astype(jnp.float32))
    last_rows = (starts_at == starts_at[row_count - 1]).astype(jnp.float32)
    restart = (starts_at[row_count - 1] >= block_start).astype(jnp.float32)
    phi_last = phi_key * last_rows[:, None, None]
    local_state = jnp.einsum(
        "shp,she->hpe", phi_last, value_heads.astype(jnp.float32)
    )
    local_norm = jnp.sum(phi_last, axis=0)
    state_in, norm_in = carry_forward(local_state, local_norm, restart)
    carried_in = (starts_at < block_start).astype(jnp.float32)
    numerator = jnp.einsum(
        "hts,she->the", attn_weights, value_heads, preferred_element_type=jnp.float32
    ) + carried_in[:, None, None] * jnp.einsum(
        "thp,hpe->the", phi_query, state_in
    )
    denominator = jnp.transpose(jnp.sum(attn_weights, axis=2, dtype=jnp.float32)) + carried_in[
        :, None
    ] * jnp.einsum("thp,hp->th", phi_query, norm_in)
    attended = (numerator / denominator[:, :, None]).reshape(row_count, -1)
    edge_rows = from_behind(attended[row_count - 2 :], "seq", 1)
    extended = jnp.concatenate([edge_rows, attended], axis=0)
    conv_out = taps_local[0] * extended[2:]
    for offset in range(1, KW):
        allowed = (positions - offset >= starts_at).astype(jnp.float32)
        conv_out = (
            conv_out
            + taps_local[offset] * extended[2 - offset : 2 - offset + row_count] * allowed[:, None]
        )
    gated_out = (conv_out * gate_conv).astype(jnp.bfloat16)
    branch_part = jnp.einsum(
        "tc,dc->td", gated_out, out_weight, preferred_element_type=jnp.float32
    )
    middle = inputs + head_total(branch_part)
    normed_two = rms_norm(middle, gain_two).astype(jnp.bfloat16)
    gate_pre = jnp.dot(normed_two, gate_weight, preferred_element_type=jnp.float32)
    upward = jnp.dot(normed_two, up_weight, preferred_element_type=jnp.float32)
    hidden = (jax.nn.silu(gate_pre) * upward).astype(jnp.bfloat16)
    ffn_part = jnp.einsum(
        "tf,df->td", hidden, down_weight, preferred_element_type=jnp.float32
    )
    output = middle + head_total(ffn_part)
    stored = (
        inputs,
        begin_ext,
        normed,
        queries,
        keys_low,
        values_low,
        gate_conv,
        state_in,
        norm_in,
        numerator,
        denominator,
        extended,
        conv_out,
        gated_out,
        middle,
        normed_two,
        gate_pre,
        upward,
        hidden,
    )
    return (output, stored)


def backward_layer(grad_out, stored, setting):
    weights_all, gain_one, gain_two, taps_local, block_start = setting
    (
        query_weight,
        key_weight,
        value_weight,
        gconv_weight,
        out_weight,
        gate_weight,
        up_weight,
        down_weight,
    ) = weights_all
    (
        inputs,
        begin_ext,
        normed,
        queries,
        keys_low,
        values_low,
        gate_conv,
        state_in,
        norm_in,
        numerator,
        denominator,
        extended,
        conv_out,
        gated_out,
        middle,
        normed_two,
        gate_pre,
        upward,
        hidden,
    ) = stored
    row_count = inputs.shape[0]
    starts_at = begin_ext[:row_count]
    positions_ext = block_start + jnp.arange(row_count + 2, dtype=jnp.int32)
    grad_low = grad_out.astype(jnp.bfloat16)
    grad_down = jnp.einsum("tf,td->df", hidden, grad_low, preferred_element_type=jnp.float32)
    back_hidden = jnp.einsum("td,df->tf", grad_low, down_weight, preferred_element_type=jnp.float32)
    silu_value, silu_back = jax.vjp(jax.nn.silu, gate_pre)
    back_gate = silu_back(back_hidden * upward)[0].astype(jnp.bfloat16)
    back_up = (back_hidden * silu_value).astype(jnp.bfloat16)
    grad_gate = jnp.einsum("tc,tf->cf", normed_two, back_gate, preferred_element_type=jnp.float32)
    grad_up = jnp.einsum("tc,tf->cf", normed_two, back_up, preferred_element_type=jnp.float32)
    part_two = jnp.einsum(
        "tf,cf->tc", back_gate, gate_weight, preferred_element_type=jnp.float32
    ) + jnp.einsum("tf,cf->tc", back_up, up_weight, preferred_element_type=jnp.float32)
    back_norm_two = head_back(part_two)
    unused_two, norm_back_two = jax.vjp(rms_norm, middle, gain_two)
    back_middle, grad_gain_two = norm_back_two(back_norm_two)
    back_middle = grad_out + back_middle
    back_branch = back_middle.astype(jnp.bfloat16)
    grad_out_weight = jnp.einsum(
        "tc,td->dc", gated_out, back_branch, preferred_element_type=jnp.float32
    )
    back_gated = jnp.einsum(
        "td,dc->tc", back_branch, out_weight, preferred_element_type=jnp.float32
    )
    back_conv = back_gated * gate_conv
    back_gconv = (back_gated * conv_out).astype(jnp.bfloat16)
    grad_gconv = jnp.einsum("tc,tf->cf", normed, back_gconv, preferred_element_type=jnp.float32)
    edge_back = from_behind(back_conv[:2], "seq", -1)
    conv_ext = jnp.concatenate([back_conv, edge_back], axis=0)
    back_attended = taps_local[0] * back_conv
    taps_rows = [jnp.sum(back_conv * extended[2:], axis=0)]
    for offset in range(1, KW):
        allowed_ext = (positions_ext - offset >= begin_ext).astype(jnp.float32)
        back_attended = (
            back_attended
            + taps_local[offset]
            * conv_ext[offset : offset + row_count]
            * allowed_ext[offset : offset + row_count, None]
        )
        allowed = allowed_ext[:row_count]
        taps_rows.append(
            jnp.sum(
                back_conv * extended[2 - offset : 2 - offset + row_count] * allowed[:, None], axis=0
            )
        )
    local_heads = queries.shape[1] // FK
    query_heads = queries.reshape(row_count, local_heads, FK)
    key_heads = keys_low.reshape(row_count, local_heads, FK)
    value_heads = values_low.reshape(row_count, local_heads, -1)
    back_out = back_attended.reshape(row_count, local_heads, -1)
    back_numer = (back_out / denominator[:, :, None]).astype(jnp.bfloat16)
    back_numer_wide = back_numer.astype(jnp.float32)
    back_denom = -jnp.sum(back_out * numerator, axis=2) / (denominator * denominator)
    scores, visible = own_scores(query_heads, key_heads, starts_at)
    attn_weights = jnp.where(visible[None], 1.0 + scores + 0.5 * scores * scores, 0.0).astype(
        jnp.bfloat16
    )
    back_weights = (
        jnp.einsum("the,she->hts", back_numer, value_heads, preferred_element_type=jnp.float32)
        + jnp.transpose(back_denom)[:, :, None]
    )
    back_scores = jnp.where(visible[None], back_weights * (1.0 + scores), 0.0).astype(jnp.bfloat16)
    back_query = (
        jnp.einsum("hts,shf->thf", back_scores, key_heads, preferred_element_type=jnp.float32)
        * 0.25
    )
    back_key = (
        jnp.einsum("hts,thf->shf", back_scores, query_heads, preferred_element_type=jnp.float32)
        * 0.25
    )
    back_value = jnp.einsum(
        "hts,the->she", attn_weights, back_numer, preferred_element_type=jnp.float32
    )
    phi_query, phi_back_query = jax.vjp(features, query_heads.astype(jnp.float32))
    phi_key, phi_back_key = jax.vjp(features, key_heads.astype(jnp.float32))
    carried_in = (starts_at < block_start).astype(jnp.float32)
    back_phi_query = carried_in[:, None, None] * (
        jnp.einsum("the,hpe->thp", back_numer_wide, state_in)
        + back_denom[:, :, None] * norm_in[None]
    )
    phi_used = phi_query * carried_in[:, None, None]
    state_grad = jnp.einsum("thp,the->hpe", phi_used, back_numer_wide)
    norm_grad = jnp.einsum("thp,th->hp", phi_used, back_denom)
    last_rows = (starts_at == starts_at[row_count - 1]).astype(jnp.float32)
    restart = (starts_at[row_count - 1] >= block_start).astype(jnp.float32)
    state_out, norm_out = carry_backward(state_grad, norm_grad, restart)
    back_phi_key = last_rows[:, None, None] * (
        jnp.einsum("she,hpe->shp", value_heads.astype(jnp.float32), state_out)
        + norm_out[None]
    )
    back_value = back_value + last_rows[:, None, None] * jnp.einsum(
        "shp,hpe->she", phi_key, state_out
    )
    back_query = back_query + phi_back_query(back_phi_query)[0]
    back_key = back_key + phi_back_key(back_phi_key)[0]
    query_low = back_query.reshape(row_count, -1).astype(jnp.bfloat16)
    key_low = back_key.reshape(row_count, -1).astype(jnp.bfloat16)
    value_low = back_value.reshape(row_count, -1).astype(jnp.bfloat16)
    grad_query = jnp.einsum("tc,tf->cf", normed, query_low, preferred_element_type=jnp.float32)
    grad_key = jnp.einsum("tc,tf->cf", normed, key_low, preferred_element_type=jnp.float32)
    grad_value = jnp.einsum("tc,tf->cf", normed, value_low, preferred_element_type=jnp.float32)
    part_one = (
        jnp.einsum("tf,cf->tc", query_low, query_weight, preferred_element_type=jnp.float32)
        + jnp.einsum("tf,cf->tc", key_low, key_weight, preferred_element_type=jnp.float32)
        + jnp.einsum("tf,cf->tc", value_low, value_weight, preferred_element_type=jnp.float32)
        + jnp.einsum("tf,cf->tc", back_gconv, gconv_weight, preferred_element_type=jnp.float32)
    )
    back_normed = head_back(part_one)
    unused_one, norm_back_one = jax.vjp(rms_norm, inputs, gain_one)
    back_inputs, grad_gain_one = norm_back_one(back_normed)
    back_inputs = back_middle + back_inputs
    weight_grads = (
        grad_query,
        grad_key,
        grad_value,
        grad_gconv,
        grad_out_weight,
        grad_gate,
        grad_up,
        grad_down,
    )
    small_grads = (grad_gain_one, grad_gain_two, jnp.stack(taps_rows))
    return (back_inputs, weight_grads, small_grads)


def both_layers(weight):
    gathered = lax.all_gather(weight, ("section", "seq"), axis=0, tiled=True)
    rows = gathered.shape[0] // 2
    return (gathered[:rows], gathered[rows:])


def scatter_layers(first_grad, second_grad):
    both = jnp.concatenate([first_grad, second_grad], axis=0).astype(jnp.bfloat16)
    return lax.psum_scatter(both, ("section", "seq"), scatter_dimension=0, tiled=True).astype(
        jnp.float32
    )


def on_device(
    tokens,
    lengths,
    gain_attn,
    w_query,
    w_key,
    w_value,
    w_gate_conv,
    conv_taps,
    w_out,
    gain_ffn,
    w_gate,
    w_up,
    w_down,
    cotangent,
):
    head_count = lax.axis_size("head")
    head_index = lax.axis_index("head")
    micro = lax.axis_index("section")
    micro_count, row_count, model_width = tokens.shape
    channels = model_width // head_count
    query_both = both_layers(w_query[0])
    key_both = both_layers(w_key[0])
    value_both = both_layers(w_value[0])
    gconv_both = both_layers(w_gate_conv[0])
    out_both = both_layers(w_out[0].T)
    gate_both = both_layers(w_gate[0])
    up_both = both_layers(w_up[0])
    down_both = both_layers(w_down[0].T)
    gains_one = lax.all_gather(gain_attn[0], "section").astype(jnp.float32)
    gains_two = lax.all_gather(gain_ffn[0], "section").astype(jnp.float32)
    taps_both = lax.dynamic_slice_in_dim(
        lax.all_gather(conv_taps[0], "section").astype(jnp.float32),
        head_index * channels,
        channels,
        2,
    )
    block_start = lax.axis_index("seq") * row_count
    positions_ext = block_start + jnp.arange(row_count + 2, dtype=jnp.int32)
    starts_at = seq_begin(lax.dynamic_index_in_dim(lengths, micro, 0, False), positions_ext)
    settings = [
        (
            (
                query_both[layer],
                key_both[layer],
                value_both[layer],
                gconv_both[layer],
                out_both[layer],
                gate_both[layer],
                up_both[layer],
                down_both[layer],
            ),
            gains_one[layer],
            gains_two[layer],
            taps_both[layer],
            block_start,
        )
        for layer in range(2)
    ]
    current = lax.dynamic_index_in_dim(tokens, micro, 0, False)
    outputs = []
    stored = []
    for layer in range(2):
        layer_out, kept = forward_layer(current.astype(jnp.float32), starts_at, settings[layer])
        current = layer_out.astype(jnp.bfloat16)
        outputs.append(current)
        stored.append(kept)
    grad_in = lax.dynamic_index_in_dim(cotangent, micro, 0, False)
    back = [None, None]
    grads = [None, None]
    smalls = [None, None]
    for layer in (1, 0):
        back_inputs, grads[layer], smalls[layer] = backward_layer(
            grad_in.astype(jnp.float32), stored[layer], settings[layer]
        )
        grad_in = back_inputs.astype(jnp.bfloat16)
        back[layer] = grad_in
    shards = [scatter_layers(a, b) for a, b in zip(grads[0], grads[1])]
    shards[4] = shards[4].T
    shards[7] = shards[7].T
    column_mask = (jnp.arange(model_width, dtype=jnp.int32) // channels == head_index).astype(
        jnp.float32
    )
    packed = []
    for layer in range(2):
        gain_one_sum, gain_two_sum, taps_sum = smalls[layer]
        taps_full = lax.dynamic_update_slice_in_dim(
            jnp.zeros((taps_sum.shape[0], model_width), jnp.float32),
            taps_sum,
            head_index * channels,
            1,
        )
        packed.append(
            jnp.concatenate(
                [
                    (gain_one_sum * column_mask)[None],
                    (gain_two_sum * column_mask)[None],
                    taps_full,
                ],
                axis=0,
            )
        )
    totals = lax.dynamic_index_in_dim(
        lax.psum(jnp.stack(packed), ("section", "seq", "head")), micro, 0, False
    )

    def to_layers(pair):
        mine = lax.dynamic_index_in_dim(jnp.stack(pair), micro, 0, False)
        theirs = lax.dynamic_index_in_dim(jnp.stack(pair), 1 - micro, 0, False)
        swapped = lax.ppermute(theirs, "section", [(0, 1), (1, 0)])
        first = jnp.where(micro == 0, mine, swapped)
        second = jnp.where(micro == 0, swapped, mine)
        return jnp.stack([first, second])[None]

    return (
        to_layers(outputs),
        to_layers(back),
        totals[0][None],
        shards[0][None],
        shards[1][None],
        shards[2][None],
        shards[3][None],
        totals[2:][None],
        shards[4][None],
        totals[1][None],
        shards[5][None],
        shards[6][None],
        shards[7][None],
    )


def solution(mesh):
    placed = (
        P(None, "seq", None),
        P(),
        P("section", None),
        P("section", "seq", "head"),
        P("section", "seq", "head"),
        P("section", "seq", "head"),
        P("section", "seq", "head"),
        P("section", None, None),
        P("section", "head", "seq"),
        P("section", None),
        P("section", "seq", "head"),
        P("section", "seq", "head"),
        P("section", "head", "seq"),
        P(None, "seq", None),
    )
    return jax.shard_map(
        on_device,
        mesh=mesh,
        in_specs=placed,
        out_specs=(
            P("section", None, "seq", None),
            P("section", None, "seq", None),
            P("section", None),
            P("section", "seq", "head"),
            P("section", "seq", "head"),
            P("section", "seq", "head"),
            P("section", "seq", "head"),
            P("section", None, None),
            P("section", "head", "seq"),
            P("section", None),
            P("section", "seq", "head"),
            P("section", "seq", "head"),
            P("section", "head", "seq"),
        ),
        check_vma=False,
    )
```

```python
import functools
import math

import jax
import jax.numpy as jnp
from jax import lax
from jax.experimental import pallas as pl
from jax.experimental.pallas import tpu as pltpu
from jax.sharding import PartitionSpec as P

FK = 16
KW = 3
MESH = pl.DeviceIdType.MESH
epsilon = 1e-05


def remote(src, dst, send, recv, **where):
    return pltpu.make_async_remote_copy(
        src_ref=src,
        dst_ref=dst,
        send_sem=send,
        recv_sem=recv,
        device_id=where,
        device_id_type=MESH,
    )


def greet(line, spread):
    core, z, q = lax.axis_index("section"), lax.axis_index("head"), lax.axis_index("seq")
    depth, count = lax.axis_size("head"), lax.axis_size("seq")
    barrier = pltpu.get_barrier_semaphore()

    def hello(**where):
        pl.semaphore_signal(barrier, inc=1, device_id=where, device_id_type=MESH)

    hello(section=1 - core)
    expected = 1
    if spread:
        for j in range(1, count):
            for h in range(2):
                hello(section=h, seq=lax.rem(q + j, count))
        expected += 2 * (count - 1)
    if line:

        @pl.when(z > 0)
        def _():
            hello(head=z - 1)

        @pl.when(z < depth - 1)
        def _():
            hello(head=z + 1)

        expected = expected + jnp.where(z > 0, 1, 0) + jnp.where(z < depth - 1, 1, 0)
    pl.semaphore_wait(barrier, expected)


class LineSum:
    def __init__(self, p_ref, o_ref, scratch, chunks, lag):
        self.p_ref, self.o_ref, self.chunks, self.lag = p_ref, o_ref, chunks, lag
        self.pin, self.low, self.high, self.out = scratch[:4]
        self.ps, self.pr, self.rs, self.rl, self.rh, self.bs, self.br, self.ts, self.tr = scratch[4:]
        self.z, self.n = lax.axis_index("head"), lax.axis_size("head")
        self.core = lax.axis_index("section")
        self.half = p_ref.shape[1] // 2
        self.step = self.half // chunks
        self.depth = max((self.n - 1) // 2, self.n - 1 - (self.n - 1) // 2)
        self.turns = chunks + 2 * self.depth * lag

    @staticmethod
    def scratch(rows, width, chunks):
        sem = pltpu.SemaphoreType.DMA((2, chunks))
        bank = pltpu.SemaphoreType.DMA((2, 2, chunks))
        return [pltpu.VMEM((rows, width), jnp.bfloat16)] * 4 + [
            sem, sem, sem, sem, sem, bank, sem, sem, sem
        ]

    def root(self, d):
        return (self.n - 1) // 2 if d == 0 else self.n - 1 - (self.n - 1) // 2

    def rng(self, d, k):
        return pl.ds(pl.multiple_of(d * self.half + k * self.step, self.step), self.step)

    def part(self, d, k):
        r = self.rng(d, k)
        other = 1 - self.core
        return remote(
            self.p_ref.at[other, r], self.pin.at[r], self.ps.at[d, k], self.pr.at[d, k], section=other
        )

    def up(self, d, k):
        r = self.rng(d, k)
        return remote(
            self.out.at[r], self.low.at[r], self.rs.at[d, k], self.rl.at[d, k], head=self.z + 1
        )

    def down(self, d, k):
        r = self.rng(d, k)
        return remote(
            self.out.at[r], self.high.at[r], self.rs.at[d, k], self.rh.at[d, k], head=self.z - 1
        )

    def share(self, d, k, side):
        r = self.rng(d, k)
        at = self.o_ref.at[self.core, r]
        return remote(
            at, at, self.bs.at[side, d, k], self.br.at[d, k], head=self.z + (1 if side else -1)
        )

    def give(self, d, k):
        r = self.rng(d, k)
        at = self.o_ref.at[self.core, r]
        return remote(at, at, self.ts.at[d, k], self.tr.at[d, k], section=1 - self.core)

    def start(self):
        for k in range(self.chunks):
            for d in range(2):
                self.part(d, k).start()

    def gathered(self, d, k):
        r = self.rng(d, k)
        z, n, root = self.z, self.n, self.root(d)
        self.part(d, k).wait_recv()
        mine = self.p_ref[self.core, r, :].astype(jnp.float32) + self.pin[r, :].astype(jnp.float32)

        @pl.when((z == 0) & (root > 0))
        def _():
            self.out[r, :] = mine.astype(jnp.bfloat16)
            self.up(d, k).start()

        @pl.when((z == n - 1) & (root < n - 1))
        def _():
            self.out[r, :] = mine.astype(jnp.bfloat16)
            self.down(d, k).start()

        @pl.when((z > 0) & (z < root))
        def _():
            self.up(d, k).wait_recv()
            self.out[r, :] = (mine + self.low[r, :].astype(jnp.float32)).astype(jnp.bfloat16)
            self.up(d, k).start()

        @pl.when((z < n - 1) & (z > root))
        def _():
            self.down(d, k).wait_recv()
            self.out[r, :] = (mine + self.high[r, :].astype(jnp.float32)).astype(jnp.bfloat16)
            self.down(d, k).start()

        @pl.when(z == root)
        def _():
            total = mine
            if root > 0:
                self.up(d, k).wait_recv()
                total = total + self.low[r, :].astype(jnp.float32)
            if root < n - 1:
                self.down(d, k).wait_recv()
                total = total + self.high[r, :].astype(jnp.float32)
            self.o_ref[self.core, r, :] = total.astype(jnp.bfloat16)
            if root > 0:
                self.share(d, k, 0).start()
            if root < n - 1:
                self.share(d, k, 1).start()
            self.give(d, k).start()

    def passed(self, d, k):
        z, n, root = self.z, self.n, self.root(d)
        self.share(d, k, 0).wait_recv()

        @pl.when((z < root) & (z > 0))
        def _():
            self.share(d, k, 0).start()

        @pl.when((z > root) & (z < n - 1))
        def _():
            self.share(d, k, 1).start()

        self.give(d, k).start()

    def turn(self, t):
        z, n = self.z, self.n
        for d in range(2):
            root = self.root(d)
            deep = max(root, n - 1 - root)
            below = jnp.where(z < root, z, jnp.where(z > root, n - 1 - z, deep))
            k = t - below * self.lag
            far = jnp.abs(z - root)

            @pl.when((k >= 0) & (k < self.chunks))
            def _():
                self.gathered(d, k)

            b = t - (deep + far) * self.lag

            @pl.when((b >= 0) & (b < self.chunks) & (far > 0))
            def _():
                self.passed(d, b)

    def finish(self):
        z, n = self.z, self.n
        for d in range(2):
            root = self.root(d)
            for k in range(self.chunks):
                self.part(d, k).wait_send()
                self.give(d, k).wait_recv()
                self.give(d, k).wait_send()

                @pl.when(z < root)
                def _():
                    self.up(d, k).wait_send()

                @pl.when(z > root)
                def _():
                    self.down(d, k).wait_send()

                if root > 0:

                    @pl.when((z <= root) & (z > 0))
                    def _():
                        self.share(d, k, 0).wait_send()

                if root < n - 1:

                    @pl.when((z >= root) & (z < n - 1))
                    def _():
                        self.share(d, k, 1).wait_send()


class Gather:
    def __init__(self, layer, srcs, dsts, sems):
        self.layer, self.srcs, self.dsts = layer, srcs, dsts
        self.ss, self.rr, self.ls = sems
        self.core, self.q = lax.axis_index("section"), lax.axis_index("seq")
        self.n = lax.axis_size("seq")

    @staticmethod
    def scratch(count, n):
        return [
            pltpu.SemaphoreType.DMA((count, n, 2)),
            pltpu.SemaphoreType.DMA((count, n)),
            pltpu.SemaphoreType.DMA((count,)),
        ]

    def copies(self, a):
        for j in range(1, self.n):
            for h in range(2):
                yield remote(
                    self.srcs[a].at[h], self.dsts[a].at[self.q], self.ss.at[a, j, h],
                    self.rr.at[a, self.q], section=h, seq=lax.rem(self.q + j, self.n),
                )
        yield remote(
            self.srcs[a].at[1 - self.layer], self.dsts[a].at[self.q], self.ss.at[a, 0, 0],
            self.rr.at[a, self.q], section=1 - self.layer,
        )

    def local(self, a):
        return pltpu.make_async_copy(
            self.srcs[a].at[self.layer], self.dsts[a].at[self.q], self.ls.at[a]
        )

    def arrival(self, a, s):
        return remote(
            self.srcs[a].at[0], self.dsts[a].at[s], self.ss.at[a, 0, 0], self.rr.at[a, s],
            section=1 - self.core,
        )

    def start(self):
        @pl.when(self.core == self.layer)
        def _():
            for a in range(len(self.srcs)):
                for copy in self.copies(a):
                    copy.start()
                self.local(a).start()

    def finish(self):
        for a in range(len(self.srcs)):
            for j in range(1, self.n):
                self.arrival(a, lax.rem(self.q + j, self.n)).wait_recv()

            @pl.when(self.core == self.layer)
            def _():
                self.local(a).wait()
                for copy in self.copies(a):
                    copy.wait_send()

            @pl.when(self.core != self.layer)
            def _():
                self.arrival(a, self.q).wait_recv()


class Scatter:
    def __init__(self, layer, srcs, dsts, sems):
        self.layer, self.srcs, self.dsts = layer, srcs, dsts
        self.ss, self.rr, self.ls = sems
        self.core, self.q = lax.axis_index("section"), lax.axis_index("seq")
        self.n = lax.axis_size("seq")

    @staticmethod
    def scratch(count, n):
        return [
            pltpu.SemaphoreType.DMA((count, n)),
            pltpu.SemaphoreType.DMA((count, 2, n)),
            pltpu.SemaphoreType.DMA((count,)),
        ]

    def copies(self, a):
        for j in range(1, self.n):
            t = lax.rem(self.q + j, self.n)
            yield remote(
                self.srcs[a].at[t], self.dsts[a].at[self.core, self.q], self.ss.at[a, j],
                self.rr.at[a, self.core, self.q], section=self.layer, seq=t,
            )

    def near(self, a):
        return remote(
            self.srcs[a].at[self.q], self.dsts[a].at[self.core, self.q], self.ss.at[a, 0],
            self.rr.at[a, self.core, self.q], section=self.layer,
        )

    def local(self, a):
        return pltpu.make_async_copy(
            self.srcs[a].at[self.q], self.dsts[a].at[self.core, self.q], self.ls.at[a]
        )

    def arrival(self, a, h, s):
        return remote(
            self.srcs[a].at[self.q], self.dsts[a].at[h, s], self.ss.at[a, 0], self.rr.at[a, h, s],
            section=1 - self.core,
        )

    def start(self):
        for a in range(len(self.srcs)):
            for copy in self.copies(a):
                copy.start()

            @pl.when(self.core == self.layer)
            def _():
                self.local(a).start()

            @pl.when(self.core != self.layer)
            def _():
                self.near(a).start()

    def finish(self):
        for a in range(len(self.srcs)):

            @pl.when(self.core == self.layer)
            def _():
                for j in range(1, self.n):
                    for h in range(2):
                        self.arrival(a, h, lax.rem(self.q + j, self.n)).wait_recv()
                self.arrival(a, 1 - self.layer, self.q).wait_recv()
                self.local(a).wait()

            @pl.when(self.core != self.layer)
            def _():
                self.near(a).wait_send()

            for copy in self.copies(a):
                copy.wait_send()


def comm_kernel(plan, *refs):
    has_sum, layer_in, count_in, layer_out, count_out, chunks, lag = plan
    refs = list(refs)

    def take(count):
        taken = refs[:count]
        del refs[:count]
        return taken

    p_in, w_in, g_in = take(has_sum), take(count_in), take(count_out)
    p_out, w_out, g_out = take(has_sum), take(count_in), take(count_out)
    greet(has_sum, count_in + count_out > 0)
    jobs = []
    if has_sum:
        line = LineSum(p_in[0], p_out[0], take(13), chunks, lag)
        line.start()
    if count_in:
        jobs.append(Gather(layer_in, w_in, w_out, take(3)))
    if count_out:
        jobs.append(Scatter(layer_out, g_in, g_out, take(3)))
    for job in jobs:
        job.start()
    if has_sum:

        def turn(t, carry):
            line.turn(t)
            return carry

        lax.fori_loop(0, line.turns, turn, 0)
        line.finish()
    for job in jobs:
        job.finish()


def communicate(cid, partial=None, gather=None, scatter=None, chunks=16, lag=3):
    n = lax.axis_size("seq")
    layer_in, w_in = gather if gather else (0, [])
    layer_out, g_in = scatter if scatter else (0, [])
    p_in = [] if partial is None else [partial]
    vmem, anywhere = pl.BlockSpec(memory_space=pltpu.VMEM), pl.BlockSpec(memory_space=pl.ANY)
    scratch = []
    if p_in:
        scratch += LineSum.scratch(partial.shape[1], partial.shape[2], chunks)
    if w_in:
        scratch += Gather.scratch(len(w_in), n)
    if g_in:
        scratch += Scatter.scratch(len(g_in), n)
    shapes = (
        [jax.ShapeDtypeStruct(p.shape, jnp.bfloat16) for p in p_in]
        + [jax.ShapeDtypeStruct((n,) + w.shape[1:], jnp.bfloat16) for w in w_in]
        + [jax.ShapeDtypeStruct((2,) + g.shape, jnp.bfloat16) for g in g_in]
    )
    plan = (len(p_in), layer_in, len(w_in), layer_out, len(g_in), chunks, lag)
    outs = pl.pallas_call(
        functools.partial(comm_kernel, plan),
        out_shape=shapes,
        in_specs=[vmem] * (len(p_in) + len(w_in)) + [anywhere] * len(g_in),
        out_specs=[vmem] * len(p_in) + [anywhere] * (len(w_in) + len(g_in)),
        scratch_shapes=scratch,
        name=f"comm{cid}",
        compiler_params=pltpu.CompilerParams(
            collective_id=cid, has_side_effects=True, vmem_limit_bytes=48 << 20
        ),
    )(*p_in, *w_in, *g_in)
    p, w = outs[: len(p_in)], outs[len(p_in) : len(p_in) + len(w_in)]
    return (
        p[0] if p else None,
        [a.reshape((-1,) + a.shape[2:]) for a in w],
        outs[len(p_in) + len(w_in) :],
    )


def exchange_kernel(x_ref, o_ref, ss, rr):
    q, n = lax.axis_index("seq"), lax.axis_size("seq")
    barrier = pltpu.get_barrier_semaphore()
    for j in range(1, n):
        pl.semaphore_signal(
            barrier, inc=1, device_id={"seq": lax.rem(q + j, n)}, device_id_type=MESH
        )
    pl.semaphore_wait(barrier, n - 1)

    def copy(j):
        return remote(x_ref, o_ref.at[q], ss.at[j], rr.at[q], seq=lax.rem(q + j, n))

    for j in range(1, n):
        copy(j).start()
    o_ref[q] = x_ref[...]
    for j in range(1, n):
        s = lax.rem(q + j, n)
        remote(x_ref, o_ref.at[s], ss.at[j], rr.at[s], seq=s).wait_recv()
    for j in range(1, n):
        copy(j).wait_send()


def exchange(x, cid):
    n = lax.axis_size("seq")
    vmem = pl.BlockSpec(memory_space=pltpu.VMEM)
    return pl.pallas_call(
        exchange_kernel,
        out_shape=jax.ShapeDtypeStruct((n,) + x.shape, x.dtype),
        in_specs=[vmem],
        out_specs=vmem,
        scratch_shapes=[pltpu.SemaphoreType.DMA((n,)), pltpu.SemaphoreType.DMA((n,))],
        name=f"exchange{cid}",
        compiler_params=pltpu.CompilerParams(collective_id=cid, has_side_effects=True),
    )(x)


def rms_norm(vector, scale_gain):
    return (
        vector * lax.rsqrt(jnp.mean(vector * vector, axis=-1, keepdims=True) + epsilon) * scale_gain
    )


def features(vector):
    second = vector[..., :, None] * vector[..., None, :] / (4.0 * math.sqrt(2.0))
    constant = jnp.ones(vector.shape[:-1] + (1,), jnp.float32)
    squares = second.reshape(vector.shape[:-1] + (vector.shape[-1] * vector.shape[-1],))
    return jnp.concatenate([constant, vector * 0.5, squares], axis=-1)


def seq_begin(lengths_row, positions):
    seq_starts = jnp.cumsum(lengths_row) - lengths_row
    chosen = jnp.where(seq_starts[None, :] <= positions[:, None], seq_starts[None, :], 0)
    return jnp.max(chosen, axis=1)


def own_scores(query_heads, key_heads, starts_at):
    row_count = starts_at.shape[0]
    scores = (
        jnp.einsum("thf,shf->hts", query_heads, key_heads, preferred_element_type=jnp.float32)
        * 0.25
    )
    places = jnp.arange(row_count, dtype=jnp.int32)
    visible = (starts_at[:, None] == starts_at[None, :]) & (places[None, :] <= places[:, None])
    return (scores, visible)


def split_heads(proj, rows):
    query = proj[:, :32].astype(jnp.bfloat16).reshape(2, rows, 2, FK)
    key = proj[:, 32:64].astype(jnp.bfloat16).reshape(2, rows, 2, FK)
    value = proj[:, 64:288].astype(jnp.bfloat16).reshape(2, rows, 2, -1)
    return query, key, value


def mb_state(key, value, last_rows):
    phi_last = features(key.astype(jnp.float32)) * last_rows[:, None, None]
    wide = jnp.concatenate(
        [value.astype(jnp.float32), jnp.ones(value.shape[:2] + (1,), jnp.float32)], axis=-1
    )
    return jnp.einsum("shp,she->hpe", phi_last, wide)


def mb_attend(query, key, value, state_in, starts_at, carried_in):
    scores, visible = own_scores(query, key, starts_at)
    weights = jnp.where(visible[None], 1.0 + scores + 0.5 * scores * scores, 0.0).astype(
        jnp.bfloat16
    )
    wide = jnp.concatenate([value, jnp.ones(value.shape[:2] + (1,), jnp.bfloat16)], axis=-1)
    both = jnp.einsum("hts,she->the", weights, wide, preferred_element_type=jnp.float32)
    both = both + carried_in[:, None, None] * jnp.einsum(
        "thp,hpe->the", features(query.astype(jnp.float32)), state_in
    )
    return both[..., :-1], both[..., -1]


def mb_back_before(back_attended, numerator, denominator, query, carried_in):
    back_out = back_attended.reshape(numerator.shape)
    back_numer = (back_out / denominator[:, :, None]).astype(jnp.bfloat16)
    back_denom = -jnp.sum(back_out * numerator, axis=2) / (denominator * denominator)
    wide = jnp.concatenate([back_numer.astype(jnp.float32), back_denom[:, :, None]], axis=-1)
    phi_used = features(query.astype(jnp.float32)) * carried_in[:, None, None]
    return wide, jnp.einsum("thp,the->hpe", phi_used, wide)


def mb_back_after(wide, query, key, value, state_in, state_out, starts_at, carried_in, last_rows):
    back_numer = wide[..., :-1].astype(jnp.bfloat16)
    back_denom = wide[..., -1]
    scores, visible = own_scores(query, key, starts_at)
    weights = jnp.where(visible[None], 1.0 + scores + 0.5 * scores * scores, 0.0).astype(
        jnp.bfloat16
    )
    back_weights = (
        jnp.einsum("the,she->hts", back_numer, value, preferred_element_type=jnp.float32)
        + jnp.transpose(back_denom)[:, :, None]
    )
    back_scores = jnp.where(visible[None], back_weights * (1.0 + scores), 0.0).astype(jnp.bfloat16)
    back_query = 0.25 * jnp.einsum(
        "hts,shf->thf", back_scores, key, preferred_element_type=jnp.float32
    )
    back_key = 0.25 * jnp.einsum(
        "hts,thf->shf", back_scores, query, preferred_element_type=jnp.float32
    )
    back_value = jnp.einsum("hts,the->she", weights, back_numer, preferred_element_type=jnp.float32)
    phi_query, phi_back_query = jax.vjp(features, query.astype(jnp.float32))
    phi_key, phi_back_key = jax.vjp(features, key.astype(jnp.float32))
    back_phi_query = carried_in[:, None, None] * jnp.einsum("the,hpe->thp", wide, state_in)
    value_wide = jnp.concatenate(
        [value.astype(jnp.float32), jnp.ones(value.shape[:2] + (1,), jnp.float32)], axis=-1
    )
    back_phi_key = last_rows[:, None, None] * jnp.einsum("she,hpe->shp", value_wide, state_out)
    back_value = back_value + last_rows[:, None, None] * jnp.einsum(
        "shp,hpe->she", phi_key, state_out[..., :-1]
    )
    return (
        back_query + phi_back_query(back_phi_query)[0],
        back_key + phi_back_key(back_phi_key)[0],
        back_value,
    )


def attention_forward(proj, taps, marks, cids):
    rows = proj.shape[0] // 2
    mine = lax.axis_index("seq")
    query, key, value = split_heads(proj, rows)
    gate_conv = proj[:, 288:].reshape(2, rows, -1)
    state = jax.vmap(mb_state)(key, value, marks["last"])
    states = exchange(state.reshape(2, -1, state.shape[-1]).astype(jnp.bfloat16), cids[0])
    state_in = jnp.einsum("nm,nmpe->mpe", marks["before"], states.astype(jnp.float32)).reshape(
        state.shape
    )
    numerator, denominator = jax.vmap(mb_attend)(
        query, key, value, state_in, marks["begin"], marks["carried"]
    )
    attended = (numerator / denominator[..., None]).reshape(2, rows, -1)
    edges = exchange(attended[:, rows - 2 :], cids[1])
    edge = lax.dynamic_index_in_dim(edges, jnp.maximum(mine - 1, 0), 0, False)
    edge = jnp.where(mine > 0, edge, 0.0)
    extended = jnp.concatenate([edge, attended], axis=1)
    conv_out = taps[0] * attended
    for offset in range(1, KW):
        conv_out = (
            conv_out
            + taps[offset]
            * extended[:, 2 - offset : 2 - offset + rows]
            * marks["allowed"][offset][:, :rows, None]
        )
    gated = (conv_out * gate_conv).astype(jnp.bfloat16)
    return gated.reshape(2 * rows, -1), (state_in, numerator, denominator, extended, conv_out)


def attention_backward(back_gated, proj, kept, taps, marks, cids):
    state_in, numerator, denominator, extended, conv_out = kept
    rows = proj.shape[0] // 2
    count, mine = lax.axis_size("seq"), lax.axis_index("seq")
    query, key, value = split_heads(proj, rows)
    gate_conv = proj[:, 288:].reshape(2, rows, -1)
    back_gated = back_gated.reshape(2, rows, -1)
    back_conv = back_gated * gate_conv
    back_gconv = (back_gated * conv_out).astype(jnp.bfloat16)
    edges = exchange(back_conv[:, :2], cids[0])
    edge = lax.dynamic_index_in_dim(edges, jnp.minimum(mine + 1, count - 1), 0, False)
    edge = jnp.where(mine < count - 1, edge, 0.0)
    conv_ext = jnp.concatenate([back_conv, edge], axis=1)
    back_attended = taps[0] * back_conv
    taps_rows = [jnp.sum(back_conv * extended[:, 2:], axis=(0, 1))]
    for offset in range(1, KW):
        allowed = marks["allowed"][offset]
        back_attended = (
            back_attended
            + taps[offset]
            * conv_ext[:, offset : offset + rows]
            * allowed[:, offset : offset + rows, None]
        )
        taps_rows.append(
            jnp.sum(
                back_conv
                * extended[:, 2 - offset : 2 - offset + rows]
                * allowed[:, :rows, None],
                axis=(0, 1),
            )
        )
    wide, state_grad = jax.vmap(mb_back_before)(
        back_attended, numerator, denominator, query, marks["carried"]
    )
    states = exchange(
        state_grad.reshape(2, -1, state_grad.shape[-1]).astype(jnp.bfloat16), cids[1]
    )
    state_out = jnp.einsum("nm,nmpe->mpe", marks["after"], states.astype(jnp.float32)).reshape(
        state_grad.shape
    )
    back_query, back_key, back_value = jax.vmap(mb_back_after)(
        wide, query, key, value, state_in, state_out, marks["begin"], marks["carried"],
        marks["last"],
    )
    flat = [a.astype(jnp.bfloat16).reshape(2 * rows, -1) for a in (back_query, back_key, back_value)]
    back_proj = jnp.concatenate(flat + [back_gconv.reshape(2 * rows, -1)], axis=1)
    return back_proj, jnp.stack(taps_rows)


def sequence_marks(lengths, rows):
    count, mine = lax.axis_size("seq"), lax.axis_index("seq")
    start = mine * rows
    positions = start + jnp.arange(rows + 2, dtype=jnp.int32)
    begin_ext = jax.vmap(lambda row: seq_begin(row, positions))(lengths)
    begin = begin_ext[:, :rows]
    ends = (jnp.arange(count, dtype=jnp.int32) + 1) * rows - 1
    stays = jax.vmap(lambda row: seq_begin(row, ends))(lengths) < (ends - rows + 1)[None, :]
    stays = stays.astype(jnp.float32)
    before = []
    after = []
    for b in range(count):
        through = jnp.where(mine > b, 1.0, 0.0) * jnp.ones_like(stays[:, 0])
        for j in range(b + 1, count):
            through = through * jnp.where(j < mine, stays[:, j], 1.0)
        before.append(through)
        through = jnp.where(mine < b, 1.0, 0.0) * jnp.ones_like(stays[:, 0])
        for j in range(b):
            through = through * jnp.where(j > mine, stays[:, j], 1.0)
        after.append(through)
    return {
        "begin": begin,
        "carried": (begin < start).astype(jnp.float32),
        "last": (begin == begin[:, rows - 1 :]).astype(jnp.float32),
        "before": jnp.stack(before),
        "after": jnp.stack(after),
        "allowed": [(positions - j >= begin_ext).astype(jnp.float32) for j in range(KW)],
    }


def by_seq(grad):
    n = lax.axis_size("seq")
    return grad.reshape((n, grad.shape[0] // n) + grad.shape[1:])


def dot_t(a, b):
    return jnp.einsum("tc,dc->td", a, b, preferred_element_type=jnp.float32)


def dot_n(a, b):
    return jnp.dot(a, b, preferred_element_type=jnp.float32)


def outer(a, b):
    return jnp.einsum("tc,tf->cf", a, b, preferred_element_type=jnp.float32).astype(jnp.bfloat16)


def on_device(
    tokens,
    lengths,
    gain_attn,
    w_query,
    w_key,
    w_value,
    w_gate_conv,
    conv_taps,
    w_out,
    gain_ffn,
    w_gate,
    w_up,
    w_down,
    cotangent,
):
    head_index = lax.axis_index("head")
    core = lax.axis_index("section")
    micro_count, rows, width = tokens.shape
    total = micro_count * rows

    def halves(weight):
        cols = weight.shape[1] // 2
        return jnp.stack([weight[:, :cols], weight[:, cols:]])

    own_mix = jnp.concatenate(
        [halves(w[0]) for w in (w_query, w_key, w_value, w_gate_conv)], axis=2
    )
    own_out = halves(w_out[0].T)
    own_ffn = jnp.concatenate([halves(w_gate[0]), halves(w_up[0])], axis=2)
    own_down = halves(w_down[0].T)
    gains_one = lax.all_gather(gain_attn[0], "section").astype(jnp.float32)
    gains_two = lax.all_gather(gain_ffn[0], "section").astype(jnp.float32)
    taps_all = lax.all_gather(conv_taps[0], "section").astype(jnp.float32)
    channels = own_out.shape[2]
    taps_both = lax.dynamic_slice_in_dim(
        taps_all, (head_index * 2 + core) * channels, channels, 2
    )
    marks = sequence_marks(lengths, rows)
    hidden_cols = own_down.shape[2]

    def as_parts(flat):
        return flat.astype(jnp.bfloat16).reshape(micro_count, rows, width)

    def wide(summed):
        return summed.astype(jnp.float32).reshape(total, width)

    mix = [None, None]
    ffn = [None, None]
    _, mix[0], _ = communicate(1, gather=(0, [own_mix, own_out]))
    x = tokens.reshape(total, width).astype(jnp.float32)
    kept = [None, None]
    outputs = []
    for layer in range(2):
        w_mix, w_o = mix[layer]
        normed = rms_norm(x, gains_one[layer]).astype(jnp.bfloat16)
        proj = dot_n(normed, w_mix)
        gated, attn = attention_forward(proj, taps_both[layer], marks, (10, 11))
        summed, ffn[layer], _ = communicate(
            2 + layer, partial=as_parts(dot_t(gated, w_o)), gather=(layer, [own_ffn, own_down])
        )
        w_gu, w_d = ffn[layer]
        middle = x + wide(summed)
        normed_two = rms_norm(middle, gains_two[layer]).astype(jnp.bfloat16)
        both = dot_n(normed_two, w_gu)
        hidden = (jax.nn.silu(both[:, :hidden_cols]) * both[:, hidden_cols:]).astype(jnp.bfloat16)
        partial = as_parts(dot_t(hidden, w_d))
        if layer == 0:
            summed, mix[1], _ = communicate(4, partial=partial, gather=(1, [own_mix, own_out]))
        else:
            summed, _, _ = communicate(5, partial=partial)
        out = (middle + wide(summed)).astype(jnp.bfloat16)
        outputs.append(out)
        kept[layer] = (x, normed, proj, gated, attn, middle, normed_two, both, hidden)
        x = out.astype(jnp.float32)

    grad = cotangent.reshape(total, width)
    back = [None, None]
    smalls = [None, None]
    received = [[None] * 4, [None] * 4]
    late = None
    for layer in (1, 0):
        x, normed, proj, gated, attn, middle, normed_two, both, hidden = kept[layer]
        w_mix, w_o = mix[layer]
        w_gu, w_d = ffn[layer]
        grad_wide = grad.astype(jnp.float32)
        back_hidden = dot_n(grad, w_d)
        gate_pre, upward = both[:, :hidden_cols], both[:, hidden_cols:]
        silu_value, silu_back = jax.vjp(jax.nn.silu, gate_pre)
        back_both = jnp.concatenate(
            [
                silu_back(back_hidden * upward)[0].astype(jnp.bfloat16),
                (back_hidden * silu_value).astype(jnp.bfloat16),
            ],
            axis=1,
        )
        partial = as_parts(dot_t(back_both, w_gu))
        if layer == 1:
            summed, _, _ = communicate(5, partial=partial)
        else:
            summed, _, received[1][:2] = communicate(6, partial=partial, scatter=(1, late))
        grad_gu = outer(normed_two, back_both)
        grad_d = outer(grad, hidden)
        _, norm_back_two = jax.vjp(rms_norm, middle, gains_two[layer])
        back_middle, gain_two = norm_back_two(wide(summed))
        back_middle = grad_wide + back_middle
        back_branch = back_middle.astype(jnp.bfloat16)
        grad_o = outer(back_branch, gated)
        back_gated = dot_n(back_branch, w_o)
        back_proj, taps_grad = attention_backward(
            back_gated, proj, attn, taps_both[layer], marks, (12, 13)
        )
        grad_mix = outer(normed, back_proj)
        partial = as_parts(dot_t(back_proj, w_mix))
        summed, _, received[layer][2:] = communicate(
            7 + layer, partial=partial, scatter=(layer, [by_seq(grad_gu), by_seq(grad_d)])
        )
        late = [by_seq(grad_mix), by_seq(grad_o)]
        _, norm_back_one = jax.vjp(rms_norm, x, gains_one[layer])
        back_x, gain_one = norm_back_one(wide(summed))
        grad = (back_middle + back_x).astype(jnp.bfloat16)
        back[layer] = grad
        smalls[layer] = (gain_one, gain_two, taps_grad)
    _, _, received[0][:2] = communicate(9, scatter=(0, late))

    def collect(index):
        picked = jnp.where(core == 0, received[0][index], received[1][index])
        return jnp.sum(picked.astype(jnp.float32), axis=1)

    grad_mix, grad_o, grad_gu, grad_d = [collect(i) for i in range(4)]

    def joined(pair):
        return jnp.concatenate([pair[0], pair[1]], axis=1)

    qk = w_query.shape[2] // 2
    vg = w_value.shape[2] // 2
    grad_query = joined(grad_mix[:, :, :qk])
    grad_key = joined(grad_mix[:, :, qk : 2 * qk])
    grad_value = joined(grad_mix[:, :, 2 * qk : 2 * qk + vg])
    grad_gconv = joined(grad_mix[:, :, 2 * qk + vg :])
    grad_out = joined(grad_o).T
    grad_gate = joined(grad_gu[:, :, :hidden_cols])
    grad_up = joined(grad_gu[:, :, hidden_cols:])
    grad_down = joined(grad_d).T

    block = width // (2 * lax.axis_size("head"))
    column_mask = (
        jnp.arange(width, dtype=jnp.int32) // block == head_index * 2 + core
    ).astype(jnp.float32)
    packed = []
    for gain_one, gain_two, taps_grad in smalls:
        taps_full = lax.dynamic_update_slice_in_dim(
            jnp.zeros((KW, width), jnp.float32), taps_grad, (head_index * 2 + core) * channels, 1
        )
        packed.append(
            jnp.concatenate(
                [(gain_one * column_mask)[None], (gain_two * column_mask)[None], taps_full], axis=0
            )
        )
    totals = lax.psum(jnp.stack(packed), ("section", "seq", "head"))
    totals = lax.dynamic_index_in_dim(totals, core, 0, False)

    def chosen(pair):
        return jnp.where(core == 0, pair[0], pair[1]).reshape(1, micro_count, rows, width)

    return (
        chosen(outputs),
        chosen(back),
        totals[0][None],
        grad_query[None],
        grad_key[None],
        grad_value[None],
        grad_gconv[None],
        totals[2:][None],
        grad_out[None],
        totals[1][None],
        grad_gate[None],
        grad_up[None],
        grad_down[None],
    )


def solution(mesh):
    placed = (
        P(None, "seq", None),
        P(),
        P("section", None),
        P("section", "seq", "head"),
        P("section", "seq", "head"),
        P("section", "seq", "head"),
        P("section", "seq", "head"),
        P("section", None, None),
        P("section", "head", "seq"),
        P("section", None),
        P("section", "seq", "head"),
        P("section", "seq", "head"),
        P("section", "head", "seq"),
        P(None, "seq", None),
    )
    return jax.shard_map(
        on_device,
        mesh=mesh,
        in_specs=placed,
        out_specs=(
            P("section", None, "seq", None),
            P("section", None, "seq", None),
            P("section", None),
            P("section", "seq", "head"),
            P("section", "seq", "head"),
            P("section", "seq", "head"),
            P("section", "seq", "head"),
            P("section", None, None),
            P("section", "head", "seq"),
            P("section", None),
            P("section", "seq", "head"),
            P("section", "seq", "head"),
            P("section", "head", "seq"),
        ),
        check_vma=False,
    )
```

```python
import functools
import math

import jax
import jax.numpy as jnp
from jax import lax
from jax.experimental import pallas as pl
from jax.experimental.pallas import tpu as pltpu
import numpy as np
from jax.sharding import PartitionSpec as P

FK = 16
KW = 3
MESH = pl.DeviceIdType.MESH
epsilon = 1e-05


def remote(src, dst, send, recv, **where):
    return pltpu.make_async_remote_copy(
        src_ref=src,
        dst_ref=dst,
        send_sem=send,
        recv_sem=recv,
        device_id=where,
        device_id_type=MESH,
    )


def greet(line, spread):
    core, z, q = lax.axis_index("section"), lax.axis_index("head"), lax.axis_index("seq")
    depth, count = lax.axis_size("head"), lax.axis_size("seq")
    barrier = pltpu.get_barrier_semaphore()

    def hello(**where):
        pl.semaphore_signal(barrier, inc=1, device_id=where, device_id_type=MESH)

    hello(section=1 - core)
    expected = 1
    if spread:
        for j in range(1, count):
            for h in range(2):
                hello(section=h, seq=lax.rem(q + j, count))
        expected += 2 * (count - 1)
    if line:

        @pl.when(z > 0)
        def _():
            hello(head=z - 1)

        @pl.when(z < depth - 1)
        def _():
            hello(head=z + 1)

        expected = expected + jnp.where(z > 0, 1, 0) + jnp.where(z < depth - 1, 1, 0)
    pl.semaphore_wait(barrier, expected)


class LineSum:
    def __init__(self, p_ref, o_ref, scratch, chunks, lag):
        self.p_ref, self.o_ref, self.chunks, self.lag = p_ref, o_ref, chunks, lag
        self.pin, self.low, self.high, self.out = scratch[:4]
        self.ps, self.pr, self.rs, self.rl, self.rh, self.bs, self.br, self.ts, self.tr = scratch[4:]
        self.z, self.n = lax.axis_index("head"), lax.axis_size("head")
        self.core = lax.axis_index("section")
        self.half = p_ref.shape[1] // 2
        self.step = self.half // chunks
        self.depth = max((self.n - 1) // 2, self.n - 1 - (self.n - 1) // 2)
        self.turns = chunks + 2 * self.depth * lag

    @staticmethod
    def scratch(rows, width, chunks):
        sem = pltpu.SemaphoreType.DMA((2, chunks))
        bank = pltpu.SemaphoreType.DMA((2, 2, chunks))
        return [pltpu.VMEM((rows, width), jnp.bfloat16)] * 4 + [
            sem, sem, sem, sem, sem, bank, sem, sem, sem
        ]

    def root(self, d):
        return (self.n - 1) // 2 if d == 0 else self.n - 1 - (self.n - 1) // 2

    def rng(self, d, k):
        return pl.ds(pl.multiple_of(d * self.half + k * self.step, self.step), self.step)

    def part(self, d, k):
        r = self.rng(d, k)
        other = 1 - self.core
        return remote(
            self.p_ref.at[other, r], self.pin.at[r], self.ps.at[d, k], self.pr.at[d, k], section=other
        )

    def up(self, d, k):
        r = self.rng(d, k)
        return remote(
            self.out.at[r], self.low.at[r], self.rs.at[d, k], self.rl.at[d, k], head=self.z + 1
        )

    def down(self, d, k):
        r = self.rng(d, k)
        return remote(
            self.out.at[r], self.high.at[r], self.rs.at[d, k], self.rh.at[d, k], head=self.z - 1
        )

    def share(self, d, k, side):
        r = self.rng(d, k)
        at = self.o_ref.at[self.core, r]
        return remote(
            at, at, self.bs.at[side, d, k], self.br.at[d, k], head=self.z + (1 if side else -1)
        )

    def give(self, d, k):
        r = self.rng(d, k)
        at = self.o_ref.at[self.core, r]
        return remote(at, at, self.ts.at[d, k], self.tr.at[d, k], section=1 - self.core)

    def start(self):
        for k in range(self.chunks):
            for d in range(2):
                self.part(d, k).start()

    def gathered(self, d, k):
        r = self.rng(d, k)
        z, n, root = self.z, self.n, self.root(d)
        self.part(d, k).wait_recv()
        mine = self.p_ref[self.core, r, :].astype(jnp.float32) + self.pin[r, :].astype(jnp.float32)

        @pl.when((z == 0) & (root > 0))
        def _():
            self.out[r, :] = mine.astype(jnp.bfloat16)
            self.up(d, k).start()

        @pl.when((z == n - 1) & (root < n - 1))
        def _():
            self.out[r, :] = mine.astype(jnp.bfloat16)
            self.down(d, k).start()

        @pl.when((z > 0) & (z < root))
        def _():
            self.up(d, k).wait_recv()
            self.out[r, :] = (mine + self.low[r, :].astype(jnp.float32)).astype(jnp.bfloat16)
            self.up(d, k).start()

        @pl.when((z < n - 1) & (z > root))
        def _():
            self.down(d, k).wait_recv()
            self.out[r, :] = (mine + self.high[r, :].astype(jnp.float32)).astype(jnp.bfloat16)
            self.down(d, k).start()

        @pl.when(z == root)
        def _():
            total = mine
            if root > 0:
                self.up(d, k).wait_recv()
                total = total + self.low[r, :].astype(jnp.float32)
            if root < n - 1:
                self.down(d, k).wait_recv()
                total = total + self.high[r, :].astype(jnp.float32)
            self.o_ref[self.core, r, :] = total.astype(jnp.bfloat16)
            if root > 0:
                self.share(d, k, 0).start()
            if root < n - 1:
                self.share(d, k, 1).start()
            self.give(d, k).start()

    def passed(self, d, k):
        z, n, root = self.z, self.n, self.root(d)
        self.share(d, k, 0).wait_recv()

        @pl.when((z < root) & (z > 0))
        def _():
            self.share(d, k, 0).start()

        @pl.when((z > root) & (z < n - 1))
        def _():
            self.share(d, k, 1).start()

        self.give(d, k).start()

    def turn(self, t):
        z, n = self.z, self.n
        for d in range(2):
            root = self.root(d)
            deep = max(root, n - 1 - root)
            below = jnp.where(z < root, z, jnp.where(z > root, n - 1 - z, deep))
            k = t - below * self.lag
            far = jnp.abs(z - root)

            @pl.when((k >= 0) & (k < self.chunks))
            def _():
                self.gathered(d, k)

            b = t - (deep + far) * self.lag

            @pl.when((b >= 0) & (b < self.chunks) & (far > 0))
            def _():
                self.passed(d, b)

    def finish(self):
        z, n = self.z, self.n
        for d in range(2):
            root = self.root(d)
            for k in range(self.chunks):
                self.part(d, k).wait_send()
                self.give(d, k).wait_recv()
                self.give(d, k).wait_send()

                @pl.when(z < root)
                def _():
                    self.up(d, k).wait_send()

                @pl.when(z > root)
                def _():
                    self.down(d, k).wait_send()

                if root > 0:

                    @pl.when((z <= root) & (z > 0))
                    def _():
                        self.share(d, k, 0).wait_send()

                if root < n - 1:

                    @pl.when((z >= root) & (z < n - 1))
                    def _():
                        self.share(d, k, 1).wait_send()


class Gather:
    def __init__(self, layer, srcs, dsts, sems):
        self.layer, self.srcs, self.dsts = layer, srcs, dsts
        self.ss, self.rr, self.ls = sems
        self.core, self.q = lax.axis_index("section"), lax.axis_index("seq")
        self.n = lax.axis_size("seq")

    @staticmethod
    def scratch(count, n):
        return [
            pltpu.SemaphoreType.DMA((count, n, 2)),
            pltpu.SemaphoreType.DMA((count, n)),
            pltpu.SemaphoreType.DMA((count,)),
        ]

    def copies(self, a):
        for j in range(1, self.n):
            for h in range(2):
                yield remote(
                    self.srcs[a].at[h], self.dsts[a].at[self.q], self.ss.at[a, j, h],
                    self.rr.at[a, self.q], section=h, seq=lax.rem(self.q + j, self.n),
                )
        yield remote(
            self.srcs[a].at[1 - self.layer], self.dsts[a].at[self.q], self.ss.at[a, 0, 0],
            self.rr.at[a, self.q], section=1 - self.layer,
        )

    def local(self, a):
        return pltpu.make_async_copy(
            self.srcs[a].at[self.layer], self.dsts[a].at[self.q], self.ls.at[a]
        )

    def arrival(self, a, s):
        return remote(
            self.srcs[a].at[0], self.dsts[a].at[s], self.ss.at[a, 0, 0], self.rr.at[a, s],
            section=1 - self.core,
        )

    def start(self):
        @pl.when(self.core == self.layer)
        def _():
            for a in range(len(self.srcs)):
                for copy in self.copies(a):
                    copy.start()
                self.local(a).start()

    def finish(self):
        for a in range(len(self.srcs)):
            for j in range(1, self.n):
                self.arrival(a, lax.rem(self.q + j, self.n)).wait_recv()

            @pl.when(self.core == self.layer)
            def _():
                self.local(a).wait()
                for copy in self.copies(a):
                    copy.wait_send()

            @pl.when(self.core != self.layer)
            def _():
                self.arrival(a, self.q).wait_recv()


class Scatter:
    def __init__(self, layer, srcs, dsts, sems):
        self.layer, self.srcs, self.dsts = layer, srcs, dsts
        self.ss, self.rr, self.ls = sems
        self.core, self.q = lax.axis_index("section"), lax.axis_index("seq")
        self.n = lax.axis_size("seq")

    @staticmethod
    def scratch(count, n):
        return [
            pltpu.SemaphoreType.DMA((count, n)),
            pltpu.SemaphoreType.DMA((count, 2, n)),
            pltpu.SemaphoreType.DMA((count,)),
        ]

    def copies(self, a):
        for j in range(1, self.n):
            t = lax.rem(self.q + j, self.n)
            yield remote(
                self.srcs[a].at[t], self.dsts[a].at[self.core, self.q], self.ss.at[a, j],
                self.rr.at[a, self.core, self.q], section=self.layer, seq=t,
            )

    def near(self, a):
        return remote(
            self.srcs[a].at[self.q], self.dsts[a].at[self.core, self.q], self.ss.at[a, 0],
            self.rr.at[a, self.core, self.q], section=self.layer,
        )

    def local(self, a):
        return pltpu.make_async_copy(
            self.srcs[a].at[self.q], self.dsts[a].at[self.core, self.q], self.ls.at[a]
        )

    def arrival(self, a, h, s):
        return remote(
            self.srcs[a].at[self.q], self.dsts[a].at[h, s], self.ss.at[a, 0], self.rr.at[a, h, s],
            section=1 - self.core,
        )

    def start(self):
        for a in range(len(self.srcs)):
            for copy in self.copies(a):
                copy.start()

            @pl.when(self.core == self.layer)
            def _():
                self.local(a).start()

            @pl.when(self.core != self.layer)
            def _():
                self.near(a).start()

    def finish(self):
        for a in range(len(self.srcs)):

            @pl.when(self.core == self.layer)
            def _():
                for j in range(1, self.n):
                    for h in range(2):
                        self.arrival(a, h, lax.rem(self.q + j, self.n)).wait_recv()
                self.arrival(a, 1 - self.layer, self.q).wait_recv()
                self.local(a).wait()

            @pl.when(self.core != self.layer)
            def _():
                self.near(a).wait_send()

            for copy in self.copies(a):
                copy.wait_send()


def comm_kernel(plan, *refs):
    has_sum, layer_in, count_in, layer_out, count_out, chunks, lag = plan
    refs = list(refs)

    def take(count):
        taken = refs[:count]
        del refs[:count]
        return taken

    p_in, w_in, g_in = take(has_sum), take(count_in), take(count_out)
    p_out, w_out, g_out = take(has_sum), take(count_in), take(count_out)
    greet(has_sum, count_in + count_out > 0)
    jobs = []
    if has_sum:
        line = LineSum(p_in[0], p_out[0], take(13), chunks, lag)
        line.start()
    if count_in:
        jobs.append(Gather(layer_in, w_in, w_out, take(3)))
    if count_out:
        jobs.append(Scatter(layer_out, g_in, g_out, take(3)))
    for job in jobs:
        job.start()
    if has_sum:

        def turn(t, carry):
            line.turn(t)
            return carry

        lax.fori_loop(0, line.turns, turn, 0)
        line.finish()
    for job in jobs:
        job.finish()


def communicate(cid, partial=None, gather=None, scatter=None, chunks=16, lag=3):
    n = lax.axis_size("seq")
    layer_in, w_in = gather if gather else (0, [])
    layer_out, g_in = scatter if scatter else (0, [])
    p_in = [] if partial is None else [partial]
    vmem, anywhere = pl.BlockSpec(memory_space=pltpu.VMEM), pl.BlockSpec(memory_space=pl.ANY)
    scratch = []
    if p_in:
        scratch += LineSum.scratch(partial.shape[1], partial.shape[2], chunks)
    if w_in:
        scratch += Gather.scratch(len(w_in), n)
    if g_in:
        scratch += Scatter.scratch(len(g_in), n)
    shapes = (
        [jax.ShapeDtypeStruct(p.shape, jnp.bfloat16) for p in p_in]
        + [jax.ShapeDtypeStruct((n,) + w.shape[1:], jnp.bfloat16) for w in w_in]
        + [jax.ShapeDtypeStruct((2,) + g.shape, jnp.bfloat16) for g in g_in]
    )
    plan = (len(p_in), layer_in, len(w_in), layer_out, len(g_in), chunks, lag)
    outs = pl.pallas_call(
        functools.partial(comm_kernel, plan),
        out_shape=shapes,
        in_specs=[vmem] * (len(p_in) + len(w_in)) + [anywhere] * len(g_in),
        out_specs=[vmem] * len(p_in) + [anywhere] * (len(w_in) + len(g_in)),
        scratch_shapes=scratch,
        name=f"comm{cid}",
        compiler_params=pltpu.CompilerParams(
            collective_id=cid, has_side_effects=True, vmem_limit_bytes=48 << 20
        ),
    )(*p_in, *w_in, *g_in)
    p, w = outs[: len(p_in)], outs[len(p_in) : len(p_in) + len(w_in)]
    return (
        p[0] if p else None,
        [a.reshape((-1,) + a.shape[2:]) for a in w],
        outs[len(p_in) + len(w_in) :],
    )


def rms_norm(vector, scale_gain):
    return (
        vector * lax.rsqrt(jnp.mean(vector * vector, axis=-1, keepdims=True) + epsilon) * scale_gain
    )


def seq_begin(lengths_row, positions):
    seq_starts = jnp.cumsum(lengths_row) - lengths_row
    chosen = jnp.where(seq_starts[None, :] <= positions[:, None], seq_starts[None, :], 0)
    return jnp.max(chosen, axis=1)


HEADS = 2
PAIRS = FK * (FK + 1) // 2
STATE = 160
BLOCK = 128


def feature_tables(values):
    wide = values + HEADS * FK
    first = np.zeros((HEADS, wide, wide), np.float32)
    second = np.zeros((HEADS, wide, wide), np.float32)
    rest = np.zeros((8, wide), np.float32)
    for h in range(HEADS):
        at = values + h * FK
        lane = 0
        for a in range(FK):
            for b in range(a, FK):
                first[h, at + a, lane] = 1
                second[h, at + b, lane] = 1
                rest[2, lane] = 0.25 if a < b else 1 / (4.0 * math.sqrt(2.0))
                lane += 1
        for a in range(FK):
            first[h, at + a, lane] = 1
            rest[1, lane] = 1
            rest[2, lane] = 0.5
            lane += 1
        rest[0, lane] = rest[1, lane] = rest[2, lane] = 1
    return np.stack([first, second], axis=1), rest


def mm(a, b):
    return lax.dot_general(a, b, (((1,), (0,)), ((), ())), preferred_element_type=jnp.float32)


def mm_nt(a, b):
    return lax.dot_general(a, b, (((1,), (1,)), ((), ())), preferred_element_type=jnp.float32)


def mm_tn(a, b):
    return lax.dot_general(a, b, (((0,), (0,)), ((), ())), preferred_element_type=jnp.float32)


class Lanes:
    def __init__(self, wide, values):
        self.values = values
        self.lane = lax.broadcasted_iota(jnp.int32, (1, wide), 1)
        lane, dim = self.lane, values // HEADS
        self.is_value = lane < values
        self.is_one = (lane >= values) & (lane < values + 2 * HEADS)
        self.head = jnp.where(
            self.is_value, jnp.where(lane < dim, 0, 1), jnp.where(self.is_one, (lane - values) % 2, 9)
        )

    def of(self, h, x):
        return jnp.where(self.head == h, x, jnp.zeros_like(x))

    def key(self, h, x):
        at = self.values + h * FK
        return jnp.where((self.lane >= at) & (self.lane < at + FK), x, jnp.zeros_like(x))

    def extended(self, a):
        return jnp.where(
            self.is_value, a, jnp.where(self.is_one, jnp.ones_like(a), jnp.zeros_like(a))
        )

    def column(self, x, index):
        return jnp.sum(
            jnp.where(self.lane == self.values + index, x, 0.0), axis=1, keepdims=True
        )

    def denominator(self, x):
        return jnp.where(
            self.lane < self.values // HEADS, self.column(x, 0), self.column(x, 1)
        )


def meet(direction, reach):
    q, n = lax.axis_index("seq"), lax.axis_size("seq")
    barrier = pltpu.get_barrier_semaphore()
    count = 0
    for d in range(1, reach + 1):
        source = q - direction * d
        target = q + direction * d

        @pl.when((source >= 0) & (source < n))
        def _():
            pl.semaphore_signal(barrier, inc=1, device_id={"seq": source}, device_id_type=MESH)

        count = count + jnp.where((target >= 0) & (target < n), 1, 0)

    @pl.when(count > 0)
    def _():
        pl.semaphore_wait(barrier, count)


class Pass:
    def __init__(self, direction, reach, src, dst, send, recv):
        self.direction, self.reach = direction, reach
        self.src, self.dst, self.send, self.recv = src, dst, send, recv
        self.q, self.n = lax.axis_index("seq"), lax.axis_size("seq")

    def has_source(self, d):
        at = self.q - self.direction * d
        return (at >= 0) & (at < self.n)

    def has_target(self, d):
        at = self.q + self.direction * d
        return (at >= 0) & (at < self.n)

    def copy(self, d):
        return remote(
            self.src, self.dst.at[d - 1], self.send.at[d - 1], self.recv.at[d - 1],
            seq=self.q + self.direction * d,
        )

    def start(self):
        for d in range(1, self.reach + 1):

            @pl.when(self.has_target(d))
            def _():
                self.copy(d).start()

    def arrived(self):
        for d in range(1, self.reach + 1):

            @pl.when(self.has_source(d))
            def _():
                self.copy(d).wait_recv()

    def sent(self):
        for d in range(1, self.reach + 1):

            @pl.when(self.has_target(d))
            def _():
                self.copy(d).wait_send()


def sum_states(states, coef, total):
    for m in range(2):
        total[m] = jnp.zeros(total.shape[1:], total.dtype)
        for d in range(1, states.reach + 1):

            @pl.when(states.has_source(d))
            def _():
                total[m, :STATE, :] += coef[d - 1, m] * states.dst[d - 1, m].astype(jnp.float32)


def shifted(a, tail, fresh, by):
    row = lax.broadcasted_iota(jnp.int32, (a.shape[0], 1), 0)
    moved = pltpu.roll(a, by, 0)
    rows = tail.shape[0]
    for r in range(by):
        edge = jnp.where(fresh, tail[rows - by + r : rows - by + r + 1, :], 0.0)
        moved = jnp.where(row == r, edge, moved)
    return moved


def attn_forward_kernel(
    reach, proj, col, row, coef, e, c, taps, gated, att, conv, sin, edge, acc, phi, s_acc, s_src,
    s_all, s_sum, e_src, ss, sr, es, er,
):
    q = lax.axis_index("seq")
    rows, wide = proj.shape[1], proj.shape[2] // 2
    values = wide - HEADS * FK
    lanes = Lanes(wide, values)
    meet(1, reach)
    states = Pass(1, reach, s_src, s_all, ss, sr)
    edges = Pass(1, 1, e_src, edge, es, er)

    def sides(m):
        return proj[m, :, :wide].astype(jnp.bfloat16), proj[m, :, wide:].astype(jnp.bfloat16)

    def phi_of(a, h):
        return (mm(a, e[h, 0]) + c[0:1, :]) * (mm(a, e[h, 1]) + c[1:2, :]) * c[2:3, :]

    def make_state(i, carry):
        m, h = i // HEADS, i % HEADS
        a, b = sides(m)
        phi[m, h] = (phi_of(a, h) * col[m, :, 1:2]).astype(jnp.bfloat16)
        keyed = (phi_of(b, h) * col[m, :, 2:3]).astype(jnp.bfloat16)
        part = mm_tn(keyed, lanes.of(h, lanes.extended(a)))

        @pl.when(h == 0)
        def _():
            s_acc[m] = part

        @pl.when(h > 0)
        def _():
            s_acc[m] += part

        return carry

    lax.fori_loop(0, 2 * HEADS, make_state, 0)
    for m in range(2):
        s_src[m] = s_acc[m, :STATE, :].astype(jnp.bfloat16)
    states.start()

    def make_block(i, carry):
        m, h = i // HEADS, i % HEADS
        a, b = sides(m)
        asked = lanes.key(h, a)
        valued = lanes.of(h, lanes.extended(a))
        for r in range(rows // BLOCK):
            lo, hi = r * BLOCK, (r + 1) * BLOCK
            x = mm_nt(asked[lo:hi], b[:hi]) * 0.25
            seen = (col[m, lo:hi, 0:1] == row[m, 0:1, :hi]) & (
                lax.broadcasted_iota(jnp.int32, (BLOCK, hi), 1)
                <= lo + lax.broadcasted_iota(jnp.int32, (BLOCK, hi), 0)
            )
            w = jnp.where(seen, 1.0 + x + 0.5 * x * x, 0.0).astype(jnp.bfloat16)
            part = mm(w, valued[:hi])

            @pl.when(h == 0)
            def _():
                acc[m, lo:hi, :] = part

            @pl.when(h > 0)
            def _():
                acc[m, lo:hi, :] += part

        return carry

    lax.fori_loop(0, 2 * HEADS, make_block, 0)
    states.arrived()
    sum_states(states, coef, s_sum)

    def attend(m, lo):
        s = s_sum[m].astype(jnp.bfloat16)
        both = acc[m, lo:, :]
        for h in range(HEADS):
            both = both + mm(phi[m, h, lo:, :], lanes.of(h, s))
        return jnp.where(lanes.is_value, both / lanes.denominator(both), both)

    for m in range(2):
        sin[m] = s_sum[m, :STATE, :].astype(jnp.bfloat16)
        e_src[m] = attend(m, rows - 16)
    edges.start()
    for m in range(2):
        att[m] = attend(m, 0)
    edges.arrived()
    for m in range(2):
        a = att[m]
        tail = edge[0, m]
        out = taps[0:1, :] * a
        for by in (1, 2):
            out = out + taps[by : by + 1, :] * shifted(a, tail, q > 0, by) * col[m, :, 2 + by : 3 + by]
        conv[m] = out
        gated[m] = (out * proj[m, :, wide:]).astype(jnp.bfloat16)
    states.sent()
    edges.sent()


def attn_backward_kernel(
    reach, bg, proj, att, conv, sin, edge, col, row, coef, late, e, c, taps, out, grad_taps,
    phi_q, phi_k, near, acc_a, acc_b, s_acc, s_src, s_all, s_sum, e_src, e_dst, ss, sr, es, er,
):
    q, n = lax.axis_index("seq"), lax.axis_size("seq")
    rows, wide = proj.shape[1], proj.shape[2] // 2
    values = wide - HEADS * FK
    lanes = Lanes(wide, values)
    meet(-1, reach)
    states = Pass(-1, reach, s_src, s_all, ss, sr)
    edges = Pass(-1, 1, e_src, e_dst, es, er)
    for m in range(2):
        e_src[m] = bg[m, :16, :] * proj[m, :16, wide:]
    edges.start()

    def sides(m):
        return proj[m, :, :wide].astype(jnp.bfloat16), proj[m, :, wide:].astype(jnp.bfloat16)

    def factors(a, h):
        return mm(a, e[h, 0]) + c[0:1, :], mm(a, e[h, 1]) + c[1:2, :]

    def make_phi(i, carry):
        m, h = i // HEADS, i % HEADS
        a, b = sides(m)
        u, w = factors(a, h)
        phi_q[m, h] = (u * w * c[2:3, :] * col[m, :, 1:2]).astype(jnp.bfloat16)
        u, w = factors(b, h)
        phi_k[m, h] = (u * w * c[2:3, :] * col[m, :, 2:3]).astype(jnp.bfloat16)
        return carry

    lax.fori_loop(0, 2 * HEADS, make_phi, 0)
    edges.arrived()
    sums = [jnp.zeros((1, wide), jnp.float32)] * KW
    place = lax.broadcasted_iota(jnp.int32, (rows, 1), 0)
    for m in range(2):
        back = bg[m]
        back_conv = back * proj[m, :, wide:]
        a = jnp.where(lanes.is_value, att[m], 0.0)
        tail = edge[0, m]
        nxt = e_dst[0, m]
        total = taps[0:1, :] * back_conv
        sums[0] = sums[0] + jnp.sum(back_conv * a, axis=0, keepdims=True)
        for by in (1, 2):
            kept = back_conv * col[m, :, 2 + by : 3 + by]
            sums[by] = sums[by] + jnp.sum(
                kept * shifted(a, tail, q > 0, by), axis=0, keepdims=True
            )
            moved = pltpu.roll(kept, rows - by, 0)
            for r in range(by):
                fresh = jnp.where(q < n - 1, nxt[r : r + 1, :] * late[by - 1 + r, m], 0.0)
                moved = jnp.where(place == rows - by + r, fresh, moved)
            total = total + taps[by : by + 1, :] * moved
        out[m, :, wide:] = jnp.where(lanes.is_value, back * conv[m], 0.0).astype(jnp.bfloat16)
        back_numer = total / lanes.denominator(att[m])
        spent = back_numer * a
        found = jnp.where(lanes.is_value, back_numer, 0.0)
        for h in range(HEADS):
            denom = -jnp.sum(lanes.of(h, spent), axis=1, keepdims=True)
            high = denom.astype(jnp.bfloat16).astype(jnp.float32)
            found = jnp.where(lanes.lane == values + h, high, found)
            found = jnp.where(lanes.lane == values + 2 + h, denom - high, found)
        near[m] = found.astype(jnp.bfloat16)
        part = jnp.zeros((wide, wide), jnp.float32)
        for h in range(HEADS):
            part = part + mm_tn(phi_q[m, h], lanes.of(h, near[m]))
        s_src[m] = part[:STATE].astype(jnp.bfloat16)
    states.start()
    grad_taps[...] = jnp.zeros(grad_taps.shape, jnp.float32)
    for by in range(KW):
        grad_taps[by : by + 1, :] = sums[by]
    acc_a[...] = jnp.zeros(acc_a.shape, jnp.float32)
    acc_b[...] = jnp.zeros(acc_b.shape, jnp.float32)
    for m in range(2):
        s_sum[m] = jnp.zeros(s_sum.shape[1:], jnp.float32)
        s_sum[m, :STATE, :] = sin[m].astype(jnp.float32)

    def through_phi(scaled, factors_of, h):
        u, w = factors_of
        return mm_nt((scaled * w).astype(jnp.bfloat16), e[h, 0]) + mm_nt(
            (scaled * u).astype(jnp.bfloat16), e[h, 1]
        )

    def make_block(i, carry):
        m, h = i // HEADS, i % HEADS
        a, b = sides(m)
        asked, keyed = lanes.key(h, a), lanes.key(h, b)
        valued = lanes.extended(a)
        given = lanes.of(h, near[m])
        given_v = jnp.where(lanes.is_value, given, jnp.zeros_like(given))
        for r in range(rows // BLOCK):
            lo, hi = r * BLOCK, (r + 1) * BLOCK
            x = mm_nt(asked[lo:hi], b[:hi]) * 0.25
            seen = (col[m, lo:hi, 0:1] == row[m, 0:1, :hi]) & (
                lax.broadcasted_iota(jnp.int32, (BLOCK, hi), 1)
                <= lo + lax.broadcasted_iota(jnp.int32, (BLOCK, hi), 0)
            )
            w = jnp.where(seen, 1.0 + x + 0.5 * x * x, 0.0).astype(jnp.bfloat16)
            back_w = mm_nt(given[lo:hi], valued[:hi])
            back_s = jnp.where(seen, back_w * (1.0 + x), 0.0).astype(jnp.bfloat16)
            acc_a[m, lo:hi, :] += 0.25 * mm(back_s, keyed[:hi])
            acc_b[m, :hi, :] += 0.25 * mm_tn(back_s, asked[lo:hi])
            acc_a[m, :hi, :] += mm_tn(w, given_v[lo:hi])
        s = s_sum[m].astype(jnp.bfloat16)
        scaled = mm_nt(given, s) * col[m, :, 1:2] * c[2:3, :]
        acc_a[m] += through_phi(scaled, factors(a, h), h)
        return carry

    lax.fori_loop(0, 2 * HEADS, make_block, 0)
    states.arrived()
    sum_states(states, coef, s_sum)

    def make_late(i, carry):
        m, h = i // HEADS, i % HEADS
        a, b = sides(m)
        s = s_sum[m].astype(jnp.bfloat16)
        scaled = mm_nt(lanes.of(h, lanes.extended(a)), s) * col[m, :, 2:3] * c[2:3, :]
        acc_b[m] += through_phi(scaled, factors(b, h), h)
        s_v = lanes.of(h, jnp.where(lanes.is_value, s, jnp.zeros_like(s)))
        acc_a[m] += mm(phi_k[m, h], s_v)
        return carry

    lax.fori_loop(0, 2 * HEADS, make_late, 0)
    for m in range(2):
        out[m, :, :wide] = acc_a[m].astype(jnp.bfloat16)
        out[m, :, wide:] = jnp.where(
            lanes.is_value, out[m, :, wide:].astype(jnp.float32), acc_b[m]
        ).astype(jnp.bfloat16)
    states.sent()
    edges.sent()


def seq_reach():
    n = lax.axis_size("seq")
    return n // 2 if n % 2 == 0 else n - 1


def attention_call(kernel, cid, inputs, scalars, shapes, scratch):
    vmem, smem = pl.BlockSpec(memory_space=pltpu.VMEM), pl.BlockSpec(memory_space=pltpu.SMEM)
    return pl.pallas_call(
        functools.partial(kernel, seq_reach()),
        out_shape=shapes,
        in_specs=[smem if i in scalars else vmem for i in range(len(inputs))],
        out_specs=[vmem] * len(shapes),
        scratch_shapes=scratch,
        name=f"attention{cid}",
        compiler_params=pltpu.CompilerParams(
            collective_id=cid, has_side_effects=True, vmem_limit_bytes=48 << 20
        ),
    )(*inputs)


def passing(reach, wide):
    dma = pltpu.SemaphoreType.DMA
    return (
        [
            pltpu.VMEM((2, STATE, wide), jnp.bfloat16),
            pltpu.VMEM((reach, 2, STATE, wide), jnp.bfloat16),
            pltpu.VMEM((2, wide, wide), jnp.float32),
        ],
        [dma((reach,)), dma((reach,)), dma((1,)), dma((1,))],
    )


def attention_forward(proj, taps, marks, tables):
    m, rows, double = proj.shape
    wide = double // 2
    f32, bf16 = jnp.float32, jnp.bfloat16
    buffers, sems = passing(seq_reach(), wide)
    shape = jax.ShapeDtypeStruct
    return attention_call(
        attn_forward_kernel,
        10,
        [proj, marks["col"], marks["row"], marks["before"], *tables, taps],
        (3,),
        [
            shape((m, rows, wide), bf16),
            shape((m, rows, wide), f32),
            shape((m, rows, wide), f32),
            shape((m, STATE, wide), bf16),
            shape((1, m, 16, wide), f32),
        ],
        [
            pltpu.VMEM((m, rows, wide), f32),
            pltpu.VMEM((m, HEADS, rows, wide), bf16),
            pltpu.VMEM((m, wide, wide), f32),
            *buffers,
            pltpu.VMEM((m, 16, wide), f32),
            *sems,
        ],
    )


def attention_backward(back_gated, proj, kept, taps, marks, tables):
    att, conv, sin, edge = kept
    m, rows, double = proj.shape
    wide = double // 2
    f32, bf16 = jnp.float32, jnp.bfloat16
    buffers, sems = passing(seq_reach(), wide)
    shape = jax.ShapeDtypeStruct
    return attention_call(
        attn_backward_kernel,
        11,
        [
            back_gated, proj, att, conv, sin, edge, marks["col"], marks["row"], marks["after"],
            marks["late"], *tables, taps,
        ],
        (8, 9),
        [shape((m, rows, double), bf16), shape((8, wide), f32)],
        [
            pltpu.VMEM((m, HEADS, rows, wide), bf16),
            pltpu.VMEM((m, HEADS, rows, wide), bf16),
            pltpu.VMEM((m, rows, wide), bf16),
            pltpu.VMEM((m, rows, wide), f32),
            pltpu.VMEM((m, rows, wide), f32),
            pltpu.VMEM((m, wide, wide), f32),
            *buffers,
            pltpu.VMEM((m, 16, wide), f32),
            pltpu.VMEM((1, m, 16, wide), f32),
            *sems,
        ],
    )


def sequence_marks(lengths, rows):
    count, mine = lax.axis_size("seq"), lax.axis_index("seq")
    start = mine * rows
    positions = start + jnp.arange(rows + 2, dtype=jnp.int32)
    begin_ext = jax.vmap(lambda row: seq_begin(row, positions))(lengths)
    begin = begin_ext[:, :rows]
    ends = (jnp.arange(count, dtype=jnp.int32) + 1) * rows - 1
    stays = jax.vmap(lambda row: seq_begin(row, ends))(lengths) < (ends - rows + 1)[None, :]
    stays = stays.astype(jnp.float32)
    blocks = jnp.arange(count, dtype=jnp.int32)

    def through(first, last):
        inside = (blocks >= first) & (blocks <= last)
        return jnp.min(jnp.where(inside[None, :], stays, 1.0), axis=1)

    reach = seq_reach()
    before = [through(mine - d + 1, mine - 1) for d in range(1, reach + 1)]
    after = [through(mine + 1, mine + d - 1) for d in range(1, reach + 1)]
    allowed = [(positions - j >= begin_ext).astype(jnp.float32) for j in range(KW)]
    columns = [
        begin.astype(jnp.float32),
        (begin < start).astype(jnp.float32),
        (begin == begin[:, rows - 1 :]).astype(jnp.float32),
        allowed[1][:, :rows],
        allowed[2][:, :rows],
    ]
    col = jnp.stack(columns + [jnp.zeros_like(columns[0])] * 3, axis=2)
    return {
        "col": col,
        "row": jnp.broadcast_to(columns[0][:, None, :], (2, 8, rows)),
        "before": jnp.stack(before),
        "after": jnp.stack(after),
        "late": jnp.stack([allowed[1][:, rows], allowed[2][:, rows], allowed[2][:, rows + 1]]),
    }


def by_seq(grad):
    n = lax.axis_size("seq")
    return grad.reshape((n, grad.shape[0] // n) + grad.shape[1:])


def dot_t(a, b):
    return jnp.einsum("tc,dc->td", a, b, preferred_element_type=jnp.float32)


def dot_n(a, b):
    return jnp.dot(a, b, preferred_element_type=jnp.float32)


def outer(a, b):
    return jnp.einsum("tc,tf->cf", a, b, preferred_element_type=jnp.float32).astype(jnp.bfloat16)


def on_device(
    tokens,
    lengths,
    gain_attn,
    w_query,
    w_key,
    w_value,
    w_gate_conv,
    conv_taps,
    w_out,
    gain_ffn,
    w_gate,
    w_up,
    w_down,
    cotangent,
):
    head_index = lax.axis_index("head")
    core = lax.axis_index("section")
    micro_count, rows, width = tokens.shape
    total = micro_count * rows

    def halves(weight):
        cols = weight.shape[1] // 2
        return jnp.stack([weight[:, :cols], weight[:, cols:]])

    own_mix = jnp.concatenate(
        [halves(w[0]) for w in (w_value, w_query, w_gate_conv, w_key)], axis=2
    )
    values = w_value.shape[2] // 2
    keys = w_query.shape[2] // 2
    wide = values + keys
    own_out = jnp.pad(halves(w_out[0].T), ((0, 0), (0, 0), (0, keys)))
    own_ffn = jnp.concatenate([halves(w_gate[0]), halves(w_up[0])], axis=2)
    own_down = halves(w_down[0].T)
    gains_one = lax.all_gather(gain_attn[0], "section").astype(jnp.float32)
    gains_two = lax.all_gather(gain_ffn[0], "section").astype(jnp.float32)
    taps_all = lax.all_gather(conv_taps[0], "section").astype(jnp.float32)
    taps_both = lax.dynamic_slice_in_dim(taps_all, (head_index * 2 + core) * values, values, 2)
    taps_both = jnp.pad(taps_both, ((0, 0), (0, 8 - KW), (0, keys)))
    first, rest = feature_tables(values)
    tables = (jnp.asarray(first, jnp.bfloat16), jnp.asarray(rest))
    marks = sequence_marks(lengths, rows)
    hidden_cols = own_down.shape[2]

    def as_parts(flat):
        return flat.astype(jnp.bfloat16).reshape(micro_count, rows, width)

    def spread(summed):
        return summed.astype(jnp.float32).reshape(total, width)

    mix = [None, None]
    ffn = [None, None]
    _, mix[0], _ = communicate(1, gather=(0, [own_mix, own_out]))
    x = tokens.reshape(total, width).astype(jnp.float32)
    kept = [None, None]
    outputs = []
    for layer in range(2):
        w_mix, w_o = mix[layer]
        normed = rms_norm(x, gains_one[layer]).astype(jnp.bfloat16)
        proj = dot_n(normed, w_mix).reshape(micro_count, rows, 2 * wide)
        gated, *attn = attention_forward(proj, taps_both[layer], marks, tables)
        gated = gated.reshape(total, wide)
        summed, ffn[layer], _ = communicate(
            2 + layer, partial=as_parts(dot_t(gated, w_o)), gather=(layer, [own_ffn, own_down])
        )
        w_gu, w_d = ffn[layer]
        middle = x + spread(summed)
        normed_two = rms_norm(middle, gains_two[layer]).astype(jnp.bfloat16)
        both = dot_n(normed_two, w_gu)
        hidden = (jax.nn.silu(both[:, :hidden_cols]) * both[:, hidden_cols:]).astype(jnp.bfloat16)
        partial = as_parts(dot_t(hidden, w_d))
        if layer == 0:
            summed, mix[1], _ = communicate(4, partial=partial, gather=(1, [own_mix, own_out]))
        else:
            summed, _, _ = communicate(5, partial=partial)
        out = (middle + spread(summed)).astype(jnp.bfloat16)
        outputs.append(out)
        kept[layer] = (x, normed, proj, gated, attn, middle, normed_two, both, hidden)
        x = out.astype(jnp.float32)

    grad = cotangent.reshape(total, width)
    back = [None, None]
    smalls = [None, None]
    received = [[None] * 4, [None] * 4]
    late = None
    for layer in (1, 0):
        x, normed, proj, gated, attn, middle, normed_two, both, hidden = kept[layer]
        w_mix, w_o = mix[layer]
        w_gu, w_d = ffn[layer]
        grad_wide = grad.astype(jnp.float32)
        back_hidden = dot_n(grad, w_d)
        gate_pre, upward = both[:, :hidden_cols], both[:, hidden_cols:]
        silu_value, silu_back = jax.vjp(jax.nn.silu, gate_pre)
        back_both = jnp.concatenate(
            [
                silu_back(back_hidden * upward)[0].astype(jnp.bfloat16),
                (back_hidden * silu_value).astype(jnp.bfloat16),
            ],
            axis=1,
        )
        partial = as_parts(dot_t(back_both, w_gu))
        if layer == 1:
            summed, _, _ = communicate(5, partial=partial)
        else:
            summed, _, received[1][:2] = communicate(6, partial=partial, scatter=(1, late))
        grad_gu = outer(normed_two, back_both)
        grad_d = outer(grad, hidden)
        _, norm_back_two = jax.vjp(rms_norm, middle, gains_two[layer])
        back_middle, gain_two = norm_back_two(spread(summed))
        back_middle = grad_wide + back_middle
        back_branch = back_middle.astype(jnp.bfloat16)
        grad_o = outer(back_branch, gated)
        back_gated = dot_n(back_branch, w_o)
        back_proj, taps_grad = attention_backward(
            back_gated.reshape(micro_count, rows, wide), proj, attn, taps_both[layer], marks, tables
        )
        back_proj = back_proj.reshape(total, 2 * wide)
        grad_mix = outer(normed, back_proj)
        partial = as_parts(dot_t(back_proj, w_mix))
        summed, _, received[layer][2:] = communicate(
            7 + layer, partial=partial, scatter=(layer, [by_seq(grad_gu), by_seq(grad_d)])
        )
        late = [by_seq(grad_mix), by_seq(grad_o)]
        _, norm_back_one = jax.vjp(rms_norm, x, gains_one[layer])
        back_x, gain_one = norm_back_one(spread(summed))
        grad = (back_middle + back_x).astype(jnp.bfloat16)
        back[layer] = grad
        smalls[layer] = (gain_one, gain_two, taps_grad)
    _, _, received[0][:2] = communicate(9, scatter=(0, late))

    def collect(index):
        picked = jnp.where(core == 0, received[0][index], received[1][index])
        return jnp.sum(picked.astype(jnp.float32), axis=1)

    grad_mix, grad_o, grad_gu, grad_d = [collect(i) for i in range(4)]

    def joined(pair):
        return jnp.concatenate([pair[0], pair[1]], axis=1)

    grad_value = joined(grad_mix[:, :, :values])
    grad_query = joined(grad_mix[:, :, values:wide])
    grad_gconv = joined(grad_mix[:, :, wide : wide + values])
    grad_key = joined(grad_mix[:, :, wide + values :])
    grad_out = joined(grad_o[:, :, :values]).T
    grad_gate = joined(grad_gu[:, :, :hidden_cols])
    grad_up = joined(grad_gu[:, :, hidden_cols:])
    grad_down = joined(grad_d).T

    block = width // (2 * lax.axis_size("head"))
    column_mask = (
        jnp.arange(width, dtype=jnp.int32) // block == head_index * 2 + core
    ).astype(jnp.float32)
    packed = []
    for gain_one, gain_two, taps_grad in smalls:
        taps_full = lax.dynamic_update_slice_in_dim(
            jnp.zeros((KW, width), jnp.float32),
            taps_grad[:KW, :values],
            (head_index * 2 + core) * values,
            1,
        )
        packed.append(
            jnp.concatenate(
                [(gain_one * column_mask)[None], (gain_two * column_mask)[None], taps_full], axis=0
            )
        )
    totals = lax.psum(jnp.stack(packed), ("section", "seq", "head"))
    totals = lax.dynamic_index_in_dim(totals, core, 0, False)

    def chosen(pair):
        return jnp.where(core == 0, pair[0], pair[1]).reshape(1, micro_count, rows, width)

    return (
        chosen(outputs),
        chosen(back),
        totals[0][None],
        grad_query[None],
        grad_key[None],
        grad_value[None],
        grad_gconv[None],
        totals[2:][None],
        grad_out[None],
        totals[1][None],
        grad_gate[None],
        grad_up[None],
        grad_down[None],
    )


def solution(mesh):
    placed = (
        P(None, "seq", None),
        P(),
        P("section", None),
        P("section", "seq", "head"),
        P("section", "seq", "head"),
        P("section", "seq", "head"),
        P("section", "seq", "head"),
        P("section", None, None),
        P("section", "head", "seq"),
        P("section", None),
        P("section", "seq", "head"),
        P("section", "seq", "head"),
        P("section", "head", "seq"),
        P(None, "seq", None),
    )
    return jax.shard_map(
        on_device,
        mesh=mesh,
        in_specs=placed,
        out_specs=(
            P("section", None, "seq", None),
            P("section", None, "seq", None),
            P("section", None),
            P("section", "seq", "head"),
            P("section", "seq", "head"),
            P("section", "seq", "head"),
            P("section", "seq", "head"),
            P("section", None, None),
            P("section", "head", "seq"),
            P("section", None),
            P("section", "seq", "head"),
            P("section", "seq", "head"),
            P("section", "head", "seq"),
        ),
        check_vma=False,
    )
```

```python
import functools
import math

import jax
import jax.numpy as jnp
from jax import lax
from jax.experimental import pallas as pl
from jax.experimental.pallas import tpu as pltpu
import numpy as np
from jax.sharding import PartitionSpec as P

FK = 16
KW = 3
MESH = pl.DeviceIdType.MESH
epsilon = 1e-05


def remote(src, dst, send, recv, **where):
    return pltpu.make_async_remote_copy(
        src_ref=src,
        dst_ref=dst,
        send_sem=send,
        recv_sem=recv,
        device_id=where,
        device_id_type=MESH,
    )


def greet(line, spread):
    core, z, q = lax.axis_index("section"), lax.axis_index("head"), lax.axis_index("seq")
    depth, count = lax.axis_size("head"), lax.axis_size("seq")
    barrier = pltpu.get_barrier_semaphore()

    def hello(**where):
        pl.semaphore_signal(barrier, inc=1, device_id=where, device_id_type=MESH)

    hello(section=1 - core)
    expected = 1
    if spread:
        for j in range(1, count):
            for h in range(2):
                hello(section=h, seq=lax.rem(q + j, count))
        expected += 2 * (count - 1)
    if line:

        @pl.when(z > 0)
        def _():
            hello(head=z - 1)

        @pl.when(z < depth - 1)
        def _():
            hello(head=z + 1)

        expected = expected + jnp.where(z > 0, 1, 0) + jnp.where(z < depth - 1, 1, 0)
    pl.semaphore_wait(barrier, expected)


class LineSum:
    def __init__(self, p_ref, o_ref, scratch, chunks, lag):
        self.p_ref, self.o_ref, self.chunks, self.lag = p_ref, o_ref, chunks, lag
        self.pin, self.low, self.high, self.out = scratch[:4]
        self.ps, self.pr, self.rs, self.rl, self.rh, self.bs, self.br, self.ts, self.tr = scratch[4:]
        self.z, self.n = lax.axis_index("head"), lax.axis_size("head")
        self.core = lax.axis_index("section")
        self.half = p_ref.shape[1] // 2
        self.step = self.half // chunks
        self.depth = max((self.n - 1) // 2, self.n - 1 - (self.n - 1) // 2)
        self.turns = chunks + 2 * self.depth * lag

    @staticmethod
    def scratch(rows, width, chunks):
        sem = pltpu.SemaphoreType.DMA((2, chunks))
        bank = pltpu.SemaphoreType.DMA((2, 2, chunks))
        return [pltpu.VMEM((rows, width), jnp.bfloat16)] * 4 + [
            sem, sem, sem, sem, sem, bank, sem, sem, sem
        ]

    def root(self, d):
        return (self.n - 1) // 2 if d == 0 else self.n - 1 - (self.n - 1) // 2

    def rng(self, d, k):
        return pl.ds(pl.multiple_of(d * self.half + k * self.step, self.step), self.step)

    def part(self, d, k):
        r = self.rng(d, k)
        other = 1 - self.core
        return remote(
            self.p_ref.at[other, r], self.pin.at[r], self.ps.at[d, k], self.pr.at[d, k], section=other
        )

    def up(self, d, k):
        r = self.rng(d, k)
        return remote(
            self.out.at[r], self.low.at[r], self.rs.at[d, k], self.rl.at[d, k], head=self.z + 1
        )

    def down(self, d, k):
        r = self.rng(d, k)
        return remote(
            self.out.at[r], self.high.at[r], self.rs.at[d, k], self.rh.at[d, k], head=self.z - 1
        )

    def share(self, d, k, side):
        r = self.rng(d, k)
        at = self.o_ref.at[self.core, r]
        return remote(
            at, at, self.bs.at[side, d, k], self.br.at[d, k], head=self.z + (1 if side else -1)
        )

    def give(self, d, k):
        r = self.rng(d, k)
        at = self.o_ref.at[self.core, r]
        return remote(at, at, self.ts.at[d, k], self.tr.at[d, k], section=1 - self.core)

    def start(self):
        for k in range(self.chunks):
            for d in range(2):
                self.part(d, k).start()

    def gathered(self, d, k):
        r = self.rng(d, k)
        z, n, root = self.z, self.n, self.root(d)
        self.part(d, k).wait_recv()
        mine = self.p_ref[self.core, r, :].astype(jnp.float32) + self.pin[r, :].astype(jnp.float32)

        @pl.when((z == 0) & (root > 0))
        def _():
            self.out[r, :] = mine.astype(jnp.bfloat16)
            self.up(d, k).start()

        @pl.when((z == n - 1) & (root < n - 1))
        def _():
            self.out[r, :] = mine.astype(jnp.bfloat16)
            self.down(d, k).start()

        @pl.when((z > 0) & (z < root))
        def _():
            self.up(d, k).wait_recv()
            self.out[r, :] = (mine + self.low[r, :].astype(jnp.float32)).astype(jnp.bfloat16)
            self.up(d, k).start()

        @pl.when((z < n - 1) & (z > root))
        def _():
            self.down(d, k).wait_recv()
            self.out[r, :] = (mine + self.high[r, :].astype(jnp.float32)).astype(jnp.bfloat16)
            self.down(d, k).start()

        @pl.when(z == root)
        def _():
            total = mine
            if root > 0:
                self.up(d, k).wait_recv()
                total = total + self.low[r, :].astype(jnp.float32)
            if root < n - 1:
                self.down(d, k).wait_recv()
                total = total + self.high[r, :].astype(jnp.float32)
            self.o_ref[self.core, r, :] = total.astype(jnp.bfloat16)
            if root > 0:
                self.share(d, k, 0).start()
            if root < n - 1:
                self.share(d, k, 1).start()
            self.give(d, k).start()

    def passed(self, d, k):
        z, n, root = self.z, self.n, self.root(d)
        self.share(d, k, 0).wait_recv()

        @pl.when((z < root) & (z > 0))
        def _():
            self.share(d, k, 0).start()

        @pl.when((z > root) & (z < n - 1))
        def _():
            self.share(d, k, 1).start()

        self.give(d, k).start()

    def turn(self, t):
        z, n = self.z, self.n
        for d in range(2):
            root = self.root(d)
            deep = max(root, n - 1 - root)
            below = jnp.where(z < root, z, jnp.where(z > root, n - 1 - z, deep))
            k = t - below * self.lag
            far = jnp.abs(z - root)

            @pl.when((k >= 0) & (k < self.chunks))
            def _():
                self.gathered(d, k)

            b = t - (deep + far) * self.lag

            @pl.when((b >= 0) & (b < self.chunks) & (far > 0))
            def _():
                self.passed(d, b)

    def finish(self):
        z, n = self.z, self.n
        for d in range(2):
            root = self.root(d)
            for k in range(self.chunks):
                self.part(d, k).wait_send()
                self.give(d, k).wait_recv()
                self.give(d, k).wait_send()

                @pl.when(z < root)
                def _():
                    self.up(d, k).wait_send()

                @pl.when(z > root)
                def _():
                    self.down(d, k).wait_send()

                if root > 0:

                    @pl.when((z <= root) & (z > 0))
                    def _():
                        self.share(d, k, 0).wait_send()

                if root < n - 1:

                    @pl.when((z >= root) & (z < n - 1))
                    def _():
                        self.share(d, k, 1).wait_send()


class Gather:
    def __init__(self, layer, srcs, dsts, sems):
        self.layer, self.srcs, self.dsts = layer, srcs, dsts
        self.ss, self.rr, self.ls = sems
        self.core, self.q = lax.axis_index("section"), lax.axis_index("seq")
        self.n = lax.axis_size("seq")

    @staticmethod
    def scratch(count, n):
        return [
            pltpu.SemaphoreType.DMA((count, n, 2)),
            pltpu.SemaphoreType.DMA((count, n)),
            pltpu.SemaphoreType.DMA((count,)),
        ]

    def copies(self, a):
        for j in range(1, self.n):
            for h in range(2):
                yield remote(
                    self.srcs[a].at[h], self.dsts[a].at[self.q], self.ss.at[a, j, h],
                    self.rr.at[a, self.q], section=h, seq=lax.rem(self.q + j, self.n),
                )
        yield remote(
            self.srcs[a].at[1 - self.layer], self.dsts[a].at[self.q], self.ss.at[a, 0, 0],
            self.rr.at[a, self.q], section=1 - self.layer,
        )

    def local(self, a):
        return pltpu.make_async_copy(
            self.srcs[a].at[self.layer], self.dsts[a].at[self.q], self.ls.at[a]
        )

    def arrival(self, a, s):
        return remote(
            self.srcs[a].at[0], self.dsts[a].at[s], self.ss.at[a, 0, 0], self.rr.at[a, s],
            section=1 - self.core,
        )

    def start(self):
        @pl.when(self.core == self.layer)
        def _():
            for a in range(len(self.srcs)):
                for copy in self.copies(a):
                    copy.start()
                self.local(a).start()

    def finish(self):
        for a in range(len(self.srcs)):
            for j in range(1, self.n):
                self.arrival(a, lax.rem(self.q + j, self.n)).wait_recv()

            @pl.when(self.core == self.layer)
            def _():
                self.local(a).wait()
                for copy in self.copies(a):
                    copy.wait_send()

            @pl.when(self.core != self.layer)
            def _():
                self.arrival(a, self.q).wait_recv()


class Scatter:
    def __init__(self, layer, srcs, dsts, sems):
        self.layer, self.srcs, self.dsts = layer, srcs, dsts
        self.ss, self.rr, self.ls = sems
        self.core, self.q = lax.axis_index("section"), lax.axis_index("seq")
        self.n = lax.axis_size("seq")

    @staticmethod
    def scratch(count, n):
        return [
            pltpu.SemaphoreType.DMA((count, n)),
            pltpu.SemaphoreType.DMA((count, 2, n)),
            pltpu.SemaphoreType.DMA((count,)),
        ]

    def copies(self, a):
        for j in range(1, self.n):
            t = lax.rem(self.q + j, self.n)
            yield remote(
                self.srcs[a].at[t], self.dsts[a].at[self.core, self.q], self.ss.at[a, j],
                self.rr.at[a, self.core, self.q], section=self.layer, seq=t,
            )

    def near(self, a):
        return remote(
            self.srcs[a].at[self.q], self.dsts[a].at[self.core, self.q], self.ss.at[a, 0],
            self.rr.at[a, self.core, self.q], section=self.layer,
        )

    def local(self, a):
        return pltpu.make_async_copy(
            self.srcs[a].at[self.q], self.dsts[a].at[self.core, self.q], self.ls.at[a]
        )

    def arrival(self, a, h, s):
        return remote(
            self.srcs[a].at[self.q], self.dsts[a].at[h, s], self.ss.at[a, 0], self.rr.at[a, h, s],
            section=1 - self.core,
        )

    def start(self):
        for a in range(len(self.srcs)):
            for copy in self.copies(a):
                copy.start()

            @pl.when(self.core == self.layer)
            def _():
                self.local(a).start()

            @pl.when(self.core != self.layer)
            def _():
                self.near(a).start()

    def finish(self):
        for a in range(len(self.srcs)):

            @pl.when(self.core == self.layer)
            def _():
                for j in range(1, self.n):
                    for h in range(2):
                        self.arrival(a, h, lax.rem(self.q + j, self.n)).wait_recv()
                self.arrival(a, 1 - self.layer, self.q).wait_recv()
                self.local(a).wait()

            @pl.when(self.core != self.layer)
            def _():
                self.near(a).wait_send()

            for copy in self.copies(a):
                copy.wait_send()


TILE = 256


class Product:
    def __init__(self, lhs, rhs, out, scratch):
        self.lhs, self.rhs, self.out = lhs, rhs, out
        self.left, self.right, self.stage, self.loads, self.stores = scratch
        self.tiles = lhs.shape[1] // TILE

    @staticmethod
    def scratch(lhs, rhs):
        return [
            pltpu.VMEM(lhs.shape, jnp.bfloat16),
            pltpu.VMEM(rhs.shape, jnp.bfloat16),
            pltpu.VMEM((2, TILE, rhs.shape[1]), jnp.bfloat16),
            pltpu.SemaphoreType.DMA((2,)),
            pltpu.SemaphoreType.DMA((2,)),
        ]

    def load(self, side):
        src, dst = ((self.lhs, self.left), (self.rhs, self.right))[side]
        return pltpu.make_async_copy(src, dst, self.loads.at[side])

    def store(self, i):
        at = pl.ds(pl.multiple_of(i * TILE, TILE), TILE)
        return pltpu.make_async_copy(self.stage.at[i % 2], self.out.at[at], self.stores.at[i % 2])

    def start(self):
        self.load(0).start()
        self.load(1).start()

    def step(self, i):
        @pl.when(i == 0)
        def _():
            self.load(0).wait()
            self.load(1).wait()

        @pl.when(i >= 2)
        def _():
            self.store(i - 2).wait()

        at = pl.ds(pl.multiple_of(i * TILE, TILE), TILE)
        self.stage[i % 2] = lax.dot_general(
            self.left[:, at],
            self.right[...],
            (((0,), (0,)), ((), ())),
            preferred_element_type=jnp.float32,
        ).astype(jnp.bfloat16)
        self.store(i).start()

    def finish(self):
        for i in range(max(self.tiles - 2, 0), self.tiles):
            self.store(i).wait()


def comm_kernel(plan, *refs):
    has_sum, layer_in, count_in, layer_out, count_out, kept, count_made, chunks, lag = plan
    refs = list(refs)

    def take(count):
        taken = refs[:count]
        del refs[:count]
        return taken

    p_in, w_in, g_in, _, m_in = (
        take(has_sum), take(count_in), take(count_out), take(kept), take(2 * count_made)
    )
    p_out, w_out, g_out, m_out = (
        take(has_sum), take(count_in), take(count_out), take(count_made)
    )
    greet(has_sum, count_in + count_out > 0)
    jobs = []
    if has_sum:
        line = LineSum(p_in[0], p_out[0], take(13), chunks, lag)
        line.start()
    if count_in:
        jobs.append(Gather(layer_in, w_in, w_out, take(3)))
    if count_out:
        jobs.append(Scatter(layer_out, g_in, g_out, take(3)))
    made = [
        Product(m_in[2 * i], m_in[2 * i + 1], m_out[i], take(5)) for i in range(count_made)
    ]
    for job in made + jobs:
        job.start()
    if has_sum:
        tiles = sum(product.tiles for product in made)

        def turn(t, carry):
            line.turn(t)
            i = t - 2
            for product in made:

                @pl.when((i >= 0) & (i < product.tiles))
                def _(product=product, i=i):
                    product.step(i)

                i = i - product.tiles
            return carry

        lax.fori_loop(0, max(line.turns, tiles + 2), turn, 0)
        line.finish()
    for job in made + jobs:
        job.finish()


def communicate(
    cid, partial=None, gather=None, scatter=None, into=(), products=(), chunks=16, lag=2
):
    n = lax.axis_size("seq")
    layer_in, w_in = gather if gather else (0, [])
    layer_out, g_in = scatter if scatter else (0, [])
    p_in = [] if partial is None else [partial]
    m_in = [a for pair in products for a in pair]
    vmem, anywhere = pl.BlockSpec(memory_space=pltpu.VMEM), pl.BlockSpec(memory_space=pl.ANY)
    scratch = []
    if p_in:
        scratch += LineSum.scratch(partial.shape[1], partial.shape[2], chunks)
    if w_in:
        scratch += Gather.scratch(len(w_in), n)
    if g_in:
        scratch += Scatter.scratch(len(g_in), n)
    for pair in products:
        scratch += Product.scratch(*pair)
    shapes = (
        [jax.ShapeDtypeStruct(p.shape, jnp.bfloat16) for p in p_in]
        + [jax.ShapeDtypeStruct((n,) + w.shape[1:], jnp.bfloat16) for w in w_in]
        + [jax.ShapeDtypeStruct((2,) + g.shape, jnp.bfloat16) for g in g_in]
        + [jax.ShapeDtypeStruct((a.shape[1], b.shape[1]), jnp.bfloat16) for a, b in products]
    )
    plan = (
        len(p_in), layer_in, len(w_in), layer_out, len(g_in), len(into), len(products), chunks, lag
    )
    first = len(p_in) + len(w_in)
    outs = pl.pallas_call(
        functools.partial(comm_kernel, plan),
        out_shape=shapes,
        in_specs=[vmem] * first + [anywhere] * (len(g_in) + len(into) + len(m_in)),
        out_specs=[vmem] * len(p_in) + [anywhere] * (len(w_in) + len(g_in) + len(products)),
        scratch_shapes=scratch,
        input_output_aliases={first + len(g_in) + i: first + i for i in range(len(into))},
        name=f"comm{cid}",
        compiler_params=pltpu.CompilerParams(
            collective_id=cid, has_side_effects=True, vmem_limit_bytes=52 << 20
        ),
    )(*p_in, *w_in, *g_in, *into, *m_in)
    return (
        outs[0] if p_in else None,
        [a.reshape((-1,) + a.shape[2:]) for a in outs[len(p_in) : first]],
        outs[first : first + len(g_in)],
        outs[first + len(g_in) :],
    )


def rms_norm(vector, scale_gain):
    return (
        vector * lax.rsqrt(jnp.mean(vector * vector, axis=-1, keepdims=True) + epsilon) * scale_gain
    )


def seq_begin(lengths_row, positions):
    seq_starts = jnp.cumsum(lengths_row) - lengths_row
    chosen = jnp.where(seq_starts[None, :] <= positions[:, None], seq_starts[None, :], 0)
    return jnp.max(chosen, axis=1)


HEADS = 2
PAIRS = FK * (FK + 1) // 2
STATE = 160
BLOCK = 128


def feature_tables(values):
    wide = values + HEADS * FK
    first = np.zeros((HEADS, wide, wide), np.float32)
    second = np.zeros((HEADS, wide, wide), np.float32)
    rest = np.zeros((8, wide), np.float32)
    for h in range(HEADS):
        at = values + h * FK
        lane = 0
        for a in range(FK):
            for b in range(a, FK):
                first[h, at + a, lane] = 1
                second[h, at + b, lane] = 1
                rest[2, lane] = 0.25 if a < b else 1 / (4.0 * math.sqrt(2.0))
                lane += 1
        for a in range(FK):
            first[h, at + a, lane] = 1
            rest[1, lane] = 1
            rest[2, lane] = 0.5
            lane += 1
        rest[0, lane] = rest[1, lane] = rest[2, lane] = 1
    return np.stack([first, second], axis=1), rest


def mm(a, b):
    return lax.dot_general(a, b, (((1,), (0,)), ((), ())), preferred_element_type=jnp.float32)


def mm_nt(a, b):
    return lax.dot_general(a, b, (((1,), (1,)), ((), ())), preferred_element_type=jnp.float32)


def mm_tn(a, b):
    return lax.dot_general(a, b, (((0,), (0,)), ((), ())), preferred_element_type=jnp.float32)


class Lanes:
    def __init__(self, wide, values):
        self.values = values
        self.lane = lax.broadcasted_iota(jnp.int32, (1, wide), 1)
        lane, dim = self.lane, values // HEADS
        self.is_value = lane < values
        self.is_one = (lane >= values) & (lane < values + 2 * HEADS)
        self.head = jnp.where(
            self.is_value, jnp.where(lane < dim, 0, 1), jnp.where(self.is_one, (lane - values) % 2, 9)
        )

    def of(self, h, x):
        return jnp.where(self.head == h, x, jnp.zeros_like(x))

    def key(self, h, x):
        at = self.values + h * FK
        return jnp.where((self.lane >= at) & (self.lane < at + FK), x, jnp.zeros_like(x))

    def extended(self, a):
        return jnp.where(
            self.is_value, a, jnp.where(self.is_one, jnp.ones_like(a), jnp.zeros_like(a))
        )

    def column(self, x, index):
        return jnp.sum(
            jnp.where(self.lane == self.values + index, x, 0.0), axis=1, keepdims=True
        )

    def denominator(self, x):
        return jnp.where(
            self.lane < self.values // HEADS, self.column(x, 0), self.column(x, 1)
        )


def meet(direction, reach):
    q, n = lax.axis_index("seq"), lax.axis_size("seq")
    barrier = pltpu.get_barrier_semaphore()
    count = 0
    for d in range(1, reach + 1):
        source = q - direction * d
        target = q + direction * d

        @pl.when((source >= 0) & (source < n))
        def _():
            pl.semaphore_signal(barrier, inc=1, device_id={"seq": source}, device_id_type=MESH)

        count = count + jnp.where((target >= 0) & (target < n), 1, 0)

    @pl.when(count > 0)
    def _():
        pl.semaphore_wait(barrier, count)


class Pass:
    def __init__(self, direction, reach, src, dst, send, recv):
        self.direction, self.reach = direction, reach
        self.src, self.dst, self.send, self.recv = src, dst, send, recv
        self.q, self.n = lax.axis_index("seq"), lax.axis_size("seq")

    def has_source(self, d):
        at = self.q - self.direction * d
        return (at >= 0) & (at < self.n)

    def has_target(self, d):
        at = self.q + self.direction * d
        return (at >= 0) & (at < self.n)

    def copy(self, d):
        return remote(
            self.src, self.dst.at[d - 1], self.send.at[d - 1], self.recv.at[d - 1],
            seq=self.q + self.direction * d,
        )

    def start(self):
        for d in range(1, self.reach + 1):

            @pl.when(self.has_target(d))
            def _():
                self.copy(d).start()

    def arrived(self):
        for d in range(1, self.reach + 1):

            @pl.when(self.has_source(d))
            def _():
                self.copy(d).wait_recv()

    def sent(self):
        for d in range(1, self.reach + 1):

            @pl.when(self.has_target(d))
            def _():
                self.copy(d).wait_send()


def sum_states(states, coef, total):
    for m in range(2):
        total[m] = jnp.zeros(total.shape[1:], total.dtype)
        for d in range(1, states.reach + 1):

            @pl.when(states.has_source(d))
            def _():
                total[m, :STATE, :] += coef[d - 1, m] * states.dst[d - 1, m].astype(jnp.float32)


def shifted(a, tail, fresh, by):
    row = lax.broadcasted_iota(jnp.int32, (a.shape[0], 1), 0)
    moved = pltpu.roll(a, by, 0)
    rows = tail.shape[0]
    for r in range(by):
        edge = jnp.where(fresh, tail[rows - by + r : rows - by + r + 1, :], 0.0)
        moved = jnp.where(row == r, edge, moved)
    return moved


def attn_forward_kernel(
    reach, proj, col, row, coef, e, c, taps, gated, att, conv, sin, edge, acc, phi, s_acc, s_src,
    s_all, s_sum, e_src, ss, sr, es, er,
):
    q = lax.axis_index("seq")
    rows, wide = proj.shape[1], proj.shape[2] // 2
    values = wide - HEADS * FK
    lanes = Lanes(wide, values)
    meet(1, reach)
    states = Pass(1, reach, s_src, s_all, ss, sr)
    edges = Pass(1, 1, e_src, edge, es, er)

    def sides(m):
        return proj[m, :, :wide].astype(jnp.bfloat16), proj[m, :, wide:].astype(jnp.bfloat16)

    def phi_of(a, h):
        return (mm(a, e[h, 0]) + c[0:1, :]) * (mm(a, e[h, 1]) + c[1:2, :]) * c[2:3, :]

    def make_state(i, carry):
        m, h = i // HEADS, i % HEADS
        a, b = sides(m)
        phi[m, h] = (phi_of(a, h) * col[m, :, 1:2]).astype(jnp.bfloat16)
        keyed = (phi_of(b, h) * col[m, :, 2:3]).astype(jnp.bfloat16)
        part = mm_tn(keyed, lanes.of(h, lanes.extended(a)))

        @pl.when(h == 0)
        def _():
            s_acc[m] = part

        @pl.when(h > 0)
        def _():
            s_acc[m] += part

        return carry

    lax.fori_loop(0, 2 * HEADS, make_state, 0)
    for m in range(2):
        s_src[m] = s_acc[m, :STATE, :].astype(jnp.bfloat16)
    states.start()

    def make_block(i, carry):
        m, h = i // HEADS, i % HEADS
        a, b = sides(m)
        asked = lanes.key(h, a)
        valued = lanes.of(h, lanes.extended(a))
        for r in range(rows // BLOCK):
            lo, hi = r * BLOCK, (r + 1) * BLOCK
            x = mm_nt(asked[lo:hi], b[:hi]) * 0.25
            seen = (col[m, lo:hi, 0:1] == row[m, 0:1, :hi]) & (
                lax.broadcasted_iota(jnp.int32, (BLOCK, hi), 1)
                <= lo + lax.broadcasted_iota(jnp.int32, (BLOCK, hi), 0)
            )
            w = jnp.where(seen, 1.0 + x + 0.5 * x * x, 0.0).astype(jnp.bfloat16)
            part = mm(w, valued[:hi])

            @pl.when(h == 0)
            def _():
                acc[m, lo:hi, :] = part

            @pl.when(h > 0)
            def _():
                acc[m, lo:hi, :] += part

        return carry

    lax.fori_loop(0, 2 * HEADS, make_block, 0)
    states.arrived()
    sum_states(states, coef, s_sum)

    def attend(m, lo):
        s = s_sum[m].astype(jnp.bfloat16)
        both = acc[m, lo:, :]
        for h in range(HEADS):
            both = both + mm(phi[m, h, lo:, :], lanes.of(h, s))
        return jnp.where(lanes.is_value, both / lanes.denominator(both), both)

    for m in range(2):
        sin[m] = s_sum[m, :STATE, :].astype(jnp.bfloat16)
        e_src[m] = attend(m, rows - 16)
    edges.start()
    for m in range(2):
        att[m] = attend(m, 0)
    edges.arrived()
    for m in range(2):
        a = att[m]
        tail = edge[0, m]
        out = taps[0:1, :] * a
        for by in (1, 2):
            out = out + taps[by : by + 1, :] * shifted(a, tail, q > 0, by) * col[m, :, 2 + by : 3 + by]
        conv[m] = out
        gated[m] = (out * proj[m, :, wide:]).astype(jnp.bfloat16)
    states.sent()
    edges.sent()


def attn_backward_kernel(
    reach, bg, proj, att, conv, sin, edge, col, row, coef, late, e, c, taps, out, grad_taps,
    phi_q, phi_k, near, acc_a, acc_b, s_acc, s_src, s_all, s_sum, e_src, e_dst, ss, sr, es, er,
):
    q, n = lax.axis_index("seq"), lax.axis_size("seq")
    rows, wide = proj.shape[1], proj.shape[2] // 2
    values = wide - HEADS * FK
    lanes = Lanes(wide, values)
    meet(-1, reach)
    states = Pass(-1, reach, s_src, s_all, ss, sr)
    edges = Pass(-1, 1, e_src, e_dst, es, er)
    for m in range(2):
        e_src[m] = bg[m, :16, :] * proj[m, :16, wide:]
    edges.start()

    def sides(m):
        return proj[m, :, :wide].astype(jnp.bfloat16), proj[m, :, wide:].astype(jnp.bfloat16)

    def factors(a, h):
        return mm(a, e[h, 0]) + c[0:1, :], mm(a, e[h, 1]) + c[1:2, :]

    def make_phi(i, carry):
        m, h = i // HEADS, i % HEADS
        a, b = sides(m)
        u, w = factors(a, h)
        phi_q[m, h] = (u * w * c[2:3, :] * col[m, :, 1:2]).astype(jnp.bfloat16)
        u, w = factors(b, h)
        phi_k[m, h] = (u * w * c[2:3, :] * col[m, :, 2:3]).astype(jnp.bfloat16)
        return carry

    lax.fori_loop(0, 2 * HEADS, make_phi, 0)
    edges.arrived()
    sums = [jnp.zeros((1, wide), jnp.float32)] * KW
    place = lax.broadcasted_iota(jnp.int32, (rows, 1), 0)
    for m in range(2):
        back = bg[m]
        back_conv = back * proj[m, :, wide:]
        a = jnp.where(lanes.is_value, att[m], 0.0)
        tail = edge[0, m]
        nxt = e_dst[0, m]
        total = taps[0:1, :] * back_conv
        sums[0] = sums[0] + jnp.sum(back_conv * a, axis=0, keepdims=True)
        for by in (1, 2):
            kept = back_conv * col[m, :, 2 + by : 3 + by]
            sums[by] = sums[by] + jnp.sum(
                kept * shifted(a, tail, q > 0, by), axis=0, keepdims=True
            )
            moved = pltpu.roll(kept, rows - by, 0)
            for r in range(by):
                fresh = jnp.where(q < n - 1, nxt[r : r + 1, :] * late[by - 1 + r, m], 0.0)
                moved = jnp.where(place == rows - by + r, fresh, moved)
            total = total + taps[by : by + 1, :] * moved
        out[m, :, wide:] = jnp.where(lanes.is_value, back * conv[m], 0.0).astype(jnp.bfloat16)
        back_numer = total / lanes.denominator(att[m])
        spent = back_numer * a
        found = jnp.where(lanes.is_value, back_numer, 0.0)
        for h in range(HEADS):
            denom = -jnp.sum(lanes.of(h, spent), axis=1, keepdims=True)
            high = denom.astype(jnp.bfloat16).astype(jnp.float32)
            found = jnp.where(lanes.lane == values + h, high, found)
            found = jnp.where(lanes.lane == values + 2 + h, denom - high, found)
        near[m] = found.astype(jnp.bfloat16)
        part = jnp.zeros((wide, wide), jnp.float32)
        for h in range(HEADS):
            part = part + mm_tn(phi_q[m, h], lanes.of(h, near[m]))
        s_src[m] = part[:STATE].astype(jnp.bfloat16)
    states.start()
    grad_taps[...] = jnp.zeros(grad_taps.shape, jnp.float32)
    for by in range(KW):
        grad_taps[by : by + 1, :] = sums[by]
    acc_a[...] = jnp.zeros(acc_a.shape, jnp.float32)
    acc_b[...] = jnp.zeros(acc_b.shape, jnp.float32)
    for m in range(2):
        s_sum[m] = jnp.zeros(s_sum.shape[1:], jnp.float32)
        s_sum[m, :STATE, :] = sin[m].astype(jnp.float32)

    def through_phi(scaled, factors_of, h):
        u, w = factors_of
        return mm_nt((scaled * w).astype(jnp.bfloat16), e[h, 0]) + mm_nt(
            (scaled * u).astype(jnp.bfloat16), e[h, 1]
        )

    def make_block(i, carry):
        m, h = i // HEADS, i % HEADS
        a, b = sides(m)
        asked, keyed = lanes.key(h, a), lanes.key(h, b)
        valued = lanes.extended(a)
        given = lanes.of(h, near[m])
        given_v = jnp.where(lanes.is_value, given, jnp.zeros_like(given))
        for r in range(rows // BLOCK):
            lo, hi = r * BLOCK, (r + 1) * BLOCK
            x = mm_nt(asked[lo:hi], b[:hi]) * 0.25
            seen = (col[m, lo:hi, 0:1] == row[m, 0:1, :hi]) & (
                lax.broadcasted_iota(jnp.int32, (BLOCK, hi), 1)
                <= lo + lax.broadcasted_iota(jnp.int32, (BLOCK, hi), 0)
            )
            w = jnp.where(seen, 1.0 + x + 0.5 * x * x, 0.0).astype(jnp.bfloat16)
            back_w = mm_nt(given[lo:hi], valued[:hi])
            back_s = jnp.where(seen, back_w * (1.0 + x), 0.0).astype(jnp.bfloat16)
            acc_a[m, lo:hi, :] += 0.25 * mm(back_s, keyed[:hi])
            acc_b[m, :hi, :] += 0.25 * mm_tn(back_s, asked[lo:hi])
            acc_a[m, :hi, :] += mm_tn(w, given_v[lo:hi])
        s = s_sum[m].astype(jnp.bfloat16)
        scaled = mm_nt(given, s) * col[m, :, 1:2] * c[2:3, :]
        acc_a[m] += through_phi(scaled, factors(a, h), h)
        return carry

    lax.fori_loop(0, 2 * HEADS, make_block, 0)
    states.arrived()
    sum_states(states, coef, s_sum)

    def make_late(i, carry):
        m, h = i // HEADS, i % HEADS
        a, b = sides(m)
        s = s_sum[m].astype(jnp.bfloat16)
        scaled = mm_nt(lanes.of(h, lanes.extended(a)), s) * col[m, :, 2:3] * c[2:3, :]
        acc_b[m] += through_phi(scaled, factors(b, h), h)
        s_v = lanes.of(h, jnp.where(lanes.is_value, s, jnp.zeros_like(s)))
        acc_a[m] += mm(phi_k[m, h], s_v)
        return carry

    lax.fori_loop(0, 2 * HEADS, make_late, 0)
    for m in range(2):
        out[m, :, :wide] = acc_a[m].astype(jnp.bfloat16)
        out[m, :, wide:] = jnp.where(
            lanes.is_value, out[m, :, wide:].astype(jnp.float32), acc_b[m]
        ).astype(jnp.bfloat16)
    states.sent()
    edges.sent()


def seq_reach():
    n = lax.axis_size("seq")
    return n // 2 if n % 2 == 0 else n - 1


def attention_call(kernel, cid, inputs, scalars, shapes, scratch):
    vmem, smem = pl.BlockSpec(memory_space=pltpu.VMEM), pl.BlockSpec(memory_space=pltpu.SMEM)
    return pl.pallas_call(
        functools.partial(kernel, seq_reach()),
        out_shape=shapes,
        in_specs=[smem if i in scalars else vmem for i in range(len(inputs))],
        out_specs=[vmem] * len(shapes),
        scratch_shapes=scratch,
        name=f"attention{cid}",
        compiler_params=pltpu.CompilerParams(
            collective_id=cid, has_side_effects=True, vmem_limit_bytes=48 << 20
        ),
    )(*inputs)


def passing(reach, wide):
    dma = pltpu.SemaphoreType.DMA
    return (
        [
            pltpu.VMEM((2, STATE, wide), jnp.bfloat16),
            pltpu.VMEM((reach, 2, STATE, wide), jnp.bfloat16),
            pltpu.VMEM((2, wide, wide), jnp.float32),
        ],
        [dma((reach,)), dma((reach,)), dma((1,)), dma((1,))],
    )


def attention_forward(proj, taps, marks, tables):
    m, rows, double = proj.shape
    wide = double // 2
    f32, bf16 = jnp.float32, jnp.bfloat16
    buffers, sems = passing(seq_reach(), wide)
    shape = jax.ShapeDtypeStruct
    return attention_call(
        attn_forward_kernel,
        10,
        [proj, marks["col"], marks["row"], marks["before"], *tables, taps],
        (3,),
        [
            shape((m, rows, wide), bf16),
            shape((m, rows, wide), f32),
            shape((m, rows, wide), f32),
            shape((m, STATE, wide), bf16),
            shape((1, m, 16, wide), f32),
        ],
        [
            pltpu.VMEM((m, rows, wide), f32),
            pltpu.VMEM((m, HEADS, rows, wide), bf16),
            pltpu.VMEM((m, wide, wide), f32),
            *buffers,
            pltpu.VMEM((m, 16, wide), f32),
            *sems,
        ],
    )


def attention_backward(back_gated, proj, kept, taps, marks, tables):
    att, conv, sin, edge = kept
    m, rows, double = proj.shape
    wide = double // 2
    f32, bf16 = jnp.float32, jnp.bfloat16
    buffers, sems = passing(seq_reach(), wide)
    shape = jax.ShapeDtypeStruct
    return attention_call(
        attn_backward_kernel,
        11,
        [
            back_gated, proj, att, conv, sin, edge, marks["col"], marks["row"], marks["after"],
            marks["late"], *tables, taps,
        ],
        (8, 9),
        [shape((m, rows, double), bf16), shape((8, wide), f32)],
        [
            pltpu.VMEM((m, HEADS, rows, wide), bf16),
            pltpu.VMEM((m, HEADS, rows, wide), bf16),
            pltpu.VMEM((m, rows, wide), bf16),
            pltpu.VMEM((m, rows, wide), f32),
            pltpu.VMEM((m, rows, wide), f32),
            pltpu.VMEM((m, wide, wide), f32),
            *buffers,
            pltpu.VMEM((m, 16, wide), f32),
            pltpu.VMEM((1, m, 16, wide), f32),
            *sems,
        ],
    )


def sequence_marks(lengths, rows):
    count, mine = lax.axis_size("seq"), lax.axis_index("seq")
    start = mine * rows
    positions = start + jnp.arange(rows + 2, dtype=jnp.int32)
    begin_ext = jax.vmap(lambda row: seq_begin(row, positions))(lengths)
    begin = begin_ext[:, :rows]
    ends = (jnp.arange(count, dtype=jnp.int32) + 1) * rows - 1
    stays = jax.vmap(lambda row: seq_begin(row, ends))(lengths) < (ends - rows + 1)[None, :]
    stays = stays.astype(jnp.float32)
    blocks = jnp.arange(count, dtype=jnp.int32)

    def through(first, last):
        inside = (blocks >= first) & (blocks <= last)
        return jnp.min(jnp.where(inside[None, :], stays, 1.0), axis=1)

    reach = seq_reach()
    before = [through(mine - d + 1, mine - 1) for d in range(1, reach + 1)]
    after = [through(mine + 1, mine + d - 1) for d in range(1, reach + 1)]
    allowed = [(positions - j >= begin_ext).astype(jnp.float32) for j in range(KW)]
    columns = [
        begin.astype(jnp.float32),
        (begin < start).astype(jnp.float32),
        (begin == begin[:, rows - 1 :]).astype(jnp.float32),
        allowed[1][:, :rows],
        allowed[2][:, :rows],
    ]
    col = jnp.stack(columns + [jnp.zeros_like(columns[0])] * 3, axis=2)
    return {
        "col": col,
        "row": jnp.broadcast_to(columns[0][:, None, :], (2, 8, rows)),
        "before": jnp.stack(before),
        "after": jnp.stack(after),
        "late": jnp.stack([allowed[1][:, rows], allowed[2][:, rows], allowed[2][:, rows + 1]]),
    }


def by_seq(grad):
    n = lax.axis_size("seq")
    return grad.reshape((n, grad.shape[0] // n) + grad.shape[1:])


def dot_t(a, b):
    return jnp.einsum("tc,dc->td", a, b, preferred_element_type=jnp.float32)


def dot_n(a, b):
    return jnp.dot(a, b, preferred_element_type=jnp.float32)


def on_device(
    tokens,
    lengths,
    gain_attn,
    w_query,
    w_key,
    w_value,
    w_gate_conv,
    conv_taps,
    w_out,
    gain_ffn,
    w_gate,
    w_up,
    w_down,
    cotangent,
):
    head_index = lax.axis_index("head")
    core = lax.axis_index("section")
    micro_count, rows, width = tokens.shape
    total = micro_count * rows

    def halves(weight):
        cols = weight.shape[1] // 2
        return jnp.stack([weight[:, :cols], weight[:, cols:]])

    own_mix = jnp.concatenate(
        [halves(w[0]) for w in (w_value, w_query, w_gate_conv, w_key)], axis=2
    )
    values = w_value.shape[2] // 2
    keys = w_query.shape[2] // 2
    wide = values + keys
    own_out = jnp.pad(halves(w_out[0].T), ((0, 0), (0, 0), (0, keys)))
    own_ffn = jnp.concatenate([halves(w_gate[0]), halves(w_up[0])], axis=2)
    own_down = halves(w_down[0].T)
    gains_one = lax.all_gather(gain_attn[0], "section").astype(jnp.float32)
    gains_two = lax.all_gather(gain_ffn[0], "section").astype(jnp.float32)
    taps_all = lax.all_gather(conv_taps[0], "section").astype(jnp.float32)
    taps_both = lax.dynamic_slice_in_dim(taps_all, (head_index * 2 + core) * values, values, 2)
    taps_both = jnp.pad(taps_both, ((0, 0), (0, 8 - KW), (0, keys)))
    first, rest = feature_tables(values)
    tables = (jnp.asarray(first, jnp.bfloat16), jnp.asarray(rest))
    marks = sequence_marks(lengths, rows)
    hidden_cols = own_down.shape[2]

    def as_parts(flat):
        return flat.astype(jnp.bfloat16).reshape(micro_count, rows, width)

    def spread(summed):
        return summed.astype(jnp.float32).reshape(total, width)

    _, (mix_0, out_0), _, _ = communicate(1, gather=(0, [own_mix, own_out]))
    w_mix, w_o, w_gu, w_d = [mix_0, None], [out_0, None], [None, None], [None, None]
    x = tokens.reshape(total, width).astype(jnp.float32)
    kept = [None, None]
    outputs = []
    last_partial = None
    for layer in range(2):
        normed = rms_norm(x, gains_one[layer]).astype(jnp.bfloat16)
        proj = dot_n(normed, w_mix[layer]).reshape(micro_count, rows, 2 * wide)
        gated, *attn = attention_forward(proj, taps_both[layer], marks, tables)
        gated = gated.reshape(total, wide)
        partial = as_parts(dot_t(gated, w_o[layer]))
        if layer == 0:
            summed, (w_gu[0], w_d[0]), _, _ = communicate(
                2, partial=partial, gather=(0, [own_ffn, own_down])
            )
        else:
            summed, (w_gu[1],), _, _ = communicate(3, partial=partial, gather=(1, [own_ffn]))
        middle = x + spread(summed)
        normed_two = rms_norm(middle, gains_two[layer]).astype(jnp.bfloat16)
        both = dot_n(normed_two, w_gu[layer])
        hidden = (jax.nn.silu(both[:, :hidden_cols]) * both[:, hidden_cols:]).astype(jnp.bfloat16)
        partial = as_parts(dot_t(hidden, w_d[layer]))
        kept[layer] = (x, normed, proj, gated, attn, middle, normed_two, both, hidden)
        if layer == 0:
            summed, (w_mix[1], w_o[1], w_d[1]), _, _ = communicate(
                4, partial=partial, gather=(1, [own_mix, own_out, own_down])
            )
            outputs.append((middle + spread(summed)).astype(jnp.bfloat16))
            x = outputs[0].astype(jnp.float32)
        else:
            last_partial = partial

    grad = cotangent.reshape(total, width)
    back = [None, None]
    smalls = [None, None]
    made = []
    into = [None] * 4
    for layer in (1, 0):
        x, normed, proj, gated, attn, middle, normed_two, both, hidden = kept[layer]
        grad_wide = grad.astype(jnp.float32)
        back_hidden = dot_n(grad, w_d[layer])
        gate_pre, upward = both[:, :hidden_cols], both[:, hidden_cols:]
        silu_value, silu_back = jax.vjp(jax.nn.silu, gate_pre)
        back_both = jnp.concatenate(
            [
                silu_back(back_hidden * upward)[0].astype(jnp.bfloat16),
                (back_hidden * silu_value).astype(jnp.bfloat16),
            ],
            axis=1,
        )
        partial = as_parts(dot_t(back_both, w_gu[layer]))
        products = ((normed_two, back_both), (grad, hidden))
        if layer == 1:
            summed, _, _, (grad_gu, grad_d) = communicate(5, partial=partial, products=products)
        else:
            summed, _, into[1:], (grad_gu, grad_d) = communicate(
                6, partial=partial, scatter=(1, made), products=products
            )
        _, norm_back_two = jax.vjp(rms_norm, middle, gains_two[layer])
        back_middle, gain_two = norm_back_two(spread(summed))
        back_middle = grad_wide + back_middle
        back_branch = back_middle.astype(jnp.bfloat16)
        back_gated = dot_n(back_branch, w_o[layer])
        back_proj, taps_grad = attention_backward(
            back_gated.reshape(micro_count, rows, wide), proj, attn, taps_both[layer], marks, tables
        )
        back_proj = back_proj.reshape(total, 2 * wide)
        partial = as_parts(dot_t(back_proj, w_mix[layer]))
        summed, _, into[:1], (grad_mix, grad_o) = communicate(
            7 + layer,
            partial=partial,
            scatter=(layer, [by_seq(grad_gu)]),
            into=into[:1] if layer == 0 else (),
            products=((normed, back_proj), (back_branch, gated)),
        )
        made = [by_seq(grad_d), by_seq(grad_mix), by_seq(grad_o)]
        _, norm_back_one = jax.vjp(rms_norm, x, gains_one[layer])
        back_x, gain_one = norm_back_one(spread(summed))
        grad = (back_middle + back_x).astype(jnp.bfloat16)
        back[layer] = grad
        smalls[layer] = (gain_one, gain_two, taps_grad)
    summed, _, into[1:], _ = communicate(
        9, partial=last_partial, scatter=(0, made), into=into[1:]
    )
    outputs.append((kept[1][5] + spread(summed)).astype(jnp.bfloat16))
    grad_gu, grad_d, grad_mix, grad_o = [
        jnp.sum(received.astype(jnp.float32), axis=1).reshape((2, -1) + received.shape[3:])
        for received in into
    ]

    def joined(pair):
        return jnp.concatenate([pair[0], pair[1]], axis=1)

    grad_value = joined(grad_mix[:, :, :values])
    grad_query = joined(grad_mix[:, :, values:wide])
    grad_gconv = joined(grad_mix[:, :, wide : wide + values])
    grad_key = joined(grad_mix[:, :, wide + values :])
    grad_out = joined(grad_o[:, :, :values]).T
    grad_gate = joined(grad_gu[:, :, :hidden_cols])
    grad_up = joined(grad_gu[:, :, hidden_cols:])
    grad_down = joined(grad_d).T

    block = width // (2 * lax.axis_size("head"))
    column_mask = (
        jnp.arange(width, dtype=jnp.int32) // block == head_index * 2 + core
    ).astype(jnp.float32)
    packed = []
    for gain_one, gain_two, taps_grad in smalls:
        taps_full = lax.dynamic_update_slice_in_dim(
            jnp.zeros((KW, width), jnp.float32),
            taps_grad[:KW, :values],
            (head_index * 2 + core) * values,
            1,
        )
        packed.append(
            jnp.concatenate(
                [(gain_one * column_mask)[None], (gain_two * column_mask)[None], taps_full], axis=0
            )
        )
    totals = lax.psum(jnp.stack(packed), ("section", "seq", "head"))
    totals = lax.dynamic_index_in_dim(totals, core, 0, False)

    def chosen(pair):
        return jnp.where(core == 0, pair[0], pair[1]).reshape(1, micro_count, rows, width)

    return (
        chosen(outputs),
        chosen(back),
        totals[0][None],
        grad_query[None],
        grad_key[None],
        grad_value[None],
        grad_gconv[None],
        totals[2:][None],
        grad_out[None],
        totals[1][None],
        grad_gate[None],
        grad_up[None],
        grad_down[None],
    )


def solution(mesh):
    placed = (
        P(None, "seq", None),
        P(),
        P("section", None),
        P("section", "seq", "head"),
        P("section", "seq", "head"),
        P("section", "seq", "head"),
        P("section", "seq", "head"),
        P("section", None, None),
        P("section", "head", "seq"),
        P("section", None),
        P("section", "seq", "head"),
        P("section", "seq", "head"),
        P("section", "head", "seq"),
        P(None, "seq", None),
    )
    return jax.shard_map(
        on_device,
        mesh=mesh,
        in_specs=placed,
        out_specs=(
            P("section", None, "seq", None),
            P("section", None, "seq", None),
            P("section", None),
            P("section", "seq", "head"),
            P("section", "seq", "head"),
            P("section", "seq", "head"),
            P("section", "seq", "head"),
            P("section", None, None),
            P("section", "head", "seq"),
            P("section", None),
            P("section", "seq", "head"),
            P("section", "seq", "head"),
            P("section", "head", "seq"),
        ),
        check_vma=False,
    )
```

```python
import functools
import math

import jax
import jax.numpy as jnp
from jax import lax
from jax.experimental import pallas as pl
from jax.experimental.pallas import tpu as pltpu
import numpy as np
from jax.sharding import PartitionSpec as P

FK = 16
KW = 3
MESH = pl.DeviceIdType.MESH
epsilon = 1e-05


def remote(src, dst, send, recv, **where):
    return pltpu.make_async_remote_copy(
        src_ref=src,
        dst_ref=dst,
        send_sem=send,
        recv_sem=recv,
        device_id=where,
        device_id_type=MESH,
    )


def greet(line, spread, everyone):
    core, z, q = lax.axis_index("section"), lax.axis_index("head"), lax.axis_index("seq")
    depth, count = lax.axis_size("head"), lax.axis_size("seq")
    barrier = pltpu.get_barrier_semaphore()

    def hello(**where):
        pl.semaphore_signal(barrier, inc=1, device_id=where, device_id_type=MESH)

    hello(section=1 - core)
    expected = 1
    if spread:
        for j in range(1, count):
            for h in range(2):
                hello(section=h, seq=lax.rem(q + j, count))
        expected += 2 * (count - 1)
    if everyone:
        for j in range(1, depth):
            for h in range(2):
                hello(section=h, head=lax.rem(z + j, depth))
        expected += 2 * (depth - 1)
    elif line:

        @pl.when(z > 0)
        def _():
            hello(head=z - 1)

        @pl.when(z < depth - 1)
        def _():
            hello(head=z + 1)

        expected = expected + jnp.where(z > 0, 1, 0) + jnp.where(z < depth - 1, 1, 0)
    pl.semaphore_wait(barrier, expected)


PIECES = 4


class LineSum:
    def __init__(self, p_ref, o_ref, scratch, chunks, lag):
        self.p_ref, self.o_ref, self.chunks, self.lag = p_ref, o_ref, chunks, lag
        self.pin, self.low, self.high, self.out = scratch[:4]
        self.ps, self.pr, self.rs, self.rl, self.rh, self.bs, self.br, self.ts, self.tr = scratch[4:]
        self.z, self.n = lax.axis_index("head"), lax.axis_size("head")
        self.core = lax.axis_index("section")
        self.half = p_ref.shape[1] // 2
        self.step = self.half // chunks
        self.depth = max((self.n - 1) // 2, self.n - 1 - (self.n - 1) // 2)
        self.turns = chunks + 2 * self.depth * lag

    @staticmethod
    def scratch(rows, width, chunks):
        dma = pltpu.SemaphoreType.DMA
        each = dma((2, chunks))
        return [pltpu.VMEM((rows, width), jnp.bfloat16)] * 4 + [
            dma((1,)), dma((2, PIECES)), dma((2,)), each, each, dma((2, 2)), each, dma((1,)), dma((1,))
        ]

    def root(self, d):
        return (self.n - 1) // 2 if d == 0 else self.n - 1 - (self.n - 1) // 2

    def rng(self, d, k):
        return pl.ds(pl.multiple_of(d * self.half + k * self.step, self.step), self.step)

    def part(self, d, k):
        size = self.half // PIECES
        r = pl.ds(pl.multiple_of(d * self.half + k * size, size), size)
        other = 1 - self.core
        return remote(
            self.p_ref.at[other, r], self.pin.at[r], self.ps.at[0], self.pr.at[d, k], section=other
        )

    def up(self, d, k):
        r = self.rng(d, k)
        return remote(
            self.out.at[r], self.low.at[r], self.rs.at[d], self.rl.at[d, k], head=self.z + 1
        )

    def down(self, d, k):
        r = self.rng(d, k)
        return remote(
            self.out.at[r], self.high.at[r], self.rs.at[d], self.rh.at[d, k], head=self.z - 1
        )

    def share(self, d, k, side):
        r = self.rng(d, k)
        at = self.o_ref.at[self.core, r]
        return remote(
            at, at, self.bs.at[side, d], self.br.at[d, k], head=self.z + (1 if side else -1)
        )

    def give(self, d, k):
        r = self.rng(d, k)
        at = self.o_ref.at[self.core, r]
        return remote(at, at, self.ts.at[0], self.tr.at[0], section=1 - self.core)

    def start(self):
        for k in range(PIECES):
            for d in range(2):
                self.part(d, k).start()

    def gathered(self, d, k):
        r = self.rng(d, k)
        z, n, root = self.z, self.n, self.root(d)
        group = self.chunks // PIECES

        @pl.when(k % group == 0)
        def _():
            self.part(d, k // group).wait_recv()

        mine = self.p_ref[self.core, r, :].astype(jnp.float32) + self.pin[r, :].astype(jnp.float32)

        @pl.when((z == 0) & (root > 0))
        def _():
            self.out[r, :] = mine.astype(jnp.bfloat16)
            self.up(d, k).start()

        @pl.when((z == n - 1) & (root < n - 1))
        def _():
            self.out[r, :] = mine.astype(jnp.bfloat16)
            self.down(d, k).start()

        @pl.when((z > 0) & (z < root))
        def _():
            self.up(d, k).wait_recv()
            self.out[r, :] = (mine + self.low[r, :].astype(jnp.float32)).astype(jnp.bfloat16)
            self.up(d, k).start()

        @pl.when((z < n - 1) & (z > root))
        def _():
            self.down(d, k).wait_recv()
            self.out[r, :] = (mine + self.high[r, :].astype(jnp.float32)).astype(jnp.bfloat16)
            self.down(d, k).start()

        @pl.when(z == root)
        def _():
            total = mine
            if root > 0:
                self.up(d, k).wait_recv()
                total = total + self.low[r, :].astype(jnp.float32)
            if root < n - 1:
                self.down(d, k).wait_recv()
                total = total + self.high[r, :].astype(jnp.float32)
            self.o_ref[self.core, r, :] = total.astype(jnp.bfloat16)
            if root > 0:
                self.share(d, k, 0).start()
            if root < n - 1:
                self.share(d, k, 1).start()
            self.give(d, k).start()

    def passed(self, d, k):
        z, n, root = self.z, self.n, self.root(d)
        self.share(d, k, 0).wait_recv()

        @pl.when((z < root) & (z > 0))
        def _():
            self.share(d, k, 0).start()

        @pl.when((z > root) & (z < n - 1))
        def _():
            self.share(d, k, 1).start()

        self.give(d, k).start()

    def turn(self, t):
        z, n = self.z, self.n
        for d in range(2):
            root = self.root(d)
            deep = max(root, n - 1 - root)
            below = jnp.where(z < root, z, jnp.where(z > root, n - 1 - z, deep))
            k = t - below * self.lag
            far = jnp.abs(z - root)

            @pl.when((k >= 0) & (k < self.chunks))
            def _():
                self.gathered(d, k)

            b = t - (deep + far) * self.lag

            @pl.when((b >= 0) & (b < self.chunks) & (far > 0))
            def _():
                self.passed(d, b)

    def finish(self):
        z, n, other = self.z, self.n, 1 - self.core
        remote(
            self.p_ref.at[other], self.pin, self.ps.at[0], self.pr.at[0, 0], section=other
        ).wait_send()
        mine = self.o_ref.at[self.core]
        given = remote(mine, mine, self.ts.at[0], self.tr.at[0], section=other)
        given.wait_recv()
        given.wait_send()
        for d in range(2):
            root = self.root(d)
            r = pl.ds(d * self.half, self.half)
            at = self.o_ref.at[self.core, r]

            def summed(head):
                return remote(
                    self.out.at[r], self.low.at[r], self.rs.at[d], self.rl.at[d, 0], head=head
                )

            def shared(side):
                return remote(
                    at, at, self.bs.at[side, d], self.br.at[d, 0], head=z + (1 if side else -1)
                )

            @pl.when(z < root)
            def _():
                summed(z + 1).wait_send()

            @pl.when(z > root)
            def _():
                summed(z - 1).wait_send()

            if root > 0:

                @pl.when((z <= root) & (z > 0))
                def _():
                    shared(0).wait_send()

            if root < n - 1:

                @pl.when((z >= root) & (z < n - 1))
                def _():
                    shared(1).wait_send()


class Gather:
    def __init__(self, layer, srcs, dsts, sems):
        self.layer, self.srcs, self.dsts = layer, srcs, dsts
        self.ss, self.rr, self.ls, self.fs, self.fr = sems
        self.core, self.q = lax.axis_index("section"), lax.axis_index("seq")
        self.n = lax.axis_size("seq")
        self.square = self.n == 4

    @staticmethod
    def scratch(count, n):
        dma = pltpu.SemaphoreType.DMA
        return [dma((count, n, 2)), dma((count, n)), dma((count,)), dma((count, 2)), dma((count, 2))]

    def peer(self, j):
        if not self.square:
            return lax.rem(self.q + j, self.n)
        x, y = self.q % 2, self.q // 2
        x, y = (1 - x if j % 2 else x), (1 - y if j // 2 else y)
        return y * 2 + x

    def direct(self):
        return range(1, 3 if self.square else self.n)

    def copies(self, a):
        for j in self.direct():
            for h in range(2):
                yield remote(
                    self.srcs[a].at[h], self.dsts[a].at[self.q], self.ss.at[a, j, h],
                    self.rr.at[a, self.q], section=h, seq=self.peer(j),
                )
        yield remote(
            self.srcs[a].at[1 - self.layer], self.dsts[a].at[self.q], self.ss.at[a, 0, 0],
            self.rr.at[a, self.q], section=1 - self.layer,
        )

    def local(self, a):
        return pltpu.make_async_copy(
            self.srcs[a].at[self.layer], self.dsts[a].at[self.q], self.ls.at[a]
        )

    def arrival(self, a, s):
        return remote(
            self.srcs[a].at[0], self.dsts[a].at[s], self.ss.at[a, 0, 0], self.rr.at[a, s],
            section=1 - self.core,
        )

    def relay(self, a, i):
        size = self.srcs[a].shape[1] // 2
        at = self.dsts[a].at[self.peer(1 + i), pl.ds(i * size, size)]
        return remote(at, at, self.fs.at[a, i], self.fr.at[a, i], seq=self.peer(2 - i))

    def corner(self, a, i):
        size = self.srcs[a].shape[1] // 2
        at = self.dsts[a].at[self.peer(3), pl.ds(i * size, size)]
        return remote(at, at, self.fs.at[a, i], self.fr.at[a, i], seq=self.peer(2 - i))

    def start(self):
        @pl.when(self.core == self.layer)
        def _():
            for a in range(len(self.srcs)):
                for copy in self.copies(a):
                    copy.start()
                self.local(a).start()

    def due(self):
        sent, turns = 0, []
        for src in self.srcs:
            sent += 2 * src.shape[1] * src.shape[2] * 2
            turns.append(3 + sent // 200_000)
        return turns

    def middle(self, a):
        for j in self.direct():
            self.arrival(a, self.peer(j)).wait_recv()
            if self.square:
                self.relay(a, j - 1).start()

    def finish(self):
        for a in range(len(self.srcs)):
            if self.square:
                for i in range(2):
                    self.corner(a, i).wait_recv()
                    self.relay(a, i).wait_send()

            @pl.when(self.core == self.layer)
            def _():
                self.local(a).wait()
                for copy in self.copies(a):
                    copy.wait_send()

            @pl.when(self.core != self.layer)
            def _():
                self.arrival(a, self.q).wait_recv()


class SmallSum:
    def __init__(self, g_ref, total, spread, scratch):
        self.g_ref, self.total, self.spread = g_ref, total, spread
        self.got, self.src, self.ss, self.sr, self.ts, self.tr = scratch
        self.core, self.q, self.z = (lax.axis_index(a) for a in ("section", "seq", "head"))
        self.n, self.depth = lax.axis_size("seq"), lax.axis_size("head")

    @staticmethod
    def scratch(shape, narrow, n, depth):
        dma = pltpu.SemaphoreType.DMA
        return [
            pltpu.VMEM((n,) + shape, jnp.float32),
            pltpu.VMEM((8, narrow), jnp.float32),
            dma((n,)),
            dma((n,)),
            dma((2 * depth,)),
            dma((2 * depth,)),
        ]

    def first(self, j):
        return remote(
            self.g_ref, self.got.at[self.q], self.ss.at[j], self.sr.at[self.q],
            seq=lax.rem(self.q + j, self.n),
        )

    def others(self):
        for j in range(self.depth):
            for flip in range(2):
                if j or flip:
                    core = 1 - self.core if flip else self.core
                    yield 2 * j + flip, lax.rem(self.z + j, self.depth), core

    def second(self, i, z, core):
        slot = self.z * 2 + self.core
        return remote(
            self.src, self.spread.at[slot], self.ts.at[i], self.tr.at[slot], head=z, section=core
        )

    def start(self):
        for j in range(1, self.n):
            self.first(j).start()
        self.got[self.q] = self.g_ref[...]

    def middle(self):
        for j in range(1, self.n):
            s = lax.rem(self.q + j, self.n)
            remote(
                self.g_ref, self.got.at[s], self.ss.at[j], self.sr.at[s], seq=s
            ).wait_recv()
        summed = self.got[0]
        for s in range(1, self.n):
            summed = summed + self.got[s]
        self.total[...] = summed[:8]
        own = summed[8:, : self.src.shape[1]]
        self.src[...] = own
        self.spread[self.z * 2 + self.core] = own
        for i, z, core in self.others():
            self.second(i, z, core).start()

    def finish(self):
        for i, z, core in self.others():
            slot = z * 2 + core
            remote(
                self.src, self.spread.at[slot], self.ts.at[i], self.tr.at[slot], head=z, section=core
            ).wait_recv()
            self.second(i, z, core).wait_send()
        for j in range(1, self.n):
            self.first(j).wait_send()


class Scatter:
    def __init__(self, layer, srcs, dsts, sems):
        self.layer, self.srcs, self.dsts = layer, srcs, dsts
        self.ss, self.rr, self.ls = sems
        self.core, self.q = lax.axis_index("section"), lax.axis_index("seq")
        self.n = lax.axis_size("seq")

    @staticmethod
    def scratch(count, n):
        return [
            pltpu.SemaphoreType.DMA((count, n)),
            pltpu.SemaphoreType.DMA((count, 2, n)),
            pltpu.SemaphoreType.DMA((count,)),
        ]

    def copies(self, a):
        for j in range(1, self.n):
            t = lax.rem(self.q + j, self.n)
            yield remote(
                self.srcs[a].at[t], self.dsts[a].at[self.core, self.q], self.ss.at[a, j],
                self.rr.at[a, self.core, self.q], section=self.layer, seq=t,
            )

    def near(self, a):
        return remote(
            self.srcs[a].at[self.q], self.dsts[a].at[self.core, self.q], self.ss.at[a, 0],
            self.rr.at[a, self.core, self.q], section=self.layer,
        )

    def local(self, a):
        return pltpu.make_async_copy(
            self.srcs[a].at[self.q], self.dsts[a].at[self.core, self.q], self.ls.at[a]
        )

    def arrival(self, a, h, s):
        return remote(
            self.srcs[a].at[self.q], self.dsts[a].at[h, s], self.ss.at[a, 0], self.rr.at[a, h, s],
            section=1 - self.core,
        )

    def start(self):
        for a in range(len(self.srcs)):
            for copy in self.copies(a):
                copy.start()

            @pl.when(self.core == self.layer)
            def _():
                self.local(a).start()

            @pl.when(self.core != self.layer)
            def _():
                self.near(a).start()

    def finish(self):
        for a in range(len(self.srcs)):

            @pl.when(self.core == self.layer)
            def _():
                for j in range(1, self.n):
                    for h in range(2):
                        self.arrival(a, h, lax.rem(self.q + j, self.n)).wait_recv()
                self.arrival(a, 1 - self.layer, self.q).wait_recv()
                self.local(a).wait()

            @pl.when(self.core != self.layer)
            def _():
                self.near(a).wait_send()

            for copy in self.copies(a):
                copy.wait_send()


TILE = 256


class Product:
    def __init__(self, lhs, rhs, out, scratch):
        self.lhs, self.rhs, self.out = lhs, rhs, out
        self.left, self.right, self.stage, self.loads, self.stores = scratch
        self.tiles = lhs.shape[1] // TILE

    @staticmethod
    def scratch(lhs, rhs):
        return [
            pltpu.VMEM(lhs.shape, jnp.bfloat16),
            pltpu.VMEM(rhs.shape, jnp.bfloat16),
            pltpu.VMEM((2, TILE, rhs.shape[1]), jnp.bfloat16),
            pltpu.SemaphoreType.DMA((2,)),
            pltpu.SemaphoreType.DMA((2,)),
        ]

    def load(self, side):
        src, dst = ((self.lhs, self.left), (self.rhs, self.right))[side]
        return pltpu.make_async_copy(src, dst, self.loads.at[side])

    def store(self, i):
        at = pl.ds(pl.multiple_of(i * TILE, TILE), TILE)
        return pltpu.make_async_copy(self.stage.at[i % 2], self.out.at[at], self.stores.at[i % 2])

    def start(self):
        self.load(0).start()
        self.load(1).start()

    def step(self, i):
        @pl.when(i == 0)
        def _():
            self.load(0).wait()
            self.load(1).wait()

        @pl.when(i >= 2)
        def _():
            self.store(i - 2).wait()

        at = pl.ds(pl.multiple_of(i * TILE, TILE), TILE)
        self.stage[i % 2] = lax.dot_general(
            self.left[:, at],
            self.right[...],
            (((0,), (0,)), ((), ())),
            preferred_element_type=jnp.float32,
        ).astype(jnp.bfloat16)
        self.store(i).start()

    def finish(self):
        for i in range(max(self.tiles - 2, 0), self.tiles):
            self.store(i).wait()


def comm_kernel(plan, *refs):
    has_sum, layer_in, count_in, layer_out, count_out, kept, count_made, small_in, chunks, lag = plan
    refs = list(refs)

    def take(count):
        taken = refs[:count]
        del refs[:count]
        return taken

    p_in, w_in, g_in, _, m_in, s_in = (
        take(has_sum), take(count_in), take(count_out), take(kept), take(2 * count_made),
        take(small_in),
    )
    p_out, w_out, g_out, m_out, s_out = (
        take(has_sum), take(count_in), take(count_out), take(count_made), take(2 * small_in)
    )
    greet(has_sum, count_in + count_out > 0, small_in)
    jobs = []
    later = []
    if has_sum:
        line = LineSum(p_in[0], p_out[0], take(13), chunks, lag)
        line.start()
    if count_in:
        weights = Gather(layer_in, w_in, w_out, take(5))
        jobs.append(weights)
        for a, turn in enumerate(weights.due()):
            later.append((turn, functools.partial(weights.middle, a)))
    if count_out:
        jobs.append(Scatter(layer_out, g_in, g_out, take(3)))
    made = [
        Product(m_in[2 * i], m_in[2 * i + 1], m_out[i], take(5)) for i in range(count_made)
    ]
    if small_in:
        small = SmallSum(s_in[0], s_out[0], s_out[1], take(6))
        jobs.insert(0, small)
        later.append((12, small.middle))
    for job in made + jobs:
        job.start()
    if has_sum:
        tiles = sum(product.tiles for product in made)

        def turn(t, carry):
            line.turn(t)
            i = t - 2
            for product in made:

                @pl.when((i >= 0) & (i < product.tiles))
                def _(product=product, i=i):
                    product.step(i)

                i = i - product.tiles
            for when, act in later:

                @pl.when(t == when)
                def _(act=act):
                    act()

            return carry

        last = max([line.turns, tiles + 2] + [when + 1 for when, _ in later])
        lax.fori_loop(0, last, turn, 0)
        line.finish()
    else:
        for _, act in later:
            act()
    for job in made + jobs:
        job.finish()


def communicate(
    cid, partial=None, gather=None, scatter=None, into=(), products=(), small=None, chunks=16, lag=2
):
    n = lax.axis_size("seq")
    layer_in, w_in = gather if gather else (0, [])
    layer_out, g_in = scatter if scatter else (0, [])
    p_in = [] if partial is None else [partial]
    m_in = [a for pair in products for a in pair]
    vmem, anywhere = pl.BlockSpec(memory_space=pltpu.VMEM), pl.BlockSpec(memory_space=pl.ANY)
    scratch = []
    if p_in:
        scratch += LineSum.scratch(partial.shape[1], partial.shape[2], chunks)
    if w_in:
        scratch += Gather.scratch(len(w_in), n)
    if g_in:
        scratch += Scatter.scratch(len(g_in), n)
    for pair in products:
        scratch += Product.scratch(*pair)
    s_in, s_shapes = [], []
    if small is not None:
        s_in, narrow, depth = [small[0]], small[1], lax.axis_size("head")
        scratch += SmallSum.scratch(small[0].shape, narrow, n, depth)
        s_shapes = [
            jax.ShapeDtypeStruct((8, small[0].shape[1]), jnp.float32),
            jax.ShapeDtypeStruct((2 * depth, 8, narrow), jnp.float32),
        ]
    shapes = (
        [jax.ShapeDtypeStruct(p.shape, jnp.bfloat16) for p in p_in]
        + [jax.ShapeDtypeStruct((n,) + w.shape[1:], jnp.bfloat16) for w in w_in]
        + [jax.ShapeDtypeStruct((2,) + g.shape, jnp.bfloat16) for g in g_in]
        + [jax.ShapeDtypeStruct((a.shape[1], b.shape[1]), jnp.bfloat16) for a, b in products]
        + s_shapes
    )
    plan = (
        len(p_in), layer_in, len(w_in), layer_out, len(g_in), len(into), len(products), len(s_in),
        chunks, lag,
    )
    first = len(p_in) + len(w_in)
    outs = pl.pallas_call(
        functools.partial(comm_kernel, plan),
        out_shape=shapes,
        in_specs=[vmem] * first
        + [anywhere] * (len(g_in) + len(into) + len(m_in))
        + [vmem] * len(s_in),
        out_specs=[vmem] * len(p_in)
        + [anywhere] * (len(w_in) + len(g_in) + len(products))
        + [vmem] * len(s_shapes),
        scratch_shapes=scratch,
        input_output_aliases={first + len(g_in) + i: first + i for i in range(len(into))},
        name=f"comm{cid}",
        compiler_params=pltpu.CompilerParams(
            collective_id=cid, has_side_effects=True, vmem_limit_bytes=52 << 20
        ),
    )(*p_in, *w_in, *g_in, *into, *m_in, *s_in)
    return (
        outs[0] if p_in else None,
        [a.reshape((-1,) + a.shape[2:]) for a in outs[len(p_in) : first]],
        outs[first : first + len(g_in)],
        outs[first + len(g_in) :],
    )


def rms_norm(vector, scale_gain):
    return (
        vector * lax.rsqrt(jnp.mean(vector * vector, axis=-1, keepdims=True) + epsilon) * scale_gain
    )


def seq_begin(lengths_row, positions):
    seq_starts = jnp.cumsum(lengths_row) - lengths_row
    chosen = jnp.where(seq_starts[None, :] <= positions[:, None], seq_starts[None, :], 0)
    return jnp.max(chosen, axis=1)


HEADS = 2
PAIRS = FK * (FK + 1) // 2
STATE = 160
BLOCK = 128


def feature_tables(values):
    wide = values + HEADS * FK
    first = np.zeros((HEADS, wide, wide), np.float32)
    second = np.zeros((HEADS, wide, wide), np.float32)
    rest = np.zeros((8, wide), np.float32)
    for h in range(HEADS):
        at = values + h * FK
        lane = 0
        for a in range(FK):
            for b in range(a, FK):
                first[h, at + a, lane] = 1
                second[h, at + b, lane] = 1
                rest[2, lane] = 0.25 if a < b else 1 / (4.0 * math.sqrt(2.0))
                lane += 1
        for a in range(FK):
            first[h, at + a, lane] = 1
            rest[1, lane] = 1
            rest[2, lane] = 0.5
            lane += 1
        rest[0, lane] = rest[1, lane] = rest[2, lane] = 1
    return np.stack([first, second], axis=1), rest


def mm(a, b):
    return lax.dot_general(a, b, (((1,), (0,)), ((), ())), preferred_element_type=jnp.float32)


def mm_nt(a, b):
    return lax.dot_general(a, b, (((1,), (1,)), ((), ())), preferred_element_type=jnp.float32)


def mm_tn(a, b):
    return lax.dot_general(a, b, (((0,), (0,)), ((), ())), preferred_element_type=jnp.float32)


class Lanes:
    def __init__(self, wide, values):
        self.values = values
        self.lane = lax.broadcasted_iota(jnp.int32, (1, wide), 1)
        lane, dim = self.lane, values // HEADS
        self.is_value = lane < values
        self.is_one = (lane >= values) & (lane < values + 2 * HEADS)
        self.head = jnp.where(
            self.is_value, jnp.where(lane < dim, 0, 1), jnp.where(self.is_one, (lane - values) % 2, 9)
        )

    def of(self, h, x):
        return jnp.where(self.head == h, x, jnp.zeros_like(x))

    def key(self, h, x):
        at = self.values + h * FK
        return jnp.where((self.lane >= at) & (self.lane < at + FK), x, jnp.zeros_like(x))

    def extended(self, a):
        return jnp.where(
            self.is_value, a, jnp.where(self.is_one, jnp.ones_like(a), jnp.zeros_like(a))
        )

    def column(self, x, index):
        return jnp.sum(
            jnp.where(self.lane == self.values + index, x, 0.0), axis=1, keepdims=True
        )

    def denominator(self, x):
        return jnp.where(
            self.lane < self.values // HEADS, self.column(x, 0), self.column(x, 1)
        )


def meet(direction, reach):
    q, n = lax.axis_index("seq"), lax.axis_size("seq")
    barrier = pltpu.get_barrier_semaphore()
    count = 0
    for d in range(1, reach + 1):
        source = q - direction * d
        target = q + direction * d

        @pl.when((source >= 0) & (source < n))
        def _():
            pl.semaphore_signal(barrier, inc=1, device_id={"seq": source}, device_id_type=MESH)

        count = count + jnp.where((target >= 0) & (target < n), 1, 0)

    @pl.when(count > 0)
    def _():
        pl.semaphore_wait(barrier, count)


class Pass:
    def __init__(self, direction, reach, src, dst, send, recv):
        self.direction, self.reach = direction, reach
        self.src, self.dst, self.send, self.recv = src, dst, send, recv
        self.q, self.n = lax.axis_index("seq"), lax.axis_size("seq")

    def has_source(self, d):
        at = self.q - self.direction * d
        return (at >= 0) & (at < self.n)

    def has_target(self, d):
        at = self.q + self.direction * d
        return (at >= 0) & (at < self.n)

    def copy(self, d):
        return remote(
            self.src, self.dst.at[d - 1], self.send.at[d - 1], self.recv.at[d - 1],
            seq=self.q + self.direction * d,
        )

    def start(self):
        for d in range(1, self.reach + 1):

            @pl.when(self.has_target(d))
            def _():
                self.copy(d).start()

    def arrived(self):
        for d in range(1, self.reach + 1):

            @pl.when(self.has_source(d))
            def _():
                self.copy(d).wait_recv()

    def sent(self):
        for d in range(1, self.reach + 1):

            @pl.when(self.has_target(d))
            def _():
                self.copy(d).wait_send()


def sum_states(states, coef, total):
    for m in range(2):
        total[m] = jnp.zeros(total.shape[1:], total.dtype)
        for d in range(1, states.reach + 1):

            @pl.when(states.has_source(d))
            def _():
                total[m, :STATE, :] += coef[d - 1, m] * states.dst[d - 1, m].astype(jnp.float32)


def shifted(a, tail, fresh, by):
    row = lax.broadcasted_iota(jnp.int32, (a.shape[0], 1), 0)
    moved = pltpu.roll(a, by, 0)
    rows = tail.shape[0]
    for r in range(by):
        edge = jnp.where(fresh, tail[rows - by + r : rows - by + r + 1, :], 0.0)
        moved = jnp.where(row == r, edge, moved)
    return moved


def attn_forward_kernel(
    reach, proj, col, row, coef, e, c, taps, gated, att, conv, sin, edge, acc, phi, s_acc, s_src,
    s_all, s_sum, e_src, ss, sr, es, er,
):
    q = lax.axis_index("seq")
    rows, wide = proj.shape[1], proj.shape[2] // 2
    values = wide - HEADS * FK
    lanes = Lanes(wide, values)
    meet(1, reach)
    states = Pass(1, reach, s_src, s_all, ss, sr)
    edges = Pass(1, 1, e_src, edge, es, er)

    def sides(m):
        return proj[m, :, :wide].astype(jnp.bfloat16), proj[m, :, wide:].astype(jnp.bfloat16)

    def phi_of(a, h):
        return (mm(a, e[h, 0]) + c[0:1, :]) * (mm(a, e[h, 1]) + c[1:2, :]) * c[2:3, :]

    def make_state(i, carry):
        m, h = i // HEADS, i % HEADS
        a, b = sides(m)
        phi[m, h] = (phi_of(a, h) * col[m, :, 1:2]).astype(jnp.bfloat16)
        keyed = (phi_of(b, h) * col[m, :, 2:3]).astype(jnp.bfloat16)
        part = mm_tn(keyed, lanes.of(h, lanes.extended(a)))

        @pl.when(h == 0)
        def _():
            s_acc[m] = part

        @pl.when(h > 0)
        def _():
            s_acc[m] += part

        return carry

    lax.fori_loop(0, 2 * HEADS, make_state, 0)
    for m in range(2):
        s_src[m] = s_acc[m, :STATE, :].astype(jnp.bfloat16)
    states.start()

    def make_block(i, carry):
        m, h = i // HEADS, i % HEADS
        a, b = sides(m)
        asked = lanes.key(h, a)
        valued = lanes.of(h, lanes.extended(a))
        for r in range(rows // BLOCK):
            lo, hi = r * BLOCK, (r + 1) * BLOCK
            x = mm_nt(asked[lo:hi], b[:hi]) * 0.25
            seen = (col[m, lo:hi, 0:1] == row[m, 0:1, :hi]) & (
                lax.broadcasted_iota(jnp.int32, (BLOCK, hi), 1)
                <= lo + lax.broadcasted_iota(jnp.int32, (BLOCK, hi), 0)
            )
            w = jnp.where(seen, 1.0 + x + 0.5 * x * x, 0.0).astype(jnp.bfloat16)
            part = mm(w, valued[:hi])

            @pl.when(h == 0)
            def _():
                acc[m, lo:hi, :] = part

            @pl.when(h > 0)
            def _():
                acc[m, lo:hi, :] += part

        return carry

    lax.fori_loop(0, 2 * HEADS, make_block, 0)
    states.arrived()
    sum_states(states, coef, s_sum)

    def attend(m, lo):
        s = s_sum[m].astype(jnp.bfloat16)
        both = acc[m, lo:, :]
        for h in range(HEADS):
            both = both + mm(phi[m, h, lo:, :], lanes.of(h, s))
        return jnp.where(lanes.is_value, both / lanes.denominator(both), both)

    for m in range(2):
        sin[m] = s_sum[m, :STATE, :].astype(jnp.bfloat16)
        e_src[m] = attend(m, rows - 16)
    edges.start()
    for m in range(2):
        att[m] = attend(m, 0)
    edges.arrived()
    for m in range(2):
        a = att[m]
        tail = edge[0, m]
        out = taps[0:1, :] * a
        for by in (1, 2):
            out = out + taps[by : by + 1, :] * shifted(a, tail, q > 0, by) * col[m, :, 2 + by : 3 + by]
        conv[m] = out
        gated[m] = (out * proj[m, :, wide:]).astype(jnp.bfloat16)
    states.sent()
    edges.sent()


def attn_backward_kernel(
    reach, bg, proj, att, conv, sin, edge, col, row, coef, late, e, c, taps, out, grad_taps,
    phi_q, phi_k, near, acc_a, acc_b, s_acc, s_src, s_all, s_sum, e_src, e_dst, ss, sr, es, er,
):
    q, n = lax.axis_index("seq"), lax.axis_size("seq")
    rows, wide = proj.shape[1], proj.shape[2] // 2
    values = wide - HEADS * FK
    lanes = Lanes(wide, values)
    meet(-1, reach)
    states = Pass(-1, reach, s_src, s_all, ss, sr)
    edges = Pass(-1, 1, e_src, e_dst, es, er)
    for m in range(2):
        e_src[m] = bg[m, :16, :] * proj[m, :16, wide:]
    edges.start()

    def sides(m):
        return proj[m, :, :wide].astype(jnp.bfloat16), proj[m, :, wide:].astype(jnp.bfloat16)

    def factors(a, h):
        return mm(a, e[h, 0]) + c[0:1, :], mm(a, e[h, 1]) + c[1:2, :]

    def make_phi(i, carry):
        m, h = i // HEADS, i % HEADS
        a, b = sides(m)
        u, w = factors(a, h)
        phi_q[m, h] = (u * w * c[2:3, :] * col[m, :, 1:2]).astype(jnp.bfloat16)
        u, w = factors(b, h)
        phi_k[m, h] = (u * w * c[2:3, :] * col[m, :, 2:3]).astype(jnp.bfloat16)
        return carry

    lax.fori_loop(0, 2 * HEADS, make_phi, 0)
    edges.arrived()
    sums = [jnp.zeros((1, wide), jnp.float32)] * KW
    place = lax.broadcasted_iota(jnp.int32, (rows, 1), 0)
    for m in range(2):
        back = bg[m]
        back_conv = back * proj[m, :, wide:]
        a = jnp.where(lanes.is_value, att[m], 0.0)
        tail = edge[0, m]
        nxt = e_dst[0, m]
        total = taps[0:1, :] * back_conv
        sums[0] = sums[0] + jnp.sum(back_conv * a, axis=0, keepdims=True)
        for by in (1, 2):
            kept = back_conv * col[m, :, 2 + by : 3 + by]
            sums[by] = sums[by] + jnp.sum(
                kept * shifted(a, tail, q > 0, by), axis=0, keepdims=True
            )
            moved = pltpu.roll(kept, rows - by, 0)
            for r in range(by):
                fresh = jnp.where(q < n - 1, nxt[r : r + 1, :] * late[by - 1 + r, m], 0.0)
                moved = jnp.where(place == rows - by + r, fresh, moved)
            total = total + taps[by : by + 1, :] * moved
        out[m, :, wide:] = jnp.where(lanes.is_value, back * conv[m], 0.0).astype(jnp.bfloat16)
        back_numer = total / lanes.denominator(att[m])
        spent = back_numer * a
        found = jnp.where(lanes.is_value, back_numer, 0.0)
        for h in range(HEADS):
            denom = -jnp.sum(lanes.of(h, spent), axis=1, keepdims=True)
            high = denom.astype(jnp.bfloat16).astype(jnp.float32)
            found = jnp.where(lanes.lane == values + h, high, found)
            found = jnp.where(lanes.lane == values + 2 + h, denom - high, found)
        near[m] = found.astype(jnp.bfloat16)
        part = jnp.zeros((wide, wide), jnp.float32)
        for h in range(HEADS):
            part = part + mm_tn(phi_q[m, h], lanes.of(h, near[m]))
        s_src[m] = part[:STATE].astype(jnp.bfloat16)
    states.start()
    grad_taps[...] = jnp.zeros(grad_taps.shape, jnp.float32)
    for by in range(KW):
        grad_taps[by : by + 1, :] = sums[by]
    acc_a[...] = jnp.zeros(acc_a.shape, jnp.float32)
    acc_b[...] = jnp.zeros(acc_b.shape, jnp.float32)
    for m in range(2):
        s_sum[m] = jnp.zeros(s_sum.shape[1:], jnp.float32)
        s_sum[m, :STATE, :] = sin[m].astype(jnp.float32)

    def through_phi(scaled, factors_of, h):
        u, w = factors_of
        return mm_nt((scaled * w).astype(jnp.bfloat16), e[h, 0]) + mm_nt(
            (scaled * u).astype(jnp.bfloat16), e[h, 1]
        )

    def make_block(i, carry):
        m, h = i // HEADS, i % HEADS
        a, b = sides(m)
        asked, keyed = lanes.key(h, a), lanes.key(h, b)
        valued = lanes.extended(a)
        given = lanes.of(h, near[m])
        given_v = jnp.where(lanes.is_value, given, jnp.zeros_like(given))
        for r in range(rows // BLOCK):
            lo, hi = r * BLOCK, (r + 1) * BLOCK
            x = mm_nt(asked[lo:hi], b[:hi]) * 0.25
            seen = (col[m, lo:hi, 0:1] == row[m, 0:1, :hi]) & (
                lax.broadcasted_iota(jnp.int32, (BLOCK, hi), 1)
                <= lo + lax.broadcasted_iota(jnp.int32, (BLOCK, hi), 0)
            )
            w = jnp.where(seen, 1.0 + x + 0.5 * x * x, 0.0).astype(jnp.bfloat16)
            back_w = mm_nt(given[lo:hi], valued[:hi])
            back_s = jnp.where(seen, back_w * (1.0 + x), 0.0).astype(jnp.bfloat16)
            acc_a[m, lo:hi, :] += 0.25 * mm(back_s, keyed[:hi])
            acc_b[m, :hi, :] += 0.25 * mm_tn(back_s, asked[lo:hi])
            acc_a[m, :hi, :] += mm_tn(w, given_v[lo:hi])
        s = s_sum[m].astype(jnp.bfloat16)
        scaled = mm_nt(given, s) * col[m, :, 1:2] * c[2:3, :]
        acc_a[m] += through_phi(scaled, factors(a, h), h)
        return carry

    lax.fori_loop(0, 2 * HEADS, make_block, 0)
    states.arrived()
    sum_states(states, coef, s_sum)

    def make_late(i, carry):
        m, h = i // HEADS, i % HEADS
        a, b = sides(m)
        s = s_sum[m].astype(jnp.bfloat16)
        scaled = mm_nt(lanes.of(h, lanes.extended(a)), s) * col[m, :, 2:3] * c[2:3, :]
        acc_b[m] += through_phi(scaled, factors(b, h), h)
        s_v = lanes.of(h, jnp.where(lanes.is_value, s, jnp.zeros_like(s)))
        acc_a[m] += mm(phi_k[m, h], s_v)
        return carry

    lax.fori_loop(0, 2 * HEADS, make_late, 0)
    for m in range(2):
        out[m, :, :wide] = acc_a[m].astype(jnp.bfloat16)
        out[m, :, wide:] = jnp.where(
            lanes.is_value, out[m, :, wide:].astype(jnp.float32), acc_b[m]
        ).astype(jnp.bfloat16)
    states.sent()
    edges.sent()


def seq_reach():
    n = lax.axis_size("seq")
    return n // 2 if n % 2 == 0 else n - 1


def attention_call(kernel, cid, inputs, scalars, shapes, scratch):
    vmem, smem = pl.BlockSpec(memory_space=pltpu.VMEM), pl.BlockSpec(memory_space=pltpu.SMEM)
    return pl.pallas_call(
        functools.partial(kernel, seq_reach()),
        out_shape=shapes,
        in_specs=[smem if i in scalars else vmem for i in range(len(inputs))],
        out_specs=[vmem] * len(shapes),
        scratch_shapes=scratch,
        name=f"attention{cid}",
        compiler_params=pltpu.CompilerParams(
            collective_id=cid, has_side_effects=True, vmem_limit_bytes=48 << 20
        ),
    )(*inputs)


def passing(reach, wide):
    dma = pltpu.SemaphoreType.DMA
    return (
        [
            pltpu.VMEM((2, STATE, wide), jnp.bfloat16),
            pltpu.VMEM((reach, 2, STATE, wide), jnp.bfloat16),
            pltpu.VMEM((2, wide, wide), jnp.float32),
        ],
        [dma((reach,)), dma((reach,)), dma((1,)), dma((1,))],
    )


def attention_forward(proj, taps, marks, tables):
    m, rows, double = proj.shape
    wide = double // 2
    f32, bf16 = jnp.float32, jnp.bfloat16
    buffers, sems = passing(seq_reach(), wide)
    shape = jax.ShapeDtypeStruct
    return attention_call(
        attn_forward_kernel,
        10,
        [proj, marks["col"], marks["row"], marks["before"], *tables, taps],
        (3,),
        [
            shape((m, rows, wide), bf16),
            shape((m, rows, wide), f32),
            shape((m, rows, wide), f32),
            shape((m, STATE, wide), bf16),
            shape((1, m, 16, wide), f32),
        ],
        [
            pltpu.VMEM((m, rows, wide), f32),
            pltpu.VMEM((m, HEADS, rows, wide), bf16),
            pltpu.VMEM((m, wide, wide), f32),
            *buffers,
            pltpu.VMEM((m, 16, wide), f32),
            *sems,
        ],
    )


def attention_backward(back_gated, proj, kept, taps, marks, tables):
    att, conv, sin, edge = kept
    m, rows, double = proj.shape
    wide = double // 2
    f32, bf16 = jnp.float32, jnp.bfloat16
    buffers, sems = passing(seq_reach(), wide)
    shape = jax.ShapeDtypeStruct
    return attention_call(
        attn_backward_kernel,
        11,
        [
            back_gated, proj, att, conv, sin, edge, marks["col"], marks["row"], marks["after"],
            marks["late"], *tables, taps,
        ],
        (8, 9),
        [shape((m, rows, double), bf16), shape((8, wide), f32)],
        [
            pltpu.VMEM((m, HEADS, rows, wide), bf16),
            pltpu.VMEM((m, HEADS, rows, wide), bf16),
            pltpu.VMEM((m, rows, wide), bf16),
            pltpu.VMEM((m, rows, wide), f32),
            pltpu.VMEM((m, rows, wide), f32),
            pltpu.VMEM((m, wide, wide), f32),
            *buffers,
            pltpu.VMEM((m, 16, wide), f32),
            pltpu.VMEM((1, m, 16, wide), f32),
            *sems,
        ],
    )


def sequence_marks(lengths, rows):
    count, mine = lax.axis_size("seq"), lax.axis_index("seq")
    start = mine * rows
    positions = start + jnp.arange(rows + 2, dtype=jnp.int32)
    begin_ext = jax.vmap(lambda row: seq_begin(row, positions))(lengths)
    begin = begin_ext[:, :rows]
    ends = (jnp.arange(count, dtype=jnp.int32) + 1) * rows - 1
    stays = jax.vmap(lambda row: seq_begin(row, ends))(lengths) < (ends - rows + 1)[None, :]
    stays = stays.astype(jnp.float32)
    blocks = jnp.arange(count, dtype=jnp.int32)

    def through(first, last):
        inside = (blocks >= first) & (blocks <= last)
        return jnp.min(jnp.where(inside[None, :], stays, 1.0), axis=1)

    reach = seq_reach()
    before = [through(mine - d + 1, mine - 1) for d in range(1, reach + 1)]
    after = [through(mine + 1, mine + d - 1) for d in range(1, reach + 1)]
    allowed = [(positions - j >= begin_ext).astype(jnp.float32) for j in range(KW)]
    columns = [
        begin.astype(jnp.float32),
        (begin < start).astype(jnp.float32),
        (begin == begin[:, rows - 1 :]).astype(jnp.float32),
        allowed[1][:, :rows],
        allowed[2][:, :rows],
    ]
    col = jnp.stack(columns + [jnp.zeros_like(columns[0])] * 3, axis=2)
    return {
        "col": col,
        "row": jnp.broadcast_to(columns[0][:, None, :], (2, 8, rows)),
        "before": jnp.stack(before),
        "after": jnp.stack(after),
        "late": jnp.stack([allowed[1][:, rows], allowed[2][:, rows], allowed[2][:, rows + 1]]),
    }


def by_seq(grad):
    n = lax.axis_size("seq")
    return grad.reshape((n, grad.shape[0] // n) + grad.shape[1:])


def dot_t(a, b):
    return jnp.einsum("tc,dc->td", a, b, preferred_element_type=jnp.float32)


def dot_n(a, b):
    return jnp.dot(a, b, preferred_element_type=jnp.float32)


def on_device(
    tokens,
    lengths,
    gain_attn,
    w_query,
    w_key,
    w_value,
    w_gate_conv,
    conv_taps,
    w_out,
    gain_ffn,
    w_gate,
    w_up,
    w_down,
    cotangent,
):
    head_index = lax.axis_index("head")
    core = lax.axis_index("section")
    micro_count, rows, width = tokens.shape
    total = micro_count * rows

    def halves(weight):
        cols = weight.shape[1] // 2
        return jnp.stack([weight[:, :cols], weight[:, cols:]])

    own_mix = jnp.concatenate(
        [halves(w[0]) for w in (w_value, w_query, w_gate_conv, w_key)], axis=2
    )
    values = w_value.shape[2] // 2
    keys = w_query.shape[2] // 2
    wide = values + keys
    own_out = jnp.pad(halves(w_out[0].T), ((0, 0), (0, 0), (0, keys)))
    own_ffn = jnp.concatenate([halves(w_gate[0]), halves(w_up[0])], axis=2)
    own_down = halves(w_down[0].T)
    gains_one = lax.all_gather(gain_attn[0], "section").astype(jnp.float32)
    gains_two = lax.all_gather(gain_ffn[0], "section").astype(jnp.float32)
    taps_all = lax.all_gather(conv_taps[0], "section").astype(jnp.float32)
    taps_both = lax.dynamic_slice_in_dim(taps_all, (head_index * 2 + core) * values, values, 2)
    taps_both = jnp.pad(taps_both, ((0, 0), (0, 8 - KW), (0, keys)))
    first, rest = feature_tables(values)
    tables = (jnp.asarray(first, jnp.bfloat16), jnp.asarray(rest))
    marks = sequence_marks(lengths, rows)
    hidden_cols = own_down.shape[2]

    def as_parts(flat):
        return flat.astype(jnp.bfloat16).reshape(micro_count, rows, width)

    def spread(summed):
        return summed.astype(jnp.float32).reshape(total, width)

    _, (mix_0, out_0), _, _ = communicate(1, gather=(0, [own_mix, own_out]))
    w_mix, w_o, w_gu, w_d = [mix_0, None], [out_0, None], [None, None], [None, None]
    x = tokens.reshape(total, width).astype(jnp.float32)
    kept = [None, None]
    outputs = []
    last_partial = None
    for layer in range(2):
        normed = rms_norm(x, gains_one[layer]).astype(jnp.bfloat16)
        proj = dot_n(normed, w_mix[layer]).reshape(micro_count, rows, 2 * wide)
        gated, *attn = attention_forward(proj, taps_both[layer], marks, tables)
        gated = gated.reshape(total, wide)
        partial = as_parts(dot_t(gated, w_o[layer]))
        if layer == 0:
            summed, (w_gu[0], w_d[0]), _, _ = communicate(
                2, partial=partial, gather=(0, [own_ffn, own_down])
            )
        else:
            summed, (w_gu[1],), _, _ = communicate(3, partial=partial, gather=(1, [own_ffn]))
        middle = x + spread(summed)
        normed_two = rms_norm(middle, gains_two[layer]).astype(jnp.bfloat16)
        both = dot_n(normed_two, w_gu[layer])
        hidden = (jax.nn.silu(both[:, :hidden_cols]) * both[:, hidden_cols:]).astype(jnp.bfloat16)
        partial = as_parts(dot_t(hidden, w_d[layer]))
        kept[layer] = (x, normed, proj, gated, attn, middle, normed_two, both, hidden)
        if layer == 0:
            summed, (w_mix[1], w_o[1], w_d[1]), _, _ = communicate(
                4, partial=partial, gather=(1, [own_mix, own_out, own_down])
            )
            outputs.append((middle + spread(summed)).astype(jnp.bfloat16))
            x = outputs[0].astype(jnp.float32)
        else:
            last_partial = partial

    grad = cotangent.reshape(total, width)
    back = [None, None]
    smalls = [None, None]
    made = []
    into = [None] * 4
    for layer in (1, 0):
        x, normed, proj, gated, attn, middle, normed_two, both, hidden = kept[layer]
        grad_wide = grad.astype(jnp.float32)
        back_hidden = dot_n(grad, w_d[layer])
        gate_pre, upward = both[:, :hidden_cols], both[:, hidden_cols:]
        silu_value, silu_back = jax.vjp(jax.nn.silu, gate_pre)
        back_both = jnp.concatenate(
            [
                silu_back(back_hidden * upward)[0].astype(jnp.bfloat16),
                (back_hidden * silu_value).astype(jnp.bfloat16),
            ],
            axis=1,
        )
        partial = as_parts(dot_t(back_both, w_gu[layer]))
        products = ((normed_two, back_both), (grad, hidden))
        if layer == 1:
            summed, _, _, (grad_gu, grad_d) = communicate(5, partial=partial, products=products)
        else:
            summed, _, into[1:], (grad_gu, grad_d) = communicate(
                6, partial=partial, scatter=(1, made), products=products
            )
        _, norm_back_two = jax.vjp(rms_norm, middle, gains_two[layer])
        back_middle, gain_two = norm_back_two(spread(summed))
        back_middle = grad_wide + back_middle
        back_branch = back_middle.astype(jnp.bfloat16)
        back_gated = dot_n(back_branch, w_o[layer])
        back_proj, taps_grad = attention_backward(
            back_gated.reshape(micro_count, rows, wide), proj, attn, taps_both[layer], marks, tables
        )
        back_proj = back_proj.reshape(total, 2 * wide)
        partial = as_parts(dot_t(back_proj, w_mix[layer]))
        summed, _, into[:1], (grad_mix, grad_o) = communicate(
            7 + layer,
            partial=partial,
            scatter=(layer, [by_seq(grad_gu)]),
            into=into[:1] if layer == 0 else (),
            products=((normed, back_proj), (back_branch, gated)),
        )
        made = [by_seq(grad_d), by_seq(grad_mix), by_seq(grad_o)]
        _, norm_back_one = jax.vjp(rms_norm, x, gains_one[layer])
        back_x, gain_one = norm_back_one(spread(summed))
        grad = (back_middle + back_x).astype(jnp.bfloat16)
        back[layer] = grad
        smalls[layer] = (gain_one, gain_two, taps_grad)
    gains = jnp.stack([smalls[0][0], smalls[1][0], smalls[0][1], smalls[1][1]])
    taps_rows = jnp.concatenate([smalls[0][2][:KW], smalls[1][2][:KW]])
    packed = jnp.concatenate(
        [
            jnp.pad(gains, ((0, 4), (0, 0))),
            jnp.pad(taps_rows, ((0, 8 - 2 * KW), (0, width - wide))),
        ]
    )
    summed, _, into[1:], (gains, taps_rows) = communicate(
        9, partial=last_partial, scatter=(0, made), into=into[1:], small=(packed, wide)
    )
    outputs.append((kept[1][5] + spread(summed)).astype(jnp.bfloat16))
    grad_gu, grad_d, grad_mix, grad_o = [
        jnp.sum(received.astype(jnp.float32), axis=1).reshape((2, -1) + received.shape[3:])
        for received in into
    ]

    def joined(pair):
        return jnp.concatenate([pair[0], pair[1]], axis=1)

    grad_value = joined(grad_mix[:, :, :values])
    grad_query = joined(grad_mix[:, :, values:wide])
    grad_gconv = joined(grad_mix[:, :, wide : wide + values])
    grad_key = joined(grad_mix[:, :, wide + values :])
    grad_out = joined(grad_o[:, :, :values]).T
    grad_gate = joined(grad_gu[:, :, :hidden_cols])
    grad_up = joined(grad_gu[:, :, hidden_cols:])
    grad_down = joined(grad_d).T

    gains = lax.dynamic_index_in_dim(gains[:4].reshape(2, 2, width), core, 1, False)
    taps_rows = lax.dynamic_index_in_dim(
        taps_rows[:, : 2 * KW, :values].reshape(-1, 2, KW, values), core, 1, False
    )
    grad_taps = jnp.transpose(taps_rows, (1, 0, 2)).reshape(KW, width)

    def chosen(pair):
        return jnp.where(core == 0, pair[0], pair[1]).reshape(1, micro_count, rows, width)

    return (
        chosen(outputs),
        chosen(back),
        gains[0][None],
        grad_query[None],
        grad_key[None],
        grad_value[None],
        grad_gconv[None],
        grad_taps[None],
        grad_out[None],
        gains[1][None],
        grad_gate[None],
        grad_up[None],
        grad_down[None],
    )


def solution(mesh):
    placed = (
        P(None, "seq", None),
        P(),
        P("section", None),
        P("section", "seq", "head"),
        P("section", "seq", "head"),
        P("section", "seq", "head"),
        P("section", "seq", "head"),
        P("section", None, None),
        P("section", "head", "seq"),
        P("section", None),
        P("section", "seq", "head"),
        P("section", "seq", "head"),
        P("section", "head", "seq"),
        P(None, "seq", None),
    )
    return jax.shard_map(
        on_device,
        mesh=mesh,
        in_specs=placed,
        out_specs=(
            P("section", None, "seq", None),
            P("section", None, "seq", None),
            P("section", None),
            P("section", "seq", "head"),
            P("section", "seq", "head"),
            P("section", "seq", "head"),
            P("section", "seq", "head"),
            P("section", None, None),
            P("section", "head", "seq"),
            P("section", None),
            P("section", "seq", "head"),
            P("section", "seq", "head"),
            P("section", "head", "seq"),
        ),
        check_vma=False,
    )
```

```python
import functools
import math

import jax
import jax.numpy as jnp
from jax import lax
from jax.experimental import pallas as pl
from jax.experimental.pallas import tpu as pltpu
import numpy as np
from jax.sharding import PartitionSpec as P

FK = 16
KW = 3
MESH = pl.DeviceIdType.MESH
epsilon = 1e-05


def remote(src, dst, send, recv, **where):
    return pltpu.make_async_remote_copy(
        src_ref=src,
        dst_ref=dst,
        send_sem=send,
        recv_sem=recv,
        device_id=where,
        device_id_type=MESH,
    )


def greet(line, spread, everyone):
    core, z, q = lax.axis_index("section"), lax.axis_index("head"), lax.axis_index("seq")
    depth, count = lax.axis_size("head"), lax.axis_size("seq")
    barrier = pltpu.get_barrier_semaphore()

    def hello(**where):
        pl.semaphore_signal(barrier, inc=1, device_id=where, device_id_type=MESH)

    hello(section=1 - core)
    expected = 1
    if spread:
        for j in range(1, count):
            for h in range(2):
                hello(section=h, seq=lax.rem(q + j, count))
        expected += 2 * (count - 1)
    if everyone:
        for j in range(1, depth):
            for h in range(2):
                hello(section=h, head=lax.rem(z + j, depth))
        expected += 2 * (depth - 1)
    elif line:

        @pl.when(z > 0)
        def _():
            hello(head=z - 1)

        @pl.when(z < depth - 1)
        def _():
            hello(head=z + 1)

        expected = expected + jnp.where(z > 0, 1, 0) + jnp.where(z < depth - 1, 1, 0)
    pl.semaphore_wait(barrier, expected)


PIECES = 4
FIRST_TILE = 8
LEAD = 3


class LineSum:
    def __init__(self, lhs, w, o_ref, scratch, chunks, lag):
        self.lhs, self.w, self.o_ref, self.chunks, self.lag = lhs, w, o_ref, chunks, lag
        self.p_ref, self.pin, self.low, self.high, self.out = scratch[:5]
        self.ps, self.pr, self.rs, self.rl, self.rh, self.bs, self.br, self.ts, self.tr = scratch[5:]
        self.z, self.n = lax.axis_index("head"), lax.axis_size("head")
        self.core = lax.axis_index("section")
        self.half = lhs.shape[1] // 2
        self.step = self.half // chunks
        self.depth = max((self.n - 1) // 2, self.n - 1 - (self.n - 1) // 2)
        self.turns = chunks + 2 * self.depth * lag

    @staticmethod
    def scratch(rows, width, chunks):
        dma = pltpu.SemaphoreType.DMA
        each = dma((2, chunks))
        whole = pltpu.VMEM((2, rows, width), jnp.bfloat16)
        return [whole] + [pltpu.VMEM((rows, width), jnp.bfloat16)] * 4 + [
            dma((1,)), dma((2, PIECES)), dma((2,)), each, each, dma((2, 2)), each, dma((1,)), dma((1,))
        ]

    def root(self, d):
        return (self.n - 1) // 2 if d == 0 else self.n - 1 - (self.n - 1) // 2

    def rng(self, d, k):
        return pl.ds(pl.multiple_of(d * self.half + k * self.step, self.step), self.step)

    def part(self, d, k):
        size = self.half // PIECES
        r = pl.ds(pl.multiple_of(d * self.half + k * size, size), size)
        other = 1 - self.core
        return remote(
            self.p_ref.at[other, r], self.pin.at[r], self.ps.at[0], self.pr.at[d, k], section=other
        )

    def up(self, d, k):
        r = self.rng(d, k)
        return remote(
            self.out.at[r], self.low.at[r], self.rs.at[d], self.rl.at[d, k], head=self.z + 1
        )

    def down(self, d, k):
        r = self.rng(d, k)
        return remote(
            self.out.at[r], self.high.at[r], self.rs.at[d], self.rh.at[d, k], head=self.z - 1
        )

    def share(self, d, k, side):
        r = self.rng(d, k)
        at = self.o_ref.at[self.core, r]
        return remote(
            at, at, self.bs.at[side, d], self.br.at[d, k], head=self.z + (1 if side else -1)
        )

    def give(self, d, k):
        r = self.rng(d, k)
        at = self.o_ref.at[self.core, r]
        return remote(at, at, self.ts.at[0], self.tr.at[0], section=1 - self.core)

    def make(self, i):
        size = self.half // PIECES
        places = [
            (m, pl.ds(pl.multiple_of(d * self.half + i * size, size), size))
            for m in range(2)
            for d in range(2)
        ]
        left = jnp.concatenate([self.lhs[m, r, :] for m, r in places], axis=0)
        made = lax.dot_general(
            left, self.w[...], (((1,), (1,)), ((), ())), preferred_element_type=jnp.float32
        ).astype(jnp.bfloat16)
        for at, (m, r) in enumerate(places):
            self.p_ref[m, r, :] = made[at * size : (at + 1) * size]
        for d in range(2):
            self.part(d, i).start()

    def gathered(self, d, k):
        r = self.rng(d, k)
        z, n, root = self.z, self.n, self.root(d)
        group = self.chunks // PIECES

        @pl.when(k % group == 0)
        def _():
            self.part(d, k // group).wait_recv()

        mine = self.p_ref[self.core, r, :].astype(jnp.float32) + self.pin[r, :].astype(jnp.float32)

        @pl.when((z == 0) & (root > 0))
        def _():
            self.out[r, :] = mine.astype(jnp.bfloat16)
            self.up(d, k).start()

        @pl.when((z == n - 1) & (root < n - 1))
        def _():
            self.out[r, :] = mine.astype(jnp.bfloat16)
            self.down(d, k).start()

        @pl.when((z > 0) & (z < root))
        def _():
            self.up(d, k).wait_recv()
            self.out[r, :] = (mine + self.low[r, :].astype(jnp.float32)).astype(jnp.bfloat16)
            self.up(d, k).start()

        @pl.when((z < n - 1) & (z > root))
        def _():
            self.down(d, k).wait_recv()
            self.out[r, :] = (mine + self.high[r, :].astype(jnp.float32)).astype(jnp.bfloat16)
            self.down(d, k).start()

        @pl.when(z == root)
        def _():
            total = mine
            if root > 0:
                self.up(d, k).wait_recv()
                total = total + self.low[r, :].astype(jnp.float32)
            if root < n - 1:
                self.down(d, k).wait_recv()
                total = total + self.high[r, :].astype(jnp.float32)
            self.o_ref[self.core, r, :] = total.astype(jnp.bfloat16)
            if root > 0:
                self.share(d, k, 0).start()
            if root < n - 1:
                self.share(d, k, 1).start()
            self.give(d, k).start()

    def passed(self, d, k):
        z, n, root = self.z, self.n, self.root(d)
        self.share(d, k, 0).wait_recv()

        @pl.when((z < root) & (z > 0))
        def _():
            self.share(d, k, 0).start()

        @pl.when((z > root) & (z < n - 1))
        def _():
            self.share(d, k, 1).start()

        self.give(d, k).start()

    def turn(self, t):
        z, n = self.z, self.n
        for d in range(2):
            root = self.root(d)
            deep = max(root, n - 1 - root)
            below = jnp.where(z < root, z, jnp.where(z > root, n - 1 - z, deep))
            k = t - below * self.lag
            far = jnp.abs(z - root)

            @pl.when((k >= 0) & (k < self.chunks))
            def _():
                self.gathered(d, k)

            b = t - (deep + far) * self.lag

            @pl.when((b >= 0) & (b < self.chunks) & (far > 0))
            def _():
                self.passed(d, b)

    def finish(self):
        z, n, other = self.z, self.n, 1 - self.core
        remote(
            self.p_ref.at[other], self.pin, self.ps.at[0], self.pr.at[0, 0], section=other
        ).wait_send()
        mine = self.o_ref.at[self.core]
        given = remote(mine, mine, self.ts.at[0], self.tr.at[0], section=other)
        given.wait_recv()
        given.wait_send()
        for d in range(2):
            root = self.root(d)
            r = pl.ds(d * self.half, self.half)
            at = self.o_ref.at[self.core, r]

            def summed(head):
                return remote(
                    self.out.at[r], self.low.at[r], self.rs.at[d], self.rl.at[d, 0], head=head
                )

            def shared(side):
                return remote(
                    at, at, self.bs.at[side, d], self.br.at[d, 0], head=z + (1 if side else -1)
                )

            @pl.when(z < root)
            def _():
                summed(z + 1).wait_send()

            @pl.when(z > root)
            def _():
                summed(z - 1).wait_send()

            if root > 0:

                @pl.when((z <= root) & (z > 0))
                def _():
                    shared(0).wait_send()

            if root < n - 1:

                @pl.when((z >= root) & (z < n - 1))
                def _():
                    shared(1).wait_send()


class Gather:
    def __init__(self, layer, srcs, dsts, sems):
        self.layer, self.srcs, self.dsts = layer, srcs, dsts
        self.ss, self.rr, self.ls, self.fs, self.fr = sems
        self.core, self.q = lax.axis_index("section"), lax.axis_index("seq")
        self.n = lax.axis_size("seq")
        self.square = self.n == 4

    @staticmethod
    def scratch(count, n):
        dma = pltpu.SemaphoreType.DMA
        return [dma((count, n, 2)), dma((count, n)), dma((count,)), dma((count, 2)), dma((count, 2))]

    def peer(self, j):
        if not self.square:
            return lax.rem(self.q + j, self.n)
        x, y = self.q % 2, self.q // 2
        x, y = (1 - x if j % 2 else x), (1 - y if j // 2 else y)
        return y * 2 + x

    def direct(self):
        return range(1, 3 if self.square else self.n)

    def copies(self, a):
        for j in self.direct():
            for h in range(2):
                yield remote(
                    self.srcs[a].at[h], self.dsts[a].at[self.q], self.ss.at[a, j, h],
                    self.rr.at[a, self.q], section=h, seq=self.peer(j),
                )
        yield remote(
            self.srcs[a].at[1 - self.layer], self.dsts[a].at[self.q], self.ss.at[a, 0, 0],
            self.rr.at[a, self.q], section=1 - self.layer,
        )

    def local(self, a):
        return pltpu.make_async_copy(
            self.srcs[a].at[self.layer], self.dsts[a].at[self.q], self.ls.at[a]
        )

    def arrival(self, a, s):
        return remote(
            self.srcs[a].at[0], self.dsts[a].at[s], self.ss.at[a, 0, 0], self.rr.at[a, s],
            section=1 - self.core,
        )

    def relay(self, a, i):
        size = self.srcs[a].shape[1] // 2
        at = self.dsts[a].at[self.peer(1 + i), pl.ds(i * size, size)]
        return remote(at, at, self.fs.at[a, i], self.fr.at[a, i], seq=self.peer(2 - i))

    def corner(self, a, i):
        size = self.srcs[a].shape[1] // 2
        at = self.dsts[a].at[self.peer(3), pl.ds(i * size, size)]
        return remote(at, at, self.fs.at[a, i], self.fr.at[a, i], seq=self.peer(2 - i))

    def start(self):
        @pl.when(self.core == self.layer)
        def _():
            for a in range(len(self.srcs)):
                for copy in self.copies(a):
                    copy.start()
                self.local(a).start()

    def due(self):
        sent, turns = 0, []
        for src in self.srcs:
            sent += 2 * src.shape[1] * src.shape[2] * 2
            turns.append(3 + sent // 200_000)
        return turns

    def middle(self, a):
        for j in self.direct():
            self.arrival(a, self.peer(j)).wait_recv()
            if self.square:
                self.relay(a, j - 1).start()

    def finish(self):
        for a in range(len(self.srcs)):
            if self.square:
                for i in range(2):
                    self.corner(a, i).wait_recv()
                    self.relay(a, i).wait_send()

            @pl.when(self.core == self.layer)
            def _():
                self.local(a).wait()
                for copy in self.copies(a):
                    copy.wait_send()

            @pl.when(self.core != self.layer)
            def _():
                self.arrival(a, self.q).wait_recv()


class SmallSum:
    def __init__(self, g_ref, total, spread, scratch):
        self.g_ref, self.total, self.spread = g_ref, total, spread
        self.got, self.src, self.ss, self.sr, self.ts, self.tr = scratch
        self.core, self.q, self.z = (lax.axis_index(a) for a in ("section", "seq", "head"))
        self.n, self.depth = lax.axis_size("seq"), lax.axis_size("head")

    @staticmethod
    def scratch(shape, narrow, n, depth):
        dma = pltpu.SemaphoreType.DMA
        return [
            pltpu.VMEM((n,) + shape, jnp.float32),
            pltpu.VMEM((8, narrow), jnp.float32),
            dma((n,)),
            dma((n,)),
            dma((2 * depth,)),
            dma((2 * depth,)),
        ]

    def first(self, j):
        return remote(
            self.g_ref, self.got.at[self.q], self.ss.at[j], self.sr.at[self.q],
            seq=lax.rem(self.q + j, self.n),
        )

    def others(self):
        for j in range(self.depth):
            for flip in range(2):
                if j or flip:
                    core = 1 - self.core if flip else self.core
                    yield 2 * j + flip, lax.rem(self.z + j, self.depth), core

    def second(self, i, z, core):
        slot = self.z * 2 + self.core
        return remote(
            self.src, self.spread.at[slot], self.ts.at[i], self.tr.at[slot], head=z, section=core
        )

    def start(self):
        for j in range(1, self.n):
            self.first(j).start()
        self.got[self.q] = self.g_ref[...]

    def middle(self):
        for j in range(1, self.n):
            s = lax.rem(self.q + j, self.n)
            remote(
                self.g_ref, self.got.at[s], self.ss.at[j], self.sr.at[s], seq=s
            ).wait_recv()
        summed = self.got[0]
        for s in range(1, self.n):
            summed = summed + self.got[s]
        self.total[...] = summed[:8]
        own = summed[8:, : self.src.shape[1]]
        self.src[...] = own
        self.spread[self.z * 2 + self.core] = own
        for i, z, core in self.others():
            self.second(i, z, core).start()

    def finish(self):
        for i, z, core in self.others():
            slot = z * 2 + core
            remote(
                self.src, self.spread.at[slot], self.ts.at[i], self.tr.at[slot], head=z, section=core
            ).wait_recv()
            self.second(i, z, core).wait_send()
        for j in range(1, self.n):
            self.first(j).wait_send()


class Scatter:
    def __init__(self, layer, srcs, dsts, sems):
        self.layer, self.srcs, self.dsts = layer, srcs, dsts
        self.ss, self.rr, self.ls = sems
        self.core, self.q = lax.axis_index("section"), lax.axis_index("seq")
        self.n = lax.axis_size("seq")

    @staticmethod
    def scratch(count, n):
        return [
            pltpu.SemaphoreType.DMA((count, n)),
            pltpu.SemaphoreType.DMA((count, 2, n)),
            pltpu.SemaphoreType.DMA((count,)),
        ]

    def copies(self, a):
        for j in range(1, self.n):
            t = lax.rem(self.q + j, self.n)
            yield remote(
                self.srcs[a].at[t], self.dsts[a].at[self.core, self.q], self.ss.at[a, j],
                self.rr.at[a, self.core, self.q], section=self.layer, seq=t,
            )

    def near(self, a):
        return remote(
            self.srcs[a].at[self.q], self.dsts[a].at[self.core, self.q], self.ss.at[a, 0],
            self.rr.at[a, self.core, self.q], section=self.layer,
        )

    def local(self, a):
        return pltpu.make_async_copy(
            self.srcs[a].at[self.q], self.dsts[a].at[self.core, self.q], self.ls.at[a]
        )

    def arrival(self, a, h, s):
        return remote(
            self.srcs[a].at[self.q], self.dsts[a].at[h, s], self.ss.at[a, 0], self.rr.at[a, h, s],
            section=1 - self.core,
        )

    def start(self):
        for a in range(len(self.srcs)):
            for copy in self.copies(a):
                copy.start()

            @pl.when(self.core == self.layer)
            def _():
                self.local(a).start()

            @pl.when(self.core != self.layer)
            def _():
                self.near(a).start()

    def finish(self):
        for a in range(len(self.srcs)):

            @pl.when(self.core == self.layer)
            def _():
                for j in range(1, self.n):
                    for h in range(2):
                        self.arrival(a, h, lax.rem(self.q + j, self.n)).wait_recv()
                self.arrival(a, 1 - self.layer, self.q).wait_recv()
                self.local(a).wait()

            @pl.when(self.core != self.layer)
            def _():
                self.near(a).wait_send()

            for copy in self.copies(a):
                copy.wait_send()


TILE = 256


class Product:
    def __init__(self, lhs, rhs, out, scratch):
        self.lhs, self.rhs, self.out = lhs, rhs, out
        self.left, self.right, self.stage, self.loads, self.stores = scratch
        self.tiles = lhs.shape[1] // TILE

    @staticmethod
    def scratch(lhs, rhs):
        return [
            pltpu.VMEM(lhs.shape, jnp.bfloat16),
            pltpu.VMEM(rhs.shape, jnp.bfloat16),
            pltpu.VMEM((2, TILE, rhs.shape[1]), jnp.bfloat16),
            pltpu.SemaphoreType.DMA((2,)),
            pltpu.SemaphoreType.DMA((2,)),
        ]

    def load(self, side):
        src, dst = ((self.lhs, self.left), (self.rhs, self.right))[side]
        return pltpu.make_async_copy(src, dst, self.loads.at[side])

    def store(self, i):
        at = pl.ds(pl.multiple_of(i * TILE, TILE), TILE)
        return pltpu.make_async_copy(self.stage.at[i % 2], self.out.at[at], self.stores.at[i % 2])

    def start(self):
        self.load(0).start()
        self.load(1).start()

    def step(self, i):
        @pl.when(i == 0)
        def _():
            self.load(0).wait()
            self.load(1).wait()

        @pl.when(i >= 2)
        def _():
            self.store(i - 2).wait()

        at = pl.ds(pl.multiple_of(i * TILE, TILE), TILE)
        self.stage[i % 2] = lax.dot_general(
            self.left[:, at],
            self.right[...],
            (((0,), (0,)), ((), ())),
            preferred_element_type=jnp.float32,
        ).astype(jnp.bfloat16)
        self.store(i).start()

    def finish(self):
        for i in range(max(self.tiles - 2, 0), self.tiles):
            self.store(i).wait()


def comm_kernel(plan, *refs):
    has_sum, layer_in, count_in, layer_out, count_out, kept, count_made, small_in, chunks, lag = plan
    refs = list(refs)

    def take(count):
        taken = refs[:count]
        del refs[:count]
        return taken

    p_in, w_in, g_in, _, m_in, s_in = (
        take(2 * has_sum), take(count_in), take(count_out), take(kept), take(2 * count_made),
        take(small_in),
    )
    p_out, w_out, g_out, m_out, s_out = (
        take(has_sum), take(count_in), take(count_out), take(count_made), take(2 * small_in)
    )
    greet(has_sum, count_in + count_out > 0, small_in)
    jobs = []
    later = []
    if has_sum:
        line = LineSum(p_in[0], p_in[1], p_out[0], take(14), chunks, lag)
    if count_in:
        weights = Gather(layer_in, w_in, w_out, take(5))
        jobs.append(weights)
        for a, turn in enumerate(weights.due()):
            later.append((turn, functools.partial(weights.middle, a)))
    if count_out:
        jobs.append(Scatter(layer_out, g_in, g_out, take(3)))
    made = [
        Product(m_in[2 * i], m_in[2 * i + 1], m_out[i], take(5)) for i in range(count_made)
    ]
    if small_in:
        small = SmallSum(s_in[0], s_out[0], s_out[1], take(6))
        jobs.insert(0, small)
        later.append((12, small.middle))
    for job in made + jobs:
        job.start()
    if has_sum:
        tiles = sum(product.tiles for product in made)

        def turn(t, carry):
            @pl.when((t < LEAD * PIECES) & (t % LEAD == 0))
            def _():
                line.make(t // LEAD)

            line.turn(t - LEAD)
            i = t - LEAD - FIRST_TILE
            for product in made:

                @pl.when((i >= 0) & (i < product.tiles))
                def _(product=product, i=i):
                    product.step(i)

                i = i - product.tiles
            for when, act in later:

                @pl.when(t == when + LEAD)
                def _(act=act):
                    act()

            return carry

        last = max([line.turns, tiles + FIRST_TILE] + [when + 1 for when, _ in later])
        lax.fori_loop(0, last + LEAD, turn, 0)
        line.finish()
    else:
        for _, act in later:
            act()
    for job in made + jobs:
        job.finish()


def communicate(
    cid, partial=None, gather=None, scatter=None, into=(), products=(), small=None, chunks=16, lag=2
):
    n = lax.axis_size("seq")
    layer_in, w_in = gather if gather else (0, [])
    layer_out, g_in = scatter if scatter else (0, [])
    p_in = [] if partial is None else list(partial)
    has_sum = 0 if partial is None else 1
    if has_sum:
        summed = (partial[0].shape[0], partial[0].shape[1], partial[1].shape[0])
    m_in = [a for pair in products for a in pair]
    vmem, anywhere = pl.BlockSpec(memory_space=pltpu.VMEM), pl.BlockSpec(memory_space=pl.ANY)
    scratch = []
    if p_in:
        scratch += LineSum.scratch(summed[1], summed[2], chunks)
    if w_in:
        scratch += Gather.scratch(len(w_in), n)
    if g_in:
        scratch += Scatter.scratch(len(g_in), n)
    for pair in products:
        scratch += Product.scratch(*pair)
    s_in, s_shapes = [], []
    if small is not None:
        s_in, narrow, depth = [small[0]], small[1], lax.axis_size("head")
        scratch += SmallSum.scratch(small[0].shape, narrow, n, depth)
        s_shapes = [
            jax.ShapeDtypeStruct((8, small[0].shape[1]), jnp.float32),
            jax.ShapeDtypeStruct((2 * depth, 8, narrow), jnp.float32),
        ]
    shapes = (
        ([jax.ShapeDtypeStruct(summed, jnp.bfloat16)] if has_sum else [])
        + [jax.ShapeDtypeStruct((n,) + w.shape[1:], jnp.bfloat16) for w in w_in]
        + [jax.ShapeDtypeStruct((2,) + g.shape, jnp.bfloat16) for g in g_in]
        + [jax.ShapeDtypeStruct((a.shape[1], b.shape[1]), jnp.bfloat16) for a, b in products]
        + s_shapes
    )
    plan = (
        has_sum, layer_in, len(w_in), layer_out, len(g_in), len(into), len(products), len(s_in),
        chunks, lag,
    )
    first = len(p_in) + len(w_in)
    first_out = has_sum + len(w_in)
    outs = pl.pallas_call(
        functools.partial(comm_kernel, plan),
        out_shape=shapes,
        in_specs=[vmem] * first
        + [anywhere] * (len(g_in) + len(into) + len(m_in))
        + [vmem] * len(s_in),
        out_specs=[vmem] * has_sum
        + [anywhere] * (len(w_in) + len(g_in) + len(products))
        + [vmem] * len(s_shapes),
        scratch_shapes=scratch,
        input_output_aliases={first + len(g_in) + i: first_out + i for i in range(len(into))},
        name=f"comm{cid}",
        compiler_params=pltpu.CompilerParams(
            collective_id=cid, has_side_effects=True, vmem_limit_bytes=52 << 20
        ),
    )(*p_in, *w_in, *g_in, *into, *m_in, *s_in)
    return (
        outs[0] if p_in else None,
        [a.reshape((-1,) + a.shape[2:]) for a in outs[has_sum : first_out]],
        outs[first_out : first_out + len(g_in)],
        outs[first_out + len(g_in) :],
    )


def rms_norm(vector, scale_gain):
    return (
        vector * lax.rsqrt(jnp.mean(vector * vector, axis=-1, keepdims=True) + epsilon) * scale_gain
    )


def seq_begin(lengths_row, positions):
    seq_starts = jnp.cumsum(lengths_row) - lengths_row
    chosen = jnp.where(seq_starts[None, :] <= positions[:, None], seq_starts[None, :], 0)
    return jnp.max(chosen, axis=1)


HEADS = 2
PAIRS = FK * (FK + 1) // 2
STATE = 160
BLOCK = 128


def feature_tables(values):
    wide = values + HEADS * FK
    first = np.zeros((HEADS, wide, wide), np.float32)
    second = np.zeros((HEADS, wide, wide), np.float32)
    rest = np.zeros((8, wide), np.float32)
    for h in range(HEADS):
        at = values + h * FK
        lane = 0
        for a in range(FK):
            for b in range(a, FK):
                first[h, at + a, lane] = 1
                second[h, at + b, lane] = 1
                rest[2, lane] = 0.25 if a < b else 1 / (4.0 * math.sqrt(2.0))
                lane += 1
        for a in range(FK):
            first[h, at + a, lane] = 1
            rest[1, lane] = 1
            rest[2, lane] = 0.5
            lane += 1
        rest[0, lane] = rest[1, lane] = rest[2, lane] = 1
    return np.stack([first, second], axis=1), rest


def mm(a, b):
    return lax.dot_general(a, b, (((1,), (0,)), ((), ())), preferred_element_type=jnp.float32)


def mm_nt(a, b):
    return lax.dot_general(a, b, (((1,), (1,)), ((), ())), preferred_element_type=jnp.float32)


def mm_tn(a, b):
    return lax.dot_general(a, b, (((0,), (0,)), ((), ())), preferred_element_type=jnp.float32)


class Lanes:
    def __init__(self, wide, values):
        self.values = values
        self.lane = lax.broadcasted_iota(jnp.int32, (1, wide), 1)
        lane, dim = self.lane, values // HEADS
        self.is_value = lane < values
        self.is_one = (lane >= values) & (lane < values + 2 * HEADS)
        self.head = jnp.where(
            self.is_value, jnp.where(lane < dim, 0, 1), jnp.where(self.is_one, (lane - values) % 2, 9)
        )

    def of(self, h, x):
        return jnp.where(self.head == h, x, jnp.zeros_like(x))

    def key(self, h, x):
        at = self.values + h * FK
        return jnp.where((self.lane >= at) & (self.lane < at + FK), x, jnp.zeros_like(x))

    def extended(self, a):
        return jnp.where(
            self.is_value, a, jnp.where(self.is_one, jnp.ones_like(a), jnp.zeros_like(a))
        )

    def column(self, x, index):
        return jnp.sum(
            jnp.where(self.lane == self.values + index, x, 0.0), axis=1, keepdims=True
        )

    def denominator(self, x):
        return jnp.where(
            self.lane < self.values // HEADS, self.column(x, 0), self.column(x, 1)
        )


def meet(direction, reach):
    q, n = lax.axis_index("seq"), lax.axis_size("seq")
    barrier = pltpu.get_barrier_semaphore()
    count = 0
    for d in range(1, reach + 1):
        source = q - direction * d
        target = q + direction * d

        @pl.when((source >= 0) & (source < n))
        def _():
            pl.semaphore_signal(barrier, inc=1, device_id={"seq": source}, device_id_type=MESH)

        count = count + jnp.where((target >= 0) & (target < n), 1, 0)

    @pl.when(count > 0)
    def _():
        pl.semaphore_wait(barrier, count)


class Pass:
    def __init__(self, direction, reach, src, dst, send, recv):
        self.direction, self.reach = direction, reach
        self.src, self.dst, self.send, self.recv = src, dst, send, recv
        self.q, self.n = lax.axis_index("seq"), lax.axis_size("seq")

    def has_source(self, d):
        at = self.q - self.direction * d
        return (at >= 0) & (at < self.n)

    def has_target(self, d):
        at = self.q + self.direction * d
        return (at >= 0) & (at < self.n)

    def copy(self, d):
        return remote(
            self.src, self.dst.at[d - 1], self.send.at[d - 1], self.recv.at[d - 1],
            seq=self.q + self.direction * d,
        )

    def start(self):
        for d in range(1, self.reach + 1):

            @pl.when(self.has_target(d))
            def _():
                self.copy(d).start()

    def arrived(self):
        for d in range(1, self.reach + 1):

            @pl.when(self.has_source(d))
            def _():
                self.copy(d).wait_recv()

    def sent(self):
        for d in range(1, self.reach + 1):

            @pl.when(self.has_target(d))
            def _():
                self.copy(d).wait_send()


def sum_states(states, coef, total):
    for m in range(2):
        total[m] = jnp.zeros(total.shape[1:], total.dtype)
        for d in range(1, states.reach + 1):

            @pl.when(states.has_source(d))
            def _():
                total[m, :STATE, :] += coef[d - 1, m] * states.dst[d - 1, m].astype(jnp.float32)


def shifted(a, tail, fresh, by):
    row = lax.broadcasted_iota(jnp.int32, (a.shape[0], 1), 0)
    moved = pltpu.roll(a, by, 0)
    rows = tail.shape[0]
    for r in range(by):
        edge = jnp.where(fresh, tail[rows - by + r : rows - by + r + 1, :], 0.0)
        moved = jnp.where(row == r, edge, moved)
    return moved


def attn_forward_kernel(
    reach, proj, col, row, coef, e, c, taps, gated, att, conv, sin, edge, acc, phi, s_acc, s_src,
    s_all, s_sum, e_src, ss, sr, es, er,
):
    q = lax.axis_index("seq")
    rows, wide = proj.shape[1], proj.shape[2] // 2
    values = wide - HEADS * FK
    lanes = Lanes(wide, values)
    meet(1, reach)
    states = Pass(1, reach, s_src, s_all, ss, sr)
    edges = Pass(1, 1, e_src, edge, es, er)

    def sides(m):
        return proj[m, :, :wide].astype(jnp.bfloat16), proj[m, :, wide:].astype(jnp.bfloat16)

    def phi_of(a, h):
        return (mm(a, e[h, 0]) + c[0:1, :]) * (mm(a, e[h, 1]) + c[1:2, :]) * c[2:3, :]

    def make_state(i, carry):
        m, h = i // HEADS, i % HEADS
        a, b = sides(m)
        phi[m, h] = (phi_of(a, h) * col[m, :, 1:2]).astype(jnp.bfloat16)
        keyed = (phi_of(b, h) * col[m, :, 2:3]).astype(jnp.bfloat16)
        part = mm_tn(keyed, lanes.of(h, lanes.extended(a)))

        @pl.when(h == 0)
        def _():
            s_acc[m] = part

        @pl.when(h > 0)
        def _():
            s_acc[m] += part

        return carry

    lax.fori_loop(0, 2 * HEADS, make_state, 0)
    for m in range(2):
        s_src[m] = s_acc[m, :STATE, :].astype(jnp.bfloat16)
    states.start()

    def make_block(i, carry):
        m, h = i // HEADS, i % HEADS
        a, b = sides(m)
        asked = lanes.key(h, a)
        valued = lanes.of(h, lanes.extended(a))
        for r in range(rows // BLOCK):
            lo, hi = r * BLOCK, (r + 1) * BLOCK
            x = mm_nt(asked[lo:hi], b[:hi]) * 0.25
            seen = (col[m, lo:hi, 0:1] == row[m, 0:1, :hi]) & (
                lax.broadcasted_iota(jnp.int32, (BLOCK, hi), 1)
                <= lo + lax.broadcasted_iota(jnp.int32, (BLOCK, hi), 0)
            )
            w = jnp.where(seen, 1.0 + x + 0.5 * x * x, 0.0).astype(jnp.bfloat16)
            part = mm(w, valued[:hi])

            @pl.when(h == 0)
            def _():
                acc[m, lo:hi, :] = part

            @pl.when(h > 0)
            def _():
                acc[m, lo:hi, :] += part

        return carry

    lax.fori_loop(0, 2 * HEADS, make_block, 0)
    states.arrived()
    sum_states(states, coef, s_sum)

    def attend(m, lo):
        s = s_sum[m].astype(jnp.bfloat16)
        both = acc[m, lo:, :]
        for h in range(HEADS):
            both = both + mm(phi[m, h, lo:, :], lanes.of(h, s))
        return jnp.where(lanes.is_value, both / lanes.denominator(both), both)

    for m in range(2):
        sin[m] = s_sum[m, :STATE, :].astype(jnp.bfloat16)
        e_src[m] = attend(m, rows - 16)
    edges.start()
    for m in range(2):
        att[m] = attend(m, 0)
    edges.arrived()
    for m in range(2):
        a = att[m]
        tail = edge[0, m]
        out = taps[0:1, :] * a
        for by in (1, 2):
            out = out + taps[by : by + 1, :] * shifted(a, tail, q > 0, by) * col[m, :, 2 + by : 3 + by]
        conv[m] = out
        gated[m] = (out * proj[m, :, wide:]).astype(jnp.bfloat16)
    states.sent()
    edges.sent()


def attn_backward_kernel(
    reach, bg, proj, att, conv, sin, edge, col, row, coef, late, e, c, taps, out, grad_taps,
    phi_q, phi_k, near, acc_a, acc_b, s_acc, s_src, s_all, s_sum, e_src, e_dst, ss, sr, es, er,
):
    q, n = lax.axis_index("seq"), lax.axis_size("seq")
    rows, wide = proj.shape[1], proj.shape[2] // 2
    values = wide - HEADS * FK
    lanes = Lanes(wide, values)
    meet(-1, reach)
    states = Pass(-1, reach, s_src, s_all, ss, sr)
    edges = Pass(-1, 1, e_src, e_dst, es, er)
    for m in range(2):
        e_src[m] = bg[m, :16, :] * proj[m, :16, wide:]
    edges.start()

    def sides(m):
        return proj[m, :, :wide].astype(jnp.bfloat16), proj[m, :, wide:].astype(jnp.bfloat16)

    def factors(a, h):
        return mm(a, e[h, 0]) + c[0:1, :], mm(a, e[h, 1]) + c[1:2, :]

    def make_phi(i, carry):
        m, h = i // HEADS, i % HEADS
        a, b = sides(m)
        u, w = factors(a, h)
        phi_q[m, h] = (u * w * c[2:3, :] * col[m, :, 1:2]).astype(jnp.bfloat16)
        u, w = factors(b, h)
        phi_k[m, h] = (u * w * c[2:3, :] * col[m, :, 2:3]).astype(jnp.bfloat16)
        return carry

    lax.fori_loop(0, 2 * HEADS, make_phi, 0)
    edges.arrived()
    sums = [jnp.zeros((1, wide), jnp.float32)] * KW
    place = lax.broadcasted_iota(jnp.int32, (rows, 1), 0)
    for m in range(2):
        back = bg[m]
        back_conv = back * proj[m, :, wide:]
        a = jnp.where(lanes.is_value, att[m], 0.0)
        tail = edge[0, m]
        nxt = e_dst[0, m]
        total = taps[0:1, :] * back_conv
        sums[0] = sums[0] + jnp.sum(back_conv * a, axis=0, keepdims=True)
        for by in (1, 2):
            kept = back_conv * col[m, :, 2 + by : 3 + by]
            sums[by] = sums[by] + jnp.sum(
                kept * shifted(a, tail, q > 0, by), axis=0, keepdims=True
            )
            moved = pltpu.roll(kept, rows - by, 0)
            for r in range(by):
                fresh = jnp.where(q < n - 1, nxt[r : r + 1, :] * late[by - 1 + r, m], 0.0)
                moved = jnp.where(place == rows - by + r, fresh, moved)
            total = total + taps[by : by + 1, :] * moved
        out[m, :, wide:] = jnp.where(lanes.is_value, back * conv[m], 0.0).astype(jnp.bfloat16)
        back_numer = total / lanes.denominator(att[m])
        spent = back_numer * a
        found = jnp.where(lanes.is_value, back_numer, 0.0)
        for h in range(HEADS):
            denom = -jnp.sum(lanes.of(h, spent), axis=1, keepdims=True)
            high = denom.astype(jnp.bfloat16).astype(jnp.float32)
            found = jnp.where(lanes.lane == values + h, high, found)
            found = jnp.where(lanes.lane == values + 2 + h, denom - high, found)
        near[m] = found.astype(jnp.bfloat16)
        part = jnp.zeros((wide, wide), jnp.float32)
        for h in range(HEADS):
            part = part + mm_tn(phi_q[m, h], lanes.of(h, near[m]))
        s_src[m] = part[:STATE].astype(jnp.bfloat16)
    states.start()
    grad_taps[...] = jnp.zeros(grad_taps.shape, jnp.float32)
    for by in range(KW):
        grad_taps[by : by + 1, :] = sums[by]
    acc_a[...] = jnp.zeros(acc_a.shape, jnp.float32)
    acc_b[...] = jnp.zeros(acc_b.shape, jnp.float32)
    for m in range(2):
        s_sum[m] = jnp.zeros(s_sum.shape[1:], jnp.float32)
        s_sum[m, :STATE, :] = sin[m].astype(jnp.float32)

    def through_phi(scaled, factors_of, h):
        u, w = factors_of
        return mm_nt((scaled * w).astype(jnp.bfloat16), e[h, 0]) + mm_nt(
            (scaled * u).astype(jnp.bfloat16), e[h, 1]
        )

    def make_block(i, carry):
        m, h = i // HEADS, i % HEADS
        a, b = sides(m)
        asked, keyed = lanes.key(h, a), lanes.key(h, b)
        valued = lanes.extended(a)
        given = lanes.of(h, near[m])
        given_v = jnp.where(lanes.is_value, given, jnp.zeros_like(given))
        for r in range(rows // BLOCK):
            lo, hi = r * BLOCK, (r + 1) * BLOCK
            x = mm_nt(asked[lo:hi], b[:hi]) * 0.25
            seen = (col[m, lo:hi, 0:1] == row[m, 0:1, :hi]) & (
                lax.broadcasted_iota(jnp.int32, (BLOCK, hi), 1)
                <= lo + lax.broadcasted_iota(jnp.int32, (BLOCK, hi), 0)
            )
            w = jnp.where(seen, 1.0 + x + 0.5 * x * x, 0.0).astype(jnp.bfloat16)
            back_w = mm_nt(given[lo:hi], valued[:hi])
            back_s = jnp.where(seen, back_w * (1.0 + x), 0.0).astype(jnp.bfloat16)
            acc_a[m, lo:hi, :] += 0.25 * mm(back_s, keyed[:hi])
            acc_b[m, :hi, :] += 0.25 * mm_tn(back_s, asked[lo:hi])
            acc_a[m, :hi, :] += mm_tn(w, given_v[lo:hi])
        s = s_sum[m].astype(jnp.bfloat16)
        scaled = mm_nt(given, s) * col[m, :, 1:2] * c[2:3, :]
        acc_a[m] += through_phi(scaled, factors(a, h), h)
        return carry

    lax.fori_loop(0, 2 * HEADS, make_block, 0)
    states.arrived()
    sum_states(states, coef, s_sum)

    def make_late(i, carry):
        m, h = i // HEADS, i % HEADS
        a, b = sides(m)
        s = s_sum[m].astype(jnp.bfloat16)
        scaled = mm_nt(lanes.of(h, lanes.extended(a)), s) * col[m, :, 2:3] * c[2:3, :]
        acc_b[m] += through_phi(scaled, factors(b, h), h)
        s_v = lanes.of(h, jnp.where(lanes.is_value, s, jnp.zeros_like(s)))
        acc_a[m] += mm(phi_k[m, h], s_v)
        return carry

    lax.fori_loop(0, 2 * HEADS, make_late, 0)
    for m in range(2):
        out[m, :, :wide] = acc_a[m].astype(jnp.bfloat16)
        out[m, :, wide:] = jnp.where(
            lanes.is_value, out[m, :, wide:].astype(jnp.float32), acc_b[m]
        ).astype(jnp.bfloat16)
    states.sent()
    edges.sent()


def seq_reach():
    n = lax.axis_size("seq")
    return n // 2 if n % 2 == 0 else n - 1


def attention_call(kernel, cid, inputs, scalars, shapes, scratch):
    vmem, smem = pl.BlockSpec(memory_space=pltpu.VMEM), pl.BlockSpec(memory_space=pltpu.SMEM)
    return pl.pallas_call(
        functools.partial(kernel, seq_reach()),
        out_shape=shapes,
        in_specs=[smem if i in scalars else vmem for i in range(len(inputs))],
        out_specs=[vmem] * len(shapes),
        scratch_shapes=scratch,
        name=f"attention{cid}",
        compiler_params=pltpu.CompilerParams(
            collective_id=cid, has_side_effects=True, vmem_limit_bytes=48 << 20
        ),
    )(*inputs)


def passing(reach, wide):
    dma = pltpu.SemaphoreType.DMA
    return (
        [
            pltpu.VMEM((2, STATE, wide), jnp.bfloat16),
            pltpu.VMEM((reach, 2, STATE, wide), jnp.bfloat16),
            pltpu.VMEM((2, wide, wide), jnp.float32),
        ],
        [dma((reach,)), dma((reach,)), dma((1,)), dma((1,))],
    )


def attention_forward(proj, taps, marks, tables):
    m, rows, double = proj.shape
    wide = double // 2
    f32, bf16 = jnp.float32, jnp.bfloat16
    buffers, sems = passing(seq_reach(), wide)
    shape = jax.ShapeDtypeStruct
    return attention_call(
        attn_forward_kernel,
        10,
        [proj, marks["col"], marks["row"], marks["before"], *tables, taps],
        (3,),
        [
            shape((m, rows, wide), bf16),
            shape((m, rows, wide), f32),
            shape((m, rows, wide), f32),
            shape((m, STATE, wide), bf16),
            shape((1, m, 16, wide), f32),
        ],
        [
            pltpu.VMEM((m, rows, wide), f32),
            pltpu.VMEM((m, HEADS, rows, wide), bf16),
            pltpu.VMEM((m, wide, wide), f32),
            *buffers,
            pltpu.VMEM((m, 16, wide), f32),
            *sems,
        ],
    )


def attention_backward(back_gated, proj, kept, taps, marks, tables):
    att, conv, sin, edge = kept
    m, rows, double = proj.shape
    wide = double // 2
    f32, bf16 = jnp.float32, jnp.bfloat16
    buffers, sems = passing(seq_reach(), wide)
    shape = jax.ShapeDtypeStruct
    return attention_call(
        attn_backward_kernel,
        11,
        [
            back_gated, proj, att, conv, sin, edge, marks["col"], marks["row"], marks["after"],
            marks["late"], *tables, taps,
        ],
        (8, 9),
        [shape((m, rows, double), bf16), shape((8, wide), f32)],
        [
            pltpu.VMEM((m, HEADS, rows, wide), bf16),
            pltpu.VMEM((m, HEADS, rows, wide), bf16),
            pltpu.VMEM((m, rows, wide), bf16),
            pltpu.VMEM((m, rows, wide), f32),
            pltpu.VMEM((m, rows, wide), f32),
            pltpu.VMEM((m, wide, wide), f32),
            *buffers,
            pltpu.VMEM((m, 16, wide), f32),
            pltpu.VMEM((1, m, 16, wide), f32),
            *sems,
        ],
    )


def sequence_marks(lengths, rows):
    count, mine = lax.axis_size("seq"), lax.axis_index("seq")
    start = mine * rows
    positions = start + jnp.arange(rows + 2, dtype=jnp.int32)
    begin_ext = jax.vmap(lambda row: seq_begin(row, positions))(lengths)
    begin = begin_ext[:, :rows]
    ends = (jnp.arange(count, dtype=jnp.int32) + 1) * rows - 1
    stays = jax.vmap(lambda row: seq_begin(row, ends))(lengths) < (ends - rows + 1)[None, :]
    stays = stays.astype(jnp.float32)
    blocks = jnp.arange(count, dtype=jnp.int32)

    def through(first, last):
        inside = (blocks >= first) & (blocks <= last)
        return jnp.min(jnp.where(inside[None, :], stays, 1.0), axis=1)

    reach = seq_reach()
    before = [through(mine - d + 1, mine - 1) for d in range(1, reach + 1)]
    after = [through(mine + 1, mine + d - 1) for d in range(1, reach + 1)]
    allowed = [(positions - j >= begin_ext).astype(jnp.float32) for j in range(KW)]
    columns = [
        begin.astype(jnp.float32),
        (begin < start).astype(jnp.float32),
        (begin == begin[:, rows - 1 :]).astype(jnp.float32),
        allowed[1][:, :rows],
        allowed[2][:, :rows],
    ]
    col = jnp.stack(columns + [jnp.zeros_like(columns[0])] * 3, axis=2)
    return {
        "col": col,
        "row": jnp.broadcast_to(columns[0][:, None, :], (2, 8, rows)),
        "before": jnp.stack(before),
        "after": jnp.stack(after),
        "late": jnp.stack([allowed[1][:, rows], allowed[2][:, rows], allowed[2][:, rows + 1]]),
    }


def by_seq(grad):
    n = lax.axis_size("seq")
    return grad.reshape((n, grad.shape[0] // n) + grad.shape[1:])


def held(a):
    return lax.optimization_barrier(a.astype(jnp.bfloat16))


def dot_n(a, b):
    return jnp.dot(a, b, preferred_element_type=jnp.float32)


def on_device(
    tokens,
    lengths,
    gain_attn,
    w_query,
    w_key,
    w_value,
    w_gate_conv,
    conv_taps,
    w_out,
    gain_ffn,
    w_gate,
    w_up,
    w_down,
    cotangent,
):
    head_index = lax.axis_index("head")
    core = lax.axis_index("section")
    micro_count, rows, width = tokens.shape
    total = micro_count * rows

    def halves(weight):
        cols = weight.shape[1] // 2
        return jnp.stack([weight[:, :cols], weight[:, cols:]])

    own_mix = jnp.concatenate(
        [halves(w[0]) for w in (w_value, w_query, w_gate_conv, w_key)], axis=2
    )
    values = w_value.shape[2] // 2
    keys = w_query.shape[2] // 2
    wide = values + keys
    own_out = jnp.pad(halves(w_out[0].T), ((0, 0), (0, 0), (0, keys)))
    own_ffn = jnp.concatenate([halves(w_gate[0]), halves(w_up[0])], axis=2)
    own_down = halves(w_down[0].T)
    gains_one = lax.all_gather(gain_attn[0], "section").astype(jnp.float32)
    gains_two = lax.all_gather(gain_ffn[0], "section").astype(jnp.float32)
    taps_all = lax.all_gather(conv_taps[0], "section").astype(jnp.float32)
    taps_both = lax.dynamic_slice_in_dim(taps_all, (head_index * 2 + core) * values, values, 2)
    taps_both = jnp.pad(taps_both, ((0, 0), (0, 8 - KW), (0, keys)))
    first, rest = feature_tables(values)
    tables = (jnp.asarray(first, jnp.bfloat16), jnp.asarray(rest))
    marks = sequence_marks(lengths, rows)
    hidden_cols = own_down.shape[2]

    def as_parts(flat):
        return flat.reshape(micro_count, rows, -1)

    def spread(summed):
        return summed.astype(jnp.float32).reshape(total, width)

    _, (mix_0, out_0), _, _ = communicate(1, gather=(0, [own_mix, own_out]))
    w_mix, w_o, w_gu, w_d = [mix_0, None], [out_0, None], [None, None], [None, None]
    x = tokens.reshape(total, width).astype(jnp.float32)
    kept = [None, None]
    outputs = []
    last_partial = None
    for layer in range(2):
        normed = rms_norm(x, gains_one[layer]).astype(jnp.bfloat16)
        proj = dot_n(normed, w_mix[layer]).reshape(micro_count, rows, 2 * wide)
        gated, *attn = attention_forward(proj, taps_both[layer], marks, tables)
        gated_flat = gated.reshape(total, wide)
        partial = (gated, w_o[layer])
        if layer == 0:
            summed, (w_gu[0], w_d[0]), _, _ = communicate(
                2, partial=partial, gather=(0, [own_ffn, own_down])
            )
        else:
            summed, (w_gu[1],), _, _ = communicate(3, partial=partial, gather=(1, [own_ffn]))
        middle = x + spread(summed)
        normed_two = rms_norm(middle, gains_two[layer]).astype(jnp.bfloat16)
        middle = held(middle).astype(jnp.float32)
        both = held(dot_n(normed_two, w_gu[layer])).astype(jnp.float32)
        hidden = (jax.nn.silu(both[:, :hidden_cols]) * both[:, hidden_cols:]).astype(jnp.bfloat16)
        partial = (as_parts(hidden), w_d[layer])
        kept[layer] = (x, normed, proj, gated_flat, attn, middle, normed_two, both, hidden)
        if layer == 0:
            summed, (w_mix[1], w_o[1], w_d[1]), _, _ = communicate(
                4, partial=partial, gather=(1, [own_mix, own_out, own_down])
            )
            outputs.append(held(middle + spread(summed)))
            x = outputs[0].astype(jnp.float32)
        else:
            last_partial = partial

    grad = cotangent.reshape(total, width)
    back = [None, None]
    smalls = [None, None]
    made = []
    into = [None] * 4
    for layer in (1, 0):
        x, normed, proj, gated_flat, attn, middle, normed_two, both, hidden = kept[layer]
        grad_wide = grad.astype(jnp.float32)
        back_hidden = dot_n(grad, w_d[layer])
        gate_pre, upward = both[:, :hidden_cols], both[:, hidden_cols:]
        silu_value, silu_back = jax.vjp(jax.nn.silu, gate_pre)
        back_both = jnp.concatenate(
            [
                silu_back(back_hidden * upward)[0].astype(jnp.bfloat16),
                (back_hidden * silu_value).astype(jnp.bfloat16),
            ],
            axis=1,
        )
        partial = (as_parts(back_both), w_gu[layer])
        products = ((normed_two, back_both), (grad, hidden))
        if layer == 1:
            summed, _, _, (grad_gu, grad_d) = communicate(5, partial=partial, products=products)
        else:
            summed, _, into[1:], (grad_gu, grad_d) = communicate(
                6, partial=partial, scatter=(1, made), products=products
            )
        _, norm_back_two = jax.vjp(rms_norm, middle, gains_two[layer])
        back_middle, gain_two = norm_back_two(spread(summed))
        back_middle = grad_wide + back_middle
        back_branch = held(back_middle)
        back_middle = back_branch.astype(jnp.float32)
        back_gated = dot_n(back_branch, w_o[layer])
        back_proj, taps_grad = attention_backward(
            back_gated.reshape(micro_count, rows, wide), proj, attn, taps_both[layer], marks, tables
        )
        back_flat = back_proj.reshape(total, 2 * wide)
        partial = (back_proj, w_mix[layer])
        summed, _, into[:1], (grad_mix, grad_o) = communicate(
            7 + layer,
            partial=partial,
            scatter=(layer, [by_seq(grad_gu)]),
            into=into[:1] if layer == 0 else (),
            products=((normed, back_flat), (back_branch, gated_flat)),
        )
        made = [by_seq(grad_d), by_seq(grad_mix), by_seq(grad_o)]
        _, norm_back_one = jax.vjp(rms_norm, x, gains_one[layer])
        back_x, gain_one = norm_back_one(spread(summed))
        grad = (back_middle + back_x).astype(jnp.bfloat16)
        back[layer] = grad
        smalls[layer] = (gain_one, gain_two, taps_grad)
    gains = jnp.stack([smalls[0][0], smalls[1][0], smalls[0][1], smalls[1][1]])
    taps_rows = jnp.concatenate([smalls[0][2][:KW], smalls[1][2][:KW]])
    packed = jnp.concatenate(
        [
            jnp.pad(gains, ((0, 4), (0, 0))),
            jnp.pad(taps_rows, ((0, 8 - 2 * KW), (0, width - wide))),
        ]
    )
    summed, _, into[1:], (gains, taps_rows) = communicate(
        9, partial=last_partial, scatter=(0, made), into=into[1:], small=(packed, wide)
    )
    outputs.append((kept[1][5] + spread(summed)).astype(jnp.bfloat16))
    grad_gu, grad_d, grad_mix, grad_o = [
        jnp.sum(received.astype(jnp.float32), axis=1).reshape((2, -1) + received.shape[3:])
        for received in into
    ]

    def joined(pair):
        return jnp.concatenate([pair[0], pair[1]], axis=1)

    grad_value = joined(grad_mix[:, :, :values])
    grad_query = joined(grad_mix[:, :, values:wide])
    grad_gconv = joined(grad_mix[:, :, wide : wide + values])
    grad_key = joined(grad_mix[:, :, wide + values :])
    grad_out = joined(grad_o[:, :, :values]).T
    grad_gate = joined(grad_gu[:, :, :hidden_cols])
    grad_up = joined(grad_gu[:, :, hidden_cols:])
    grad_down = joined(grad_d).T

    gains = lax.dynamic_index_in_dim(gains[:4].reshape(2, 2, width), core, 1, False)
    taps_rows = lax.dynamic_index_in_dim(
        taps_rows[:, : 2 * KW, :values].reshape(-1, 2, KW, values), core, 1, False
    )
    grad_taps = jnp.transpose(taps_rows, (1, 0, 2)).reshape(KW, width)

    def chosen(pair):
        return jnp.where(core == 0, pair[0], pair[1]).reshape(1, micro_count, rows, width)

    return (
        chosen(outputs),
        chosen(back),
        gains[0][None],
        grad_query[None],
        grad_key[None],
        grad_value[None],
        grad_gconv[None],
        grad_taps[None],
        grad_out[None],
        gains[1][None],
        grad_gate[None],
        grad_up[None],
        grad_down[None],
    )


def solution(mesh):
    placed = (
        P(None, "seq", None),
        P(),
        P("section", None),
        P("section", "seq", "head"),
        P("section", "seq", "head"),
        P("section", "seq", "head"),
        P("section", "seq", "head"),
        P("section", None, None),
        P("section", "head", "seq"),
        P("section", None),
        P("section", "seq", "head"),
        P("section", "seq", "head"),
        P("section", "head", "seq"),
        P(None, "seq", None),
    )
    return jax.shard_map(
        on_device,
        mesh=mesh,
        in_specs=placed,
        out_specs=(
            P("section", None, "seq", None),
            P("section", None, "seq", None),
            P("section", None),
            P("section", "seq", "head"),
            P("section", "seq", "head"),
            P("section", "seq", "head"),
            P("section", "seq", "head"),
            P("section", None, None),
            P("section", "head", "seq"),
            P("section", None),
            P("section", "seq", "head"),
            P("section", "seq", "head"),
            P("section", "head", "seq"),
        ),
        check_vma=False,
    )
```

```python
import functools
import math

import jax
import jax.numpy as jnp
from jax import lax
from jax.experimental import pallas as pl
from jax.experimental.pallas import tpu as pltpu
import numpy as np
from jax.sharding import PartitionSpec as P

FK = 16
KW = 3
MESH = pl.DeviceIdType.MESH
epsilon = 1e-05


def remote(src, dst, send, recv, **where):
    return pltpu.make_async_remote_copy(
        src_ref=src,
        dst_ref=dst,
        send_sem=send,
        recv_sem=recv,
        device_id=where,
        device_id_type=MESH,
    )


def greet(line, spread, everyone):
    core, z, q = lax.axis_index("section"), lax.axis_index("head"), lax.axis_index("seq")
    depth, count = lax.axis_size("head"), lax.axis_size("seq")
    barrier = pltpu.get_barrier_semaphore()

    def hello(**where):
        pl.semaphore_signal(barrier, inc=1, device_id=where, device_id_type=MESH)

    hello(section=1 - core)
    expected = 1
    if spread:
        for j in range(1, count):
            for h in range(2):
                hello(section=h, seq=lax.rem(q + j, count))
        expected += 2 * (count - 1)
    if everyone:
        for j in range(1, depth):
            for h in range(2):
                hello(section=h, head=lax.rem(z + j, depth))
        expected += 2 * (depth - 1)
    elif line:

        @pl.when(z > 0)
        def _():
            hello(head=z - 1)

        @pl.when(z < depth - 1)
        def _():
            hello(head=z + 1)

        expected = expected + jnp.where(z > 0, 1, 0) + jnp.where(z < depth - 1, 1, 0)
    pl.semaphore_wait(barrier, expected)


PIECES = 4
FIRST_TILE = 8
LEAD = 3


class LineSum:
    def __init__(self, lhs, w, o_ref, scratch, chunks, lag):
        self.lhs, self.w, self.o_ref, self.chunks, self.lag = lhs, w, o_ref, chunks, lag
        self.p_ref, self.pin, self.low, self.high, self.out = scratch[:5]
        self.ps, self.pr, self.rs, self.rl, self.rh, self.bs, self.br, self.ts, self.tr = scratch[5:]
        self.z, self.n = lax.axis_index("head"), lax.axis_size("head")
        self.core = lax.axis_index("section")
        self.half = lhs.shape[1] // 2
        self.step = self.half // chunks
        self.depth = max((self.n - 1) // 2, self.n - 1 - (self.n - 1) // 2)
        self.turns = chunks + 2 * self.depth * lag

    @staticmethod
    def scratch(rows, width, chunks):
        dma = pltpu.SemaphoreType.DMA
        each = dma((2, chunks))
        whole = pltpu.VMEM((2, rows, width), jnp.bfloat16)
        return [whole] + [pltpu.VMEM((rows, width), jnp.bfloat16)] * 4 + [
            dma((1,)), dma((2, PIECES)), dma((2,)), each, each, dma((2, 2)), each, dma((1,)), dma((1,))
        ]

    def root(self, d):
        return (self.n - 1) // 2 if d == 0 else self.n - 1 - (self.n - 1) // 2

    def rng(self, d, k):
        return pl.ds(pl.multiple_of(d * self.half + k * self.step, self.step), self.step)

    def part(self, d, k):
        size = self.half // PIECES
        r = pl.ds(pl.multiple_of(d * self.half + k * size, size), size)
        other = 1 - self.core
        return remote(
            self.p_ref.at[other, r], self.pin.at[r], self.ps.at[0], self.pr.at[d, k], section=other
        )

    def up(self, d, k):
        r = self.rng(d, k)
        return remote(
            self.out.at[r], self.low.at[r], self.rs.at[d], self.rl.at[d, k], head=self.z + 1
        )

    def down(self, d, k):
        r = self.rng(d, k)
        return remote(
            self.out.at[r], self.high.at[r], self.rs.at[d], self.rh.at[d, k], head=self.z - 1
        )

    def share(self, d, k, side):
        r = self.rng(d, k)
        at = self.o_ref.at[self.core, r]
        return remote(
            at, at, self.bs.at[side, d], self.br.at[d, k], head=self.z + (1 if side else -1)
        )

    def give(self, d, k):
        r = self.rng(d, k)
        at = self.o_ref.at[self.core, r]
        return remote(at, at, self.ts.at[0], self.tr.at[0], section=1 - self.core)

    def make(self, i):
        size = self.half // PIECES
        places = [
            (m, pl.ds(pl.multiple_of(d * self.half + i * size, size), size))
            for m in range(2)
            for d in range(2)
        ]
        left = jnp.concatenate([self.lhs[m, r, :] for m, r in places], axis=0)
        made = lax.dot_general(
            left, self.w[...], (((1,), (1,)), ((), ())), preferred_element_type=jnp.float32
        ).astype(jnp.bfloat16)
        for at, (m, r) in enumerate(places):
            self.p_ref[m, r, :] = made[at * size : (at + 1) * size]
        for d in range(2):
            self.part(d, i).start()

    def gathered(self, d, k):
        r = self.rng(d, k)
        z, n, root = self.z, self.n, self.root(d)
        group = self.chunks // PIECES

        @pl.when(k % group == 0)
        def _():
            self.part(d, k // group).wait_recv()

        mine = self.p_ref[self.core, r, :].astype(jnp.float32) + self.pin[r, :].astype(jnp.float32)

        @pl.when((z == 0) & (root > 0))
        def _():
            self.out[r, :] = mine.astype(jnp.bfloat16)
            self.up(d, k).start()

        @pl.when((z == n - 1) & (root < n - 1))
        def _():
            self.out[r, :] = mine.astype(jnp.bfloat16)
            self.down(d, k).start()

        @pl.when((z > 0) & (z < root))
        def _():
            self.up(d, k).wait_recv()
            self.out[r, :] = (mine + self.low[r, :].astype(jnp.float32)).astype(jnp.bfloat16)
            self.up(d, k).start()

        @pl.when((z < n - 1) & (z > root))
        def _():
            self.down(d, k).wait_recv()
            self.out[r, :] = (mine + self.high[r, :].astype(jnp.float32)).astype(jnp.bfloat16)
            self.down(d, k).start()

        @pl.when(z == root)
        def _():
            total = mine
            if root > 0:
                self.up(d, k).wait_recv()
                total = total + self.low[r, :].astype(jnp.float32)
            if root < n - 1:
                self.down(d, k).wait_recv()
                total = total + self.high[r, :].astype(jnp.float32)
            self.o_ref[self.core, r, :] = total.astype(jnp.bfloat16)
            if root > 0:
                self.share(d, k, 0).start()
            if root < n - 1:
                self.share(d, k, 1).start()
            self.give(d, k).start()

    def passed(self, d, k):
        z, n, root = self.z, self.n, self.root(d)
        self.share(d, k, 0).wait_recv()

        @pl.when((z < root) & (z > 0))
        def _():
            self.share(d, k, 0).start()

        @pl.when((z > root) & (z < n - 1))
        def _():
            self.share(d, k, 1).start()

        self.give(d, k).start()

    def turn(self, t):
        z, n = self.z, self.n
        for d in range(2):
            root = self.root(d)
            deep = max(root, n - 1 - root)
            below = jnp.where(z < root, z, jnp.where(z > root, n - 1 - z, deep))
            k = t - below * self.lag
            far = jnp.abs(z - root)

            @pl.when((k >= 0) & (k < self.chunks))
            def _():
                self.gathered(d, k)

            b = t - (deep + far) * self.lag

            @pl.when((b >= 0) & (b < self.chunks) & (far > 0))
            def _():
                self.passed(d, b)

    def finish(self):
        z, n, other = self.z, self.n, 1 - self.core
        remote(
            self.p_ref.at[other], self.pin, self.ps.at[0], self.pr.at[0, 0], section=other
        ).wait_send()
        mine = self.o_ref.at[self.core]
        given = remote(mine, mine, self.ts.at[0], self.tr.at[0], section=other)
        given.wait_recv()
        given.wait_send()
        for d in range(2):
            root = self.root(d)
            r = pl.ds(d * self.half, self.half)
            at = self.o_ref.at[self.core, r]

            def summed(head):
                return remote(
                    self.out.at[r], self.low.at[r], self.rs.at[d], self.rl.at[d, 0], head=head
                )

            def shared(side):
                return remote(
                    at, at, self.bs.at[side, d], self.br.at[d, 0], head=z + (1 if side else -1)
                )

            @pl.when(z < root)
            def _():
                summed(z + 1).wait_send()

            @pl.when(z > root)
            def _():
                summed(z - 1).wait_send()

            if root > 0:

                @pl.when((z <= root) & (z > 0))
                def _():
                    shared(0).wait_send()

            if root < n - 1:

                @pl.when((z >= root) & (z < n - 1))
                def _():
                    shared(1).wait_send()


class Gather:
    def __init__(self, layer, srcs, dsts, sems):
        self.layer, self.srcs, self.dsts = layer, srcs, dsts
        self.ss, self.rr, self.ls, self.fs, self.fr = sems
        self.core, self.q = lax.axis_index("section"), lax.axis_index("seq")
        self.n = lax.axis_size("seq")
        self.square = self.n == 4

    @staticmethod
    def scratch(count, n):
        dma = pltpu.SemaphoreType.DMA
        return [dma((count, n, 2)), dma((count, n)), dma((count,)), dma((count, 2)), dma((count, 2))]

    def peer(self, j):
        if not self.square:
            return lax.rem(self.q + j, self.n)
        x, y = self.q % 2, self.q // 2
        x, y = (1 - x if j % 2 else x), (1 - y if j // 2 else y)
        return y * 2 + x

    def direct(self):
        return range(1, 3 if self.square else self.n)

    def copies(self, a):
        for j in self.direct():
            for h in range(2):
                yield remote(
                    self.srcs[a].at[h], self.dsts[a].at[self.q], self.ss.at[a, j, h],
                    self.rr.at[a, self.q], section=h, seq=self.peer(j),
                )
        yield remote(
            self.srcs[a].at[1 - self.layer], self.dsts[a].at[self.q], self.ss.at[a, 0, 0],
            self.rr.at[a, self.q], section=1 - self.layer,
        )

    def local(self, a):
        return pltpu.make_async_copy(
            self.srcs[a].at[self.layer], self.dsts[a].at[self.q], self.ls.at[a]
        )

    def arrival(self, a, s):
        return remote(
            self.srcs[a].at[0], self.dsts[a].at[s], self.ss.at[a, 0, 0], self.rr.at[a, s],
            section=1 - self.core,
        )

    def relay(self, a, i):
        size = self.srcs[a].shape[1] // 2
        at = self.dsts[a].at[self.peer(1 + i), pl.ds(i * size, size)]
        return remote(at, at, self.fs.at[a, i], self.fr.at[a, i], seq=self.peer(2 - i))

    def corner(self, a, i):
        size = self.srcs[a].shape[1] // 2
        at = self.dsts[a].at[self.peer(3), pl.ds(i * size, size)]
        return remote(at, at, self.fs.at[a, i], self.fr.at[a, i], seq=self.peer(2 - i))

    def start(self):
        @pl.when(self.core == self.layer)
        def _():
            for a in range(len(self.srcs)):
                for copy in self.copies(a):
                    copy.start()
                self.local(a).start()

    def due(self):
        sent, turns = 0, []
        for src in self.srcs:
            sent += 2 * src.shape[1] * src.shape[2] * 2
            turns.append(3 + sent // 200_000)
        return turns

    def middle(self, a):
        for j in self.direct():
            self.arrival(a, self.peer(j)).wait_recv()
            if self.square:
                self.relay(a, j - 1).start()

    def finish(self):
        for a in range(len(self.srcs)):
            if self.square:
                for i in range(2):
                    self.corner(a, i).wait_recv()
                    self.relay(a, i).wait_send()

            @pl.when(self.core == self.layer)
            def _():
                self.local(a).wait()
                for copy in self.copies(a):
                    copy.wait_send()

            @pl.when(self.core != self.layer)
            def _():
                self.arrival(a, self.q).wait_recv()


class SmallSum:
    def __init__(self, g_ref, total, spread, scratch):
        self.g_ref, self.total, self.spread = g_ref, total, spread
        self.got, self.src, self.ss, self.sr, self.ts, self.tr = scratch
        self.core, self.q, self.z = (lax.axis_index(a) for a in ("section", "seq", "head"))
        self.n, self.depth = lax.axis_size("seq"), lax.axis_size("head")

    @staticmethod
    def scratch(shape, narrow, n, depth):
        dma = pltpu.SemaphoreType.DMA
        return [
            pltpu.VMEM((n,) + shape, jnp.float32),
            pltpu.VMEM((8, narrow), jnp.float32),
            dma((n,)),
            dma((n,)),
            dma((2 * depth,)),
            dma((2 * depth,)),
        ]

    def first(self, j):
        return remote(
            self.g_ref, self.got.at[self.q], self.ss.at[j], self.sr.at[self.q],
            seq=lax.rem(self.q + j, self.n),
        )

    def others(self):
        for j in range(self.depth):
            for flip in range(2):
                if j or flip:
                    core = 1 - self.core if flip else self.core
                    yield 2 * j + flip, lax.rem(self.z + j, self.depth), core

    def second(self, i, z, core):
        slot = self.z * 2 + self.core
        return remote(
            self.src, self.spread.at[slot], self.ts.at[i], self.tr.at[slot], head=z, section=core
        )

    def start(self):
        for j in range(1, self.n):
            self.first(j).start()
        self.got[self.q] = self.g_ref[...]

    def middle(self):
        for j in range(1, self.n):
            s = lax.rem(self.q + j, self.n)
            remote(
                self.g_ref, self.got.at[s], self.ss.at[j], self.sr.at[s], seq=s
            ).wait_recv()
        summed = self.got[0]
        for s in range(1, self.n):
            summed = summed + self.got[s]
        self.total[...] = summed[:8]
        own = summed[8:, : self.src.shape[1]]
        self.src[...] = own
        self.spread[self.z * 2 + self.core] = own
        for i, z, core in self.others():
            self.second(i, z, core).start()

    def finish(self):
        for i, z, core in self.others():
            slot = z * 2 + core
            remote(
                self.src, self.spread.at[slot], self.ts.at[i], self.tr.at[slot], head=z, section=core
            ).wait_recv()
            self.second(i, z, core).wait_send()
        for j in range(1, self.n):
            self.first(j).wait_send()


class Scatter:
    def __init__(self, layer, srcs, dsts, sems):
        self.layer, self.srcs, self.dsts = layer, srcs, dsts
        self.ss, self.rr, self.ls = sems
        self.core, self.q = lax.axis_index("section"), lax.axis_index("seq")
        self.n = lax.axis_size("seq")

    @staticmethod
    def scratch(count, n):
        return [
            pltpu.SemaphoreType.DMA((count, n)),
            pltpu.SemaphoreType.DMA((count, 2, n)),
            pltpu.SemaphoreType.DMA((count,)),
        ]

    def copies(self, a):
        for j in range(1, self.n):
            t = lax.rem(self.q + j, self.n)
            yield remote(
                self.srcs[a].at[t], self.dsts[a].at[self.core, self.q], self.ss.at[a, j],
                self.rr.at[a, self.core, self.q], section=self.layer, seq=t,
            )

    def near(self, a):
        return remote(
            self.srcs[a].at[self.q], self.dsts[a].at[self.core, self.q], self.ss.at[a, 0],
            self.rr.at[a, self.core, self.q], section=self.layer,
        )

    def local(self, a):
        return pltpu.make_async_copy(
            self.srcs[a].at[self.q], self.dsts[a].at[self.core, self.q], self.ls.at[a]
        )

    def arrival(self, a, h, s):
        return remote(
            self.srcs[a].at[self.q], self.dsts[a].at[h, s], self.ss.at[a, 0], self.rr.at[a, h, s],
            section=1 - self.core,
        )

    def start(self):
        for a in range(len(self.srcs)):
            for copy in self.copies(a):
                copy.start()

            @pl.when(self.core == self.layer)
            def _():
                self.local(a).start()

            @pl.when(self.core != self.layer)
            def _():
                self.near(a).start()

    def finish(self):
        for a in range(len(self.srcs)):

            @pl.when(self.core == self.layer)
            def _():
                for j in range(1, self.n):
                    for h in range(2):
                        self.arrival(a, h, lax.rem(self.q + j, self.n)).wait_recv()
                self.arrival(a, 1 - self.layer, self.q).wait_recv()
                self.local(a).wait()

            @pl.when(self.core != self.layer)
            def _():
                self.near(a).wait_send()

            for copy in self.copies(a):
                copy.wait_send()


TILE = 256


class Product:
    def __init__(self, lhs, rhs, out, scratch):
        self.lhs, self.rhs, self.out = lhs, rhs, out
        self.left, self.right, self.stage, self.loads, self.stores = scratch
        self.tiles = lhs.shape[1] // TILE

    @staticmethod
    def scratch(lhs, rhs):
        return [
            pltpu.VMEM(lhs.shape, jnp.bfloat16),
            pltpu.VMEM(rhs.shape, jnp.bfloat16),
            pltpu.VMEM((2, TILE, rhs.shape[1]), jnp.bfloat16),
            pltpu.SemaphoreType.DMA((2,)),
            pltpu.SemaphoreType.DMA((2,)),
        ]

    def load(self, side):
        src, dst = ((self.lhs, self.left), (self.rhs, self.right))[side]
        return pltpu.make_async_copy(src, dst, self.loads.at[side])

    def store(self, i):
        at = pl.ds(pl.multiple_of(i * TILE, TILE), TILE)
        return pltpu.make_async_copy(self.stage.at[i % 2], self.out.at[at], self.stores.at[i % 2])

    def start(self):
        self.load(0).start()
        self.load(1).start()

    def step(self, i):
        @pl.when(i == 0)
        def _():
            self.load(0).wait()
            self.load(1).wait()

        @pl.when(i >= 2)
        def _():
            self.store(i - 2).wait()

        at = pl.ds(pl.multiple_of(i * TILE, TILE), TILE)
        self.stage[i % 2] = lax.dot_general(
            self.left[:, at],
            self.right[...],
            (((0,), (0,)), ((), ())),
            preferred_element_type=jnp.float32,
        ).astype(jnp.bfloat16)
        self.store(i).start()

    def finish(self):
        for i in range(max(self.tiles - 2, 0), self.tiles):
            self.store(i).wait()


def comm_kernel(plan, *refs):
    has_sum, layer_in, count_in, layer_out, count_out, kept, count_made, small_in, chunks, lag = plan
    refs = list(refs)

    def take(count):
        taken = refs[:count]
        del refs[:count]
        return taken

    p_in, w_in, g_in, _, m_in, s_in = (
        take(2 * has_sum), take(count_in), take(count_out), take(kept), take(2 * count_made),
        take(small_in),
    )
    p_out, w_out, g_out, m_out, s_out = (
        take(has_sum), take(count_in), take(count_out), take(count_made), take(2 * small_in)
    )
    greet(has_sum, count_in + count_out > 0, small_in)
    jobs = []
    later = []
    if has_sum:
        line = LineSum(p_in[0], p_in[1], p_out[0], take(14), chunks, lag)
    if count_in:
        weights = Gather(layer_in, w_in, w_out, take(5))
        jobs.append(weights)
        for a, turn in enumerate(weights.due()):
            later.append((turn, functools.partial(weights.middle, a)))
    if count_out:
        jobs.append(Scatter(layer_out, g_in, g_out, take(3)))
    made = [
        Product(m_in[2 * i], m_in[2 * i + 1], m_out[i], take(5)) for i in range(count_made)
    ]
    if small_in:
        small = SmallSum(s_in[0], s_out[0], s_out[1], take(6))
        jobs.insert(0, small)
        later.append((12, small.middle))
    for job in made + jobs:
        job.start()
    if has_sum:
        tiles = sum(product.tiles for product in made)

        def turn(t, carry):
            @pl.when((t < LEAD * PIECES) & (t % LEAD == 0))
            def _():
                line.make(t // LEAD)

            line.turn(t - LEAD)
            i = t - LEAD - FIRST_TILE
            for product in made:

                @pl.when((i >= 0) & (i < product.tiles))
                def _(product=product, i=i):
                    product.step(i)

                i = i - product.tiles
            for when, act in later:

                @pl.when(t == when + LEAD)
                def _(act=act):
                    act()

            return carry

        last = max([line.turns, tiles + FIRST_TILE] + [when + 1 for when, _ in later])
        lax.fori_loop(0, last + LEAD, turn, 0)
        line.finish()
    else:
        for _, act in later:
            act()
    for job in made + jobs:
        job.finish()


def communicate(
    cid, partial=None, gather=None, scatter=None, into=(), products=(), small=None, chunks=16, lag=2
):
    n = lax.axis_size("seq")
    layer_in, w_in = gather if gather else (0, [])
    layer_out, g_in = scatter if scatter else (0, [])
    p_in = [] if partial is None else list(partial)
    has_sum = 0 if partial is None else 1
    if has_sum:
        summed = (partial[0].shape[0], partial[0].shape[1], partial[1].shape[0])
    m_in = [a for pair in products for a in pair]
    vmem, anywhere = pl.BlockSpec(memory_space=pltpu.VMEM), pl.BlockSpec(memory_space=pl.ANY)
    scratch = []
    if p_in:
        scratch += LineSum.scratch(summed[1], summed[2], chunks)
    if w_in:
        scratch += Gather.scratch(len(w_in), n)
    if g_in:
        scratch += Scatter.scratch(len(g_in), n)
    for pair in products:
        scratch += Product.scratch(*pair)
    s_in, s_shapes = [], []
    if small is not None:
        s_in, narrow, depth = [small[0]], small[1], lax.axis_size("head")
        scratch += SmallSum.scratch(small[0].shape, narrow, n, depth)
        s_shapes = [
            jax.ShapeDtypeStruct((8, small[0].shape[1]), jnp.float32),
            jax.ShapeDtypeStruct((2 * depth, 8, narrow), jnp.float32),
        ]
    shapes = (
        ([jax.ShapeDtypeStruct(summed, jnp.bfloat16)] if has_sum else [])
        + [jax.ShapeDtypeStruct((n,) + w.shape[1:], jnp.bfloat16) for w in w_in]
        + [jax.ShapeDtypeStruct((2,) + g.shape, jnp.bfloat16) for g in g_in]
        + [jax.ShapeDtypeStruct((a.shape[1], b.shape[1]), jnp.bfloat16) for a, b in products]
        + s_shapes
    )
    plan = (
        has_sum, layer_in, len(w_in), layer_out, len(g_in), len(into), len(products), len(s_in),
        chunks, lag,
    )
    first = len(p_in) + len(w_in)
    first_out = has_sum + len(w_in)
    outs = pl.pallas_call(
        functools.partial(comm_kernel, plan),
        out_shape=shapes,
        in_specs=[vmem] * first
        + [anywhere] * (len(g_in) + len(into) + len(m_in))
        + [vmem] * len(s_in),
        out_specs=[vmem] * has_sum
        + [anywhere] * (len(w_in) + len(g_in) + len(products))
        + [vmem] * len(s_shapes),
        scratch_shapes=scratch,
        input_output_aliases={first + len(g_in) + i: first_out + i for i in range(len(into))},
        name=f"comm{cid}",
        compiler_params=pltpu.CompilerParams(
            collective_id=cid, has_side_effects=True, vmem_limit_bytes=52 << 20
        ),
    )(*p_in, *w_in, *g_in, *into, *m_in, *s_in)
    return (
        outs[0] if p_in else None,
        [a.reshape((-1,) + a.shape[2:]) for a in outs[has_sum : first_out]],
        outs[first_out : first_out + len(g_in)],
        outs[first_out + len(g_in) :],
    )


def rms_norm(vector, scale_gain):
    return (
        vector * lax.rsqrt(jnp.mean(vector * vector, axis=-1, keepdims=True) + epsilon) * scale_gain
    )


def seq_begin(lengths_row, positions):
    seq_starts = jnp.cumsum(lengths_row) - lengths_row
    chosen = jnp.where(seq_starts[None, :] <= positions[:, None], seq_starts[None, :], 0)
    return jnp.max(chosen, axis=1)


HEADS = 2
PAIRS = FK * (FK + 1) // 2
STATE = 160
BLOCK = 128


def feature_tables(values):
    wide = values + HEADS * FK
    first = np.zeros((HEADS, wide, wide), np.float32)
    second = np.zeros((HEADS, wide, wide), np.float32)
    rest = np.zeros((8, wide), np.float32)
    for h in range(HEADS):
        at = values + h * FK
        lane = 0
        for a in range(FK):
            for b in range(a, FK):
                first[h, at + a, lane] = 1
                second[h, at + b, lane] = 1
                rest[2, lane] = 0.25 if a < b else 1 / (4.0 * math.sqrt(2.0))
                lane += 1
        for a in range(FK):
            first[h, at + a, lane] = 1
            rest[1, lane] = 1
            rest[2, lane] = 0.5
            lane += 1
        rest[0, lane] = rest[1, lane] = rest[2, lane] = 1
    return np.stack([first, second], axis=1), rest


def mm(a, b):
    return lax.dot_general(a, b, (((1,), (0,)), ((), ())), preferred_element_type=jnp.float32)


def mm_nt(a, b):
    return lax.dot_general(a, b, (((1,), (1,)), ((), ())), preferred_element_type=jnp.float32)


def mm_tn(a, b):
    return lax.dot_general(a, b, (((0,), (0,)), ((), ())), preferred_element_type=jnp.float32)


class Lanes:
    def __init__(self, wide, values):
        self.values = values
        self.lane = lax.broadcasted_iota(jnp.int32, (1, wide), 1)
        lane, dim = self.lane, values // HEADS
        self.is_value = lane < values
        self.is_one = (lane >= values) & (lane < values + 2 * HEADS)
        self.head = jnp.where(
            self.is_value, jnp.where(lane < dim, 0, 1), jnp.where(self.is_one, (lane - values) % 2, 9)
        )

    def of(self, h, x):
        return jnp.where(self.head == h, x, jnp.zeros_like(x))

    def key(self, h, x):
        at = self.values + h * FK
        return jnp.where((self.lane >= at) & (self.lane < at + FK), x, jnp.zeros_like(x))

    def extended(self, a):
        return jnp.where(
            self.is_value, a, jnp.where(self.is_one, jnp.ones_like(a), jnp.zeros_like(a))
        )

    def column(self, x, index):
        return jnp.sum(
            jnp.where(self.lane == self.values + index, x, 0.0), axis=1, keepdims=True
        )

    def denominator(self, x):
        return jnp.where(
            self.lane < self.values // HEADS, self.column(x, 0), self.column(x, 1)
        )


def meet(direction, reach):
    q, n = lax.axis_index("seq"), lax.axis_size("seq")
    barrier = pltpu.get_barrier_semaphore()
    count = 0
    for d in range(1, reach + 1):
        source = q - direction * d
        target = q + direction * d

        @pl.when((source >= 0) & (source < n))
        def _():
            pl.semaphore_signal(barrier, inc=1, device_id={"seq": source}, device_id_type=MESH)

        count = count + jnp.where((target >= 0) & (target < n), 1, 0)

    @pl.when(count > 0)
    def _():
        pl.semaphore_wait(barrier, count)


class Pass:
    def __init__(self, direction, reach, src, dst, send, recv):
        self.direction, self.reach = direction, reach
        self.src, self.dst, self.send, self.recv = src, dst, send, recv
        self.q, self.n = lax.axis_index("seq"), lax.axis_size("seq")

    def has_source(self, d):
        at = self.q - self.direction * d
        return (at >= 0) & (at < self.n)

    def has_target(self, d):
        at = self.q + self.direction * d
        return (at >= 0) & (at < self.n)

    def copy(self, d):
        return remote(
            self.src, self.dst.at[d - 1], self.send.at[d - 1], self.recv.at[d - 1],
            seq=self.q + self.direction * d,
        )

    def start(self):
        for d in range(1, self.reach + 1):

            @pl.when(self.has_target(d))
            def _():
                self.copy(d).start()

    def arrived(self):
        for d in range(1, self.reach + 1):

            @pl.when(self.has_source(d))
            def _():
                self.copy(d).wait_recv()

    def sent(self):
        for d in range(1, self.reach + 1):

            @pl.when(self.has_target(d))
            def _():
                self.copy(d).wait_send()


def sum_states(states, coef, total):
    for m in range(2):
        total[m] = jnp.zeros(total.shape[1:], total.dtype)
        for d in range(1, states.reach + 1):

            @pl.when(states.has_source(d))
            def _():
                total[m, :STATE, :] += coef[d - 1, m] * states.dst[d - 1, m].astype(jnp.float32)


def shifted(a, tail, fresh, by):
    row = lax.broadcasted_iota(jnp.int32, (a.shape[0], 1), 0)
    moved = pltpu.roll(a, by, 0)
    rows = tail.shape[0]
    for r in range(by):
        edge = jnp.where(fresh, tail[rows - by + r : rows - by + r + 1, :], 0.0)
        moved = jnp.where(row == r, edge, moved)
    return moved


def attn_forward_kernel(
    reach, proj, col, row, coef, e, c, taps, gated, att, conv, sin, edge, acc, phi, s_acc, s_src,
    s_all, s_sum, e_src, ss, sr, es, er,
):
    q = lax.axis_index("seq")
    rows, wide = proj.shape[1], proj.shape[2] // 2
    values = wide - HEADS * FK
    lanes = Lanes(wide, values)
    meet(1, reach)
    states = Pass(1, reach, s_src, s_all, ss, sr)
    edges = Pass(1, 1, e_src, edge, es, er)

    def sides(m):
        return proj[m, :, :wide].astype(jnp.bfloat16), proj[m, :, wide:].astype(jnp.bfloat16)

    def phi_of(a, h):
        return (mm(a, e[h, 0]) + c[0:1, :]) * (mm(a, e[h, 1]) + c[1:2, :]) * c[2:3, :]

    def make_state(i, carry):
        m, h = i // HEADS, i % HEADS
        a, b = sides(m)
        phi[m, h] = (phi_of(a, h) * col[m, :, 1:2]).astype(jnp.bfloat16)
        keyed = (phi_of(b, h) * col[m, :, 2:3]).astype(jnp.bfloat16)
        part = mm_tn(keyed, lanes.of(h, lanes.extended(a)))

        @pl.when(h == 0)
        def _():
            s_acc[m] = part

        @pl.when(h > 0)
        def _():
            s_acc[m] += part

        return carry

    lax.fori_loop(0, 2 * HEADS, make_state, 0)
    for m in range(2):
        s_src[m] = s_acc[m, :STATE, :].astype(jnp.bfloat16)
    states.start()

    def make_block(i, carry):
        m, h = i // HEADS, i % HEADS
        a, b = sides(m)
        asked = lanes.key(h, a)
        valued = lanes.of(h, lanes.extended(a))
        for r in range(rows // BLOCK):
            lo, hi = r * BLOCK, (r + 1) * BLOCK
            x = mm_nt(asked[lo:hi], b[:hi]) * 0.25
            seen = (col[m, lo:hi, 0:1] == row[m, 0:1, :hi]) & (
                lax.broadcasted_iota(jnp.int32, (BLOCK, hi), 1)
                <= lo + lax.broadcasted_iota(jnp.int32, (BLOCK, hi), 0)
            )
            w = jnp.where(seen, 1.0 + x + 0.5 * x * x, 0.0).astype(jnp.bfloat16)
            part = mm(w, valued[:hi])

            @pl.when(h == 0)
            def _():
                acc[m, lo:hi, :] = part

            @pl.when(h > 0)
            def _():
                acc[m, lo:hi, :] += part

        return carry

    lax.fori_loop(0, 2 * HEADS, make_block, 0)
    states.arrived()
    sum_states(states, coef, s_sum)

    def attend(m, lo):
        s = s_sum[m].astype(jnp.bfloat16)
        both = acc[m, lo:, :]
        for h in range(HEADS):
            both = both + mm(phi[m, h, lo:, :], lanes.of(h, s))
        return jnp.where(lanes.is_value, both / lanes.denominator(both), both)

    for m in range(2):
        sin[m] = s_sum[m, :STATE, :].astype(jnp.bfloat16)
        e_src[m] = attend(m, rows - 16)
    edges.start()
    for m in range(2):
        att[m] = attend(m, 0)
    edges.arrived()
    for m in range(2):
        a = att[m]
        tail = edge[0, m]
        out = taps[0:1, :] * a
        for by in (1, 2):
            out = out + taps[by : by + 1, :] * shifted(a, tail, q > 0, by) * col[m, :, 2 + by : 3 + by]
        conv[m] = out
        gated[m] = (out * proj[m, :, wide:]).astype(jnp.bfloat16)
    states.sent()
    edges.sent()


def attn_backward_kernel(
    reach, bg, proj, att, conv, sin, edge, col, row, coef, late, e, c, taps, out, grad_taps,
    phi_q, phi_k, near, acc_a, acc_b, s_acc, s_src, s_all, s_sum, e_src, e_dst, ss, sr, es, er,
):
    q, n = lax.axis_index("seq"), lax.axis_size("seq")
    rows, wide = proj.shape[1], proj.shape[2] // 2
    values = wide - HEADS * FK
    lanes = Lanes(wide, values)
    meet(-1, reach)
    states = Pass(-1, reach, s_src, s_all, ss, sr)
    edges = Pass(-1, 1, e_src, e_dst, es, er)
    for m in range(2):
        e_src[m] = bg[m, :16, :] * proj[m, :16, wide:]
    edges.start()

    def sides(m):
        return proj[m, :, :wide].astype(jnp.bfloat16), proj[m, :, wide:].astype(jnp.bfloat16)

    def factors(a, h):
        return mm(a, e[h, 0]) + c[0:1, :], mm(a, e[h, 1]) + c[1:2, :]

    def make_phi(i, carry):
        m, h = i // HEADS, i % HEADS
        a, b = sides(m)
        u, w = factors(a, h)
        phi_q[m, h] = (u * w * c[2:3, :] * col[m, :, 1:2]).astype(jnp.bfloat16)
        u, w = factors(b, h)
        phi_k[m, h] = (u * w * c[2:3, :] * col[m, :, 2:3]).astype(jnp.bfloat16)
        return carry

    lax.fori_loop(0, 2 * HEADS, make_phi, 0)
    edges.arrived()
    sums = [jnp.zeros((1, wide), jnp.float32)] * KW
    place = lax.broadcasted_iota(jnp.int32, (rows, 1), 0)
    for m in range(2):
        back = bg[m]
        back_conv = back * proj[m, :, wide:]
        a = jnp.where(lanes.is_value, att[m], 0.0)
        tail = edge[0, m]
        nxt = e_dst[0, m]
        total = taps[0:1, :] * back_conv
        sums[0] = sums[0] + jnp.sum(back_conv * a, axis=0, keepdims=True)
        for by in (1, 2):
            kept = back_conv * col[m, :, 2 + by : 3 + by]
            sums[by] = sums[by] + jnp.sum(
                kept * shifted(a, tail, q > 0, by), axis=0, keepdims=True
            )
            moved = pltpu.roll(kept, rows - by, 0)
            for r in range(by):
                fresh = jnp.where(q < n - 1, nxt[r : r + 1, :] * late[by - 1 + r, m], 0.0)
                moved = jnp.where(place == rows - by + r, fresh, moved)
            total = total + taps[by : by + 1, :] * moved
        out[m, :, wide:] = jnp.where(lanes.is_value, back * conv[m], 0.0).astype(jnp.bfloat16)
        back_numer = total / lanes.denominator(att[m])
        spent = back_numer * a
        found = jnp.where(lanes.is_value, back_numer, 0.0)
        for h in range(HEADS):
            denom = -jnp.sum(lanes.of(h, spent), axis=1, keepdims=True)
            high = denom.astype(jnp.bfloat16).astype(jnp.float32)
            found = jnp.where(lanes.lane == values + h, high, found)
            found = jnp.where(lanes.lane == values + 2 + h, denom - high, found)
        near[m] = found.astype(jnp.bfloat16)
        part = jnp.zeros((wide, wide), jnp.float32)
        for h in range(HEADS):
            part = part + mm_tn(phi_q[m, h], lanes.of(h, near[m]))
        s_src[m] = part[:STATE].astype(jnp.bfloat16)
    states.start()
    grad_taps[...] = jnp.zeros(grad_taps.shape, jnp.float32)
    for by in range(KW):
        grad_taps[by : by + 1, :] = sums[by]
    acc_a[...] = jnp.zeros(acc_a.shape, jnp.float32)
    acc_b[...] = jnp.zeros(acc_b.shape, jnp.float32)
    for m in range(2):
        s_sum[m] = jnp.zeros(s_sum.shape[1:], jnp.float32)
        s_sum[m, :STATE, :] = sin[m].astype(jnp.float32)

    def through_phi(scaled, factors_of, h):
        u, w = factors_of
        return mm_nt((scaled * w).astype(jnp.bfloat16), e[h, 0]) + mm_nt(
            (scaled * u).astype(jnp.bfloat16), e[h, 1]
        )

    def make_block(i, carry):
        m, h = i // HEADS, i % HEADS
        a, b = sides(m)
        asked, keyed = lanes.key(h, a), lanes.key(h, b)
        valued = lanes.extended(a)
        given = lanes.of(h, near[m])
        given_v = jnp.where(lanes.is_value, given, jnp.zeros_like(given))
        for r in range(rows // BLOCK):
            lo, hi = r * BLOCK, (r + 1) * BLOCK
            x = mm_nt(asked[lo:hi], b[:hi]) * 0.25
            seen = (col[m, lo:hi, 0:1] == row[m, 0:1, :hi]) & (
                lax.broadcasted_iota(jnp.int32, (BLOCK, hi), 1)
                <= lo + lax.broadcasted_iota(jnp.int32, (BLOCK, hi), 0)
            )
            w = jnp.where(seen, 1.0 + x + 0.5 * x * x, 0.0).astype(jnp.bfloat16)
            back_w = mm_nt(given[lo:hi], valued[:hi])
            back_s = jnp.where(seen, back_w * (1.0 + x), 0.0).astype(jnp.bfloat16)
            acc_a[m, lo:hi, :] += 0.25 * mm(back_s, keyed[:hi])
            acc_b[m, :hi, :] += 0.25 * mm_tn(back_s, asked[lo:hi])
            acc_a[m, :hi, :] += mm_tn(w, given_v[lo:hi])
        s = s_sum[m].astype(jnp.bfloat16)
        scaled = mm_nt(given, s) * col[m, :, 1:2] * c[2:3, :]
        acc_a[m] += through_phi(scaled, factors(a, h), h)
        return carry

    lax.fori_loop(0, 2 * HEADS, make_block, 0)
    states.arrived()
    sum_states(states, coef, s_sum)

    def make_late(i, carry):
        m, h = i // HEADS, i % HEADS
        a, b = sides(m)
        s = s_sum[m].astype(jnp.bfloat16)
        scaled = mm_nt(lanes.of(h, lanes.extended(a)), s) * col[m, :, 2:3] * c[2:3, :]
        acc_b[m] += through_phi(scaled, factors(b, h), h)
        s_v = lanes.of(h, jnp.where(lanes.is_value, s, jnp.zeros_like(s)))
        acc_a[m] += mm(phi_k[m, h], s_v)
        return carry

    lax.fori_loop(0, 2 * HEADS, make_late, 0)
    for m in range(2):
        out[m, :, :wide] = acc_a[m].astype(jnp.bfloat16)
        out[m, :, wide:] = jnp.where(
            lanes.is_value, out[m, :, wide:].astype(jnp.float32), acc_b[m]
        ).astype(jnp.bfloat16)
    states.sent()
    edges.sent()


def seq_reach():
    n = lax.axis_size("seq")
    return n // 2 if n % 2 == 0 else n - 1


def attention_call(kernel, cid, inputs, scalars, shapes, scratch):
    vmem, smem = pl.BlockSpec(memory_space=pltpu.VMEM), pl.BlockSpec(memory_space=pltpu.SMEM)
    return pl.pallas_call(
        functools.partial(kernel, seq_reach()),
        out_shape=shapes,
        in_specs=[smem if i in scalars else vmem for i in range(len(inputs))],
        out_specs=[vmem] * len(shapes),
        scratch_shapes=scratch,
        name=f"attention{cid}",
        compiler_params=pltpu.CompilerParams(
            collective_id=cid, has_side_effects=True, vmem_limit_bytes=48 << 20
        ),
    )(*inputs)


def passing(reach, wide):
    dma = pltpu.SemaphoreType.DMA
    return (
        [
            pltpu.VMEM((2, STATE, wide), jnp.bfloat16),
            pltpu.VMEM((reach, 2, STATE, wide), jnp.bfloat16),
            pltpu.VMEM((2, wide, wide), jnp.float32),
        ],
        [dma((reach,)), dma((reach,)), dma((1,)), dma((1,))],
    )


def attention_forward(proj, taps, marks, tables):
    m, rows, double = proj.shape
    wide = double // 2
    f32, bf16 = jnp.float32, jnp.bfloat16
    buffers, sems = passing(seq_reach(), wide)
    shape = jax.ShapeDtypeStruct
    return attention_call(
        attn_forward_kernel,
        10,
        [proj, marks["col"], marks["row"], marks["before"], *tables, taps],
        (3,),
        [
            shape((m, rows, wide), bf16),
            shape((m, rows, wide), f32),
            shape((m, rows, wide), f32),
            shape((m, STATE, wide), bf16),
            shape((1, m, 16, wide), f32),
        ],
        [
            pltpu.VMEM((m, rows, wide), f32),
            pltpu.VMEM((m, HEADS, rows, wide), bf16),
            pltpu.VMEM((m, wide, wide), f32),
            *buffers,
            pltpu.VMEM((m, 16, wide), f32),
            *sems,
        ],
    )


def attention_backward(back_gated, proj, kept, taps, marks, tables):
    att, conv, sin, edge = kept
    m, rows, double = proj.shape
    wide = double // 2
    f32, bf16 = jnp.float32, jnp.bfloat16
    buffers, sems = passing(seq_reach(), wide)
    shape = jax.ShapeDtypeStruct
    return attention_call(
        attn_backward_kernel,
        11,
        [
            back_gated, proj, att, conv, sin, edge, marks["col"], marks["row"], marks["after"],
            marks["late"], *tables, taps,
        ],
        (8, 9),
        [shape((m, rows, double), bf16), shape((8, wide), f32)],
        [
            pltpu.VMEM((m, HEADS, rows, wide), bf16),
            pltpu.VMEM((m, HEADS, rows, wide), bf16),
            pltpu.VMEM((m, rows, wide), bf16),
            pltpu.VMEM((m, rows, wide), f32),
            pltpu.VMEM((m, rows, wide), f32),
            pltpu.VMEM((m, wide, wide), f32),
            *buffers,
            pltpu.VMEM((m, 16, wide), f32),
            pltpu.VMEM((1, m, 16, wide), f32),
            *sems,
        ],
    )


def sequence_marks(lengths, rows):
    count, mine = lax.axis_size("seq"), lax.axis_index("seq")
    start = mine * rows
    positions = start + jnp.arange(rows + 2, dtype=jnp.int32)
    begin_ext = jax.vmap(lambda row: seq_begin(row, positions))(lengths)
    begin = begin_ext[:, :rows]
    ends = (jnp.arange(count, dtype=jnp.int32) + 1) * rows - 1
    stays = jax.vmap(lambda row: seq_begin(row, ends))(lengths) < (ends - rows + 1)[None, :]
    stays = stays.astype(jnp.float32)
    blocks = jnp.arange(count, dtype=jnp.int32)

    def through(first, last):
        inside = (blocks >= first) & (blocks <= last)
        return jnp.min(jnp.where(inside[None, :], stays, 1.0), axis=1)

    reach = seq_reach()
    before = [through(mine - d + 1, mine - 1) for d in range(1, reach + 1)]
    after = [through(mine + 1, mine + d - 1) for d in range(1, reach + 1)]
    allowed = [(positions - j >= begin_ext).astype(jnp.float32) for j in range(KW)]
    columns = [
        begin.astype(jnp.float32),
        (begin < start).astype(jnp.float32),
        (begin == begin[:, rows - 1 :]).astype(jnp.float32),
        allowed[1][:, :rows],
        allowed[2][:, :rows],
    ]
    col = jnp.stack(columns + [jnp.zeros_like(columns[0])] * 3, axis=2)
    return {
        "col": col,
        "row": jnp.broadcast_to(columns[0][:, None, :], (2, 8, rows)),
        "before": jnp.stack(before),
        "after": jnp.stack(after),
        "late": jnp.stack([allowed[1][:, rows], allowed[2][:, rows], allowed[2][:, rows + 1]]),
    }


def by_seq(grad):
    n = lax.axis_size("seq")
    return grad.reshape((n, grad.shape[0] // n) + grad.shape[1:])


def held(a):
    return lax.optimization_barrier(a.astype(jnp.bfloat16))


def dot_n(a, b):
    return jnp.dot(a, b, preferred_element_type=jnp.float32)


def on_device(
    tokens,
    lengths,
    gain_attn,
    w_query,
    w_key,
    w_value,
    w_gate_conv,
    conv_taps,
    w_out,
    gain_ffn,
    w_gate,
    w_up,
    w_down,
    cotangent,
):
    head_index = lax.axis_index("head")
    core = lax.axis_index("section")
    micro_count, rows, width = tokens.shape
    total = micro_count * rows

    def halves(weight):
        middle = weight.shape[1] // 2
        return jnp.stack([weight[:, :middle], weight[:, middle:]])

    own_mix = jnp.concatenate(
        [halves(w[0]) for w in (w_value, w_query, w_gate_conv, w_key)], axis=2
    )
    values = w_value.shape[2] // 2
    keys = w_query.shape[2] // 2
    wide = values + keys
    own_out = jnp.pad(halves(w_out[0].T), ((0, 0), (0, 0), (0, keys)))
    cols = w_gate.shape[2] // 2

    def filled(half):
        return jnp.pad(half, ((0, 0), (0, 0), (0, -cols % 128)))

    own_ffn = jnp.concatenate([filled(halves(w_gate[0])), filled(halves(w_up[0]))], axis=2)
    own_down = filled(halves(w_down[0].T))
    gains_one = lax.all_gather(gain_attn[0], "section").astype(jnp.float32)
    gains_two = lax.all_gather(gain_ffn[0], "section").astype(jnp.float32)
    taps_all = lax.all_gather(conv_taps[0], "section").astype(jnp.float32)
    taps_both = lax.dynamic_slice_in_dim(taps_all, (head_index * 2 + core) * values, values, 2)
    taps_both = jnp.pad(taps_both, ((0, 0), (0, 8 - KW), (0, keys)))
    first, rest = feature_tables(values)
    tables = (jnp.asarray(first, jnp.bfloat16), jnp.asarray(rest))
    marks = sequence_marks(lengths, rows)
    hidden_cols = own_down.shape[2]

    def as_parts(flat):
        return flat.reshape(micro_count, rows, -1)

    def spread(summed):
        return summed.astype(jnp.float32).reshape(total, width)

    _, (mix_0, out_0), _, _ = communicate(1, gather=(0, [own_mix, own_out]))
    w_mix, w_o, w_gu, w_d = [mix_0, None], [out_0, None], [None, None], [None, None]
    x = tokens.reshape(total, width).astype(jnp.float32)
    kept = [None, None]
    outputs = []
    last_partial = None
    for layer in range(2):
        normed = rms_norm(x, gains_one[layer]).astype(jnp.bfloat16)
        proj = dot_n(normed, w_mix[layer]).reshape(micro_count, rows, 2 * wide)
        gated, *attn = attention_forward(proj, taps_both[layer], marks, tables)
        gated_flat = gated.reshape(total, wide)
        partial = (gated, w_o[layer])
        if layer == 0:
            summed, (w_gu[0], w_d[0]), _, _ = communicate(
                2, partial=partial, gather=(0, [own_ffn, own_down])
            )
        else:
            summed, (w_gu[1],), _, _ = communicate(3, partial=partial, gather=(1, [own_ffn]))
        middle = x + spread(summed)
        normed_two = rms_norm(middle, gains_two[layer]).astype(jnp.bfloat16)
        middle = held(middle).astype(jnp.float32)
        both = held(dot_n(normed_two, w_gu[layer])).astype(jnp.float32)
        hidden = (jax.nn.silu(both[:, :hidden_cols]) * both[:, hidden_cols:]).astype(jnp.bfloat16)
        partial = (as_parts(hidden), w_d[layer])
        kept[layer] = (x, normed, proj, gated_flat, attn, middle, normed_two, both, hidden)
        if layer == 0:
            summed, (w_mix[1], w_o[1], w_d[1]), _, _ = communicate(
                4, partial=partial, gather=(1, [own_mix, own_out, own_down])
            )
            outputs.append(held(middle + spread(summed)))
            x = outputs[0].astype(jnp.float32)
        else:
            last_partial = partial

    grad = cotangent.reshape(total, width)
    back = [None, None]
    smalls = [None, None]
    made = []
    into = [None] * 4
    for layer in (1, 0):
        x, normed, proj, gated_flat, attn, middle, normed_two, both, hidden = kept[layer]
        grad_wide = grad.astype(jnp.float32)
        back_hidden = dot_n(grad, w_d[layer])
        gate_pre, upward = both[:, :hidden_cols], both[:, hidden_cols:]
        silu_value, silu_back = jax.vjp(jax.nn.silu, gate_pre)
        back_both = jnp.concatenate(
            [
                silu_back(back_hidden * upward)[0].astype(jnp.bfloat16),
                (back_hidden * silu_value).astype(jnp.bfloat16),
            ],
            axis=1,
        )
        partial = (as_parts(back_both), w_gu[layer])
        products = ((normed_two, back_both), (grad, hidden))
        if layer == 1:
            summed, _, _, (grad_gu, grad_d) = communicate(5, partial=partial, products=products)
        else:
            summed, _, into[1:], (grad_gu, grad_d) = communicate(
                6, partial=partial, scatter=(1, made), products=products
            )
        _, norm_back_two = jax.vjp(rms_norm, middle, gains_two[layer])
        back_middle, gain_two = norm_back_two(spread(summed))
        back_middle = grad_wide + back_middle
        back_branch = held(back_middle)
        back_middle = back_branch.astype(jnp.float32)
        back_gated = dot_n(back_branch, w_o[layer])
        back_proj, taps_grad = attention_backward(
            back_gated.reshape(micro_count, rows, wide), proj, attn, taps_both[layer], marks, tables
        )
        back_flat = back_proj.reshape(total, 2 * wide)
        partial = (back_proj, w_mix[layer])
        summed, _, into[:1], (grad_mix, grad_o) = communicate(
            7 + layer,
            partial=partial,
            scatter=(layer, [by_seq(grad_gu)]),
            into=into[:1] if layer == 0 else (),
            products=((normed, back_flat), (back_branch, gated_flat)),
        )
        made = [by_seq(grad_d), by_seq(grad_mix), by_seq(grad_o)]
        _, norm_back_one = jax.vjp(rms_norm, x, gains_one[layer])
        back_x, gain_one = norm_back_one(spread(summed))
        grad = (back_middle + back_x).astype(jnp.bfloat16)
        back[layer] = grad
        smalls[layer] = (gain_one, gain_two, taps_grad)
    gains = jnp.stack([smalls[0][0], smalls[1][0], smalls[0][1], smalls[1][1]])
    taps_rows = jnp.concatenate([smalls[0][2][:KW], smalls[1][2][:KW]])
    packed = jnp.concatenate(
        [
            jnp.pad(gains, ((0, 4), (0, 0))),
            jnp.pad(taps_rows, ((0, 8 - 2 * KW), (0, width - wide))),
        ]
    )
    summed, _, into[1:], (gains, taps_rows) = communicate(
        9, partial=last_partial, scatter=(0, made), into=into[1:], small=(packed, wide)
    )
    outputs.append((kept[1][5] + spread(summed)).astype(jnp.bfloat16))
    grad_gu, grad_d, grad_mix, grad_o = [
        jnp.sum(received.astype(jnp.float32), axis=1).reshape((2, -1) + received.shape[3:])
        for received in into
    ]

    def joined(pair):
        return jnp.concatenate([pair[0], pair[1]], axis=1)

    grad_value = joined(grad_mix[:, :, :values])
    grad_query = joined(grad_mix[:, :, values:wide])
    grad_gconv = joined(grad_mix[:, :, wide : wide + values])
    grad_key = joined(grad_mix[:, :, wide + values :])
    grad_out = joined(grad_o[:, :, :values]).T
    grad_gate = joined(grad_gu[:, :, :cols])
    grad_up = joined(grad_gu[:, :, hidden_cols : hidden_cols + cols])
    grad_down = joined(grad_d[:, :, :cols]).T

    gains = lax.dynamic_index_in_dim(gains[:4].reshape(2, 2, width), core, 1, False)
    taps_rows = lax.dynamic_index_in_dim(
        taps_rows[:, : 2 * KW, :values].reshape(-1, 2, KW, values), core, 1, False
    )
    grad_taps = jnp.transpose(taps_rows, (1, 0, 2)).reshape(KW, width)

    def chosen(pair):
        return jnp.where(core == 0, pair[0], pair[1]).reshape(1, micro_count, rows, width)

    return (
        chosen(outputs),
        chosen(back),
        gains[0][None],
        grad_query[None],
        grad_key[None],
        grad_value[None],
        grad_gconv[None],
        grad_taps[None],
        grad_out[None],
        gains[1][None],
        grad_gate[None],
        grad_up[None],
        grad_down[None],
    )


def solution(mesh):
    placed = (
        P(None, "seq", None),
        P(),
        P("section", None),
        P("section", "seq", "head"),
        P("section", "seq", "head"),
        P("section", "seq", "head"),
        P("section", "seq", "head"),
        P("section", None, None),
        P("section", "head", "seq"),
        P("section", None),
        P("section", "seq", "head"),
        P("section", "seq", "head"),
        P("section", "head", "seq"),
        P(None, "seq", None),
    )
    return jax.shard_map(
        on_device,
        mesh=mesh,
        in_specs=placed,
        out_specs=(
            P("section", None, "seq", None),
            P("section", None, "seq", None),
            P("section", None),
            P("section", "seq", "head"),
            P("section", "seq", "head"),
            P("section", "seq", "head"),
            P("section", "seq", "head"),
            P("section", None, None),
            P("section", "head", "seq"),
            P("section", None),
            P("section", "seq", "head"),
            P("section", "seq", "head"),
            P("section", "head", "seq"),
        ),
        check_vma=False,
    )
```

```python
import functools
import math

import jax
import jax.numpy as jnp
from jax import lax
from jax.experimental import pallas as pl
from jax.experimental.pallas import tpu as pltpu
import numpy as np
from jax.sharding import PartitionSpec as P

FK = 16
KW = 3
MESH = pl.DeviceIdType.MESH
epsilon = 1e-05


def remote(src, dst, send, recv, **where):
    return pltpu.make_async_remote_copy(
        src_ref=src,
        dst_ref=dst,
        send_sem=send,
        recv_sem=recv,
        device_id=where,
        device_id_type=MESH,
    )


def greet(line, spread, everyone):
    core, z, q = lax.axis_index("section"), lax.axis_index("head"), lax.axis_index("seq")
    depth, count = lax.axis_size("head"), lax.axis_size("seq")
    barrier = pltpu.get_barrier_semaphore()

    def hello(**where):
        pl.semaphore_signal(barrier, inc=1, device_id=where, device_id_type=MESH)

    hello(section=1 - core)
    expected = 1
    if spread:
        for j in range(1, count):
            for h in range(2):
                hello(section=h, seq=lax.rem(q + j, count))
        expected += 2 * (count - 1)
    if everyone:
        for j in range(1, depth):
            for h in range(2):
                hello(section=h, head=lax.rem(z + j, depth))
        expected += 2 * (depth - 1)
    elif line:

        @pl.when(z > 0)
        def _():
            hello(head=z - 1)

        @pl.when(z < depth - 1)
        def _():
            hello(head=z + 1)

        expected = expected + jnp.where(z > 0, 1, 0) + jnp.where(z < depth - 1, 1, 0)
    pl.semaphore_wait(barrier, expected)


PIECES = 4
FIRST_TILE = 8
LEAD = 3


class LineSum:
    def __init__(self, lhs, w, o_ref, scratch, chunks, lag):
        self.lhs, self.w, self.o_ref, self.chunks, self.lag = lhs, w, o_ref, chunks, lag
        self.p_ref, self.pin, self.low, self.high, self.out = scratch[:5]
        self.ps, self.pr, self.rs, self.rl, self.rh, self.bs, self.br, self.ts, self.tr = scratch[5:]
        self.z, self.n = lax.axis_index("head"), lax.axis_size("head")
        self.core = lax.axis_index("section")
        self.half = lhs.shape[1] // 2
        self.step = self.half // chunks
        self.depth = max((self.n - 1) // 2, self.n - 1 - (self.n - 1) // 2)
        self.turns = chunks + 2 * self.depth * lag

    @staticmethod
    def scratch(rows, width, chunks):
        dma = pltpu.SemaphoreType.DMA
        each = dma((2, chunks))
        whole = pltpu.VMEM((2, rows, width), jnp.bfloat16)
        return [whole] + [pltpu.VMEM((rows, width), jnp.bfloat16)] * 4 + [
            dma((1,)), dma((2, PIECES)), dma((2,)), each, each, dma((2, 2)), each, dma((1,)), dma((1,))
        ]

    def root(self, d):
        return (self.n - 1) // 2 if d == 0 else self.n - 1 - (self.n - 1) // 2

    def rng(self, d, k):
        return pl.ds(pl.multiple_of(d * self.half + k * self.step, self.step), self.step)

    def part(self, d, k):
        size = self.half // PIECES
        r = pl.ds(pl.multiple_of(d * self.half + k * size, size), size)
        other = 1 - self.core
        return remote(
            self.p_ref.at[other, r], self.pin.at[r], self.ps.at[0], self.pr.at[d, k], section=other
        )

    def up(self, d, k):
        r = self.rng(d, k)
        return remote(
            self.out.at[r], self.low.at[r], self.rs.at[d], self.rl.at[d, k], head=self.z + 1
        )

    def down(self, d, k):
        r = self.rng(d, k)
        return remote(
            self.out.at[r], self.high.at[r], self.rs.at[d], self.rh.at[d, k], head=self.z - 1
        )

    def share(self, d, k, side):
        r = self.rng(d, k)
        at = self.o_ref.at[self.core, r]
        return remote(
            at, at, self.bs.at[side, d], self.br.at[d, k], head=self.z + (1 if side else -1)
        )

    def give(self, d, k):
        r = self.rng(d, k)
        at = self.o_ref.at[self.core, r]
        return remote(at, at, self.ts.at[0], self.tr.at[0], section=1 - self.core)

    def make(self, i):
        size = self.half // PIECES
        places = [
            (m, pl.ds(pl.multiple_of(d * self.half + i * size, size), size))
            for m in range(2)
            for d in range(2)
        ]
        left = jnp.concatenate([self.lhs[m, r, :] for m, r in places], axis=0)
        made = lax.dot_general(
            left, self.w[...], (((1,), (1,)), ((), ())), preferred_element_type=jnp.float32
        ).astype(jnp.bfloat16)
        for at, (m, r) in enumerate(places):
            self.p_ref[m, r, :] = made[at * size : (at + 1) * size]
        for d in range(2):
            self.part(d, i).start()

    def gathered(self, d, k):
        r = self.rng(d, k)
        z, n, root = self.z, self.n, self.root(d)
        group = self.chunks // PIECES

        @pl.when(k % group == 0)
        def _():
            self.part(d, k // group).wait_recv()

        mine = self.p_ref[self.core, r, :].astype(jnp.float32) + self.pin[r, :].astype(jnp.float32)

        @pl.when((z == 0) & (root > 0))
        def _():
            self.out[r, :] = mine.astype(jnp.bfloat16)
            self.up(d, k).start()

        @pl.when((z == n - 1) & (root < n - 1))
        def _():
            self.out[r, :] = mine.astype(jnp.bfloat16)
            self.down(d, k).start()

        @pl.when((z > 0) & (z < root))
        def _():
            self.up(d, k).wait_recv()
            self.out[r, :] = (mine + self.low[r, :].astype(jnp.float32)).astype(jnp.bfloat16)
            self.up(d, k).start()

        @pl.when((z < n - 1) & (z > root))
        def _():
            self.down(d, k).wait_recv()
            self.out[r, :] = (mine + self.high[r, :].astype(jnp.float32)).astype(jnp.bfloat16)
            self.down(d, k).start()

        @pl.when(z == root)
        def _():
            total = mine
            if root > 0:
                self.up(d, k).wait_recv()
                total = total + self.low[r, :].astype(jnp.float32)
            if root < n - 1:
                self.down(d, k).wait_recv()
                total = total + self.high[r, :].astype(jnp.float32)
            self.o_ref[self.core, r, :] = total.astype(jnp.bfloat16)
            if root > 0:
                self.share(d, k, 0).start()
            if root < n - 1:
                self.share(d, k, 1).start()
            self.give(d, k).start()

    def passed(self, d, k):
        z, n, root = self.z, self.n, self.root(d)
        self.share(d, k, 0).wait_recv()

        @pl.when((z < root) & (z > 0))
        def _():
            self.share(d, k, 0).start()

        @pl.when((z > root) & (z < n - 1))
        def _():
            self.share(d, k, 1).start()

        self.give(d, k).start()

    def turn(self, t):
        z, n = self.z, self.n
        for d in range(2):
            root = self.root(d)
            deep = max(root, n - 1 - root)
            below = jnp.where(z < root, z, jnp.where(z > root, n - 1 - z, deep))
            k = t - below * self.lag
            far = jnp.abs(z - root)

            @pl.when((k >= 0) & (k < self.chunks))
            def _():
                self.gathered(d, k)

            b = t - (deep + far) * self.lag

            @pl.when((b >= 0) & (b < self.chunks) & (far > 0))
            def _():
                self.passed(d, b)

    def finish(self):
        z, n, other = self.z, self.n, 1 - self.core
        remote(
            self.p_ref.at[other], self.pin, self.ps.at[0], self.pr.at[0, 0], section=other
        ).wait_send()
        mine = self.o_ref.at[self.core]
        given = remote(mine, mine, self.ts.at[0], self.tr.at[0], section=other)
        given.wait_recv()
        given.wait_send()
        for d in range(2):
            root = self.root(d)
            r = pl.ds(d * self.half, self.half)
            at = self.o_ref.at[self.core, r]

            def summed(head):
                return remote(
                    self.out.at[r], self.low.at[r], self.rs.at[d], self.rl.at[d, 0], head=head
                )

            def shared(side):
                return remote(
                    at, at, self.bs.at[side, d], self.br.at[d, 0], head=z + (1 if side else -1)
                )

            @pl.when(z < root)
            def _():
                summed(z + 1).wait_send()

            @pl.when(z > root)
            def _():
                summed(z - 1).wait_send()

            if root > 0:

                @pl.when((z <= root) & (z > 0))
                def _():
                    shared(0).wait_send()

            if root < n - 1:

                @pl.when((z >= root) & (z < n - 1))
                def _():
                    shared(1).wait_send()


class Gather:
    def __init__(self, layer, srcs, dsts, sems):
        self.layer, self.srcs, self.dsts = layer, srcs, dsts
        self.ss, self.rr, self.ls, self.fs, self.fr = sems
        self.core, self.q = lax.axis_index("section"), lax.axis_index("seq")
        self.n = lax.axis_size("seq")
        self.square = self.n == 4

    @staticmethod
    def scratch(count, n):
        dma = pltpu.SemaphoreType.DMA
        return [dma((count, n, 2)), dma((count, n)), dma((count,)), dma((count, 2)), dma((count, 2))]

    def peer(self, j):
        if not self.square:
            return lax.rem(self.q + j, self.n)
        x, y = self.q % 2, self.q // 2
        x, y = (1 - x if j % 2 else x), (1 - y if j // 2 else y)
        return y * 2 + x

    def direct(self):
        return range(1, 3 if self.square else self.n)

    def copies(self, a):
        for j in self.direct():
            for h in range(2):
                yield remote(
                    self.srcs[a].at[h], self.dsts[a].at[self.q], self.ss.at[a, j, h],
                    self.rr.at[a, self.q], section=h, seq=self.peer(j),
                )
        yield remote(
            self.srcs[a].at[1 - self.layer], self.dsts[a].at[self.q], self.ss.at[a, 0, 0],
            self.rr.at[a, self.q], section=1 - self.layer,
        )

    def local(self, a):
        return pltpu.make_async_copy(
            self.srcs[a].at[self.layer], self.dsts[a].at[self.q], self.ls.at[a]
        )

    def arrival(self, a, s):
        return remote(
            self.srcs[a].at[0], self.dsts[a].at[s], self.ss.at[a, 0, 0], self.rr.at[a, s],
            section=1 - self.core,
        )

    def relay(self, a, i):
        size = self.srcs[a].shape[1] // 2
        at = self.dsts[a].at[self.peer(1 + i), pl.ds(i * size, size)]
        return remote(at, at, self.fs.at[a, i], self.fr.at[a, i], seq=self.peer(2 - i))

    def corner(self, a, i):
        size = self.srcs[a].shape[1] // 2
        at = self.dsts[a].at[self.peer(3), pl.ds(i * size, size)]
        return remote(at, at, self.fs.at[a, i], self.fr.at[a, i], seq=self.peer(2 - i))

    def start(self):
        @pl.when(self.core == self.layer)
        def _():
            for a in range(len(self.srcs)):
                for copy in self.copies(a):
                    copy.start()
                self.local(a).start()

    def due(self):
        sent, turns = 0, []
        for src in self.srcs:
            sent += 2 * src.shape[1] * src.shape[2] * 2
            turns.append(3 + sent // 200_000)
        return turns

    def middle(self, a):
        for j in self.direct():
            self.arrival(a, self.peer(j)).wait_recv()
            if self.square:
                self.relay(a, j - 1).start()

    def finish(self):
        for a in range(len(self.srcs)):
            if self.square:
                for i in range(2):
                    self.corner(a, i).wait_recv()
                    self.relay(a, i).wait_send()

            @pl.when(self.core == self.layer)
            def _():
                self.local(a).wait()
                for copy in self.copies(a):
                    copy.wait_send()

            @pl.when(self.core != self.layer)
            def _():
                self.arrival(a, self.q).wait_recv()


class SmallSum:
    def __init__(self, g_ref, total, spread, scratch):
        self.g_ref, self.total, self.spread = g_ref, total, spread
        self.got, self.src, self.ss, self.sr, self.ts, self.tr = scratch
        self.core, self.q, self.z = (lax.axis_index(a) for a in ("section", "seq", "head"))
        self.n, self.depth = lax.axis_size("seq"), lax.axis_size("head")

    @staticmethod
    def scratch(shape, narrow, n, depth):
        dma = pltpu.SemaphoreType.DMA
        return [
            pltpu.VMEM((n,) + shape, jnp.float32),
            pltpu.VMEM((8, narrow), jnp.float32),
            dma((n,)),
            dma((n,)),
            dma((2 * depth,)),
            dma((2 * depth,)),
        ]

    def first(self, j):
        return remote(
            self.g_ref, self.got.at[self.q], self.ss.at[j], self.sr.at[self.q],
            seq=lax.rem(self.q + j, self.n),
        )

    def others(self):
        for j in range(self.depth):
            for flip in range(2):
                if j or flip:
                    core = 1 - self.core if flip else self.core
                    yield 2 * j + flip, lax.rem(self.z + j, self.depth), core

    def second(self, i, z, core):
        slot = self.z * 2 + self.core
        return remote(
            self.src, self.spread.at[slot], self.ts.at[i], self.tr.at[slot], head=z, section=core
        )

    def start(self):
        for j in range(1, self.n):
            self.first(j).start()
        self.got[self.q] = self.g_ref[...]

    def middle(self):
        for j in range(1, self.n):
            s = lax.rem(self.q + j, self.n)
            remote(
                self.g_ref, self.got.at[s], self.ss.at[j], self.sr.at[s], seq=s
            ).wait_recv()
        summed = self.got[0]
        for s in range(1, self.n):
            summed = summed + self.got[s]
        self.total[...] = summed[:8]
        own = summed[8:, : self.src.shape[1]]
        self.src[...] = own
        self.spread[self.z * 2 + self.core] = own
        for i, z, core in self.others():
            self.second(i, z, core).start()

    def finish(self):
        for i, z, core in self.others():
            slot = z * 2 + core
            remote(
                self.src, self.spread.at[slot], self.ts.at[i], self.tr.at[slot], head=z, section=core
            ).wait_recv()
            self.second(i, z, core).wait_send()
        for j in range(1, self.n):
            self.first(j).wait_send()


class Scatter:
    def __init__(self, layer, srcs, dsts, sems):
        self.layer, self.srcs, self.dsts = layer, srcs, dsts
        self.ss, self.rr, self.ls = sems
        self.core, self.q = lax.axis_index("section"), lax.axis_index("seq")
        self.n = lax.axis_size("seq")

    @staticmethod
    def scratch(count, n):
        return [
            pltpu.SemaphoreType.DMA((count, n)),
            pltpu.SemaphoreType.DMA((count, 2, n)),
            pltpu.SemaphoreType.DMA((count,)),
        ]

    def copies(self, a):
        for j in range(1, self.n):
            t = lax.rem(self.q + j, self.n)
            yield remote(
                self.srcs[a].at[t], self.dsts[a].at[self.core, self.q], self.ss.at[a, j],
                self.rr.at[a, self.core, self.q], section=self.layer, seq=t,
            )

    def near(self, a):
        return remote(
            self.srcs[a].at[self.q], self.dsts[a].at[self.core, self.q], self.ss.at[a, 0],
            self.rr.at[a, self.core, self.q], section=self.layer,
        )

    def local(self, a):
        return pltpu.make_async_copy(
            self.srcs[a].at[self.q], self.dsts[a].at[self.core, self.q], self.ls.at[a]
        )

    def arrival(self, a, h, s):
        return remote(
            self.srcs[a].at[self.q], self.dsts[a].at[h, s], self.ss.at[a, 0], self.rr.at[a, h, s],
            section=1 - self.core,
        )

    def start(self):
        for a in range(len(self.srcs)):
            for copy in self.copies(a):
                copy.start()

            @pl.when(self.core == self.layer)
            def _():
                self.local(a).start()

            @pl.when(self.core != self.layer)
            def _():
                self.near(a).start()

    def finish(self):
        for a in range(len(self.srcs)):

            @pl.when(self.core == self.layer)
            def _():
                for j in range(1, self.n):
                    for h in range(2):
                        self.arrival(a, h, lax.rem(self.q + j, self.n)).wait_recv()
                self.arrival(a, 1 - self.layer, self.q).wait_recv()
                self.local(a).wait()

            @pl.when(self.core != self.layer)
            def _():
                self.near(a).wait_send()

            for copy in self.copies(a):
                copy.wait_send()


TILE = 256


class Product:
    def __init__(self, lhs, rhs, out, scratch):
        self.lhs, self.rhs, self.out = lhs, rhs, out
        self.left, self.right, self.stage, self.loads, self.stores = scratch
        self.tiles = lhs.shape[1] // TILE

    @staticmethod
    def scratch(lhs, rhs):
        return [
            pltpu.VMEM(lhs.shape, jnp.bfloat16),
            pltpu.VMEM(rhs.shape, jnp.bfloat16),
            pltpu.VMEM((2, TILE, rhs.shape[1]), jnp.bfloat16),
            pltpu.SemaphoreType.DMA((2,)),
            pltpu.SemaphoreType.DMA((2,)),
        ]

    def load(self, side):
        src, dst = ((self.lhs, self.left), (self.rhs, self.right))[side]
        return pltpu.make_async_copy(src, dst, self.loads.at[side])

    def store(self, i):
        at = pl.ds(pl.multiple_of(i * TILE, TILE), TILE)
        return pltpu.make_async_copy(self.stage.at[i % 2], self.out.at[at], self.stores.at[i % 2])

    def start(self):
        self.load(0).start()
        self.load(1).start()

    def step(self, i):
        @pl.when(i == 0)
        def _():
            self.load(0).wait()
            self.load(1).wait()

        @pl.when(i >= 2)
        def _():
            self.store(i - 2).wait()

        at = pl.ds(pl.multiple_of(i * TILE, TILE), TILE)
        self.stage[i % 2] = lax.dot_general(
            self.left[:, at],
            self.right[...],
            (((0,), (0,)), ((), ())),
            preferred_element_type=jnp.float32,
        ).astype(jnp.bfloat16)
        self.store(i).start()

    def finish(self):
        for i in range(max(self.tiles - 2, 0), self.tiles):
            self.store(i).wait()


def comm_kernel(plan, *refs):
    has_sum, layer_in, count_in, layer_out, count_out, kept, count_made, small_in, chunks, lag = plan
    refs = list(refs)

    def take(count):
        taken = refs[:count]
        del refs[:count]
        return taken

    p_in, w_in, g_in, _, m_in, s_in = (
        take(2 * has_sum), take(count_in), take(count_out), take(kept), take(2 * count_made),
        take(small_in),
    )
    p_out, w_out, g_out, m_out, s_out = (
        take(has_sum), take(count_in), take(count_out), take(count_made), take(2 * small_in)
    )
    greet(has_sum, count_in + count_out > 0, small_in)
    jobs = []
    later = []
    if has_sum:
        line = LineSum(p_in[0], p_in[1], p_out[0], take(14), chunks, lag)
    if count_in:
        weights = Gather(layer_in, w_in, w_out, take(5))
        jobs.append(weights)
        for a, turn in enumerate(weights.due()):
            later.append((turn, functools.partial(weights.middle, a)))
    if count_out:
        jobs.append(Scatter(layer_out, g_in, g_out, take(3)))
    made = [
        Product(m_in[2 * i], m_in[2 * i + 1], m_out[i], take(5)) for i in range(count_made)
    ]
    if small_in:
        small = SmallSum(s_in[0], s_out[0], s_out[1], take(6))
        jobs.insert(0, small)
        later.append((12, small.middle))
    for job in made + jobs:
        job.start()
    if has_sum:
        tiles = sum(product.tiles for product in made)

        def turn(t, carry):
            @pl.when((t < LEAD * PIECES) & (t % LEAD == 0))
            def _():
                line.make(t // LEAD)

            line.turn(t - LEAD)
            i = t - LEAD - FIRST_TILE
            for product in made:

                @pl.when((i >= 0) & (i < product.tiles))
                def _(product=product, i=i):
                    product.step(i)

                i = i - product.tiles
            for when, act in later:

                @pl.when(t == when + LEAD)
                def _(act=act):
                    act()

            return carry

        last = max([line.turns, tiles + FIRST_TILE] + [when + 1 for when, _ in later])
        lax.fori_loop(0, last + LEAD, turn, 0)
        line.finish()
    else:
        for _, act in later:
            act()
    for job in made + jobs:
        job.finish()


def communicate(
    cid, partial=None, gather=None, scatter=None, into=(), products=(), small=None, chunks=16, lag=2
):
    n = lax.axis_size("seq")
    layer_in, w_in = gather if gather else (0, [])
    layer_out, g_in = scatter if scatter else (0, [])
    p_in = [] if partial is None else list(partial)
    has_sum = 0 if partial is None else 1
    if has_sum:
        summed = (partial[0].shape[0], partial[0].shape[1], partial[1].shape[0])
    m_in = [a for pair in products for a in pair]
    vmem, anywhere = pl.BlockSpec(memory_space=pltpu.VMEM), pl.BlockSpec(memory_space=pl.ANY)
    scratch = []
    if p_in:
        scratch += LineSum.scratch(summed[1], summed[2], chunks)
    if w_in:
        scratch += Gather.scratch(len(w_in), n)
    if g_in:
        scratch += Scatter.scratch(len(g_in), n)
    for pair in products:
        scratch += Product.scratch(*pair)
    s_in, s_shapes = [], []
    if small is not None:
        s_in, narrow, depth = [small[0]], small[1], lax.axis_size("head")
        scratch += SmallSum.scratch(small[0].shape, narrow, n, depth)
        s_shapes = [
            jax.ShapeDtypeStruct((8, small[0].shape[1]), jnp.float32),
            jax.ShapeDtypeStruct((2 * depth, 8, narrow), jnp.float32),
        ]
    shapes = (
        ([jax.ShapeDtypeStruct(summed, jnp.bfloat16)] if has_sum else [])
        + [jax.ShapeDtypeStruct((n,) + w.shape[1:], jnp.bfloat16) for w in w_in]
        + [jax.ShapeDtypeStruct((2,) + g.shape, jnp.bfloat16) for g in g_in]
        + [jax.ShapeDtypeStruct((a.shape[1], b.shape[1]), jnp.bfloat16) for a, b in products]
        + s_shapes
    )
    plan = (
        has_sum, layer_in, len(w_in), layer_out, len(g_in), len(into), len(products), len(s_in),
        chunks, lag,
    )
    first = len(p_in) + len(w_in)
    first_out = has_sum + len(w_in)
    outs = pl.pallas_call(
        functools.partial(comm_kernel, plan),
        out_shape=shapes,
        in_specs=[vmem] * first
        + [anywhere] * (len(g_in) + len(into) + len(m_in))
        + [vmem] * len(s_in),
        out_specs=[vmem] * has_sum
        + [anywhere] * (len(w_in) + len(g_in) + len(products))
        + [vmem] * len(s_shapes),
        scratch_shapes=scratch,
        input_output_aliases={first + len(g_in) + i: first_out + i for i in range(len(into))},
        name=f"comm{cid}",
        compiler_params=pltpu.CompilerParams(
            collective_id=cid, has_side_effects=True, vmem_limit_bytes=52 << 20
        ),
    )(*p_in, *w_in, *g_in, *into, *m_in, *s_in)
    return (
        outs[0] if p_in else None,
        [a.reshape((-1,) + a.shape[2:]) for a in outs[has_sum : first_out]],
        outs[first_out : first_out + len(g_in)],
        outs[first_out + len(g_in) :],
    )


def rms_norm(vector, scale_gain):
    return (
        vector * lax.rsqrt(jnp.mean(vector * vector, axis=-1, keepdims=True) + epsilon) * scale_gain
    )


def seq_begin(lengths_row, positions):
    seq_starts = jnp.cumsum(lengths_row) - lengths_row
    chosen = jnp.where(seq_starts[None, :] <= positions[:, None], seq_starts[None, :], 0)
    return jnp.max(chosen, axis=1)


HEADS = 2
PAIRS = FK * (FK + 1) // 2
STATE = 160
BLOCK = 128


def feature_tables(values):
    wide = values + HEADS * FK
    first = np.zeros((HEADS, wide, wide), np.float32)
    second = np.zeros((HEADS, wide, wide), np.float32)
    rest = np.zeros((8, wide), np.float32)
    for h in range(HEADS):
        at = values + h * FK
        lane = 0
        for a in range(FK):
            for b in range(a, FK):
                first[h, at + a, lane] = 1
                second[h, at + b, lane] = 1
                rest[2, lane] = 0.25 if a < b else 1 / (4.0 * math.sqrt(2.0))
                lane += 1
        for a in range(FK):
            first[h, at + a, lane] = 1
            rest[1, lane] = 1
            rest[2, lane] = 0.5
            lane += 1
        rest[0, lane] = rest[1, lane] = rest[2, lane] = 1
    return np.stack([first, second], axis=1), rest


def mm(a, b):
    return lax.dot_general(a, b, (((1,), (0,)), ((), ())), preferred_element_type=jnp.float32)


def mm_nt(a, b):
    return lax.dot_general(a, b, (((1,), (1,)), ((), ())), preferred_element_type=jnp.float32)


def mm_tn(a, b):
    return lax.dot_general(a, b, (((0,), (0,)), ((), ())), preferred_element_type=jnp.float32)


class Lanes:
    def __init__(self, wide, values):
        self.values = values
        self.lane = lax.broadcasted_iota(jnp.int32, (1, wide), 1)
        lane, dim = self.lane, values // HEADS
        self.is_value = lane < values
        self.is_one = (lane >= values) & (lane < values + 2 * HEADS)
        self.head = jnp.where(
            self.is_value, jnp.where(lane < dim, 0, 1), jnp.where(self.is_one, (lane - values) % 2, 9)
        )

    def of(self, h, x):
        return jnp.where(self.head == h, x, jnp.zeros_like(x))

    def key(self, h, x):
        at = self.values + h * FK
        return jnp.where((self.lane >= at) & (self.lane < at + FK), x, jnp.zeros_like(x))

    def extended(self, a):
        return jnp.where(
            self.is_value, a, jnp.where(self.is_one, jnp.ones_like(a), jnp.zeros_like(a))
        )

    def column(self, x, index):
        return jnp.sum(
            jnp.where(self.lane == self.values + index, x, 0.0), axis=1, keepdims=True
        )

    def denominator(self, x):
        return jnp.where(
            self.lane < self.values // HEADS, self.column(x, 0), self.column(x, 1)
        )


def meet(direction, reach):
    q, n = lax.axis_index("seq"), lax.axis_size("seq")
    barrier = pltpu.get_barrier_semaphore()
    count = 0
    for d in range(1, reach + 1):
        source = q - direction * d
        target = q + direction * d

        @pl.when((source >= 0) & (source < n))
        def _():
            pl.semaphore_signal(barrier, inc=1, device_id={"seq": source}, device_id_type=MESH)

        count = count + jnp.where((target >= 0) & (target < n), 1, 0)

    @pl.when(count > 0)
    def _():
        pl.semaphore_wait(barrier, count)


class Pass:
    def __init__(self, direction, reach, src, dst, send, recv):
        self.direction, self.reach = direction, reach
        self.src, self.dst, self.send, self.recv = src, dst, send, recv
        self.q, self.n = lax.axis_index("seq"), lax.axis_size("seq")

    def has_source(self, d):
        at = self.q - self.direction * d
        return (at >= 0) & (at < self.n)

    def has_target(self, d):
        at = self.q + self.direction * d
        return (at >= 0) & (at < self.n)

    def copy(self, d):
        return remote(
            self.src, self.dst.at[d - 1], self.send.at[d - 1], self.recv.at[d - 1],
            seq=self.q + self.direction * d,
        )

    def start(self):
        for d in range(1, self.reach + 1):

            @pl.when(self.has_target(d))
            def _():
                self.copy(d).start()

    def arrived(self):
        for d in range(1, self.reach + 1):

            @pl.when(self.has_source(d))
            def _():
                self.copy(d).wait_recv()

    def sent(self):
        for d in range(1, self.reach + 1):

            @pl.when(self.has_target(d))
            def _():
                self.copy(d).wait_send()


def sum_states(states, coef, total):
    for m in range(2):
        total[m] = jnp.zeros(total.shape[1:], total.dtype)
        for d in range(1, states.reach + 1):

            @pl.when(states.has_source(d))
            def _():
                total[m, :STATE, :] += coef[d - 1, m] * states.dst[d - 1, m].astype(jnp.float32)


def shifted(a, tail, fresh, by):
    row = lax.broadcasted_iota(jnp.int32, (a.shape[0], 1), 0)
    moved = pltpu.roll(a, by, 0)
    rows = tail.shape[0]
    for r in range(by):
        edge = jnp.where(fresh, tail[rows - by + r : rows - by + r + 1, :], 0.0)
        moved = jnp.where(row == r, edge, moved)
    return moved


def attn_forward_kernel(
    reach, proj, col, row, coef, e, c, taps, gated, att, conv, sin, edge, acc, phi, s_acc, s_src,
    s_all, s_sum, e_src, ss, sr, es, er,
):
    q = lax.axis_index("seq")
    rows, wide = proj.shape[1], proj.shape[2] // 2
    values = wide - HEADS * FK
    lanes = Lanes(wide, values)
    meet(1, reach)
    states = Pass(1, reach, s_src, s_all, ss, sr)
    edges = Pass(1, 1, e_src, edge, es, er)

    def sides(m):
        return proj[m, :, :wide].astype(jnp.bfloat16), proj[m, :, wide:].astype(jnp.bfloat16)

    def phi_of(a, h):
        return (mm(a, e[h, 0]) + c[0:1, :]) * (mm(a, e[h, 1]) + c[1:2, :]) * c[2:3, :]

    def make_state(i, carry):
        m, h = i // HEADS, i % HEADS
        a, b = sides(m)
        phi[m, h] = (phi_of(a, h) * col[m, :, 1:2]).astype(jnp.bfloat16)
        keyed = (phi_of(b, h) * col[m, :, 2:3]).astype(jnp.bfloat16)
        part = mm_tn(keyed, lanes.of(h, lanes.extended(a)))

        @pl.when(h == 0)
        def _():
            s_acc[m] = part

        @pl.when(h > 0)
        def _():
            s_acc[m] += part

        return carry

    lax.fori_loop(0, 2 * HEADS, make_state, 0)
    for m in range(2):
        s_src[m] = s_acc[m, :STATE, :].astype(jnp.bfloat16)
    states.start()

    def make_block(i, carry):
        m, h = i // HEADS, i % HEADS
        a, b = sides(m)
        asked = lanes.key(h, a)
        valued = lanes.of(h, lanes.extended(a))
        for r in range(rows // BLOCK):
            lo, hi = r * BLOCK, (r + 1) * BLOCK
            x = mm_nt(asked[lo:hi], b[:hi]) * 0.25
            seen = (col[m, lo:hi, 0:1] == row[m, 0:1, :hi]) & (
                lax.broadcasted_iota(jnp.int32, (BLOCK, hi), 1)
                <= lo + lax.broadcasted_iota(jnp.int32, (BLOCK, hi), 0)
            )
            w = jnp.where(seen, 1.0 + x + 0.5 * x * x, 0.0).astype(jnp.bfloat16)
            part = mm(w, valued[:hi])

            @pl.when(h == 0)
            def _():
                acc[m, lo:hi, :] = part

            @pl.when(h > 0)
            def _():
                acc[m, lo:hi, :] += part

        return carry

    lax.fori_loop(0, 2 * HEADS, make_block, 0)
    states.arrived()
    sum_states(states, coef, s_sum)

    def attend(m, lo):
        s = s_sum[m].astype(jnp.bfloat16)
        both = acc[m, lo:, :]
        for h in range(HEADS):
            both = both + mm(phi[m, h, lo:, :], lanes.of(h, s))
        return jnp.where(lanes.is_value, both / lanes.denominator(both), both)

    for m in range(2):
        sin[m] = s_sum[m, :STATE, :].astype(jnp.bfloat16)
        e_src[m] = attend(m, rows - 16)
    edges.start()
    for m in range(2):
        att[m] = attend(m, 0)
    edges.arrived()
    for m in range(2):
        a = att[m]
        tail = edge[0, m]
        out = taps[0:1, :] * a
        for by in (1, 2):
            out = out + taps[by : by + 1, :] * shifted(a, tail, q > 0, by) * col[m, :, 2 + by : 3 + by]
        conv[m] = out
        gated[m] = (out * proj[m, :, wide:]).astype(jnp.bfloat16)
    states.sent()
    edges.sent()


def attn_backward_kernel(
    reach, bg, proj, att, conv, sin, edge, col, row, coef, late, e, c, taps, out, grad_taps,
    phi_q, phi_k, near, acc_a, acc_b, s_acc, s_src, s_all, s_sum, e_src, e_dst, ss, sr, es, er,
):
    q, n = lax.axis_index("seq"), lax.axis_size("seq")
    rows, wide = proj.shape[1], proj.shape[2] // 2
    values = wide - HEADS * FK
    lanes = Lanes(wide, values)
    meet(-1, reach)
    states = Pass(-1, reach, s_src, s_all, ss, sr)
    edges = Pass(-1, 1, e_src, e_dst, es, er)
    for m in range(2):
        e_src[m] = bg[m, :16, :] * proj[m, :16, wide:]
    edges.start()

    def sides(m):
        return proj[m, :, :wide].astype(jnp.bfloat16), proj[m, :, wide:].astype(jnp.bfloat16)

    def factors(a, h):
        return mm(a, e[h, 0]) + c[0:1, :], mm(a, e[h, 1]) + c[1:2, :]

    def make_phi(i, carry):
        m, h = i // HEADS, i % HEADS
        a, b = sides(m)
        u, w = factors(a, h)
        phi_q[m, h] = (u * w * c[2:3, :] * col[m, :, 1:2]).astype(jnp.bfloat16)
        u, w = factors(b, h)
        phi_k[m, h] = (u * w * c[2:3, :] * col[m, :, 2:3]).astype(jnp.bfloat16)
        return carry

    lax.fori_loop(0, 2 * HEADS, make_phi, 0)
    edges.arrived()
    sums = [jnp.zeros((1, wide), jnp.float32)] * KW
    place = lax.broadcasted_iota(jnp.int32, (rows, 1), 0)
    for m in range(2):
        back = bg[m]
        back_conv = back * proj[m, :, wide:]
        a = jnp.where(lanes.is_value, att[m], 0.0)
        tail = edge[0, m]
        nxt = e_dst[0, m]
        total = taps[0:1, :] * back_conv
        sums[0] = sums[0] + jnp.sum(back_conv * a, axis=0, keepdims=True)
        for by in (1, 2):
            kept = back_conv * col[m, :, 2 + by : 3 + by]
            sums[by] = sums[by] + jnp.sum(
                kept * shifted(a, tail, q > 0, by), axis=0, keepdims=True
            )
            moved = pltpu.roll(kept, rows - by, 0)
            for r in range(by):
                fresh = jnp.where(q < n - 1, nxt[r : r + 1, :] * late[by - 1 + r, m], 0.0)
                moved = jnp.where(place == rows - by + r, fresh, moved)
            total = total + taps[by : by + 1, :] * moved
        out[m, :, wide:] = jnp.where(lanes.is_value, back * conv[m], 0.0).astype(jnp.bfloat16)
        back_numer = total / lanes.denominator(att[m])
        spent = back_numer * a
        found = jnp.where(lanes.is_value, back_numer, 0.0)
        for h in range(HEADS):
            denom = -jnp.sum(lanes.of(h, spent), axis=1, keepdims=True)
            high = denom.astype(jnp.bfloat16).astype(jnp.float32)
            found = jnp.where(lanes.lane == values + h, high, found)
            found = jnp.where(lanes.lane == values + 2 + h, denom - high, found)
        near[m] = found.astype(jnp.bfloat16)
        part = jnp.zeros((wide, wide), jnp.float32)
        for h in range(HEADS):
            part = part + mm_tn(phi_q[m, h], lanes.of(h, near[m]))
        s_src[m] = part[:STATE].astype(jnp.bfloat16)
    states.start()
    grad_taps[...] = jnp.zeros(grad_taps.shape, jnp.float32)
    for by in range(KW):
        grad_taps[by : by + 1, :] = sums[by]
    acc_a[...] = jnp.zeros(acc_a.shape, jnp.float32)
    acc_b[...] = jnp.zeros(acc_b.shape, jnp.float32)
    for m in range(2):
        s_sum[m] = jnp.zeros(s_sum.shape[1:], jnp.float32)
        s_sum[m, :STATE, :] = sin[m].astype(jnp.float32)

    def through_phi(scaled, factors_of, h):
        u, w = factors_of
        return mm_nt((scaled * w).astype(jnp.bfloat16), e[h, 0]) + mm_nt(
            (scaled * u).astype(jnp.bfloat16), e[h, 1]
        )

    def make_block(i, carry):
        m, h = i // HEADS, i % HEADS
        a, b = sides(m)
        asked, keyed = lanes.key(h, a), lanes.key(h, b)
        valued = lanes.extended(a)
        given = lanes.of(h, near[m])
        given_v = jnp.where(lanes.is_value, given, jnp.zeros_like(given))
        for r in range(rows // BLOCK):
            lo, hi = r * BLOCK, (r + 1) * BLOCK
            x = mm_nt(asked[lo:hi], b[:hi]) * 0.25
            seen = (col[m, lo:hi, 0:1] == row[m, 0:1, :hi]) & (
                lax.broadcasted_iota(jnp.int32, (BLOCK, hi), 1)
                <= lo + lax.broadcasted_iota(jnp.int32, (BLOCK, hi), 0)
            )
            w = jnp.where(seen, 1.0 + x + 0.5 * x * x, 0.0).astype(jnp.bfloat16)
            back_w = mm_nt(given[lo:hi], valued[:hi])
            back_s = jnp.where(seen, back_w * (1.0 + x), 0.0).astype(jnp.bfloat16)
            acc_a[m, lo:hi, :] += 0.25 * mm(back_s, keyed[:hi])
            acc_b[m, :hi, :] += 0.25 * mm_tn(back_s, asked[lo:hi])
            acc_a[m, :hi, :] += mm_tn(w, given_v[lo:hi])
        s = s_sum[m].astype(jnp.bfloat16)
        scaled = mm_nt(given, s) * col[m, :, 1:2] * c[2:3, :]
        acc_a[m] += through_phi(scaled, factors(a, h), h)
        return carry

    lax.fori_loop(0, 2 * HEADS, make_block, 0)
    states.arrived()
    sum_states(states, coef, s_sum)

    def make_late(i, carry):
        m, h = i // HEADS, i % HEADS
        a, b = sides(m)
        s = s_sum[m].astype(jnp.bfloat16)
        scaled = mm_nt(lanes.of(h, lanes.extended(a)), s) * col[m, :, 2:3] * c[2:3, :]
        acc_b[m] += through_phi(scaled, factors(b, h), h)
        s_v = lanes.of(h, jnp.where(lanes.is_value, s, jnp.zeros_like(s)))
        acc_a[m] += mm(phi_k[m, h], s_v)
        return carry

    lax.fori_loop(0, 2 * HEADS, make_late, 0)
    for m in range(2):
        out[m, :, :wide] = acc_a[m].astype(jnp.bfloat16)
        out[m, :, wide:] = jnp.where(
            lanes.is_value, out[m, :, wide:].astype(jnp.float32), acc_b[m]
        ).astype(jnp.bfloat16)
    states.sent()
    edges.sent()


def seq_reach():
    n = lax.axis_size("seq")
    return n // 2 if n % 2 == 0 else n - 1


def attention_call(kernel, cid, inputs, scalars, shapes, scratch):
    vmem, smem = pl.BlockSpec(memory_space=pltpu.VMEM), pl.BlockSpec(memory_space=pltpu.SMEM)
    return pl.pallas_call(
        functools.partial(kernel, seq_reach()),
        out_shape=shapes,
        in_specs=[smem if i in scalars else vmem for i in range(len(inputs))],
        out_specs=[vmem] * len(shapes),
        scratch_shapes=scratch,
        name=f"attention{cid}",
        compiler_params=pltpu.CompilerParams(
            collective_id=cid, has_side_effects=True, vmem_limit_bytes=48 << 20
        ),
    )(*inputs)


def passing(reach, wide):
    dma = pltpu.SemaphoreType.DMA
    return (
        [
            pltpu.VMEM((2, STATE, wide), jnp.bfloat16),
            pltpu.VMEM((reach, 2, STATE, wide), jnp.bfloat16),
            pltpu.VMEM((2, wide, wide), jnp.float32),
        ],
        [dma((reach,)), dma((reach,)), dma((1,)), dma((1,))],
    )


def attention_forward(proj, taps, marks, tables):
    m, rows, double = proj.shape
    wide = double // 2
    f32, bf16 = jnp.float32, jnp.bfloat16
    buffers, sems = passing(seq_reach(), wide)
    shape = jax.ShapeDtypeStruct
    return attention_call(
        attn_forward_kernel,
        10,
        [proj, marks["col"], marks["row"], marks["before"], *tables, taps],
        (3,),
        [
            shape((m, rows, wide), bf16),
            shape((m, rows, wide), f32),
            shape((m, rows, wide), f32),
            shape((m, STATE, wide), bf16),
            shape((1, m, 16, wide), f32),
        ],
        [
            pltpu.VMEM((m, rows, wide), f32),
            pltpu.VMEM((m, HEADS, rows, wide), bf16),
            pltpu.VMEM((m, wide, wide), f32),
            *buffers,
            pltpu.VMEM((m, 16, wide), f32),
            *sems,
        ],
    )


def attention_backward(back_gated, proj, kept, taps, marks, tables):
    att, conv, sin, edge = kept
    m, rows, double = proj.shape
    wide = double // 2
    f32, bf16 = jnp.float32, jnp.bfloat16
    buffers, sems = passing(seq_reach(), wide)
    shape = jax.ShapeDtypeStruct
    return attention_call(
        attn_backward_kernel,
        11,
        [
            back_gated, proj, att, conv, sin, edge, marks["col"], marks["row"], marks["after"],
            marks["late"], *tables, taps,
        ],
        (8, 9),
        [shape((m, rows, double), bf16), shape((8, wide), f32)],
        [
            pltpu.VMEM((m, HEADS, rows, wide), bf16),
            pltpu.VMEM((m, HEADS, rows, wide), bf16),
            pltpu.VMEM((m, rows, wide), bf16),
            pltpu.VMEM((m, rows, wide), f32),
            pltpu.VMEM((m, rows, wide), f32),
            pltpu.VMEM((m, wide, wide), f32),
            *buffers,
            pltpu.VMEM((m, 16, wide), f32),
            pltpu.VMEM((1, m, 16, wide), f32),
            *sems,
        ],
    )


def sequence_marks(lengths, rows):
    count, mine = lax.axis_size("seq"), lax.axis_index("seq")
    start = mine * rows
    positions = start + jnp.arange(rows + 2, dtype=jnp.int32)
    begin_ext = jax.vmap(lambda row: seq_begin(row, positions))(lengths)
    begin = begin_ext[:, :rows]
    ends = (jnp.arange(count, dtype=jnp.int32) + 1) * rows - 1
    stays = jax.vmap(lambda row: seq_begin(row, ends))(lengths) < (ends - rows + 1)[None, :]
    stays = stays.astype(jnp.float32)
    blocks = jnp.arange(count, dtype=jnp.int32)

    def through(first, last):
        inside = (blocks >= first) & (blocks <= last)
        return jnp.min(jnp.where(inside[None, :], stays, 1.0), axis=1)

    reach = seq_reach()
    before = [through(mine - d + 1, mine - 1) for d in range(1, reach + 1)]
    after = [through(mine + 1, mine + d - 1) for d in range(1, reach + 1)]
    allowed = [(positions - j >= begin_ext).astype(jnp.float32) for j in range(KW)]
    columns = [
        begin.astype(jnp.float32),
        (begin < start).astype(jnp.float32),
        (begin == begin[:, rows - 1 :]).astype(jnp.float32),
        allowed[1][:, :rows],
        allowed[2][:, :rows],
    ]
    col = jnp.stack(columns + [jnp.zeros_like(columns[0])] * 3, axis=2)
    return {
        "col": col,
        "row": jnp.broadcast_to(columns[0][:, None, :], (2, 8, rows)),
        "before": jnp.stack(before),
        "after": jnp.stack(after),
        "late": jnp.stack([allowed[1][:, rows], allowed[2][:, rows], allowed[2][:, rows + 1]]),
    }


def by_seq(grad):
    n = lax.axis_size("seq")
    return grad.reshape((n, grad.shape[0] // n) + grad.shape[1:])


def held(a):
    return lax.optimization_barrier(a.astype(jnp.bfloat16))


def dot_n(a, b):
    return jnp.dot(a, b, preferred_element_type=jnp.float32)


def on_device(
    tokens,
    lengths,
    gain_attn,
    w_query,
    w_key,
    w_value,
    w_gate_conv,
    conv_taps,
    w_out,
    gain_ffn,
    w_gate,
    w_up,
    w_down,
    cotangent,
):
    head_index = lax.axis_index("head")
    core = lax.axis_index("section")
    micro_count, rows, width = tokens.shape
    total = micro_count * rows

    def halves(weight):
        middle = weight.shape[1] // 2
        return jnp.stack([weight[:, :middle], weight[:, middle:]])

    own_mix = jnp.concatenate(
        [halves(w[0]) for w in (w_value, w_query, w_gate_conv, w_key)], axis=2
    )
    values = w_value.shape[2] // 2
    keys = w_query.shape[2] // 2
    wide = values + keys
    own_out = jnp.pad(halves(w_out[0].T), ((0, 0), (0, 0), (0, keys)))
    cols = w_gate.shape[2] // 2

    def filled(half):
        return jnp.pad(half, ((0, 0), (0, 0), (0, -cols % 128)))

    own_ffn = jnp.concatenate([filled(halves(w_gate[0])), filled(halves(w_up[0]))], axis=2)
    own_down = filled(halves(w_down[0].T))
    rows_of_layer = jnp.concatenate([gain_attn, gain_ffn, conv_taps[0]], axis=0)
    rows_all = lax.all_gather(rows_of_layer, "section").astype(jnp.float32)
    gains_one, gains_two, taps_all = rows_all[:, 0], rows_all[:, 1], rows_all[:, 2:]
    taps_both = lax.dynamic_slice_in_dim(taps_all, (head_index * 2 + core) * values, values, 2)
    taps_both = jnp.pad(taps_both, ((0, 0), (0, 8 - KW), (0, keys)))
    first, rest = feature_tables(values)
    tables = (jnp.asarray(first, jnp.bfloat16), jnp.asarray(rest))
    marks = sequence_marks(lengths, rows)
    hidden_cols = own_down.shape[2]

    def as_parts(flat):
        return flat.reshape(micro_count, rows, -1)

    def spread(summed):
        return summed.astype(jnp.float32).reshape(total, width)

    _, (mix_0, out_0), _, _ = communicate(1, gather=(0, [own_mix, own_out]))
    w_mix, w_o, w_gu, w_d = [mix_0, None], [out_0, None], [None, None], [None, None]
    x = tokens.reshape(total, width).astype(jnp.float32)
    kept = [None, None]
    outputs = []
    last_partial = None
    for layer in range(2):
        normed = rms_norm(x, gains_one[layer]).astype(jnp.bfloat16)
        proj = dot_n(normed, w_mix[layer]).reshape(micro_count, rows, 2 * wide)
        gated, *attn = attention_forward(proj, taps_both[layer], marks, tables)
        gated_flat = gated.reshape(total, wide)
        partial = (gated, w_o[layer])
        if layer == 0:
            summed, (w_gu[0], w_d[0]), _, _ = communicate(
                2, partial=partial, gather=(0, [own_ffn, own_down])
            )
        else:
            summed, (w_gu[1],), _, _ = communicate(3, partial=partial, gather=(1, [own_ffn]))
        middle = x + spread(summed)
        normed_two = rms_norm(middle, gains_two[layer]).astype(jnp.bfloat16)
        middle = held(middle).astype(jnp.float32)
        both = held(dot_n(normed_two, w_gu[layer])).astype(jnp.float32)
        hidden = (jax.nn.silu(both[:, :hidden_cols]) * both[:, hidden_cols:]).astype(jnp.bfloat16)
        partial = (as_parts(hidden), w_d[layer])
        kept[layer] = (x, normed, proj, gated_flat, attn, middle, normed_two, both, hidden)
        if layer == 0:
            summed, (w_mix[1], w_o[1], w_d[1]), _, _ = communicate(
                4, partial=partial, gather=(1, [own_mix, own_out, own_down])
            )
            outputs.append(held(middle + spread(summed)))
            x = outputs[0].astype(jnp.float32)
        else:
            last_partial = partial

    grad = cotangent.reshape(total, width)
    back = [None, None]
    smalls = [None, None]
    made = []
    into = [None] * 4
    for layer in (1, 0):
        x, normed, proj, gated_flat, attn, middle, normed_two, both, hidden = kept[layer]
        grad_wide = grad.astype(jnp.float32)
        back_hidden = dot_n(grad, w_d[layer])
        gate_pre, upward = both[:, :hidden_cols], both[:, hidden_cols:]
        silu_value, silu_back = jax.vjp(jax.nn.silu, gate_pre)
        back_both = jnp.concatenate(
            [
                silu_back(back_hidden * upward)[0].astype(jnp.bfloat16),
                (back_hidden * silu_value).astype(jnp.bfloat16),
            ],
            axis=1,
        )
        partial = (as_parts(back_both), w_gu[layer])
        products = ((normed_two, back_both), (grad, hidden))
        if layer == 1:
            summed, _, _, (grad_gu, grad_d) = communicate(5, partial=partial, products=products)
        else:
            summed, _, into[1:], (grad_gu, grad_d) = communicate(
                6, partial=partial, scatter=(1, made), products=products
            )
        _, norm_back_two = jax.vjp(rms_norm, middle, gains_two[layer])
        back_middle, gain_two = norm_back_two(spread(summed))
        back_middle = grad_wide + back_middle
        back_branch = held(back_middle)
        back_middle = back_branch.astype(jnp.float32)
        back_gated = dot_n(back_branch, w_o[layer])
        back_proj, taps_grad = attention_backward(
            back_gated.reshape(micro_count, rows, wide), proj, attn, taps_both[layer], marks, tables
        )
        back_flat = back_proj.reshape(total, 2 * wide)
        partial = (back_proj, w_mix[layer])
        summed, _, into[:1], (grad_mix, grad_o) = communicate(
            7 + layer,
            partial=partial,
            scatter=(layer, [by_seq(grad_gu)]),
            into=into[:1] if layer == 0 else (),
            products=((normed, back_flat), (back_branch, gated_flat)),
        )
        made = [by_seq(grad_d), by_seq(grad_mix), by_seq(grad_o)]
        _, norm_back_one = jax.vjp(rms_norm, x, gains_one[layer])
        back_x, gain_one = norm_back_one(spread(summed))
        grad = (back_middle + back_x).astype(jnp.bfloat16)
        back[layer] = grad
        smalls[layer] = (gain_one, gain_two, taps_grad)
    gains = jnp.stack([smalls[0][0], smalls[1][0], smalls[0][1], smalls[1][1]])
    taps_rows = jnp.concatenate([smalls[0][2][:KW], smalls[1][2][:KW]])
    packed = jnp.concatenate(
        [
            jnp.pad(gains, ((0, 4), (0, 0))),
            jnp.pad(taps_rows, ((0, 8 - 2 * KW), (0, width - wide))),
        ]
    )
    summed, _, into[1:], (gains, taps_rows) = communicate(
        9, partial=last_partial, scatter=(0, made), into=into[1:], small=(packed, wide)
    )
    outputs.append((kept[1][5] + spread(summed)).astype(jnp.bfloat16))
    grad_gu, grad_d, grad_mix, grad_o = [
        jnp.sum(received.astype(jnp.float32), axis=1).reshape((2, -1) + received.shape[3:])
        for received in into
    ]

    def joined(pair):
        return jnp.concatenate([pair[0], pair[1]], axis=1)

    grad_value = joined(grad_mix[:, :, :values])
    grad_query = joined(grad_mix[:, :, values:wide])
    grad_gconv = joined(grad_mix[:, :, wide : wide + values])
    grad_key = joined(grad_mix[:, :, wide + values :])
    grad_out = joined(grad_o[:, :, :values]).T
    grad_gate = joined(grad_gu[:, :, :cols])
    grad_up = joined(grad_gu[:, :, hidden_cols : hidden_cols + cols])
    grad_down = joined(grad_d[:, :, :cols]).T

    gains = lax.dynamic_index_in_dim(gains[:4].reshape(2, 2, width), core, 1, False)
    taps_rows = lax.dynamic_index_in_dim(
        taps_rows[:, : 2 * KW, :values].reshape(-1, 2, KW, values), core, 1, False
    )
    grad_taps = jnp.transpose(taps_rows, (1, 0, 2)).reshape(KW, width)

    def chosen(pair):
        return jnp.where(core == 0, pair[0], pair[1]).reshape(1, micro_count, rows, width)

    return (
        chosen(outputs),
        chosen(back),
        gains[0][None],
        grad_query[None],
        grad_key[None],
        grad_value[None],
        grad_gconv[None],
        grad_taps[None],
        grad_out[None],
        gains[1][None],
        grad_gate[None],
        grad_up[None],
        grad_down[None],
    )


def solution(mesh):
    placed = (
        P(None, "seq", None),
        P(),
        P("section", None),
        P("section", "seq", "head"),
        P("section", "seq", "head"),
        P("section", "seq", "head"),
        P("section", "seq", "head"),
        P("section", None, None),
        P("section", "head", "seq"),
        P("section", None),
        P("section", "seq", "head"),
        P("section", "seq", "head"),
        P("section", "head", "seq"),
        P(None, "seq", None),
    )
    return jax.shard_map(
        on_device,
        mesh=mesh,
        in_specs=placed,
        out_specs=(
            P("section", None, "seq", None),
            P("section", None, "seq", None),
            P("section", None),
            P("section", "seq", "head"),
            P("section", "seq", "head"),
            P("section", "seq", "head"),
            P("section", "seq", "head"),
            P("section", None, None),
            P("section", "head", "seq"),
            P("section", None),
            P("section", "seq", "head"),
            P("section", "seq", "head"),
            P("section", "head", "seq"),
        ),
        check_vma=False,
    )
```

```python
import functools
import math

import jax
import jax.numpy as jnp
from jax import lax
from jax.experimental import pallas as pl
from jax.experimental.pallas import tpu as pltpu
import numpy as np
from jax.sharding import PartitionSpec as P

FK = 16
KW = 3
MESH = pl.DeviceIdType.MESH
epsilon = 1e-05


def remote(src, dst, send, recv, **where):
    return pltpu.make_async_remote_copy(
        src_ref=src,
        dst_ref=dst,
        send_sem=send,
        recv_sem=recv,
        device_id=where,
        device_id_type=MESH,
    )


def greet(line, spread, everyone):
    core, z, q = lax.axis_index("section"), lax.axis_index("head"), lax.axis_index("seq")
    depth, count = lax.axis_size("head"), lax.axis_size("seq")
    barrier = pltpu.get_barrier_semaphore()

    def hello(**where):
        pl.semaphore_signal(barrier, inc=1, device_id=where, device_id_type=MESH)

    hello(section=1 - core)
    expected = 1
    if spread:
        for j in range(1, count):
            for h in range(2):
                hello(section=h, seq=lax.rem(q + j, count))
        expected += 2 * (count - 1)
    if everyone:
        for j in range(1, depth):
            for h in range(2):
                hello(section=h, head=lax.rem(z + j, depth))
        expected += 2 * (depth - 1)
    elif line:

        @pl.when(z > 0)
        def _():
            hello(head=z - 1)

        @pl.when(z < depth - 1)
        def _():
            hello(head=z + 1)

        expected = expected + jnp.where(z > 0, 1, 0) + jnp.where(z < depth - 1, 1, 0)
    pl.semaphore_wait(barrier, expected)


PIECES = 4
FIRST_TILE = 8
LEAD = 3


class LineSum:
    def __init__(self, lhs, w, o_ref, scratch, chunks, lag):
        self.lhs, self.w, self.o_ref, self.chunks, self.lag = lhs, w, o_ref, chunks, lag
        self.p_ref, self.pin, self.low, self.high, self.out = scratch[:5]
        self.ps, self.pr, self.rs, self.rl, self.rh, self.bs, self.br, self.ts, self.tr = scratch[5:]
        self.z, self.n = lax.axis_index("head"), lax.axis_size("head")
        self.core = lax.axis_index("section")
        self.half = lhs.shape[1] // 2
        self.step = self.half // chunks
        self.depth = max((self.n - 1) // 2, self.n - 1 - (self.n - 1) // 2)
        self.turns = chunks + 2 * self.depth * lag

    @staticmethod
    def scratch(rows, width, chunks):
        dma = pltpu.SemaphoreType.DMA
        each = dma((2, chunks))
        whole = pltpu.VMEM((2, rows, width), jnp.bfloat16)
        return [whole] + [pltpu.VMEM((rows, width), jnp.bfloat16)] * 4 + [
            dma((1,)), dma((2, PIECES)), dma((2,)), each, each, dma((2, 2)), each, dma((1,)), dma((1,))
        ]

    def root(self, d):
        return (self.n - 1) // 2 if d == 0 else self.n - 1 - (self.n - 1) // 2

    def rng(self, d, k):
        return pl.ds(pl.multiple_of(d * self.half + k * self.step, self.step), self.step)

    def part(self, d, k):
        size = self.half // PIECES
        r = pl.ds(pl.multiple_of(d * self.half + k * size, size), size)
        other = 1 - self.core
        return remote(
            self.p_ref.at[other, r], self.pin.at[r], self.ps.at[0], self.pr.at[d, k], section=other
        )

    def up(self, d, k):
        r = self.rng(d, k)
        return remote(
            self.out.at[r], self.low.at[r], self.rs.at[d], self.rl.at[d, k], head=self.z + 1
        )

    def down(self, d, k):
        r = self.rng(d, k)
        return remote(
            self.out.at[r], self.high.at[r], self.rs.at[d], self.rh.at[d, k], head=self.z - 1
        )

    def share(self, d, k, side):
        r = self.rng(d, k)
        at = self.o_ref.at[self.core, r]
        return remote(
            at, at, self.bs.at[side, d], self.br.at[d, k], head=self.z + (1 if side else -1)
        )

    def give(self, d, k):
        r = self.rng(d, k)
        at = self.o_ref.at[self.core, r]
        return remote(at, at, self.ts.at[0], self.tr.at[0], section=1 - self.core)

    def make(self, i):
        size = self.half // PIECES
        places = [
            (m, pl.ds(pl.multiple_of(d * self.half + i * size, size), size))
            for m in range(2)
            for d in range(2)
        ]
        left = jnp.concatenate([self.lhs[m, r, :] for m, r in places], axis=0)
        made = lax.dot_general(
            left, self.w[...], (((1,), (1,)), ((), ())), preferred_element_type=jnp.float32
        ).astype(jnp.bfloat16)
        for at, (m, r) in enumerate(places):
            self.p_ref[m, r, :] = made[at * size : (at + 1) * size]
        for d in range(2):
            self.part(d, i).start()

    def gathered(self, d, k):
        r = self.rng(d, k)
        z, n, root = self.z, self.n, self.root(d)
        group = self.chunks // PIECES

        @pl.when(k % group == 0)
        def _():
            self.part(d, k // group).wait_recv()

        mine = self.p_ref[self.core, r, :].astype(jnp.float32) + self.pin[r, :].astype(jnp.float32)

        @pl.when((z == 0) & (root > 0))
        def _():
            self.out[r, :] = mine.astype(jnp.bfloat16)
            self.up(d, k).start()

        @pl.when((z == n - 1) & (root < n - 1))
        def _():
            self.out[r, :] = mine.astype(jnp.bfloat16)
            self.down(d, k).start()

        @pl.when((z > 0) & (z < root))
        def _():
            self.up(d, k).wait_recv()
            self.out[r, :] = (mine + self.low[r, :].astype(jnp.float32)).astype(jnp.bfloat16)
            self.up(d, k).start()

        @pl.when((z < n - 1) & (z > root))
        def _():
            self.down(d, k).wait_recv()
            self.out[r, :] = (mine + self.high[r, :].astype(jnp.float32)).astype(jnp.bfloat16)
            self.down(d, k).start()

        @pl.when(z == root)
        def _():
            total = mine
            if root > 0:
                self.up(d, k).wait_recv()
                total = total + self.low[r, :].astype(jnp.float32)
            if root < n - 1:
                self.down(d, k).wait_recv()
                total = total + self.high[r, :].astype(jnp.float32)
            self.o_ref[self.core, r, :] = total.astype(jnp.bfloat16)
            if root > 0:
                self.share(d, k, 0).start()
            if root < n - 1:
                self.share(d, k, 1).start()
            self.give(d, k).start()

    def passed(self, d, k):
        z, n, root = self.z, self.n, self.root(d)
        self.share(d, k, 0).wait_recv()

        @pl.when((z < root) & (z > 0))
        def _():
            self.share(d, k, 0).start()

        @pl.when((z > root) & (z < n - 1))
        def _():
            self.share(d, k, 1).start()

        self.give(d, k).start()

    def turn(self, t):
        z, n = self.z, self.n
        for d in range(2):
            root = self.root(d)
            deep = max(root, n - 1 - root)
            below = jnp.where(z < root, z, jnp.where(z > root, n - 1 - z, deep))
            k = t - below * self.lag
            far = jnp.abs(z - root)

            @pl.when((k >= 0) & (k < self.chunks))
            def _():
                self.gathered(d, k)

            b = t - (deep + far) * self.lag

            @pl.when((b >= 0) & (b < self.chunks) & (far > 0))
            def _():
                self.passed(d, b)

    def finish(self):
        z, n, other = self.z, self.n, 1 - self.core
        remote(
            self.p_ref.at[other], self.pin, self.ps.at[0], self.pr.at[0, 0], section=other
        ).wait_send()
        mine = self.o_ref.at[self.core]
        given = remote(mine, mine, self.ts.at[0], self.tr.at[0], section=other)
        given.wait_recv()
        given.wait_send()
        for d in range(2):
            root = self.root(d)
            r = pl.ds(d * self.half, self.half)
            at = self.o_ref.at[self.core, r]

            def summed(head):
                return remote(
                    self.out.at[r], self.low.at[r], self.rs.at[d], self.rl.at[d, 0], head=head
                )

            def shared(side):
                return remote(
                    at, at, self.bs.at[side, d], self.br.at[d, 0], head=z + (1 if side else -1)
                )

            @pl.when(z < root)
            def _():
                summed(z + 1).wait_send()

            @pl.when(z > root)
            def _():
                summed(z - 1).wait_send()

            if root > 0:

                @pl.when((z <= root) & (z > 0))
                def _():
                    shared(0).wait_send()

            if root < n - 1:

                @pl.when((z >= root) & (z < n - 1))
                def _():
                    shared(1).wait_send()


class Gather:
    def __init__(self, layer, srcs, dsts, sems):
        self.layer, self.srcs, self.dsts = layer, srcs, dsts
        self.ss, self.rr, self.ls, self.fs, self.fr = sems
        self.core, self.q = lax.axis_index("section"), lax.axis_index("seq")
        self.n = lax.axis_size("seq")
        self.square = self.n == 4

    @staticmethod
    def scratch(count, n):
        dma = pltpu.SemaphoreType.DMA
        return [dma((count, n, 2)), dma((count, n)), dma((count,)), dma((count, 2)), dma((count, 2))]

    def peer(self, j):
        if not self.square:
            return lax.rem(self.q + j, self.n)
        x, y = self.q % 2, self.q // 2
        x, y = (1 - x if j % 2 else x), (1 - y if j // 2 else y)
        return y * 2 + x

    def direct(self):
        return range(1, 3 if self.square else self.n)

    def copies(self, a):
        for j in self.direct():
            for h in range(2):
                yield remote(
                    self.srcs[a].at[h], self.dsts[a].at[self.q], self.ss.at[a, j, h],
                    self.rr.at[a, self.q], section=h, seq=self.peer(j),
                )
        yield remote(
            self.srcs[a].at[1 - self.layer], self.dsts[a].at[self.q], self.ss.at[a, 0, 0],
            self.rr.at[a, self.q], section=1 - self.layer,
        )

    def local(self, a):
        return pltpu.make_async_copy(
            self.srcs[a].at[self.layer], self.dsts[a].at[self.q], self.ls.at[a]
        )

    def arrival(self, a, s):
        return remote(
            self.srcs[a].at[0], self.dsts[a].at[s], self.ss.at[a, 0, 0], self.rr.at[a, s],
            section=1 - self.core,
        )

    def relay(self, a, i):
        size = self.srcs[a].shape[1] // 2
        at = self.dsts[a].at[self.peer(1 + i), pl.ds(i * size, size)]
        return remote(at, at, self.fs.at[a, i], self.fr.at[a, i], seq=self.peer(2 - i))

    def corner(self, a, i):
        size = self.srcs[a].shape[1] // 2
        at = self.dsts[a].at[self.peer(3), pl.ds(i * size, size)]
        return remote(at, at, self.fs.at[a, i], self.fr.at[a, i], seq=self.peer(2 - i))

    def start(self):
        @pl.when(self.core == self.layer)
        def _():
            for a in range(len(self.srcs)):
                for copy in self.copies(a):
                    copy.start()
                self.local(a).start()

    def due(self):
        sent, turns = 0, []
        for src in self.srcs:
            sent += 2 * src.shape[1] * src.shape[2] * 2
            turns.append(3 + sent // 200_000)
        return turns

    def middle(self, a):
        for j in self.direct():
            self.arrival(a, self.peer(j)).wait_recv()
            if self.square:
                self.relay(a, j - 1).start()

    def finish(self):
        for a in range(len(self.srcs)):
            if self.square:
                for i in range(2):
                    self.corner(a, i).wait_recv()
                    self.relay(a, i).wait_send()

            @pl.when(self.core == self.layer)
            def _():
                self.local(a).wait()
                for copy in self.copies(a):
                    copy.wait_send()

            @pl.when(self.core != self.layer)
            def _():
                self.arrival(a, self.q).wait_recv()


class SmallSum:
    def __init__(self, g_ref, total, spread, scratch):
        self.g_ref, self.total, self.spread = g_ref, total, spread
        self.got, self.src, self.ss, self.sr, self.ts, self.tr = scratch
        self.core, self.q, self.z = (lax.axis_index(a) for a in ("section", "seq", "head"))
        self.n, self.depth = lax.axis_size("seq"), lax.axis_size("head")

    @staticmethod
    def scratch(shape, narrow, n, depth):
        dma = pltpu.SemaphoreType.DMA
        return [
            pltpu.VMEM((n,) + shape, jnp.float32),
            pltpu.VMEM((8, narrow), jnp.float32),
            dma((n,)),
            dma((n,)),
            dma((2 * depth,)),
            dma((2 * depth,)),
        ]

    def first(self, j):
        return remote(
            self.g_ref, self.got.at[self.q], self.ss.at[j], self.sr.at[self.q],
            seq=lax.rem(self.q + j, self.n),
        )

    def others(self):
        for j in range(self.depth):
            for flip in range(2):
                if j or flip:
                    core = 1 - self.core if flip else self.core
                    yield 2 * j + flip, lax.rem(self.z + j, self.depth), core

    def second(self, i, z, core):
        slot = self.z * 2 + self.core
        return remote(
            self.src, self.spread.at[slot], self.ts.at[i], self.tr.at[slot], head=z, section=core
        )

    def start(self):
        for j in range(1, self.n):
            self.first(j).start()
        self.got[self.q] = self.g_ref[...]

    def middle(self):
        for j in range(1, self.n):
            s = lax.rem(self.q + j, self.n)
            remote(
                self.g_ref, self.got.at[s], self.ss.at[j], self.sr.at[s], seq=s
            ).wait_recv()
        summed = self.got[0]
        for s in range(1, self.n):
            summed = summed + self.got[s]
        self.total[...] = summed[:8]
        own = summed[8:, : self.src.shape[1]]
        self.src[...] = own
        self.spread[self.z * 2 + self.core] = own
        for i, z, core in self.others():
            self.second(i, z, core).start()

    def finish(self):
        for i, z, core in self.others():
            slot = z * 2 + core
            remote(
                self.src, self.spread.at[slot], self.ts.at[i], self.tr.at[slot], head=z, section=core
            ).wait_recv()
            self.second(i, z, core).wait_send()
        for j in range(1, self.n):
            self.first(j).wait_send()


class Scatter:
    def __init__(self, layer, srcs, dsts, sems):
        self.layer, self.srcs, self.dsts = layer, srcs, dsts
        self.ss, self.rr, self.ls = sems
        self.core, self.q = lax.axis_index("section"), lax.axis_index("seq")
        self.n = lax.axis_size("seq")

    @staticmethod
    def scratch(count, n):
        return [
            pltpu.SemaphoreType.DMA((count, n)),
            pltpu.SemaphoreType.DMA((count, 2, n)),
            pltpu.SemaphoreType.DMA((count,)),
        ]

    def copies(self, a):
        for j in range(1, self.n):
            t = lax.rem(self.q + j, self.n)
            yield remote(
                self.srcs[a].at[t], self.dsts[a].at[self.core, self.q], self.ss.at[a, j],
                self.rr.at[a, self.core, self.q], section=self.layer, seq=t,
            )

    def near(self, a):
        return remote(
            self.srcs[a].at[self.q], self.dsts[a].at[self.core, self.q], self.ss.at[a, 0],
            self.rr.at[a, self.core, self.q], section=self.layer,
        )

    def local(self, a):
        return pltpu.make_async_copy(
            self.srcs[a].at[self.q], self.dsts[a].at[self.core, self.q], self.ls.at[a]
        )

    def arrival(self, a, h, s):
        return remote(
            self.srcs[a].at[self.q], self.dsts[a].at[h, s], self.ss.at[a, 0], self.rr.at[a, h, s],
            section=1 - self.core,
        )

    def start(self):
        for a in range(len(self.srcs)):
            for copy in self.copies(a):
                copy.start()

            @pl.when(self.core == self.layer)
            def _():
                self.local(a).start()

            @pl.when(self.core != self.layer)
            def _():
                self.near(a).start()

    def finish(self):
        for a in range(len(self.srcs)):

            @pl.when(self.core == self.layer)
            def _():
                for j in range(1, self.n):
                    for h in range(2):
                        self.arrival(a, h, lax.rem(self.q + j, self.n)).wait_recv()
                self.arrival(a, 1 - self.layer, self.q).wait_recv()
                self.local(a).wait()

            @pl.when(self.core != self.layer)
            def _():
                self.near(a).wait_send()

            for copy in self.copies(a):
                copy.wait_send()


TILE = 256


class Product:
    def __init__(self, lhs, rhs, out, scratch):
        self.lhs, self.rhs, self.out = lhs, rhs, out
        self.left, self.right, self.stage, self.loads, self.stores = scratch
        self.tiles = lhs.shape[1] // TILE

    @staticmethod
    def scratch(lhs, rhs):
        return [
            pltpu.VMEM(lhs.shape, jnp.bfloat16),
            pltpu.VMEM(rhs.shape, jnp.bfloat16),
            pltpu.VMEM((2, TILE, rhs.shape[1]), jnp.bfloat16),
            pltpu.SemaphoreType.DMA((2,)),
            pltpu.SemaphoreType.DMA((2,)),
        ]

    def load(self, side):
        src, dst = ((self.lhs, self.left), (self.rhs, self.right))[side]
        return pltpu.make_async_copy(src, dst, self.loads.at[side])

    def store(self, i):
        at = pl.ds(pl.multiple_of(i * TILE, TILE), TILE)
        return pltpu.make_async_copy(self.stage.at[i % 2], self.out.at[at], self.stores.at[i % 2])

    def start(self):
        self.load(0).start()
        self.load(1).start()

    def step(self, i):
        @pl.when(i == 0)
        def _():
            self.load(0).wait()
            self.load(1).wait()

        @pl.when(i >= 2)
        def _():
            self.store(i - 2).wait()

        at = pl.ds(pl.multiple_of(i * TILE, TILE), TILE)
        self.stage[i % 2] = lax.dot_general(
            self.left[:, at],
            self.right[...],
            (((0,), (0,)), ((), ())),
            preferred_element_type=jnp.float32,
        ).astype(jnp.bfloat16)
        self.store(i).start()

    def finish(self):
        for i in range(max(self.tiles - 2, 0), self.tiles):
            self.store(i).wait()


def comm_kernel(plan, *refs):
    has_sum, layer_in, count_in, layer_out, count_out, kept, count_made, small_in, chunks, lag = plan
    refs = list(refs)

    def take(count):
        taken = refs[:count]
        del refs[:count]
        return taken

    p_in, w_in, g_in, _, m_in, s_in = (
        take(2 * has_sum), take(count_in), take(count_out), take(kept), take(2 * count_made),
        take(small_in),
    )
    p_out, w_out, g_out, m_out, s_out = (
        take(has_sum), take(count_in), take(count_out), take(count_made), take(2 * small_in)
    )
    greet(has_sum, count_in + count_out > 0, small_in)
    jobs = []
    later = []
    if has_sum:
        line = LineSum(p_in[0], p_in[1], p_out[0], take(14), chunks, lag)
    if count_in:
        weights = Gather(layer_in, w_in, w_out, take(5))
        jobs.append(weights)
        for a, turn in enumerate(weights.due()):
            later.append((turn, functools.partial(weights.middle, a)))
    if count_out:
        jobs.append(Scatter(layer_out, g_in, g_out, take(3)))
    made = [
        Product(m_in[2 * i], m_in[2 * i + 1], m_out[i], take(5)) for i in range(count_made)
    ]
    if small_in:
        small = SmallSum(s_in[0], s_out[0], s_out[1], take(6))
        jobs.insert(0, small)
        later.append((12, small.middle))
    for job in made + jobs:
        job.start()
    if has_sum:
        tiles = sum(product.tiles for product in made)

        def turn(t, carry):
            @pl.when((t < LEAD * PIECES) & (t % LEAD == 0))
            def _():
                line.make(t // LEAD)

            line.turn(t - LEAD)
            i = t - LEAD - FIRST_TILE
            for product in made:

                @pl.when((i >= 0) & (i < product.tiles))
                def _(product=product, i=i):
                    product.step(i)

                i = i - product.tiles
            for when, act in later:

                @pl.when(t == when + LEAD)
                def _(act=act):
                    act()

            return carry

        last = max([line.turns, tiles + FIRST_TILE] + [when + 1 for when, _ in later])
        lax.fori_loop(0, last + LEAD, turn, 0)
        line.finish()
    else:
        for _, act in later:
            act()
    for job in made + jobs:
        job.finish()


def communicate(
    cid, partial=None, gather=None, scatter=None, into=(), products=(), small=None, chunks=16, lag=2
):
    n = lax.axis_size("seq")
    layer_in, w_in = gather if gather else (0, [])
    layer_out, g_in = scatter if scatter else (0, [])
    p_in = [] if partial is None else list(partial)
    has_sum = 0 if partial is None else 1
    if has_sum:
        summed = (partial[0].shape[0], partial[0].shape[1], partial[1].shape[0])
    m_in = [a for pair in products for a in pair]
    vmem, anywhere = pl.BlockSpec(memory_space=pltpu.VMEM), pl.BlockSpec(memory_space=pl.ANY)
    scratch = []
    if p_in:
        scratch += LineSum.scratch(summed[1], summed[2], chunks)
    if w_in:
        scratch += Gather.scratch(len(w_in), n)
    if g_in:
        scratch += Scatter.scratch(len(g_in), n)
    for pair in products:
        scratch += Product.scratch(*pair)
    s_in, s_shapes = [], []
    if small is not None:
        s_in, narrow, depth = [small[0]], small[1], lax.axis_size("head")
        scratch += SmallSum.scratch(small[0].shape, narrow, n, depth)
        s_shapes = [
            jax.ShapeDtypeStruct((8, small[0].shape[1]), jnp.float32),
            jax.ShapeDtypeStruct((2 * depth, 8, narrow), jnp.float32),
        ]
    shapes = (
        ([jax.ShapeDtypeStruct(summed, jnp.bfloat16)] if has_sum else [])
        + [jax.ShapeDtypeStruct((n,) + w.shape[1:], jnp.bfloat16) for w in w_in]
        + [jax.ShapeDtypeStruct((2,) + g.shape, jnp.bfloat16) for g in g_in]
        + [jax.ShapeDtypeStruct((a.shape[1], b.shape[1]), jnp.bfloat16) for a, b in products]
        + s_shapes
    )
    plan = (
        has_sum, layer_in, len(w_in), layer_out, len(g_in), len(into), len(products), len(s_in),
        chunks, lag,
    )
    first = len(p_in) + len(w_in)
    first_out = has_sum + len(w_in)
    outs = pl.pallas_call(
        functools.partial(comm_kernel, plan),
        out_shape=shapes,
        in_specs=[vmem] * len(p_in)
        + [anywhere if has_sum else vmem] * len(w_in)
        + [anywhere] * (len(g_in) + len(into) + len(m_in))
        + [vmem] * len(s_in),
        out_specs=[vmem] * has_sum
        + [anywhere] * (len(w_in) + len(g_in) + len(products))
        + [vmem] * len(s_shapes),
        scratch_shapes=scratch,
        input_output_aliases={first + len(g_in) + i: first_out + i for i in range(len(into))},
        name=f"comm{cid}",
        compiler_params=pltpu.CompilerParams(
            collective_id=cid, has_side_effects=True, vmem_limit_bytes=52 << 20
        ),
    )(*p_in, *w_in, *g_in, *into, *m_in, *s_in)
    return (
        outs[0] if p_in else None,
        [a.reshape((-1,) + a.shape[2:]) for a in outs[has_sum : first_out]],
        outs[first_out : first_out + len(g_in)],
        outs[first_out + len(g_in) :],
    )


def rms_norm(vector, scale_gain):
    return (
        vector * lax.rsqrt(jnp.mean(vector * vector, axis=-1, keepdims=True) + epsilon) * scale_gain
    )


def seq_begin(lengths_row, positions):
    seq_starts = jnp.cumsum(lengths_row) - lengths_row
    chosen = jnp.where(seq_starts[None, :] <= positions[:, None], seq_starts[None, :], 0)
    return jnp.max(chosen, axis=1)


HEADS = 2
PAIRS = FK * (FK + 1) // 2
STATE = 160
BLOCK = 128


def feature_tables(values):
    wide = values + HEADS * FK
    first = np.zeros((HEADS, wide, wide), np.float32)
    second = np.zeros((HEADS, wide, wide), np.float32)
    rest = np.zeros((8, wide), np.float32)
    for h in range(HEADS):
        at = values + h * FK
        lane = 0
        for a in range(FK):
            for b in range(a, FK):
                first[h, at + a, lane] = 1
                second[h, at + b, lane] = 1
                rest[2, lane] = 0.25 if a < b else 1 / (4.0 * math.sqrt(2.0))
                lane += 1
        for a in range(FK):
            first[h, at + a, lane] = 1
            rest[1, lane] = 1
            rest[2, lane] = 0.5
            lane += 1
        rest[0, lane] = rest[1, lane] = rest[2, lane] = 1
    return np.stack([first, second], axis=1), rest


def mm(a, b):
    return lax.dot_general(a, b, (((1,), (0,)), ((), ())), preferred_element_type=jnp.float32)


def mm_nt(a, b):
    return lax.dot_general(a, b, (((1,), (1,)), ((), ())), preferred_element_type=jnp.float32)


def mm_tn(a, b):
    return lax.dot_general(a, b, (((0,), (0,)), ((), ())), preferred_element_type=jnp.float32)


class Lanes:
    def __init__(self, wide, values):
        self.values = values
        self.lane = lax.broadcasted_iota(jnp.int32, (1, wide), 1)
        lane, dim = self.lane, values // HEADS
        self.is_value = lane < values
        self.is_one = (lane >= values) & (lane < values + 2 * HEADS)
        self.head = jnp.where(
            self.is_value, jnp.where(lane < dim, 0, 1), jnp.where(self.is_one, (lane - values) % 2, 9)
        )

    def of(self, h, x):
        return jnp.where(self.head == h, x, jnp.zeros_like(x))

    def key(self, h, x):
        at = self.values + h * FK
        return jnp.where((self.lane >= at) & (self.lane < at + FK), x, jnp.zeros_like(x))

    def extended(self, a):
        return jnp.where(
            self.is_value, a, jnp.where(self.is_one, jnp.ones_like(a), jnp.zeros_like(a))
        )

    def column(self, x, index):
        return jnp.sum(
            jnp.where(self.lane == self.values + index, x, 0.0), axis=1, keepdims=True
        )

    def denominator(self, x):
        return jnp.where(
            self.lane < self.values // HEADS, self.column(x, 0), self.column(x, 1)
        )


def meet(direction, reach):
    q, n = lax.axis_index("seq"), lax.axis_size("seq")
    barrier = pltpu.get_barrier_semaphore()
    count = 0
    for d in range(1, reach + 1):
        source = q - direction * d
        target = q + direction * d

        @pl.when((source >= 0) & (source < n))
        def _():
            pl.semaphore_signal(barrier, inc=1, device_id={"seq": source}, device_id_type=MESH)

        count = count + jnp.where((target >= 0) & (target < n), 1, 0)

    @pl.when(count > 0)
    def _():
        pl.semaphore_wait(barrier, count)


class Pass:
    def __init__(self, direction, reach, src, dst, send, recv):
        self.direction, self.reach = direction, reach
        self.src, self.dst, self.send, self.recv = src, dst, send, recv
        self.q, self.n = lax.axis_index("seq"), lax.axis_size("seq")

    def has_source(self, d):
        at = self.q - self.direction * d
        return (at >= 0) & (at < self.n)

    def has_target(self, d):
        at = self.q + self.direction * d
        return (at >= 0) & (at < self.n)

    def copy(self, d):
        return remote(
            self.src, self.dst.at[d - 1], self.send.at[d - 1], self.recv.at[d - 1],
            seq=self.q + self.direction * d,
        )

    def start(self):
        for d in range(1, self.reach + 1):

            @pl.when(self.has_target(d))
            def _():
                self.copy(d).start()

    def arrived(self):
        for d in range(1, self.reach + 1):

            @pl.when(self.has_source(d))
            def _():
                self.copy(d).wait_recv()

    def sent(self):
        for d in range(1, self.reach + 1):

            @pl.when(self.has_target(d))
            def _():
                self.copy(d).wait_send()


def sum_states(states, coef, total):
    for m in range(2):
        total[m] = jnp.zeros(total.shape[1:], total.dtype)
        for d in range(1, states.reach + 1):

            @pl.when(states.has_source(d))
            def _():
                total[m, :STATE, :] += coef[d - 1, m] * states.dst[d - 1, m].astype(jnp.float32)


def shifted(a, tail, fresh, by):
    row = lax.broadcasted_iota(jnp.int32, (a.shape[0], 1), 0)
    moved = pltpu.roll(a, by, 0)
    rows = tail.shape[0]
    for r in range(by):
        edge = jnp.where(fresh, tail[rows - by + r : rows - by + r + 1, :], 0.0)
        moved = jnp.where(row == r, edge, moved)
    return moved


def attn_forward_kernel(
    reach, proj, col, row, coef, e, c, taps, gated, att, conv, sin, edge, acc, phi, s_acc, s_src,
    s_all, s_sum, e_src, ss, sr, es, er,
):
    q = lax.axis_index("seq")
    rows, wide = proj.shape[1], proj.shape[2] // 2
    values = wide - HEADS * FK
    lanes = Lanes(wide, values)
    meet(1, reach)
    states = Pass(1, reach, s_src, s_all, ss, sr)
    edges = Pass(1, 1, e_src, edge, es, er)

    def sides(m):
        return proj[m, :, :wide].astype(jnp.bfloat16), proj[m, :, wide:].astype(jnp.bfloat16)

    def phi_of(a, h):
        return (mm(a, e[h, 0]) + c[0:1, :]) * (mm(a, e[h, 1]) + c[1:2, :]) * c[2:3, :]

    def make_state(i, carry):
        m, h = i // HEADS, i % HEADS
        a, b = sides(m)
        phi[m, h] = (phi_of(a, h) * col[m, :, 1:2]).astype(jnp.bfloat16)
        keyed = (phi_of(b, h) * col[m, :, 2:3]).astype(jnp.bfloat16)
        part = mm_tn(keyed, lanes.of(h, lanes.extended(a)))

        @pl.when(h == 0)
        def _():
            s_acc[m] = part

        @pl.when(h > 0)
        def _():
            s_acc[m] += part

        return carry

    lax.fori_loop(0, 2 * HEADS, make_state, 0)
    for m in range(2):
        s_src[m] = s_acc[m, :STATE, :].astype(jnp.bfloat16)
    states.start()

    def make_block(i, carry):
        m, h = i // HEADS, i % HEADS
        a, b = sides(m)
        asked = lanes.key(h, a)
        valued = lanes.of(h, lanes.extended(a))
        for r in range(rows // BLOCK):
            lo, hi = r * BLOCK, (r + 1) * BLOCK
            x = mm_nt(asked[lo:hi], b[:hi]) * 0.25
            seen = (col[m, lo:hi, 0:1] == row[m, 0:1, :hi]) & (
                lax.broadcasted_iota(jnp.int32, (BLOCK, hi), 1)
                <= lo + lax.broadcasted_iota(jnp.int32, (BLOCK, hi), 0)
            )
            w = jnp.where(seen, 1.0 + x + 0.5 * x * x, 0.0).astype(jnp.bfloat16)
            part = mm(w, valued[:hi])

            @pl.when(h == 0)
            def _():
                acc[m, lo:hi, :] = part

            @pl.when(h > 0)
            def _():
                acc[m, lo:hi, :] += part

        return carry

    lax.fori_loop(0, 2 * HEADS, make_block, 0)
    states.arrived()
    sum_states(states, coef, s_sum)

    def attend(m, lo):
        s = s_sum[m].astype(jnp.bfloat16)
        both = acc[m, lo:, :]
        for h in range(HEADS):
            both = both + mm(phi[m, h, lo:, :], lanes.of(h, s))
        return jnp.where(lanes.is_value, both / lanes.denominator(both), both)

    for m in range(2):
        sin[m] = s_sum[m, :STATE, :].astype(jnp.bfloat16)
        e_src[m] = attend(m, rows - 16)
    edges.start()
    for m in range(2):
        att[m] = attend(m, 0)
    edges.arrived()
    for m in range(2):
        a = att[m]
        tail = edge[0, m]
        out = taps[0:1, :] * a
        for by in (1, 2):
            out = out + taps[by : by + 1, :] * shifted(a, tail, q > 0, by) * col[m, :, 2 + by : 3 + by]
        conv[m] = out
        gated[m] = (out * proj[m, :, wide:]).astype(jnp.bfloat16)
    states.sent()
    edges.sent()


def attn_backward_kernel(
    reach, bg, proj, att, conv, sin, edge, col, row, coef, late, e, c, taps, out, grad_taps,
    phi_q, phi_k, near, acc_a, acc_b, s_acc, s_src, s_all, s_sum, e_src, e_dst, ss, sr, es, er,
):
    q, n = lax.axis_index("seq"), lax.axis_size("seq")
    rows, wide = proj.shape[1], proj.shape[2] // 2
    values = wide - HEADS * FK
    lanes = Lanes(wide, values)
    meet(-1, reach)
    states = Pass(-1, reach, s_src, s_all, ss, sr)
    edges = Pass(-1, 1, e_src, e_dst, es, er)
    for m in range(2):
        e_src[m] = bg[m, :16, :] * proj[m, :16, wide:]
    edges.start()

    def sides(m):
        return proj[m, :, :wide].astype(jnp.bfloat16), proj[m, :, wide:].astype(jnp.bfloat16)

    def factors(a, h):
        return mm(a, e[h, 0]) + c[0:1, :], mm(a, e[h, 1]) + c[1:2, :]

    def make_phi(i, carry):
        m, h = i // HEADS, i % HEADS
        a, b = sides(m)
        u, w = factors(a, h)
        phi_q[m, h] = (u * w * c[2:3, :] * col[m, :, 1:2]).astype(jnp.bfloat16)
        u, w = factors(b, h)
        phi_k[m, h] = (u * w * c[2:3, :] * col[m, :, 2:3]).astype(jnp.bfloat16)
        return carry

    lax.fori_loop(0, 2 * HEADS, make_phi, 0)
    edges.arrived()
    sums = [jnp.zeros((1, wide), jnp.float32)] * KW
    place = lax.broadcasted_iota(jnp.int32, (rows, 1), 0)
    for m in range(2):
        back = bg[m]
        back_conv = back * proj[m, :, wide:]
        a = jnp.where(lanes.is_value, att[m], 0.0)
        tail = edge[0, m]
        nxt = e_dst[0, m]
        total = taps[0:1, :] * back_conv
        sums[0] = sums[0] + jnp.sum(back_conv * a, axis=0, keepdims=True)
        for by in (1, 2):
            kept = back_conv * col[m, :, 2 + by : 3 + by]
            sums[by] = sums[by] + jnp.sum(
                kept * shifted(a, tail, q > 0, by), axis=0, keepdims=True
            )
            moved = pltpu.roll(kept, rows - by, 0)
            for r in range(by):
                fresh = jnp.where(q < n - 1, nxt[r : r + 1, :] * late[by - 1 + r, m], 0.0)
                moved = jnp.where(place == rows - by + r, fresh, moved)
            total = total + taps[by : by + 1, :] * moved
        out[m, :, wide:] = jnp.where(lanes.is_value, back * conv[m], 0.0).astype(jnp.bfloat16)
        back_numer = total / lanes.denominator(att[m])
        spent = back_numer * a
        found = jnp.where(lanes.is_value, back_numer, 0.0)
        for h in range(HEADS):
            denom = -jnp.sum(lanes.of(h, spent), axis=1, keepdims=True)
            high = denom.astype(jnp.bfloat16).astype(jnp.float32)
            found = jnp.where(lanes.lane == values + h, high, found)
            found = jnp.where(lanes.lane == values + 2 + h, denom - high, found)
        near[m] = found.astype(jnp.bfloat16)
        part = jnp.zeros((wide, wide), jnp.float32)
        for h in range(HEADS):
            part = part + mm_tn(phi_q[m, h], lanes.of(h, near[m]))
        s_src[m] = part[:STATE].astype(jnp.bfloat16)
    states.start()
    grad_taps[...] = jnp.zeros(grad_taps.shape, jnp.float32)
    for by in range(KW):
        grad_taps[by : by + 1, :] = sums[by]
    acc_a[...] = jnp.zeros(acc_a.shape, jnp.float32)
    acc_b[...] = jnp.zeros(acc_b.shape, jnp.float32)
    for m in range(2):
        s_sum[m] = jnp.zeros(s_sum.shape[1:], jnp.float32)
        s_sum[m, :STATE, :] = sin[m].astype(jnp.float32)

    def through_phi(scaled, factors_of, h):
        u, w = factors_of
        return mm_nt((scaled * w).astype(jnp.bfloat16), e[h, 0]) + mm_nt(
            (scaled * u).astype(jnp.bfloat16), e[h, 1]
        )

    def make_block(i, carry):
        m, h = i // HEADS, i % HEADS
        a, b = sides(m)
        asked, keyed = lanes.key(h, a), lanes.key(h, b)
        valued = lanes.extended(a)
        given = lanes.of(h, near[m])
        given_v = jnp.where(lanes.is_value, given, jnp.zeros_like(given))
        for r in range(rows // BLOCK):
            lo, hi = r * BLOCK, (r + 1) * BLOCK
            x = mm_nt(asked[lo:hi], b[:hi]) * 0.25
            seen = (col[m, lo:hi, 0:1] == row[m, 0:1, :hi]) & (
                lax.broadcasted_iota(jnp.int32, (BLOCK, hi), 1)
                <= lo + lax.broadcasted_iota(jnp.int32, (BLOCK, hi), 0)
            )
            w = jnp.where(seen, 1.0 + x + 0.5 * x * x, 0.0).astype(jnp.bfloat16)
            back_w = mm_nt(given[lo:hi], valued[:hi])
            back_s = jnp.where(seen, back_w * (1.0 + x), 0.0).astype(jnp.bfloat16)
            acc_a[m, lo:hi, :] += 0.25 * mm(back_s, keyed[:hi])
            acc_b[m, :hi, :] += 0.25 * mm_tn(back_s, asked[lo:hi])
            acc_a[m, :hi, :] += mm_tn(w, given_v[lo:hi])
        s = s_sum[m].astype(jnp.bfloat16)
        scaled = mm_nt(given, s) * col[m, :, 1:2] * c[2:3, :]
        acc_a[m] += through_phi(scaled, factors(a, h), h)
        return carry

    lax.fori_loop(0, 2 * HEADS, make_block, 0)
    states.arrived()
    sum_states(states, coef, s_sum)

    def make_late(i, carry):
        m, h = i // HEADS, i % HEADS
        a, b = sides(m)
        s = s_sum[m].astype(jnp.bfloat16)
        scaled = mm_nt(lanes.of(h, lanes.extended(a)), s) * col[m, :, 2:3] * c[2:3, :]
        acc_b[m] += through_phi(scaled, factors(b, h), h)
        s_v = lanes.of(h, jnp.where(lanes.is_value, s, jnp.zeros_like(s)))
        acc_a[m] += mm(phi_k[m, h], s_v)
        return carry

    lax.fori_loop(0, 2 * HEADS, make_late, 0)
    for m in range(2):
        out[m, :, :wide] = acc_a[m].astype(jnp.bfloat16)
        out[m, :, wide:] = jnp.where(
            lanes.is_value, out[m, :, wide:].astype(jnp.float32), acc_b[m]
        ).astype(jnp.bfloat16)
    states.sent()
    edges.sent()


def seq_reach():
    n = lax.axis_size("seq")
    return n // 2 if n % 2 == 0 else n - 1


def attention_call(kernel, cid, inputs, scalars, shapes, scratch):
    vmem, smem = pl.BlockSpec(memory_space=pltpu.VMEM), pl.BlockSpec(memory_space=pltpu.SMEM)
    return pl.pallas_call(
        functools.partial(kernel, seq_reach()),
        out_shape=shapes,
        in_specs=[smem if i in scalars else vmem for i in range(len(inputs))],
        out_specs=[vmem] * len(shapes),
        scratch_shapes=scratch,
        name=f"attention{cid}",
        compiler_params=pltpu.CompilerParams(
            collective_id=cid, has_side_effects=True, vmem_limit_bytes=48 << 20
        ),
    )(*inputs)


def passing(reach, wide):
    dma = pltpu.SemaphoreType.DMA
    return (
        [
            pltpu.VMEM((2, STATE, wide), jnp.bfloat16),
            pltpu.VMEM((reach, 2, STATE, wide), jnp.bfloat16),
            pltpu.VMEM((2, wide, wide), jnp.float32),
        ],
        [dma((reach,)), dma((reach,)), dma((1,)), dma((1,))],
    )


def attention_forward(proj, taps, marks, tables):
    m, rows, double = proj.shape
    wide = double // 2
    f32, bf16 = jnp.float32, jnp.bfloat16
    buffers, sems = passing(seq_reach(), wide)
    shape = jax.ShapeDtypeStruct
    return attention_call(
        attn_forward_kernel,
        10,
        [proj, marks["col"], marks["row"], marks["before"], *tables, taps],
        (3,),
        [
            shape((m, rows, wide), bf16),
            shape((m, rows, wide), f32),
            shape((m, rows, wide), f32),
            shape((m, STATE, wide), bf16),
            shape((1, m, 16, wide), f32),
        ],
        [
            pltpu.VMEM((m, rows, wide), f32),
            pltpu.VMEM((m, HEADS, rows, wide), bf16),
            pltpu.VMEM((m, wide, wide), f32),
            *buffers,
            pltpu.VMEM((m, 16, wide), f32),
            *sems,
        ],
    )


def attention_backward(back_gated, proj, kept, taps, marks, tables):
    att, conv, sin, edge = kept
    m, rows, double = proj.shape
    wide = double // 2
    f32, bf16 = jnp.float32, jnp.bfloat16
    buffers, sems = passing(seq_reach(), wide)
    shape = jax.ShapeDtypeStruct
    return attention_call(
        attn_backward_kernel,
        11,
        [
            back_gated, proj, att, conv, sin, edge, marks["col"], marks["row"], marks["after"],
            marks["late"], *tables, taps,
        ],
        (8, 9),
        [shape((m, rows, double), bf16), shape((8, wide), f32)],
        [
            pltpu.VMEM((m, HEADS, rows, wide), bf16),
            pltpu.VMEM((m, HEADS, rows, wide), bf16),
            pltpu.VMEM((m, rows, wide), bf16),
            pltpu.VMEM((m, rows, wide), f32),
            pltpu.VMEM((m, rows, wide), f32),
            pltpu.VMEM((m, wide, wide), f32),
            *buffers,
            pltpu.VMEM((m, 16, wide), f32),
            pltpu.VMEM((1, m, 16, wide), f32),
            *sems,
        ],
    )


def sequence_marks(lengths, rows):
    count, mine = lax.axis_size("seq"), lax.axis_index("seq")
    start = mine * rows
    positions = start + jnp.arange(rows + 2, dtype=jnp.int32)
    begin_ext = jax.vmap(lambda row: seq_begin(row, positions))(lengths)
    begin = begin_ext[:, :rows]
    ends = (jnp.arange(count, dtype=jnp.int32) + 1) * rows - 1
    stays = jax.vmap(lambda row: seq_begin(row, ends))(lengths) < (ends - rows + 1)[None, :]
    stays = stays.astype(jnp.float32)
    blocks = jnp.arange(count, dtype=jnp.int32)

    def through(first, last):
        inside = (blocks >= first) & (blocks <= last)
        return jnp.min(jnp.where(inside[None, :], stays, 1.0), axis=1)

    reach = seq_reach()
    before = [through(mine - d + 1, mine - 1) for d in range(1, reach + 1)]
    after = [through(mine + 1, mine + d - 1) for d in range(1, reach + 1)]
    allowed = [(positions - j >= begin_ext).astype(jnp.float32) for j in range(KW)]
    columns = [
        begin.astype(jnp.float32),
        (begin < start).astype(jnp.float32),
        (begin == begin[:, rows - 1 :]).astype(jnp.float32),
        allowed[1][:, :rows],
        allowed[2][:, :rows],
    ]
    col = jnp.stack(columns + [jnp.zeros_like(columns[0])] * 3, axis=2)
    return {
        "col": col,
        "row": jnp.broadcast_to(columns[0][:, None, :], (2, 8, rows)),
        "before": jnp.stack(before),
        "after": jnp.stack(after),
        "late": jnp.stack([allowed[1][:, rows], allowed[2][:, rows], allowed[2][:, rows + 1]]),
    }


def by_seq(grad):
    n = lax.axis_size("seq")
    return grad.reshape((n, grad.shape[0] // n) + grad.shape[1:])


def held(a):
    return lax.optimization_barrier(a.astype(jnp.bfloat16))


def dot_n(a, b):
    return jnp.dot(a, b, preferred_element_type=jnp.float32)


def on_device(
    tokens,
    lengths,
    gain_attn,
    w_query,
    w_key,
    w_value,
    w_gate_conv,
    conv_taps,
    w_out,
    gain_ffn,
    w_gate,
    w_up,
    w_down,
    cotangent,
):
    head_index = lax.axis_index("head")
    core = lax.axis_index("section")
    micro_count, rows, width = tokens.shape
    total = micro_count * rows

    def halves(weight):
        middle = weight.shape[1] // 2
        return jnp.stack([weight[:, :middle], weight[:, middle:]])

    own_mix = jnp.concatenate(
        [halves(w[0]) for w in (w_value, w_query, w_gate_conv, w_key)], axis=2
    )
    values = w_value.shape[2] // 2
    keys = w_query.shape[2] // 2
    wide = values + keys
    own_out = jnp.pad(halves(w_out[0].T), ((0, 0), (0, 0), (0, keys)))
    cols = w_gate.shape[2] // 2

    def filled(half):
        return jnp.pad(half, ((0, 0), (0, 0), (0, -cols % 128)))

    own_ffn = jnp.concatenate([filled(halves(w_gate[0])), filled(halves(w_up[0]))], axis=2)
    own_down = filled(halves(w_down[0].T))
    rows_of_layer = jnp.concatenate([gain_attn, gain_ffn, conv_taps[0]], axis=0)
    rows_all = lax.all_gather(rows_of_layer, "section").astype(jnp.float32)
    gains_one, gains_two, taps_all = rows_all[:, 0], rows_all[:, 1], rows_all[:, 2:]
    taps_both = lax.dynamic_slice_in_dim(taps_all, (head_index * 2 + core) * values, values, 2)
    taps_both = jnp.pad(taps_both, ((0, 0), (0, 8 - KW), (0, keys)))
    first, rest = feature_tables(values)
    tables = (jnp.asarray(first, jnp.bfloat16), jnp.asarray(rest))
    marks = sequence_marks(lengths, rows)
    hidden_cols = own_down.shape[2]

    def as_parts(flat):
        return flat.reshape(micro_count, rows, -1)

    def spread(summed):
        return summed.astype(jnp.float32).reshape(total, width)

    _, (mix_0, out_0), _, _ = communicate(1, gather=(0, [own_mix, own_out]))
    w_mix, w_o, w_gu, w_d = [mix_0, None], [out_0, None], [None, None], [None, None]
    x = tokens.reshape(total, width).astype(jnp.float32)
    kept = [None, None]
    outputs = []
    last_partial = None
    for layer in range(2):
        normed = rms_norm(x, gains_one[layer]).astype(jnp.bfloat16)
        proj = dot_n(normed, w_mix[layer]).reshape(micro_count, rows, 2 * wide)
        gated, *attn = attention_forward(proj, taps_both[layer], marks, tables)
        gated_flat = gated.reshape(total, wide)
        partial = (gated, w_o[layer])
        if layer == 0:
            summed, (w_gu[0], w_d[0]), _, _ = communicate(
                2, partial=partial, gather=(0, [own_ffn, own_down])
            )
        else:
            summed, (w_gu[1],), _, _ = communicate(3, partial=partial, gather=(1, [own_ffn]))
        middle = x + spread(summed)
        normed_two = rms_norm(middle, gains_two[layer]).astype(jnp.bfloat16)
        middle = held(middle).astype(jnp.float32)
        both = held(dot_n(normed_two, w_gu[layer])).astype(jnp.float32)
        hidden = (jax.nn.silu(both[:, :hidden_cols]) * both[:, hidden_cols:]).astype(jnp.bfloat16)
        partial = (as_parts(hidden), w_d[layer])
        kept[layer] = (x, normed, proj, gated_flat, attn, middle, normed_two, both, hidden)
        if layer == 0:
            summed, (w_mix[1], w_o[1], w_d[1]), _, _ = communicate(
                4, partial=partial, gather=(1, [own_mix, own_out, own_down])
            )
            outputs.append(held(middle + spread(summed)))
            x = outputs[0].astype(jnp.float32)
        else:
            last_partial = partial

    grad = cotangent.reshape(total, width)
    back = [None, None]
    smalls = [None, None]
    made = []
    into = [None] * 4
    for layer in (1, 0):
        x, normed, proj, gated_flat, attn, middle, normed_two, both, hidden = kept[layer]
        grad_wide = grad.astype(jnp.float32)
        back_hidden = dot_n(grad, w_d[layer])
        gate_pre, upward = both[:, :hidden_cols], both[:, hidden_cols:]
        silu_value, silu_back = jax.vjp(jax.nn.silu, gate_pre)
        back_both = jnp.concatenate(
            [
                silu_back(back_hidden * upward)[0].astype(jnp.bfloat16),
                (back_hidden * silu_value).astype(jnp.bfloat16),
            ],
            axis=1,
        )
        partial = (as_parts(back_both), w_gu[layer])
        products = ((normed_two, back_both), (grad, hidden))
        if layer == 1:
            summed, _, _, (grad_gu, grad_d) = communicate(5, partial=partial, products=products)
        else:
            summed, _, into[1:], (grad_gu, grad_d) = communicate(
                6, partial=partial, scatter=(1, made), products=products
            )
        _, norm_back_two = jax.vjp(rms_norm, middle, gains_two[layer])
        back_middle, gain_two = norm_back_two(spread(summed))
        back_middle = grad_wide + back_middle
        back_branch = held(back_middle)
        back_middle = back_branch.astype(jnp.float32)
        back_gated = dot_n(back_branch, w_o[layer])
        back_proj, taps_grad = attention_backward(
            back_gated.reshape(micro_count, rows, wide), proj, attn, taps_both[layer], marks, tables
        )
        back_flat = back_proj.reshape(total, 2 * wide)
        partial = (back_proj, w_mix[layer])
        summed, _, into[:1], (grad_mix, grad_o) = communicate(
            7 + layer,
            partial=partial,
            scatter=(layer, [by_seq(grad_gu)]),
            into=into[:1] if layer == 0 else (),
            products=((normed, back_flat), (back_branch, gated_flat)),
        )
        made = [by_seq(grad_d), by_seq(grad_mix), by_seq(grad_o)]
        _, norm_back_one = jax.vjp(rms_norm, x, gains_one[layer])
        back_x, gain_one = norm_back_one(spread(summed))
        grad = (back_middle + back_x).astype(jnp.bfloat16)
        back[layer] = grad
        smalls[layer] = (gain_one, gain_two, taps_grad)
    gains = jnp.stack([smalls[0][0], smalls[1][0], smalls[0][1], smalls[1][1]])
    taps_rows = jnp.concatenate([smalls[0][2][:KW], smalls[1][2][:KW]])
    packed = jnp.concatenate(
        [
            jnp.pad(gains, ((0, 4), (0, 0))),
            jnp.pad(taps_rows, ((0, 8 - 2 * KW), (0, width - wide))),
        ]
    )
    summed, _, into[1:], (gains, taps_rows) = communicate(
        9, partial=last_partial, scatter=(0, made), into=into[1:], small=(packed, wide)
    )
    outputs.append((kept[1][5] + spread(summed)).astype(jnp.bfloat16))
    grad_gu, grad_d, grad_mix, grad_o = [
        jnp.sum(received.astype(jnp.float32), axis=1).reshape((2, -1) + received.shape[3:])
        for received in into
    ]

    def joined(pair):
        return jnp.concatenate([pair[0], pair[1]], axis=1)

    grad_value = joined(grad_mix[:, :, :values])
    grad_query = joined(grad_mix[:, :, values:wide])
    grad_gconv = joined(grad_mix[:, :, wide : wide + values])
    grad_key = joined(grad_mix[:, :, wide + values :])
    grad_out = joined(grad_o[:, :, :values]).T
    grad_gate = joined(grad_gu[:, :, :cols])
    grad_up = joined(grad_gu[:, :, hidden_cols : hidden_cols + cols])
    grad_down = joined(grad_d[:, :, :cols]).T

    gains = lax.dynamic_index_in_dim(gains[:4].reshape(2, 2, width), core, 1, False)
    taps_rows = lax.dynamic_index_in_dim(
        taps_rows[:, : 2 * KW, :values].reshape(-1, 2, KW, values), core, 1, False
    )
    grad_taps = jnp.transpose(taps_rows, (1, 0, 2)).reshape(KW, width)

    def chosen(pair):
        return jnp.where(core == 0, pair[0], pair[1]).reshape(1, micro_count, rows, width)

    return (
        chosen(outputs),
        chosen(back),
        gains[0][None],
        grad_query[None],
        grad_key[None],
        grad_value[None],
        grad_gconv[None],
        grad_taps[None],
        grad_out[None],
        gains[1][None],
        grad_gate[None],
        grad_up[None],
        grad_down[None],
    )


def solution(mesh):
    placed = (
        P(None, "seq", None),
        P(),
        P("section", None),
        P("section", "seq", "head"),
        P("section", "seq", "head"),
        P("section", "seq", "head"),
        P("section", "seq", "head"),
        P("section", None, None),
        P("section", "head", "seq"),
        P("section", None),
        P("section", "seq", "head"),
        P("section", "seq", "head"),
        P("section", "head", "seq"),
        P(None, "seq", None),
    )
    return jax.shard_map(
        on_device,
        mesh=mesh,
        in_specs=placed,
        out_specs=(
            P("section", None, "seq", None),
            P("section", None, "seq", None),
            P("section", None),
            P("section", "seq", "head"),
            P("section", "seq", "head"),
            P("section", "seq", "head"),
            P("section", "seq", "head"),
            P("section", None, None),
            P("section", "head", "seq"),
            P("section", None),
            P("section", "seq", "head"),
            P("section", "seq", "head"),
            P("section", "head", "seq"),
        ),
        check_vma=False,
    )
```
